16 devices in a mesh: tp: 4 (over z, y), cp: 4 (over x, core).
Axes of the slice: x: 2, y: 2, z: 2, core: 2. Of those that a mesh axis runs over, the one named last changes fastest.
Arguments:
- tokens: int32 [2048], P('cp')
- pos: int32 [2048], P('cp')
- doc_id: int32 [2048], P('cp')
- dy: bfloat16 [2048, 2560], P('cp')
- table: bfloat16 [32000, 2560], P('tp')
- w_q: bfloat16 [2560, 2560], P(None, 'tp')
- w_k: bfloat16 [2560, 2560], P(None, 'tp')
- w_v: bfloat16 [2560, 2560], P(None, 'tp')
- w_o: bfloat16 [2560, 2560], P('tp')
- w_gate: bfloat16 [2560, 6912], P(None, 'tp')
- w_up: bfloat16 [2560, 6912], P(None, 'tp')
- w_down: bfloat16 [6912, 2560], P('tp')
- gain_one: bfloat16 [2560], replicated
- gain_two: bfloat16 [2560], replicated
- inv_freq: float32 [64], replicated
Outputs:
- output 1: bfloat16 [2048, 2560], P('cp')
- output 2: float32 [32000, 2560], P('tp')
- output 3: float32 [2560, 2560], P(None, 'tp')
- output 4: float32 [2560, 2560], P(None, 'tp')
- output 5: float32 [2560, 2560], P(None, 'tp')
- output 6: float32 [2560, 2560], P('tp')
- output 7: float32 [2560, 6912], P(None, 'tp')
- output 8: float32 [2560, 6912], P(None, 'tp')
- output 9: float32 [6912, 2560], P('tp')
- output 10: float32 [2560], replicated
- output 11: float32 [2560], replicated
All inputs are finite; a program needn't handle non-finite values.
Results may differ from the reference program's by a relative error of at most 0.0149397.
Values are sent between devices in bfloat16 or wider.
A program may use at most 1 GiB of HBM per device.

```python
import math
import jax
import jax.numpy as jnp
from jax import lax

VOCAB = 32000
MODEL_DIM = 2560
HEADS = 20
KV_HEADS = 20
HEAD_DIM = 128
FFN_DIM = 6912
TOK_BLOCK = 256
CP_SIZE = 4

TOKENS = 2 * CP_SIZE * TOK_BLOCK
GROUP = HEADS // KV_HEADS
HOT_COUNT = 2 ** 5
NORM_EPS = 1e-5
SCORE_SCALE = HEAD_DIM ** -0.5
NEG_BIG = -1e30


def slot_sequence():
    slot = jnp.arange(TOKENS)
    shard = slot // (2 * TOK_BLOCK)
    within = slot % (2 * TOK_BLOCK)
    block_no = jnp.where(within < TOK_BLOCK, shard, 2 * CP_SIZE - 1 - shard)
    return block_no * TOK_BLOCK + within % TOK_BLOCK


def draw_layout(key):
    keys = jax.random.split(key, 5)
    seq_pos = slot_sequence()
    cuts = jax.random.randint(keys[0], (CP_SIZE,), 1, TOKENS)
    after_cut = cuts[None, :] <= seq_pos[:, None]
    doc_id = jnp.sum(after_cut.astype(jnp.int32), axis=1)
    doc_start = jnp.max(jnp.where(after_cut, cuts[None, :], 0), axis=1)
    pos = (seq_pos - doc_start).astype(jnp.int32)
    hot_ids = jax.random.randint(keys[1], (HOT_COUNT,), 0, VOCAB // 8)
    hot_pick = jax.random.randint(keys[2], (TOKENS,), 0, HOT_COUNT)
    spread_ids = jax.random.randint(keys[3], (TOKENS,), 0, VOCAB)
    use_hot = jax.random.randint(keys[4], (TOKENS,), 0, 2)
    tokens = jnp.where(use_hot == 1, hot_ids[hot_pick], spread_ids)
    tokens = tokens.at[0].set(0).at[1].set(VOCAB - 1)
    return tokens, pos, doc_id.astype(jnp.int32)


def setup_inputs(seed: int = 0) -> dict:
    base = jax.random.key(seed)
    tokens, pos, doc_id = draw_layout(jax.random.fold_in(base, 1))
    keys = jax.random.split(jax.random.fold_in(base, 2), 14)

    def weight(which, fan_in, fan_out):
        return (jax.random.normal(keys[which], (fan_in, fan_out), jnp.float32) * fan_in ** -0.5).astype(jnp.bfloat16)

    def gain(which):
        return (1.0 + 0.25 * jax.random.normal(keys[which], (MODEL_DIM,), jnp.float32)).astype(jnp.bfloat16)

    log_theta = jax.random.uniform(keys[11], (), jnp.float32, math.log(1e4), math.log(5e5))
    exponent = jnp.arange(HEAD_DIM // 2, dtype=jnp.float32) * (2.0 / HEAD_DIM)
    jitter = jax.random.uniform(keys[12], (HEAD_DIM // 2,), jnp.float32, 0.9, 1.1)
    return {
        "tokens": tokens,
        "pos": pos,
        "doc_id": doc_id,
        "dy": jax.random.normal(keys[0], (TOKENS, MODEL_DIM), jnp.float32).astype(jnp.bfloat16),
        "table": jax.random.normal(keys[1], (VOCAB, MODEL_DIM), jnp.float32).astype(jnp.bfloat16),
        "w_q": weight(2, MODEL_DIM, HEADS * HEAD_DIM),
        "w_k": weight(3, MODEL_DIM, KV_HEADS * HEAD_DIM),
        "w_v": weight(4, MODEL_DIM, KV_HEADS * HEAD_DIM),
        "w_o": weight(5, HEADS * HEAD_DIM, MODEL_DIM),
        "w_gate": weight(6, MODEL_DIM, FFN_DIM),
        "w_up": weight(7, MODEL_DIM, FFN_DIM),
        "w_down": weight(8, FFN_DIM, MODEL_DIM),
        "gain_one": gain(9),
        "gain_two": gain(10),
        "inv_freq": jnp.exp(-log_theta * exponent) * jitter,
    }


def to_bf16(feats):
    return feats.astype(jnp.bfloat16).astype(jnp.float32)


def rms_norm(feats, gain_vec):
    return feats * lax.rsqrt(jnp.mean(feats * feats, axis=-1, keepdims=True) + NORM_EPS) * gain_vec


def rotate(tensor_in, cosine, sine):
    half = tensor_in.shape[-1] // 2
    first = tensor_in[..., :half]
    second = tensor_in[..., half:]
    return jnp.concatenate([first * cosine - second * sine, second * cosine + first * sine], axis=-1)


def forward_pass(params, tokens, pos, doc_id, inv_freq):
    table, w_q, w_k, w_v, w_o, w_gate, w_up, w_down, gain_one, gain_two = params
    embed = jnp.take(table, tokens, axis=0)
    act_one = to_bf16(rms_norm(embed, gain_one))
    angle = pos.astype(jnp.float32)[:, None, None] * inv_freq
    cosine = jnp.cos(angle)
    sine = jnp.sin(angle)
    query = jnp.dot(act_one, w_q, preferred_element_type=jnp.float32).reshape(TOKENS, HEADS, HEAD_DIM)
    query = to_bf16(rotate(query, cosine, sine)).reshape(2 * CP_SIZE, TOK_BLOCK, KV_HEADS, GROUP, HEAD_DIM)
    key_all = jnp.dot(act_one, w_k, preferred_element_type=jnp.float32).reshape(TOKENS, KV_HEADS, HEAD_DIM)
    key_all = to_bf16(rotate(key_all, cosine, sine))
    value_all = to_bf16(jnp.dot(act_one, w_v, preferred_element_type=jnp.float32)).reshape(TOKENS, KV_HEADS, HEAD_DIM)
    seq_pos = slot_sequence()

    def attend(block):
        query_blk, seq_blk, doc_blk = block
        scores = jnp.einsum("qkgd,skd->kgqs", query_blk, key_all) * SCORE_SCALE
        allowed = (doc_blk[:, None] == doc_id[None, :]) & (seq_pos[None, :] <= seq_blk[:, None])
        attn_prob = jax.nn.softmax(jnp.where(allowed, scores, NEG_BIG), axis=-1)
        return jnp.einsum("kgqs,skd->qkgd", to_bf16(attn_prob), value_all)

    blocks = (query, seq_pos.reshape(2 * CP_SIZE, TOK_BLOCK), doc_id.reshape(2 * CP_SIZE, TOK_BLOCK))
    attended = to_bf16(lax.map(jax.checkpoint(attend), blocks)).reshape(TOKENS, HEADS * HEAD_DIM)
    residual = embed + jnp.dot(attended, w_o, preferred_element_type=jnp.float32)
    act_two = to_bf16(rms_norm(residual, gain_two))
    gate = jnp.dot(act_two, w_gate, preferred_element_type=jnp.float32)
    hidden = to_bf16(jax.nn.silu(gate) * jnp.dot(act_two, w_up, preferred_element_type=jnp.float32))
    return residual + jnp.dot(hidden, w_down, preferred_element_type=jnp.float32)


def reference(tokens, pos, doc_id, dy, table, w_q, w_k, w_v, w_o, w_gate, w_up, w_down, gain_one, gain_two, inv_freq):
    params = tuple(weight.astype(jnp.float32) for weight in (table, w_q, w_k, w_v, w_o, w_gate, w_up, w_down, gain_one, gain_two))
    layer_out, pullback = jax.vjp(lambda *weights: forward_pass(weights, tokens, pos, doc_id, inv_freq), *params)
    grads = pullback(dy.astype(jnp.float32))
    return (layer_out.astype(jnp.bfloat16), grads[0], grads[1], grads[2], grads[3], grads[4], grads[5], grads[6], grads[7], grads[8], grads[9])
```

```python
import functools
import jax
import jax.numpy as jnp
from jax import lax
from jax.experimental import pallas as pl
from jax.experimental.pallas import tpu as pltpu
from jax.sharding import PartitionSpec as P

NORM_EPS = 1e-5
NEG_BIG = -1e30
F32 = jnp.float32
BF16 = jnp.bfloat16


def rms_stats(feats):
    inv_rms = lax.rsqrt(jnp.mean(feats * feats, axis=-1, keepdims=True) + NORM_EPS)
    return feats * inv_rms, inv_rms


def rms_back(d_normed, normed, inv_rms):
    return inv_rms * (d_normed - normed * jnp.mean(d_normed * normed, axis=-1, keepdims=True))


def rotate(tensor_in, cosine, sine):
    half = tensor_in.shape[-1] // 2
    first = tensor_in[..., :half]
    second = tensor_in[..., half:]
    return jnp.concatenate([first * cosine - second * sine, second * cosine + first * sine], axis=-1)


def to_bf16(feats):
    return feats.astype(BF16).astype(F32)


def dot(a, b, ca, cb):
    return lax.dot_general(a, b, (((ca,), (cb,)), ((), ())), preferred_element_type=F32)


def slot_sequence(slot, block_len, cp_count):
    shard = slot // (2 * block_len)
    within = slot % (2 * block_len)
    block_no = jnp.where(within < block_len, shard, 2 * cp_count - 1 - shard)
    return block_no * block_len + within % block_len


def slot_block(j):
    return jnp.where(j < 4, 2 * j, 15 - 2 * j)


def qkv_kernel(x, gain, wq, wk, wv, cos, sin, act, q, k, v, *, head_dim):
    feats = x[...].astype(F32)
    inv = lax.rsqrt(jnp.mean(feats * feats, axis=-1, keepdims=True) + NORM_EPS)
    a = (feats * inv * gain[...]).astype(BF16)
    act[...] = a
    for w, out, turn in ((wq, q, True), (wk, k, True), (wv, v, False)):
        t = jnp.dot(a, w[...], preferred_element_type=F32)
        for h in range(w.shape[1] // head_dim):
            cols = slice(h * head_dim, (h + 1) * head_dim)
            th = t[:, cols]
            if turn:
                th = th * cos[...] + pltpu.roll(th, head_dim // 2, 1) * sin[...]
            out[:, cols] = th.astype(BF16)


def project_qkv(x_all, gain, wq, wk, wv, cos, sin, block=256):
    total, dim = x_all.shape
    width = wq.shape[1]
    head_dim = cos.shape[1]
    rows = lambda n: pl.BlockSpec((block, n), lambda i: (i, 0))
    whole = lambda a: pl.BlockSpec(a.shape, lambda i: (0, 0))
    return pl.pallas_call(
        functools.partial(qkv_kernel, head_dim=head_dim),
        out_shape=[jax.ShapeDtypeStruct((total, n), BF16) for n in (dim, width, width, width)],
        grid=(total // block,),
        in_specs=[rows(dim), whole(gain), whole(wq), whole(wk), whole(wv), rows(head_dim), rows(head_dim)],
        out_specs=[rows(dim), rows(width), rows(width), rows(width)],
        compiler_params=pltpu.CompilerParams(vmem_limit_bytes=48 * 1024 * 1024),
        cost_estimate=pl.CostEstimate(flops=6 * total * dim * width, bytes_accessed=4 * total * dim + 6 * dim * width + 6 * total * width, transcendentals=0),
        name="project_qkv",
    )(x_all, gain, wq, wk, wv, cos, sin)


def attend_kernel(info, q, k, v, doc_col, doc_row, out, lse, sc, *, heads, head_dim, scale):
    blk = q.shape[0]
    b = info[pl.program_id(0)]
    jmin = info[2 + pl.program_id(0)]
    row_n = lax.broadcasted_iota(jnp.int32, (blk, blk), 0) + b * blk
    col_n = lax.broadcasted_iota(jnp.int32, (blk, blk), 1)

    def score(j, peaks):
        sb = slot_block(j)
        off = pl.multiple_of(sb * blk, blk)
        allowed = (doc_col[...] == doc_row[sb]) & (col_n + j * blk <= row_n)
        new = []
        for h in range(heads):
            cols = slice(h * head_dim, (h + 1) * head_dim)
            s = dot(q[:, cols], k[pl.ds(off, blk), cols], 1, 1) * scale
            s = jnp.where(allowed, s, NEG_BIG)
            sc[j, h] = s
            new.append(jnp.maximum(peaks[h], jnp.max(s, axis=1, keepdims=True)))
        return tuple(new)

    peaks = lax.fori_loop(jmin, b + 1, score, tuple(jnp.full((blk, 1), NEG_BIG, F32) for _ in range(heads)))

    def weigh(j, sums):
        new = []
        for h in range(heads):
            p = jnp.exp(sc[j, h] - peaks[h])
            sc[j, h] = p
            new.append(sums[h] + jnp.sum(p, axis=1, keepdims=True))
        return tuple(new)

    sums = lax.fori_loop(jmin, b + 1, weigh, tuple(jnp.zeros((blk, 1), F32) for _ in range(heads)))
    inv = tuple(1.0 / t for t in sums)
    for h in range(heads):
        lse[:, h:h + 1] = peaks[h] + jnp.log(sums[h])

    def mix(j, acc):
        off = pl.multiple_of(slot_block(j) * blk, blk)
        new = []
        for h in range(heads):
            cols = slice(h * head_dim, (h + 1) * head_dim)
            new.append(acc[h] + jnp.dot((sc[j, h] * inv[h]).astype(BF16), v[pl.ds(off, blk), cols], preferred_element_type=F32))
        return tuple(new)

    acc = lax.fori_loop(jmin, b + 1, mix, tuple(jnp.zeros((blk, head_dim), F32) for _ in range(heads)))
    for h in range(heads):
        out[:, h * head_dim:(h + 1) * head_dim] = acc[h].astype(BF16)


def attend(info, q, k, v, doc_col, doc_row, head_dim, blk):
    total, width = k.shape
    heads = width // head_dim
    mine = lambda n: pl.BlockSpec((blk, n), lambda i, info: (2 * info[6] + i, 0))
    whole = lambda a: pl.BlockSpec(a.shape, lambda i, info: (0,) * a.ndim)
    return pl.pallas_call(
        functools.partial(attend_kernel, heads=heads, head_dim=head_dim, scale=head_dim ** -0.5),
        out_shape=[jax.ShapeDtypeStruct((2 * blk, width), BF16), jax.ShapeDtypeStruct((2 * blk, 8), F32)],
        grid_spec=pltpu.PrefetchScalarGridSpec(
            num_scalar_prefetch=1,
            grid=(2,),
            in_specs=[mine(width), whole(k), whole(v), mine(1), whole(doc_row)],
            out_specs=[pl.BlockSpec((blk, width), lambda i, info: (i, 0)), pl.BlockSpec((blk, 8), lambda i, info: (i, 0))],
            scratch_shapes=[pltpu.VMEM((total // blk, heads, blk, blk), F32)],
        ),
        compiler_params=pltpu.CompilerParams(vmem_limit_bytes=40 * 1024 * 1024),
        cost_estimate=pl.CostEstimate(flops=4 * 2 * blk * total * width, bytes_accessed=8 * total * width, transcendentals=heads * blk * total),
        name="attend",
    )(info, q, k, v, doc_col, doc_row)


def attend_back_kernel(info, q, k, v, do, doc_col, doc_row, lse_col, lse_row, del_col, del_row, cos, sin, out, acc, *, heads, head_dim, scale):
    blk = cos.shape[0]
    width = heads * head_dim
    i = pl.program_id(0)
    b = info[i]
    jmin = info[2 + i]
    imax = info[4 + i]
    me = pl.multiple_of((2 * info[6] + i) * blk, blk)
    mine = pl.ds(me, blk)
    iota_r = lax.broadcasted_iota(jnp.int32, (blk, blk), 0)
    iota_c = lax.broadcasted_iota(jnp.int32, (blk, blk), 1)
    acc[...] = jnp.zeros_like(acc)
    spans = [slice(h * head_dim, (h + 1) * head_dim) for h in range(heads)]

    def for_query(j, c):
        sb = slot_block(j)
        there = pl.ds(pl.multiple_of(sb * blk, blk), blk)
        allowed = (doc_col[mine, :] == doc_row[sb]) & (iota_c + j * blk <= iota_r + b * blk)
        for h, cols in enumerate(spans):
            s = jnp.where(allowed, dot(q[mine, cols], k[there, cols], 1, 1) * scale, NEG_BIG)
            p = jnp.exp(s - lse_col[mine, h:h + 1])
            dp = to_bf16(dot(do[mine, cols], v[there, cols], 1, 1))
            ds = (p * (dp - del_col[mine, h:h + 1]) * scale).astype(BF16)
            acc[0, :, cols] += jnp.dot(ds, k[there, cols], preferred_element_type=F32)
        return c

    lax.fori_loop(jmin, b + 1, for_query, 0)
    my_block = 2 * info[6] + i

    def for_key(j, c):
        sb = slot_block(j)
        there = pl.ds(pl.multiple_of(sb * blk, blk), blk)
        allowed = (doc_col[mine, :] == doc_row[sb]) & (iota_r + b * blk <= iota_c + j * blk)
        for h, cols in enumerate(spans):
            s = jnp.where(allowed, dot(k[mine, cols], q[there, cols], 1, 1) * scale, NEG_BIG)
            p = jnp.exp(s - lse_row[sb, h:h + 1, :])
            dp = to_bf16(dot(v[mine, cols], do[there, cols], 1, 1))
            ds = (p * (dp - del_row[sb, h:h + 1, :]) * scale).astype(BF16)
            acc[2, :, cols] += jnp.dot(p.astype(BF16), do[there, cols], preferred_element_type=F32)
            acc[1, :, cols] += jnp.dot(ds, q[there, cols], preferred_element_type=F32)
        return c

    lax.fori_loop(b, imax + 1, for_key, 0)
    for part in range(3):
        for h, cols in enumerate(spans):
            t = acc[part, :, cols]
            if part < 2:
                t = to_bf16(t)
                t = t * cos[...] - pltpu.roll(t, head_dim // 2, 1) * sin[...]
            out[:, part * width + h * head_dim:part * width + (h + 1) * head_dim] = t.astype(BF16)


def attend_back(info, q, k, v, do, doc_col, doc_row, lse_col, lse_row, del_col, del_row, cos, sin, blk):
    total, width = k.shape
    head_dim = cos.shape[1]
    heads = width // head_dim
    mine = lambda n: pl.BlockSpec((blk, n), lambda i, info: (2 * info[6] + i, 0))
    whole = lambda a: pl.BlockSpec(a.shape, lambda i, info: (0,) * a.ndim)
    arrays = (q, k, v, do, doc_col, doc_row, lse_col, lse_row, del_col, del_row)
    return pl.pallas_call(
        functools.partial(attend_back_kernel, heads=heads, head_dim=head_dim, scale=head_dim ** -0.5),
        out_shape=jax.ShapeDtypeStruct((2 * blk, 3 * width), BF16),
        grid_spec=pltpu.PrefetchScalarGridSpec(
            num_scalar_prefetch=1,
            grid=(2,),
            in_specs=[whole(a) for a in arrays] + [mine(head_dim), mine(head_dim)],
            out_specs=pl.BlockSpec((blk, 3 * width), lambda i, info: (i, 0)),
            scratch_shapes=[pltpu.VMEM((3, blk, width), F32)],
        ),
        compiler_params=pltpu.CompilerParams(vmem_limit_bytes=48 * 1024 * 1024),
        cost_estimate=pl.CostEstimate(flops=14 * 2 * blk * total * width // 2, bytes_accessed=12 * total * width, transcendentals=heads * blk * total),
        name="attend_back",
    )(info, *arrays, cos, sin)


def scatter_kernel(order, sid, bounds, d_hbm, base_hbm, out_hbm, rows, load_sem, row_sem):
    lo = bounds[0]
    hi = bounds[1]
    load = pltpu.make_async_copy(d_hbm, rows, load_sem)
    load.start()
    load.wait()

    def add_body(p, first):
        t = order[p]
        same = jnp.logical_and(p > lo, sid[p] == sid[jnp.maximum(p - 1, 0)])

        @pl.when(same)
        def _():
            rows[pl.ds(first, 1), :] = rows[pl.ds(first, 1), :] + rows[pl.ds(t, 1), :]

        return jnp.where(same, first, t)

    lax.fori_loop(lo, hi, add_body, 0)

    def send_body(p, count):
        new = jnp.logical_or(p == lo, sid[p] != sid[jnp.maximum(p - 1, 0)])

        @pl.when(new)
        def _():
            pltpu.make_async_copy(rows.at[pl.ds(order[p], 1), :], out_hbm.at[pl.ds(sid[p], 1), :], row_sem).start()

        return count + new.astype(jnp.int32)

    count = lax.fori_loop(lo, hi, send_body, 0)

    def wait_body(p, c):
        pltpu.make_async_copy(rows.at[pl.ds(0, 1), :], out_hbm.at[pl.ds(0, 1), :], row_sem).wait()
        return c

    lax.fori_loop(0, count, wait_body, 0)


def scatter_rows(order, sid, bounds, grads, rows):
    total, dim = grads.shape
    base = jnp.zeros((rows, dim), F32)
    return pl.pallas_call(
        scatter_kernel,
        out_shape=jax.ShapeDtypeStruct((rows, dim), F32),
        grid_spec=pltpu.PrefetchScalarGridSpec(
            num_scalar_prefetch=3,
            grid=(),
            in_specs=[pl.BlockSpec(memory_space=pl.ANY), pl.BlockSpec(memory_space=pl.ANY)],
            out_specs=pl.BlockSpec(memory_space=pl.ANY),
            scratch_shapes=[pltpu.VMEM((total, dim), F32), pltpu.SemaphoreType.DMA, pltpu.SemaphoreType.DMA],
        ),
        input_output_aliases={4: 0},
        compiler_params=pltpu.CompilerParams(vmem_limit_bytes=28 * 1024 * 1024),
        name="scatter_rows",
    )(order, sid, bounds, grads, base)


def solution(mesh):
    cp_count = mesh.shape["cp"]
    tp_count = mesh.shape["tp"]
    both = ("cp", "tp")
    x_swap = [(i, i ^ 2) for i in range(cp_count)]
    core_swap = [(i, i ^ 1) for i in range(cp_count)]

    def device_step(tokens, pos, doc_id, dy, table, w_q, w_k, w_v, w_o, w_gate, w_up, w_down, gain_one, gain_two, inv_freq):
        span = tokens.shape[0]
        total = span * cp_count
        part = span // tp_count
        rows, dim = table.shape
        head_dim = 2 * inv_freq.shape[0]
        heads = w_q.shape[1] // head_dim
        width = heads * head_dim
        scale = head_dim ** -0.5
        tp_rank = lax.axis_index("tp")
        cp_rank = lax.axis_index("cp")
        core = cp_rank % 2
        gain_a = gain_one.astype(F32)
        gain_b = gain_two.astype(F32)

        def own(arr):
            return lax.dynamic_slice_in_dim(arr, cp_rank * span, span, 0)

        local_ids = tokens - tp_rank * rows
        owned = (local_ids >= 0) & (local_ids < rows)
        safe_ids = jnp.where(owned, local_ids, 0)
        picked = jnp.where(owned[:, None], jnp.take(table, safe_ids, axis=0), jnp.zeros((), BF16))
        x_slice = lax.psum_scatter(picked, "tp", scatter_dimension=0, tiled=True)
        x_all = lax.all_gather(x_slice, both, axis=0, tiled=True)

        ints = lax.all_gather(jnp.stack([tokens, pos, doc_id]), "cp", axis=1, tiled=True)
        tok_all, pos_all, doc_all = ints[0], ints[1], ints[2]

        half = dim // 2
        wo_half = lax.dynamic_slice_in_dim(w_o, core * half, half, 1)
        wo_mine = lax.all_gather(wo_half, "tp", axis=0, tiled=True)
        wo_other = lax.ppermute(wo_mine, "cp", core_swap)
        wo_full = jnp.zeros((tp_count * width, dim), BF16)
        wo_full = lax.dynamic_update_slice_in_dim(wo_full, wo_mine, core * half, 1)
        wo_full = lax.dynamic_update_slice_in_dim(wo_full, wo_other, (1 - core) * half, 1)

        dy_x = lax.ppermute(dy, "cp", x_swap)
        dy_all = jnp.zeros((total, dim), BF16)
        for piece, who in ((dy, cp_rank), (dy_x, cp_rank ^ 2), (lax.ppermute(dy, "cp", core_swap), cp_rank ^ 1), (lax.ppermute(dy_x, "cp", core_swap), cp_rank ^ 3)):
            dy_all = lax.dynamic_update_slice_in_dim(dy_all, piece, who * span, 0)

        ids_all = tok_all
        slot_ids = jnp.arange(total, dtype=jnp.int32)
        before = (ids_all[None, :] < ids_all[:, None]) | ((ids_all[None, :] == ids_all[:, None]) & (slot_ids[None, :] < slot_ids[:, None]))
        rank = jnp.sum(before.astype(jnp.int32), axis=1)
        at_rank = rank[None, :] == slot_ids[:, None]
        order = jnp.sum(jnp.where(at_rank, slot_ids[None, :], 0), axis=1)
        sid = jnp.sum(jnp.where(at_rank, ids_all[None, :], 0), axis=1) - tp_rank * rows
        bounds = jnp.stack([jnp.sum((ids_all < tp_rank * rows).astype(jnp.int32)), jnp.sum((ids_all < (tp_rank + 1) * rows).astype(jnp.int32))])

        angle = pos_all.astype(F32)[:, None] * inv_freq[None, :]
        cos = jnp.cos(angle)
        sin = jnp.sin(angle)
        cos = jnp.concatenate([cos, cos], axis=1)
        sin = jnp.concatenate([-sin, sin], axis=1)
        act_a, query, key, value = project_qkv(x_all, gain_a[None, :], w_q, w_k, w_v, cos, sin)

        blk = span // 2
        blocks = total // blk
        doc_col = doc_all[:, None]
        doc_row = doc_all.reshape(blocks, 1, blk)
        seq_block = jnp.concatenate([jnp.arange(0, blocks, 2), jnp.arange(blocks - 1, 0, -2)])
        doc_seq = doc_all.reshape(blocks, blk)[seq_block]
        first_doc, last_doc = doc_seq[:, 0], doc_seq[:, -1]
        b_own = jnp.stack([cp_rank, blocks - 1 - cp_rank])
        first_own, last_own = first_doc[b_own], last_doc[b_own]
        jmin = jnp.sum((last_doc[None, :] < first_own[:, None]).astype(jnp.int32), axis=1)
        imax = jnp.sum((first_doc[None, :] <= last_own[:, None]).astype(jnp.int32), axis=1) - 1
        info = jnp.concatenate([b_own, jmin, imax, cp_rank[None]]).astype(jnp.int32)
        attended, lse = attend(info, query, key, value, doc_col, doc_row, head_dim, blk)

        att_parts = lax.all_gather(attended, both, axis=0, tiled=False).reshape(cp_count, tp_count, span, width)
        att_own = jnp.transpose(lax.dynamic_index_in_dim(att_parts, cp_rank, 0, keepdims=False), (1, 0, 2)).reshape(span, tp_count * width)
        x_own = own(x_all).astype(F32)
        residual = x_own + dot(att_own, wo_full, 1, 0)
        normed_o, inv_o = rms_stats(residual)
        act_b = (normed_o * gain_b).astype(BF16)

        def mlp(act, dyt):
            gate = dot(act, w_gate, 1, 0)
            up_val = dot(act, w_up, 1, 0)
            gate_sig = jax.nn.sigmoid(gate)
            hidden = (gate * gate_sig * up_val).astype(BF16)
            d_hidden = to_bf16(dot(dyt, w_down, 1, 1))
            d_gate = (d_hidden * up_val * gate_sig * (1.0 + gate * (1.0 - gate_sig))).astype(BF16)
            d_up = (d_hidden * gate * gate_sig).astype(BF16)
            return hidden, d_gate, d_up

        hidden, d_gate, d_up = mlp(act_b, dy)
        d_act_b = dot(d_gate, w_gate, 1, 1) + dot(d_up, w_up, 1, 1)
        d_act_b = to_bf16(lax.psum_scatter(d_act_b, "tp", scatter_dimension=0, tiled=True))

        def mine(arr):
            return lax.dynamic_slice_in_dim(arr, tp_rank * part, part, 0)

        res_part = mine(residual)
        normed_b, inv_b = rms_stats(res_part)
        grad_gain_b = jnp.sum(d_act_b * normed_b, axis=0)
        d_resid = mine(dy).astype(F32) + rms_back(d_act_b * gain_b, normed_b, inv_b)
        d_resid_all = lax.all_gather(d_resid.astype(BF16), both, axis=0, tiled=True)

        out_part = lax.psum_scatter(dot(hidden, w_down, 1, 0), "tp", scatter_dimension=0, tiled=True)
        layer_out = lax.all_gather((res_part + out_part).astype(BF16), "tp", axis=0, tiled=True)

        d_att = dot(d_resid_all, w_o, 1, 1)
        d_att_b = d_att.astype(BF16)
        att_heads = lax.dynamic_index_in_dim(att_parts, tp_rank, 1, keepdims=False).reshape(total, width)
        head_of = (jnp.arange(width)[None, :] // head_dim == jnp.arange(8)[:, None]).astype(F32)
        prod = att_heads.astype(F32) * d_att_b.astype(F32)
        delta = lax.dot_general(head_of, prod, (((1,), (1,)), ((), ())), precision=lax.Precision.HIGHEST, preferred_element_type=F32)
        lse_all = lax.all_gather(lse, "cp", axis=0, tiled=True)

        def by_block(arr):
            return jnp.transpose(arr.reshape(8, blocks, blk), (1, 0, 2))

        dqkv = attend_back(info, query, key, value, d_att_b, doc_col, doc_row, lse_all, by_block(lse_all.T), delta.T, by_block(delta), cos, sin, blk)
        d_q_pre, d_k_pre, d_v_pre = (dqkv[:, i * width:(i + 1) * width] for i in range(3))
        d_act_a = dot(d_q_pre, w_q, 1, 1) + dot(d_k_pre, w_k, 1, 1) + dot(d_v_pre, w_v, 1, 1)
        d_act_a = to_bf16(lax.psum_scatter(d_act_a, "tp", scatter_dimension=0, tiled=True))
        dqkv_all = lax.all_gather(dqkv, "cp", axis=0, tiled=True)
        normed_a, inv_a = rms_stats(x_slice.astype(F32))
        grad_gain_a = jnp.sum(d_act_a * normed_a, axis=0)
        d_embed = d_resid + rms_back(d_act_a * gain_a, normed_a, inv_a)
        d_embed_all = lax.all_gather(d_embed, both, axis=0, tiled=True)
        gain_grads = lax.psum(jnp.stack([grad_gain_a, grad_gain_b]), both)

        att_all = jnp.transpose(att_parts, (0, 2, 1, 3)).reshape(total, tp_count * width)
        resid_all = x_all.astype(F32) + dot(att_all, wo_full, 1, 0)
        act_b_all = (rms_stats(resid_all)[0] * gain_b).astype(BF16)
        hidden_all, d_gate_all, d_up_all = mlp(act_b_all, dy_all)
        grad_down = dot(hidden_all, dy_all, 0, 0)
        grad_gate = dot(act_b_all, d_gate_all, 0, 0)
        grad_up = dot(act_b_all, d_up_all, 0, 0)
        grad_out = dot(att_heads, d_resid_all, 0, 0)
        grad_qkv = [dot(act_a, dqkv_all[:, i * width:(i + 1) * width], 0, 0) for i in range(3)]

        grad_table = scatter_rows(order, sid, bounds, d_embed_all, rows)
        return (layer_out, grad_table, *grad_qkv, grad_out, grad_gate, grad_up, grad_down, gain_grads[0], gain_grads[1])

    col_spec = P(None, "tp")
    row_spec = P("tp", None)
    tok_spec = P("cp")
    rep_spec = P(None)
    in_specs = (tok_spec, tok_spec, tok_spec, P("cp", None), row_spec, col_spec, col_spec, col_spec, row_spec, col_spec, col_spec, row_spec, rep_spec, rep_spec, rep_spec)
    out_specs = (P("cp", None), row_spec, col_spec, col_spec, col_spec, row_spec, col_spec, col_spec, row_spec, rep_spec, rep_spec)
    return jax.shard_map(device_step, mesh=mesh, in_specs=in_specs, out_specs=out_specs, check_vma=False)
```

```python
import functools
import jax
import jax.numpy as jnp
from jax import lax
from jax.experimental import pallas as pl
from jax.experimental.pallas import tpu as pltpu
from jax.sharding import PartitionSpec as P

NORM_EPS = 1e-5
NEG_BIG = -1e30
F32 = jnp.float32
BF16 = jnp.bfloat16


def rms_stats(feats):
    inv_rms = lax.rsqrt(jnp.mean(feats * feats, axis=-1, keepdims=True) + NORM_EPS)
    return feats * inv_rms, inv_rms


def rms_back(d_normed, normed, inv_rms):
    return inv_rms * (d_normed - normed * jnp.mean(d_normed * normed, axis=-1, keepdims=True))


def rotate(tensor_in, cosine, sine):
    half = tensor_in.shape[-1] // 2
    first = tensor_in[..., :half]
    second = tensor_in[..., half:]
    return jnp.concatenate([first * cosine - second * sine, second * cosine + first * sine], axis=-1)


def to_bf16(feats):
    return feats.astype(BF16).astype(F32)


def dot(a, b, ca, cb):
    return lax.dot_general(a, b, (((ca,), (cb,)), ((), ())), preferred_element_type=F32)


def slot_sequence(slot, block_len, cp_count):
    shard = slot // (2 * block_len)
    within = slot % (2 * block_len)
    block_no = jnp.where(within < block_len, shard, 2 * cp_count - 1 - shard)
    return block_no * block_len + within % block_len


def slot_block(j):
    return jnp.where(j < 4, 2 * j, 15 - 2 * j)


def qkv_kernel(x, gain, wq, wk, wv, cos, sin, act, q, k, v, *, head_dim):
    feats = x[...].astype(F32)
    inv = lax.rsqrt(jnp.mean(feats * feats, axis=-1, keepdims=True) + NORM_EPS)
    a = (feats * inv * gain[...]).astype(BF16)
    act[...] = a
    for w, out, turn in ((wq, q, True), (wk, k, True), (wv, v, False)):
        t = jnp.dot(a, w[...], preferred_element_type=F32)
        for h in range(w.shape[1] // head_dim):
            cols = slice(h * head_dim, (h + 1) * head_dim)
            th = t[:, cols]
            if turn:
                th = th * cos[...] + pltpu.roll(th, head_dim // 2, 1) * sin[...]
            out[:, cols] = th.astype(BF16)


def project_qkv(x_all, gain, wq, wk, wv, cos, sin, block=256):
    total, dim = x_all.shape
    width = wq.shape[1]
    head_dim = cos.shape[1]
    rows = lambda n: pl.BlockSpec((block, n), lambda i: (i, 0))
    whole = lambda a: pl.BlockSpec(a.shape, lambda i: (0, 0))
    return pl.pallas_call(
        functools.partial(qkv_kernel, head_dim=head_dim),
        out_shape=[jax.ShapeDtypeStruct((total, n), BF16) for n in (dim, width, width, width)],
        grid=(total // block,),
        in_specs=[rows(dim), whole(gain), whole(wq), whole(wk), whole(wv), rows(head_dim), rows(head_dim)],
        out_specs=[rows(dim), rows(width), rows(width), rows(width)],
        compiler_params=pltpu.CompilerParams(vmem_limit_bytes=48 * 1024 * 1024),
        cost_estimate=pl.CostEstimate(flops=6 * total * dim * width, bytes_accessed=4 * total * dim + 6 * dim * width + 6 * total * width, transcendentals=0),
        name="project_qkv",
    )(x_all, gain, wq, wk, wv, cos, sin)


def attend_kernel(info, q, k, v, doc_col, doc_row, out, lse, sc, *, heads, head_dim, scale):
    blk = q.shape[0]
    b = info[pl.program_id(0)]
    jmin = info[2 + pl.program_id(0)]
    row_n = lax.broadcasted_iota(jnp.int32, (blk, blk), 0) + b * blk
    col_n = lax.broadcasted_iota(jnp.int32, (blk, blk), 1)

    def score(j, peaks):
        sb = slot_block(j)
        off = pl.multiple_of(sb * blk, blk)
        allowed = (doc_col[...] == doc_row[sb]) & (col_n + j * blk <= row_n)
        new = []
        for h in range(heads):
            cols = slice(h * head_dim, (h + 1) * head_dim)
            s = dot(q[:, cols], k[pl.ds(off, blk), cols], 1, 1) * scale
            s = jnp.where(allowed, s, NEG_BIG)
            sc[j, h] = s
            new.append(jnp.maximum(peaks[h], jnp.max(s, axis=1, keepdims=True)))
        return tuple(new)

    peaks = lax.fori_loop(jmin, b + 1, score, tuple(jnp.full((blk, 1), NEG_BIG, F32) for _ in range(heads)))

    def weigh(j, sums):
        new = []
        for h in range(heads):
            p = jnp.exp(sc[j, h] - peaks[h])
            sc[j, h] = p
            new.append(sums[h] + jnp.sum(p, axis=1, keepdims=True))
        return tuple(new)

    sums = lax.fori_loop(jmin, b + 1, weigh, tuple(jnp.zeros((blk, 1), F32) for _ in range(heads)))
    inv = tuple(1.0 / t for t in sums)
    for h in range(heads):
        lse[:, h:h + 1] = peaks[h] + jnp.log(sums[h])

    def mix(j, acc):
        off = pl.multiple_of(slot_block(j) * blk, blk)
        new = []
        for h in range(heads):
            cols = slice(h * head_dim, (h + 1) * head_dim)
            new.append(acc[h] + jnp.dot((sc[j, h] * inv[h]).astype(BF16), v[pl.ds(off, blk), cols], preferred_element_type=F32))
        return tuple(new)

    acc = lax.fori_loop(jmin, b + 1, mix, tuple(jnp.zeros((blk, head_dim), F32) for _ in range(heads)))
    for h in range(heads):
        out[:, h * head_dim:(h + 1) * head_dim] = acc[h].astype(BF16)


def attend(info, q, k, v, doc_col, doc_row, head_dim, blk):
    total, width = k.shape
    heads = width // head_dim
    mine = lambda n: pl.BlockSpec((blk, n), lambda i, info: (2 * info[6] + i, 0))
    whole = lambda a: pl.BlockSpec(a.shape, lambda i, info: (0,) * a.ndim)
    return pl.pallas_call(
        functools.partial(attend_kernel, heads=heads, head_dim=head_dim, scale=head_dim ** -0.5),
        out_shape=[jax.ShapeDtypeStruct((2 * blk, width), BF16), jax.ShapeDtypeStruct((2 * blk, 8), F32)],
        grid_spec=pltpu.PrefetchScalarGridSpec(
            num_scalar_prefetch=1,
            grid=(2,),
            in_specs=[mine(width), whole(k), whole(v), mine(1), whole(doc_row)],
            out_specs=[pl.BlockSpec((blk, width), lambda i, info: (i, 0)), pl.BlockSpec((blk, 8), lambda i, info: (i, 0))],
            scratch_shapes=[pltpu.VMEM((total // blk, heads, blk, blk), F32)],
        ),
        compiler_params=pltpu.CompilerParams(vmem_limit_bytes=40 * 1024 * 1024),
        cost_estimate=pl.CostEstimate(flops=4 * 2 * blk * total * width, bytes_accessed=8 * total * width, transcendentals=heads * blk * total),
        name="attend",
    )(info, q, k, v, doc_col, doc_row)


def attend_back_kernel(info, q, k, v, do, doc_col, doc_row, lse_col, lse_row, del_col, del_row, cos, sin, out, acc, *, heads, head_dim, scale):
    blk = cos.shape[0]
    width = heads * head_dim
    i = pl.program_id(0)
    b = info[i]
    jmin = info[2 + i]
    imax = info[4 + i]
    me = pl.multiple_of((2 * info[6] + i) * blk, blk)
    mine = pl.ds(me, blk)
    iota_r = lax.broadcasted_iota(jnp.int32, (blk, blk), 0)
    iota_c = lax.broadcasted_iota(jnp.int32, (blk, blk), 1)
    acc[...] = jnp.zeros_like(acc)
    spans = [slice(h * head_dim, (h + 1) * head_dim) for h in range(heads)]

    def for_query(j, c):
        sb = slot_block(j)
        there = pl.ds(pl.multiple_of(sb * blk, blk), blk)
        allowed = (doc_col[mine, :] == doc_row[sb]) & (iota_c + j * blk <= iota_r + b * blk)
        for h, cols in enumerate(spans):
            s = jnp.where(allowed, dot(q[mine, cols], k[there, cols], 1, 1) * scale, NEG_BIG)
            p = jnp.exp(s - lse_col[mine, h:h + 1])
            dp = to_bf16(dot(do[mine, cols], v[there, cols], 1, 1))
            ds = (p * (dp - del_col[mine, h:h + 1]) * scale).astype(BF16)
            acc[0, :, cols] += jnp.dot(ds, k[there, cols], preferred_element_type=F32)
        return c

    lax.fori_loop(jmin, b + 1, for_query, 0)
    my_block = 2 * info[6] + i

    def for_key(j, c):
        sb = slot_block(j)
        there = pl.ds(pl.multiple_of(sb * blk, blk), blk)
        allowed = (doc_col[mine, :] == doc_row[sb]) & (iota_r + b * blk <= iota_c + j * blk)
        for h, cols in enumerate(spans):
            s = jnp.where(allowed, dot(k[mine, cols], q[there, cols], 1, 1) * scale, NEG_BIG)
            p = jnp.exp(s - lse_row[sb, h:h + 1, :])
            dp = to_bf16(dot(v[mine, cols], do[there, cols], 1, 1))
            ds = (p * (dp - del_row[sb, h:h + 1, :]) * scale).astype(BF16)
            acc[2, :, cols] += jnp.dot(p.astype(BF16), do[there, cols], preferred_element_type=F32)
            acc[1, :, cols] += jnp.dot(ds, q[there, cols], preferred_element_type=F32)
        return c

    lax.fori_loop(b, imax + 1, for_key, 0)
    for part in range(3):
        for h, cols in enumerate(spans):
            t = acc[part, :, cols]
            if part < 2:
                t = to_bf16(t)
                t = t * cos[...] - pltpu.roll(t, head_dim // 2, 1) * sin[...]
            out[:, part * width + h * head_dim:part * width + (h + 1) * head_dim] = t.astype(BF16)


def attend_back(info, q, k, v, do, doc_col, doc_row, lse_col, lse_row, del_col, del_row, cos, sin, blk):
    total, width = k.shape
    head_dim = cos.shape[1]
    heads = width // head_dim
    mine = lambda n: pl.BlockSpec((blk, n), lambda i, info: (2 * info[6] + i, 0))
    whole = lambda a: pl.BlockSpec(a.shape, lambda i, info: (0,) * a.ndim)
    arrays = (q, k, v, do, doc_col, doc_row, lse_col, lse_row, del_col, del_row)
    return pl.pallas_call(
        functools.partial(attend_back_kernel, heads=heads, head_dim=head_dim, scale=head_dim ** -0.5),
        out_shape=jax.ShapeDtypeStruct((2 * blk, 3 * width), BF16),
        grid_spec=pltpu.PrefetchScalarGridSpec(
            num_scalar_prefetch=1,
            grid=(2,),
            in_specs=[whole(a) for a in arrays] + [mine(head_dim), mine(head_dim)],
            out_specs=pl.BlockSpec((blk, 3 * width), lambda i, info: (i, 0)),
            scratch_shapes=[pltpu.VMEM((3, blk, width), F32)],
        ),
        compiler_params=pltpu.CompilerParams(vmem_limit_bytes=48 * 1024 * 1024),
        cost_estimate=pl.CostEstimate(flops=14 * 2 * blk * total * width // 2, bytes_accessed=12 * total * width, transcendentals=heads * blk * total),
        name="attend_back",
    )(info, *arrays, cos, sin)


def out_proj_kernel(info, x, att, w0, w1, w2, w3, gain, res, act, wbuf, sems):
    tp, rows, width = att.shape
    part = w0.shape[1]

    def fetch(r):
        for i, w in enumerate((w0, w1, w2, w3)):
            @pl.when(r == i)
            def _(i=i, w=w):
                pltpu.make_async_copy(w, wbuf.at[i % 2], sems.at[i % 2]).start()

    fetch(0)

    def step(r, c):
        slot = lax.rem(r, 2)
        fetch(r + 1)
        pltpu.make_async_copy(w0, wbuf.at[slot], sems.at[slot]).wait()
        cols = pl.ds(pl.multiple_of((info[6] ^ r) * part, 128), part)
        t = x[:, cols].astype(F32)
        for i in range(tp):
            t += jnp.dot(att[i], wbuf[slot, i * width:(i + 1) * width, :], preferred_element_type=F32)
        res[:, cols] = t
        return c

    lax.fori_loop(0, 4, step, 0)
    h = res[...]
    inv = lax.rsqrt(jnp.mean(h * h, axis=-1, keepdims=True) + NORM_EPS)
    act[...] = (h * inv * gain[...]).astype(BF16)


def out_proj(info, flip, x_all, att, pieces, gain):
    tp, rows, width = att.shape
    dim = x_all.shape[1]
    whole = lambda a: pl.BlockSpec(a.shape, lambda i, info: (0,) * a.ndim)
    full = pl.BlockSpec((rows, dim), lambda i, info: (0, 0))
    return pl.pallas_call(
        out_proj_kernel,
        out_shape=[jax.ShapeDtypeStruct((rows, dim), F32), jax.ShapeDtypeStruct((rows, dim), BF16)],
        grid_spec=pltpu.PrefetchScalarGridSpec(
            num_scalar_prefetch=1,
            grid=(1,),
            in_specs=[pl.BlockSpec((rows, dim), lambda i, info: (info[6] ^ flip, 0)), whole(att)] + [pl.BlockSpec(memory_space=pl.ANY)] * 4 + [whole(gain)],
            out_specs=[full, full],
            scratch_shapes=[pltpu.VMEM((2,) + pieces[0].shape, BF16), pltpu.SemaphoreType.DMA((2,))],
        ),
        compiler_params=pltpu.CompilerParams(vmem_limit_bytes=48 * 1024 * 1024),
        cost_estimate=pl.CostEstimate(flops=2 * rows * dim * dim, bytes_accessed=2 * dim * dim + 10 * rows * dim, transcendentals=0),
        name="out_proj",
    )(info, x_all, att, *pieces, gain)


def weight_grad_kernel(info, *refs, pieces, splits):
    lhs = refs[:pieces]
    rhs = refs[pieces:2 * pieces]
    outs = refs[2 * pieces:]
    t = dot(lhs[0][...], rhs[0][...], 0, 0)
    for a, b in zip(lhs[1:], rhs[1:]):
        t += dot(a[...], b[...], 0, 0)
    width = t.shape[1] // splits
    for i, out in enumerate(outs):
        out[...] = t[:, i * width:(i + 1) * width]


def weight_grad(info, lhs, rhs, block=256, splits=1, rows=None):
    def spec(arr, p, cols, moving):
        if arr.ndim == 3:
            return pl.BlockSpec((None, arr.shape[1], cols), lambda i, info: (info[6] ^ p, 0, i if moving else 0))
        return pl.BlockSpec((arr.shape[0], cols), lambda i, info: (0, i if moving else 0))

    tokens = lhs[0].shape[-2]
    rows, dim = rows or lhs[0].shape[-1], rhs[0].shape[-1]
    n = len(lhs)
    width = dim // splits
    outs = pl.pallas_call(
        functools.partial(weight_grad_kernel, pieces=n, splits=splits),
        out_shape=[jax.ShapeDtypeStruct((rows, width), F32)] * splits,
        grid_spec=pltpu.PrefetchScalarGridSpec(
            num_scalar_prefetch=1,
            grid=(pl.cdiv(rows, block),),
            in_specs=[spec(a, p, block, True) for p, a in enumerate(lhs)] + [spec(b, p, dim, False) for p, b in enumerate(rhs)],
            out_specs=[pl.BlockSpec((block, width), lambda i, info: (i, 0))] * splits,
        ),
        compiler_params=pltpu.CompilerParams(vmem_limit_bytes=56 * 1024 * 1024),
        cost_estimate=pl.CostEstimate(flops=2 * n * tokens * rows * dim, bytes_accessed=4 * rows * dim + 2 * n * tokens * (rows + dim), transcendentals=0),
        name="weight_grad",
    )(info, *lhs, *rhs)
    return outs if splits > 1 else outs[0]


def mlp_kernel(act, dhid, wg, wu, hidden, d_gate, d_up, *grad, limit):
    i = pl.program_id(0)
    block = wg.shape[0]
    left = limit - i * block
    row_ok = lax.broadcasted_iota(jnp.int32, (block, 1), 0) < left
    col_ok = lax.broadcasted_iota(jnp.int32, (1, block), 1) < left
    wgt = jnp.where(row_ok, wg[...], jnp.zeros((), BF16))
    wut = jnp.where(row_ok, wu[...], jnp.zeros((), BF16))
    gate = dot(act[...], wgt, 1, 1)
    up = dot(act[...], wut, 1, 1)
    dh = jnp.where(col_ok, dhid[...].astype(F32), 0.0)
    sig = jax.nn.sigmoid(gate)
    hidden[...] = (gate * sig * up).astype(BF16)
    dg = (dh * up * sig * (1.0 + gate * (1.0 - sig))).astype(BF16)
    du = (dh * gate * sig).astype(BF16)
    d_gate[...] = dg
    d_up[...] = du
    if grad:
        t = jnp.dot(dg, wgt, preferred_element_type=F32) + jnp.dot(du, wut, preferred_element_type=F32)

        @pl.when(i == 0)
        def _():
            grad[0][...] = t

        @pl.when(i > 0)
        def _():
            grad[0][...] += t


def mlp_block(act, dhid, wg, wu, with_grad, block=256):
    rows, dim = act.shape
    limit = wg.shape[0]
    cols = pl.BlockSpec((rows, block), lambda i: (0, i))
    tile = pl.BlockSpec((block, dim), lambda i: (i, 0))
    whole = pl.BlockSpec((rows, dim), lambda i: (0, 0))
    return pl.pallas_call(
        functools.partial(mlp_kernel, limit=limit),
        out_shape=[jax.ShapeDtypeStruct((rows, pl.cdiv(limit, block) * block), BF16)] * 3 + [jax.ShapeDtypeStruct((rows, dim), F32)] * with_grad,
        grid=(pl.cdiv(limit, block),),
        in_specs=[whole, cols, tile, tile],
        out_specs=[cols] * 3 + [whole] * with_grad,
        compiler_params=pltpu.CompilerParams(vmem_limit_bytes=48 * 1024 * 1024),
        cost_estimate=pl.CostEstimate(flops=(4 + 4 * with_grad) * rows * dim * limit, bytes_accessed=4 * dim * limit + 6 * rows * limit + 10 * rows * dim, transcendentals=rows * limit),
        name="mlp_block",
    )(act, dhid, wg, wu)


def zero_kernel(after, out, zeros, sem):
    zeros[...] = jnp.zeros_like(zeros)
    step = zeros.shape[0]
    count = out.shape[0] // step

    def send(i, c):
        pltpu.make_async_copy(zeros, out.at[pl.ds(pl.multiple_of(i * step, step), step), :], sem).start()
        return c

    def wait(i, c):
        pltpu.make_async_copy(zeros, out.at[pl.ds(0, step), :], sem).wait()
        return c

    lax.fori_loop(0, count, send, 0)
    lax.fori_loop(0, count, wait, 0)


def zero_rows(after, rows, dim, step=200):
    return pl.pallas_call(
        zero_kernel,
        out_shape=jax.ShapeDtypeStruct((rows, dim), F32),
        in_specs=[pl.BlockSpec(memory_space=pltpu.SMEM)],
        out_specs=pl.BlockSpec(memory_space=pl.ANY),
        scratch_shapes=[pltpu.VMEM((step, dim), F32), pltpu.SemaphoreType.DMA],
        compiler_params=pltpu.CompilerParams(vmem_limit_bytes=8 * 1024 * 1024),
        cost_estimate=pl.CostEstimate(flops=rows * dim, bytes_accessed=4 * rows * dim, transcendentals=0),
        name="zero_rows",
    )(after)


def scatter_kernel(order, sid, bounds, d_hbm, base_hbm, out_hbm, rows, load_sem, row_sem):
    lo = bounds[0]
    hi = bounds[1]
    load = pltpu.make_async_copy(d_hbm, rows, load_sem)
    load.start()
    load.wait()

    def add_body(p, first):
        t = order[p]
        same = jnp.logical_and(p > lo, sid[p] == sid[jnp.maximum(p - 1, 0)])

        @pl.when(same)
        def _():
            rows[pl.ds(first, 1), :] = rows[pl.ds(first, 1), :] + rows[pl.ds(t, 1), :]

        return jnp.where(same, first, t)

    lax.fori_loop(lo, hi, add_body, 0)

    def send_body(p, count):
        new = jnp.logical_or(p == lo, sid[p] != sid[jnp.maximum(p - 1, 0)])

        @pl.when(new)
        def _():
            pltpu.make_async_copy(rows.at[pl.ds(order[p], 1), :], out_hbm.at[pl.ds(sid[p], 1), :], row_sem).start()

        return count + new.astype(jnp.int32)

    count = lax.fori_loop(lo, hi, send_body, 0)

    def wait_body(p, c):
        pltpu.make_async_copy(rows.at[pl.ds(0, 1), :], out_hbm.at[pl.ds(0, 1), :], row_sem).wait()
        return c

    lax.fori_loop(0, count, wait_body, 0)


def scatter_rows(order, sid, bounds, grads, base):
    total, dim = grads.shape
    rows = base.shape[0]
    return pl.pallas_call(
        scatter_kernel,
        out_shape=jax.ShapeDtypeStruct((rows, dim), F32),
        grid_spec=pltpu.PrefetchScalarGridSpec(
            num_scalar_prefetch=3,
            grid=(),
            in_specs=[pl.BlockSpec(memory_space=pl.ANY), pl.BlockSpec(memory_space=pl.ANY)],
            out_specs=pl.BlockSpec(memory_space=pl.ANY),
            scratch_shapes=[pltpu.VMEM((total, dim), F32), pltpu.SemaphoreType.DMA, pltpu.SemaphoreType.DMA],
        ),
        input_output_aliases={4: 0},
        compiler_params=pltpu.CompilerParams(vmem_limit_bytes=28 * 1024 * 1024),
        name="scatter_rows",
    )(order, sid, bounds, grads, base)


def solution(mesh):
    cp_count = mesh.shape["cp"]
    tp_count = mesh.shape["tp"]
    both = ("cp", "tp")
    x_swap = [(i, i ^ 2) for i in range(cp_count)]
    core_swap = [(i, i ^ 1) for i in range(cp_count)]

    def device_step(tokens, pos, doc_id, dy, table, w_q, w_k, w_v, w_o, w_gate, w_up, w_down, gain_one, gain_two, inv_freq):
        span = tokens.shape[0]
        total = span * cp_count
        part = span // tp_count
        rows, dim = table.shape
        head_dim = 2 * inv_freq.shape[0]
        heads = w_q.shape[1] // head_dim
        width = heads * head_dim
        scale = head_dim ** -0.5
        tp_rank = lax.axis_index("tp")
        cp_rank = lax.axis_index("cp")
        core = cp_rank % 2
        gain_a = gain_one.astype(F32)
        gain_b = gain_two.astype(F32)

        def own(arr):
            return lax.dynamic_slice_in_dim(arr, cp_rank * span, span, 0)

        barrier = lax.optimization_barrier
        swap = lambda arr, pairs, axis="cp": lax.ppermute(arr, axis, pairs)
        local_ids = tokens - tp_rank * rows
        owned = (local_ids >= 0) & (local_ids < rows)
        safe_ids = jnp.where(owned, local_ids, 0)
        picked = jnp.where(owned[:, None], jnp.take(table, safe_ids, axis=0), jnp.zeros((), BF16))
        x_slice = lax.psum_scatter(picked, "tp", scatter_dimension=0, tiled=True)

        ints = lax.all_gather(jnp.stack([tokens, pos, doc_id]), "cp", axis=1, tiled=True)
        tok_all, pos_all, doc_all = ints[0], ints[1], ints[2]
        slot_ids = jnp.arange(total, dtype=jnp.int32)
        before = (tok_all[None, :] < tok_all[:, None]) | ((tok_all[None, :] == tok_all[:, None]) & (slot_ids[None, :] < slot_ids[:, None]))
        rank = jnp.sum(before.astype(jnp.int32), axis=1)
        at_rank = rank[None, :] == slot_ids[:, None]
        order = jnp.sum(jnp.where(at_rank, slot_ids[None, :], 0), axis=1)
        sid = jnp.sum(jnp.where(at_rank, tok_all[None, :], 0), axis=1) - tp_rank * rows
        order = order + 8 * (order // part)
        bounds = jnp.stack([jnp.sum((tok_all < tp_rank * rows).astype(jnp.int32)), jnp.sum((tok_all < (tp_rank + 1) * rows).astype(jnp.int32))])
        base = zero_rows(bounds, rows, dim)
        quarter = dim // cp_count
        wo_part = lax.dynamic_slice_in_dim(w_o, cp_rank * quarter, quarter, 1)
        wo_near = [wo_part] + [swap(wo_part, [(i, i ^ k) for i in range(tp_count)], "tp") for k in (1, 2, 3)]
        x_slice, base, order, sid, bounds, wo_near = barrier((x_slice, base, order, sid, bounds, wo_near))
        x_all = lax.all_gather(x_slice, both, axis=0, tiled=True)

        wo_own = jnp.zeros((tp_count * width, quarter), BF16)
        for k, piece in enumerate(wo_near):
            wo_own = lax.dynamic_update_slice_in_dim(wo_own, piece, (tp_rank ^ k) * width, 0)
        wo_core = swap(wo_own, core_swap)
        wo_x = swap(wo_own, x_swap)
        wo_diag = swap(wo_x, core_swap)
        x_all, wo_x = barrier((x_all, wo_x))

        angle = pos_all.astype(F32)[:, None] * inv_freq[None, :]
        cos = jnp.cos(angle)
        sin = jnp.sin(angle)
        cos = jnp.concatenate([cos, cos], axis=1)
        sin = jnp.concatenate([-sin, sin], axis=1)
        dy_x = swap(dy, x_swap)
        act_a, query, key, value = project_qkv(x_all, gain_a[None, :], w_q, w_k, w_v, cos, sin)

        blk = span // 2
        blocks = total // blk
        doc_col = doc_all[:, None]
        doc_row = doc_all.reshape(blocks, 1, blk)
        seq_block = jnp.concatenate([jnp.arange(0, blocks, 2), jnp.arange(blocks - 1, 0, -2)])
        doc_seq = doc_all.reshape(blocks, blk)[seq_block]
        first_doc, last_doc = doc_seq[:, 0], doc_seq[:, -1]
        b_own = jnp.stack([cp_rank, blocks - 1 - cp_rank])
        first_own, last_own = first_doc[b_own], last_doc[b_own]
        jmin = jnp.sum((last_doc[None, :] < first_own[:, None]).astype(jnp.int32), axis=1)
        imax = jnp.sum((first_doc[None, :] <= last_own[:, None]).astype(jnp.int32), axis=1) - 1
        info = jnp.concatenate([b_own, jmin, imax, cp_rank[None]]).astype(jnp.int32)
        attended, lse = attend(info, query, key, value, doc_col, doc_row, head_dim, blk)

        attended, dy_x = barrier((attended, dy_x))
        att_parts = lax.all_gather(attended, "tp", axis=0, tiled=False)
        lse_all = lax.all_gather(lse, "cp", axis=0, tiled=True)
        d_hidden = dot(dy, w_down, 1, 1).astype(BF16)
        dhid_x = dot(dy_x, w_down, 1, 1).astype(BF16)
        att_parts, lse_all, d_hidden, dhid_x = barrier((att_parts, lse_all, d_hidden, dhid_x))
        gain_row = gain_b[None, :]
        residual, act_b = out_proj(info, 0, x_all, att_parts, (wo_own, wo_core, wo_x, wo_diag), gain_row)
        att_x = swap(att_parts, x_swap)

        wg, wu = w_gate.T, w_up.T
        ffn = wg.shape[0]
        hidden, d_gate, d_up, d_act_b = mlp_block(act_b, d_hidden, wg, wu, True)
        d_act_b, att_x = barrier((d_act_b, att_x))
        d_act_b = lax.psum_scatter(d_act_b, "tp", scatter_dimension=0, tiled=True)
        act_x = out_proj(info, 2, x_all, att_x, (wo_own, wo_core, wo_x, wo_diag), gain_row)[1]
        hidden_x, d_gate_x, d_up_x = mlp_block(act_x, dhid_x, wg, wu, False)
        d_act_b, hidden_x, d_gate_x, d_up_x = barrier((d_act_b, hidden_x, d_gate_x, d_up_x))
        d_act_b = to_bf16(d_act_b)
        acts, dys, hiddens, d_gates, d_ups = [(a, swap(a, core_swap), b, swap(b, core_swap)) for a, b in (
            (act_b, act_x), (dy, dy_x), (hidden, hidden_x), (d_gate, d_gate_x), (d_up, d_up_x))]
        heads_x = lax.dynamic_index_in_dim(att_x, tp_rank, 0, keepdims=False)
        head_parts = (attended, swap(attended, core_swap), heads_x, swap(heads_x, core_swap))
        att_heads = jnp.zeros((total, width), BF16)
        for k, piece in enumerate(head_parts):
            att_heads = lax.dynamic_update_slice_in_dim(att_heads, piece, (cp_rank ^ k) * span, 0)
        grad_down = weight_grad(info, hiddens, dys, rows=ffn)
        grad_gate = weight_grad(info, d_gates, acts, rows=ffn)
        grad_up = weight_grad(info, d_ups, acts, rows=ffn)

        def mine(arr):
            return lax.dynamic_slice_in_dim(arr, tp_rank * part, part, 0)

        res_part = mine(residual)
        normed_b, inv_b = rms_stats(res_part)
        grad_gain_b = jnp.sum(d_act_b * normed_b, axis=0)
        d_resid = mine(dy).astype(F32) + rms_back(d_act_b * gain_b, normed_b, inv_b)
        d_resid_all = lax.all_gather(d_resid.astype(BF16), both, axis=0, tiled=True)
        d_resid_all, grad_down, grad_gate, grad_up, att_heads = barrier((d_resid_all, grad_down, grad_gate, grad_up, att_heads))
        tp_swap = lambda arr, k: swap(arr, [(i, i ^ k) for i in range(tp_count)], "tp")
        tp_slice = lambda arr, k: lax.dynamic_slice_in_dim(arr, (tp_rank ^ k) * part, part, 0)
        out_part = dot(hidden[:, :ffn], w_down, 1, 0)
        out_slice = res_part + tp_slice(out_part, 0)
        for k in (1, 2, 3):
            out_slice = out_slice + tp_swap(tp_slice(out_part, k), k)
        out_slice = out_slice.astype(BF16)
        layer_out = jnp.zeros((span, dim), BF16)
        for k in range(4):
            piece = tp_swap(out_slice, k) if k else out_slice
            layer_out = lax.dynamic_update_slice_in_dim(layer_out, piece, (tp_rank ^ k) * part, 0)

        d_att = dot(d_resid_all, w_o, 1, 1)
        d_att_b = d_att.astype(BF16)
        head_of = (jnp.arange(width)[None, :] // head_dim == jnp.arange(8)[:, None]).astype(F32)
        prod = att_heads.astype(F32) * d_att_b.astype(F32)
        delta = lax.dot_general(head_of, prod, (((1,), (1,)), ((), ())), precision=lax.Precision.HIGHEST, preferred_element_type=F32)

        def by_block(arr):
            return jnp.transpose(arr.reshape(8, blocks, blk), (1, 0, 2))

        dqkv = attend_back(info, query, key, value, d_att_b, doc_col, doc_row, lse_all, by_block(lse_all.T), delta.T, by_block(delta), cos, sin, blk)
        d_q_pre, d_k_pre, d_v_pre = (dqkv[:, i * width:(i + 1) * width] for i in range(3))
        d_act_a = dot(d_q_pre, w_q, 1, 1) + dot(d_k_pre, w_k, 1, 1) + dot(d_v_pre, w_v, 1, 1)
        d_act_a = to_bf16(lax.psum_scatter(d_act_a, "tp", scatter_dimension=0, tiled=True))
        dqkv_x = swap(dqkv, x_swap)
        dqkvs = (dqkv, swap(dqkv, core_swap), dqkv_x, swap(dqkv_x, core_swap))
        normed_a, inv_a = rms_stats(x_slice.astype(F32))
        grad_gain_a = jnp.sum(d_act_a * normed_a, axis=0)
        d_embed = d_resid + rms_back(d_act_a * gain_a, normed_a, inv_a)
        payload = jnp.concatenate([d_embed, grad_gain_a[None], grad_gain_b[None], jnp.zeros((6, dim), F32)], axis=0)
        gathered = lax.all_gather(payload, both, axis=0, tiled=True)
        grad_qkv = weight_grad(info, [act_a.reshape(cp_count, span, dim)] * 4, dqkvs, splits=3)
        grad_out = weight_grad(info, head_parts, [d_resid_all.reshape(cp_count, span, dim)] * 4)
        gathered, grad_qkv, grad_out = barrier((gathered, grad_qkv, grad_out))
        gain_grads = jnp.sum(gathered.reshape(cp_count * tp_count, part + 8, dim)[:, part:part + 2], axis=0)
        grad_table = scatter_rows(order, sid, bounds, gathered, base)
        return (layer_out, grad_table, *grad_qkv, grad_out, grad_gate.T, grad_up.T, grad_down, gain_grads[0], gain_grads[1])

    col_spec = P(None, "tp")
    row_spec = P("tp", None)
    tok_spec = P("cp")
    rep_spec = P(None)
    in_specs = (tok_spec, tok_spec, tok_spec, P("cp", None), row_spec, col_spec, col_spec, col_spec, row_spec, col_spec, col_spec, row_spec, rep_spec, rep_spec, rep_spec)
    out_specs = (P("cp", None), row_spec, col_spec, col_spec, col_spec, row_spec, col_spec, col_spec, row_spec, rep_spec, rep_spec)
    return jax.shard_map(device_step, mesh=mesh, in_specs=in_specs, out_specs=out_specs, check_vma=False)
```

```python
import functools
import jax
import jax.numpy as jnp
from jax import lax
from jax.experimental import pallas as pl
from jax.experimental.pallas import tpu as pltpu
from jax.sharding import PartitionSpec as P

NORM_EPS = 1e-5
NEG_BIG = -1e30
F32 = jnp.float32
BF16 = jnp.bfloat16


def rms_stats(feats):
    inv_rms = lax.rsqrt(jnp.mean(feats * feats, axis=-1, keepdims=True) + NORM_EPS)
    return feats * inv_rms, inv_rms


def rms_back(d_normed, normed, inv_rms):
    return inv_rms * (d_normed - normed * jnp.mean(d_normed * normed, axis=-1, keepdims=True))


def to_bf16(feats):
    return feats.astype(BF16).astype(F32)


def dot(a, b, ca, cb):
    return lax.dot_general(a, b, (((ca,), (cb,)), ((), ())), preferred_element_type=F32)


def slot_block(j):
    return jnp.where(j < 4, 2 * j, 15 - 2 * j)


def qkv_kernel(x, gain, wq, wk, wv, cos, sin, act, q, k, v, wide, *, head_dim):
    width = wq.shape[1]

    @pl.when(pl.program_id(0) == 0)
    def _():
        for i, w in enumerate((wq, wk, wv)):
            wide[:, i * width:(i + 1) * width] = w[...]

    feats = x[...].astype(F32)
    inv = lax.rsqrt(jnp.mean(feats * feats, axis=-1, keepdims=True) + NORM_EPS)
    a = (feats * inv * gain[...]).astype(BF16)
    act[...] = a
    t = jnp.dot(a, wide[...], preferred_element_type=F32)
    for i, out in enumerate((q, k, v)):
        for h in range(width // head_dim):
            th = t[:, i * width + h * head_dim:i * width + (h + 1) * head_dim]
            if i < 2:
                th = th * cos[...] + pltpu.roll(th, head_dim // 2, 1) * sin[...]
            out[:, h * head_dim:(h + 1) * head_dim] = th.astype(BF16)


def project_qkv(x_all, gain, wq, wk, wv, cos, sin, block=512):
    total, dim = x_all.shape
    width = wq.shape[1]
    head_dim = cos.shape[1]
    rows = lambda n: pl.BlockSpec((block, n), lambda i: (i, 0))
    whole = lambda a: pl.BlockSpec(a.shape, lambda i: (0, 0), pipeline_mode=pl.Buffered(1))
    return pl.pallas_call(
        functools.partial(qkv_kernel, head_dim=head_dim),
        out_shape=[jax.ShapeDtypeStruct((total, n), BF16) for n in (dim, width, width, width)],
        grid=(total // block,),
        in_specs=[rows(dim), whole(gain), whole(wq), whole(wk), whole(wv), rows(head_dim), rows(head_dim)],
        out_specs=[rows(dim), rows(width), rows(width), rows(width)],
        scratch_shapes=[pltpu.VMEM((dim, 3 * width), BF16)],
        compiler_params=pltpu.CompilerParams(vmem_limit_bytes=60 * 1024 * 1024),
        cost_estimate=pl.CostEstimate(flops=6 * total * dim * width, bytes_accessed=4 * total * dim + 6 * dim * width + 6 * total * width, transcendentals=0),
        name="project_qkv",
    )(x_all, gain, wq, wk, wv, cos, sin)


def attend_kernel(info, q, k, v, doc_col, doc_row, out, lse, sc, *, heads, head_dim, scale):
    blk = q.shape[0]
    b = info[pl.program_id(0)]
    jmin = info[2 + pl.program_id(0)]
    row_n = lax.broadcasted_iota(jnp.int32, (blk, blk), 0) + b * blk
    col_n = lax.broadcasted_iota(jnp.int32, (blk, blk), 1)

    def score(j, peaks):
        sb = slot_block(j)
        off = pl.multiple_of(sb * blk, blk)
        allowed = (doc_col[...] == doc_row[sb]) & (col_n + j * blk <= row_n)
        new = []
        for h in range(heads):
            cols = slice(h * head_dim, (h + 1) * head_dim)
            s = dot(q[:, cols], k[pl.ds(off, blk), cols], 1, 1) * scale
            s = jnp.where(allowed, s, NEG_BIG)
            sc[j, h] = s
            new.append(jnp.maximum(peaks[h], jnp.max(s, axis=1, keepdims=True)))
        return tuple(new)

    peaks = lax.fori_loop(jmin, b + 1, score, tuple(jnp.full((blk, 1), NEG_BIG, F32) for _ in range(heads)))

    def weigh(j, sums):
        new = []
        for h in range(heads):
            p = jnp.exp(sc[j, h] - peaks[h])
            sc[j, h] = p
            new.append(sums[h] + jnp.sum(p, axis=1, keepdims=True))
        return tuple(new)

    sums = lax.fori_loop(jmin, b + 1, weigh, tuple(jnp.zeros((blk, 1), F32) for _ in range(heads)))
    inv = tuple(1.0 / t for t in sums)
    for h in range(heads):
        lse[:, h:h + 1] = peaks[h] + jnp.log(sums[h])

    def mix(j, acc):
        off = pl.multiple_of(slot_block(j) * blk, blk)
        new = []
        for h in range(heads):
            cols = slice(h * head_dim, (h + 1) * head_dim)
            new.append(acc[h] + jnp.dot((sc[j, h] * inv[h]).astype(BF16), v[pl.ds(off, blk), cols], preferred_element_type=F32))
        return tuple(new)

    acc = lax.fori_loop(jmin, b + 1, mix, tuple(jnp.zeros((blk, head_dim), F32) for _ in range(heads)))
    for h in range(heads):
        out[:, h * head_dim:(h + 1) * head_dim] = acc[h].astype(BF16)


def attend(info, q, k, v, doc_col, doc_row, head_dim, blk):
    total, width = k.shape
    heads = width // head_dim
    mine = lambda n: pl.BlockSpec((blk, n), lambda i, info: (2 * info[6] + i, 0))
    whole = lambda a: pl.BlockSpec(a.shape, lambda i, info: (0,) * a.ndim)
    return pl.pallas_call(
        functools.partial(attend_kernel, heads=heads, head_dim=head_dim, scale=head_dim ** -0.5),
        out_shape=[jax.ShapeDtypeStruct((2 * blk, width), BF16), jax.ShapeDtypeStruct((2 * blk, 8), F32)],
        grid_spec=pltpu.PrefetchScalarGridSpec(
            num_scalar_prefetch=1,
            grid=(2,),
            in_specs=[mine(width), whole(k), whole(v), mine(1), whole(doc_row)],
            out_specs=[pl.BlockSpec((blk, width), lambda i, info: (i, 0)), pl.BlockSpec((blk, 8), lambda i, info: (i, 0))],
            scratch_shapes=[pltpu.VMEM((total // blk, heads, blk, blk), F32)],
        ),
        compiler_params=pltpu.CompilerParams(vmem_limit_bytes=40 * 1024 * 1024),
        cost_estimate=pl.CostEstimate(flops=4 * 2 * blk * total * width, bytes_accessed=8 * total * width, transcendentals=heads * blk * total),
        name="attend",
    )(info, q, k, v, doc_col, doc_row)


def attend_back_kernel(info, q, k, v, do, doc_col, doc_row, lse_col, lse_row, del_col, del_row, cos, sin, out, acc, *, heads, head_dim, scale):
    blk = cos.shape[0]
    width = heads * head_dim
    i = pl.program_id(0)
    b = info[i]
    jmin = info[2 + i]
    imax = info[4 + i]
    me = pl.multiple_of((2 * info[6] + i) * blk, blk)
    mine = pl.ds(me, blk)
    iota_r = lax.broadcasted_iota(jnp.int32, (blk, blk), 0)
    iota_c = lax.broadcasted_iota(jnp.int32, (blk, blk), 1)
    acc[...] = jnp.zeros_like(acc)
    spans = [slice(h * head_dim, (h + 1) * head_dim) for h in range(heads)]

    def for_query(j, c):
        sb = slot_block(j)
        there = pl.ds(pl.multiple_of(sb * blk, blk), blk)
        allowed = (doc_col[mine, :] == doc_row[sb]) & (iota_c + j * blk <= iota_r + b * blk)
        for h, cols in enumerate(spans):
            s = jnp.where(allowed, dot(q[mine, cols], k[there, cols], 1, 1) * scale, NEG_BIG)
            p = jnp.exp(s - lse_col[mine, h:h + 1])
            dp = to_bf16(dot(do[mine, cols], v[there, cols], 1, 1))
            ds = (p * (dp - del_col[mine, h:h + 1]) * scale).astype(BF16)
            acc[0, :, cols] += jnp.dot(ds, k[there, cols], preferred_element_type=F32)
        return c

    lax.fori_loop(jmin, b + 1, for_query, 0)

    def for_key(j, c):
        sb = slot_block(j)
        there = pl.ds(pl.multiple_of(sb * blk, blk), blk)
        allowed = (doc_col[mine, :] == doc_row[sb]) & (iota_r + b * blk <= iota_c + j * blk)
        for h, cols in enumerate(spans):
            s = jnp.where(allowed, dot(k[mine, cols], q[there, cols], 1, 1) * scale, NEG_BIG)
            p = jnp.exp(s - lse_row[sb, h:h + 1, :])
            dp = to_bf16(dot(v[mine, cols], do[there, cols], 1, 1))
            ds = (p * (dp - del_row[sb, h:h + 1, :]) * scale).astype(BF16)
            acc[2, :, cols] += jnp.dot(p.astype(BF16), do[there, cols], preferred_element_type=F32)
            acc[1, :, cols] += jnp.dot(ds, q[there, cols], preferred_element_type=F32)
        return c

    lax.fori_loop(b, imax + 1, for_key, 0)
    for part in range(3):
        for h, cols in enumerate(spans):
            t = acc[part, :, cols]
            if part < 2:
                t = to_bf16(t)
                t = t * cos[...] - pltpu.roll(t, head_dim // 2, 1) * sin[...]
            out[:, part * width + h * head_dim:part * width + (h + 1) * head_dim] = t.astype(BF16)


def attend_back(info, q, k, v, do, doc_col, doc_row, lse_col, lse_row, del_col, del_row, cos, sin, blk):
    total, width = k.shape
    head_dim = cos.shape[1]
    heads = width // head_dim
    mine = lambda n: pl.BlockSpec((blk, n), lambda i, info: (2 * info[6] + i, 0))
    whole = lambda a: pl.BlockSpec(a.shape, lambda i, info: (0,) * a.ndim)
    arrays = (q, k, v, do, doc_col, doc_row, lse_col, lse_row, del_col, del_row)
    return pl.pallas_call(
        functools.partial(attend_back_kernel, heads=heads, head_dim=head_dim, scale=head_dim ** -0.5),
        out_shape=jax.ShapeDtypeStruct((2 * blk, 3 * width), BF16),
        grid_spec=pltpu.PrefetchScalarGridSpec(
            num_scalar_prefetch=1,
            grid=(2,),
            in_specs=[whole(a) for a in arrays] + [mine(head_dim), mine(head_dim)],
            out_specs=pl.BlockSpec((blk, 3 * width), lambda i, info: (i, 0)),
            scratch_shapes=[pltpu.VMEM((3, blk, width), F32)],
        ),
        compiler_params=pltpu.CompilerParams(vmem_limit_bytes=48 * 1024 * 1024),
        cost_estimate=pl.CostEstimate(flops=14 * 2 * blk * total * width // 2, bytes_accessed=12 * total * width, transcendentals=heads * blk * total),
        name="attend_back",
    )(info, *arrays, cos, sin)


def out_proj_kernel(info, x, att, a0, b0, a1, b1, gain, res, act, wide, abuf, bbuf, sems):
    tp, _, width = att.shape
    na, nb = a0.shape[1], b0.shape[1]
    sets = ((a0, b0), (a1, b1))

    def copies(i):
        return (pltpu.make_async_copy(sets[i][0], abuf.at[i], sems.at[i, 0]), pltpu.make_async_copy(sets[i][1], bbuf.at[i], sems.at[i, 1]))

    for i in range(2):
        for c in copies(i):
            c.start()
    for t in range(tp):
        wide[:, t * width:(t + 1) * width] = att[t]
    for i in range(2):
        start = (info[7] ^ i) * (na + nb)
        first, second = copies(i)
        first.wait()
        cols = pl.ds(pl.multiple_of(start, 128), na)
        res[:, cols] = x[:, cols].astype(F32) + jnp.dot(wide[...], abuf[i], preferred_element_type=F32)
        second.wait()
        cols = pl.ds(pl.multiple_of(start + na, 128), nb)
        res[:, cols] = x[:, cols].astype(F32) + jnp.dot(wide[...], bbuf[i], preferred_element_type=F32)
    h = res[...]
    inv = lax.rsqrt(jnp.mean(h * h, axis=-1, keepdims=True) + NORM_EPS)
    act[...] = (h * inv * gain[...]).astype(BF16)


def out_proj(info, flip, x_all, att, pieces, gain):
    _, rows, _ = att.shape
    dim = x_all.shape[1]
    whole = lambda a: pl.BlockSpec(a.shape, lambda i, info: (0,) * a.ndim)
    full = pl.BlockSpec((rows, dim), lambda i, info: (0, 0))
    return pl.pallas_call(
        out_proj_kernel,
        out_shape=[jax.ShapeDtypeStruct((rows, dim), F32), jax.ShapeDtypeStruct((rows, dim), BF16)],
        grid_spec=pltpu.PrefetchScalarGridSpec(
            num_scalar_prefetch=1,
            grid=(1,),
            in_specs=[pl.BlockSpec((rows, dim), lambda i, info: (info[6] ^ flip, 0)), whole(att)] + [pl.BlockSpec(memory_space=pl.ANY)] * 4 + [whole(gain)],
            out_specs=[full, full],
            scratch_shapes=[pltpu.VMEM((rows, dim), BF16), pltpu.VMEM((2,) + pieces[0].shape, BF16), pltpu.VMEM((2,) + pieces[1].shape, BF16), pltpu.SemaphoreType.DMA((2, 2))],
        ),
        compiler_params=pltpu.CompilerParams(vmem_limit_bytes=56 * 1024 * 1024),
        cost_estimate=pl.CostEstimate(flops=2 * rows * dim * dim, bytes_accessed=2 * dim * dim + 10 * rows * dim, transcendentals=0),
        name="out_proj",
    )(info, x_all, att, *pieces, gain)


def weight_grad_kernel(info, *refs, pieces, splits):
    lhs = refs[:pieces]
    rhs = refs[pieces:2 * pieces]
    outs = refs[2 * pieces:]
    t = dot(lhs[0][...], rhs[0][...], 0, 0)
    for a, b in zip(lhs[1:], rhs[1:]):
        t += dot(a[...], b[...], 0, 0)
    width = t.shape[1] // splits
    for i, out in enumerate(outs):
        out[...] = t[:, i * width:(i + 1) * width]


def weight_grad(info, lhs, rhs, block=256, splits=1, rows=None):
    def spec(arr, p, cols, moving):
        if arr.ndim == 3:
            return pl.BlockSpec((None, arr.shape[1], cols), lambda i, info: (info[6] ^ p, 0, i if moving else 0))
        return pl.BlockSpec((arr.shape[0], cols), lambda i, info: (0, i if moving else 0))

    tokens = lhs[0].shape[-2]
    rows, dim = rows or lhs[0].shape[-1], rhs[0].shape[-1]
    n = len(lhs)
    width = dim // splits
    outs = pl.pallas_call(
        functools.partial(weight_grad_kernel, pieces=n, splits=splits),
        out_shape=[jax.ShapeDtypeStruct((rows, width), F32)] * splits,
        grid_spec=pltpu.PrefetchScalarGridSpec(
            num_scalar_prefetch=1,
            grid=(pl.cdiv(rows, block),),
            in_specs=[spec(a, p, block, True) for p, a in enumerate(lhs)] + [spec(b, p, dim, False) for p, b in enumerate(rhs)],
            out_specs=[pl.BlockSpec((block, width), lambda i, info: (i, 0))] * splits,
        ),
        compiler_params=pltpu.CompilerParams(vmem_limit_bytes=56 * 1024 * 1024),
        cost_estimate=pl.CostEstimate(flops=2 * n * tokens * rows * dim, bytes_accessed=4 * rows * dim + 2 * n * tokens * (rows + dim), transcendentals=0),
        name="weight_grad",
    )(info, *lhs, *rhs)
    return outs if splits > 1 else outs[0]


def mlp_kernel(act, dhid, wg, wu, hidden, d_gate, d_up, *grad, limit):
    i = pl.program_id(0)
    block = wg.shape[0]
    left = limit - i * block
    row_ok = lax.broadcasted_iota(jnp.int32, (block, 1), 0) < left
    col_ok = lax.broadcasted_iota(jnp.int32, (1, block), 1) < left
    wgt = jnp.where(row_ok, wg[...], jnp.zeros((), BF16))
    wut = jnp.where(row_ok, wu[...], jnp.zeros((), BF16))
    gate = dot(act[...], wgt, 1, 1)
    up = dot(act[...], wut, 1, 1)
    dh = jnp.where(col_ok, dhid[...].astype(F32), 0.0)
    sig = jax.nn.sigmoid(gate)
    hidden[...] = (gate * sig * up).astype(BF16)
    dg = (dh * up * sig * (1.0 + gate * (1.0 - sig))).astype(BF16)
    du = (dh * gate * sig).astype(BF16)
    d_gate[...] = dg
    d_up[...] = du
    if grad:
        t = jnp.dot(dg, wgt, preferred_element_type=F32) + jnp.dot(du, wut, preferred_element_type=F32)

        @pl.when(i == 0)
        def _():
            grad[0][...] = t

        @pl.when(i > 0)
        def _():
            grad[0][...] += t


def mlp_block(act, dhid, wg, wu, with_grad, block=256):
    rows, dim = act.shape
    limit = wg.shape[0]
    cols = pl.BlockSpec((rows, block), lambda i: (0, i))
    tile = pl.BlockSpec((block, dim), lambda i: (i, 0))
    whole = pl.BlockSpec((rows, dim), lambda i: (0, 0))
    return pl.pallas_call(
        functools.partial(mlp_kernel, limit=limit),
        out_shape=[jax.ShapeDtypeStruct((rows, pl.cdiv(limit, block) * block), BF16)] * 3 + [jax.ShapeDtypeStruct((rows, dim), F32)] * with_grad,
        grid=(pl.cdiv(limit, block),),
        in_specs=[whole, cols, tile, tile],
        out_specs=[cols] * 3 + [whole] * with_grad,
        compiler_params=pltpu.CompilerParams(vmem_limit_bytes=48 * 1024 * 1024),
        cost_estimate=pl.CostEstimate(flops=(4 + 4 * with_grad) * rows * dim * limit, bytes_accessed=4 * dim * limit + 6 * rows * limit + 10 * rows * dim, transcendentals=rows * limit),
        name="mlp_block",
    )(act, dhid, wg, wu)


def zero_kernel(after, out, zeros, sem):
    zeros[...] = jnp.zeros_like(zeros)
    step = zeros.shape[0]
    count = out.shape[0] // step

    def send(i, c):
        pltpu.make_async_copy(zeros, out.at[pl.ds(pl.multiple_of(i * step, step), step), :], sem).start()
        return c

    def wait(i, c):
        pltpu.make_async_copy(zeros, out.at[pl.ds(0, step), :], sem).wait()
        return c

    lax.fori_loop(0, count, send, 0)
    lax.fori_loop(0, count, wait, 0)


def zero_rows(after, rows, dim, step=200):
    return pl.pallas_call(
        zero_kernel,
        out_shape=jax.ShapeDtypeStruct((rows, dim), F32),
        in_specs=[pl.BlockSpec(memory_space=pltpu.SMEM)],
        out_specs=pl.BlockSpec(memory_space=pl.ANY),
        scratch_shapes=[pltpu.VMEM((step, dim), F32), pltpu.SemaphoreType.DMA],
        compiler_params=pltpu.CompilerParams(vmem_limit_bytes=8 * 1024 * 1024),
        cost_estimate=pl.CostEstimate(flops=rows * dim, bytes_accessed=4 * rows * dim, transcendentals=0),
        name="zero_rows",
    )(after)


def scatter_kernel(order, sid, runs, bounds, rows, base_hbm, out_hbm, sums, row_sem, sum_sem):
    lo = bounds[0]
    hi = bounds[1]

    def one(c):
        p, singles, multi = c
        n = runs[p]
        t = order[p]
        single = n == 1

        @pl.when(single)
        def _():
            pltpu.make_async_copy(rows.at[pl.ds(t, 1), :], out_hbm.at[pl.ds(sid[p], 1), :], row_sem).start()

        @pl.when(jnp.logical_not(single))
        def _():
            def add(j, acc):
                return acc + rows[pl.ds(order[p + j], 1), :]

            sums[pl.ds(multi, 1), :] = lax.fori_loop(1, n, add, rows[pl.ds(t, 1), :])

        return p + n, singles + single.astype(jnp.int32), multi + 1 - single.astype(jnp.int32)

    _, singles, multi = lax.while_loop(lambda c: c[0] < hi, one, (lo, 0, 0))

    def two(c):
        p, k = c
        n = runs[p]

        @pl.when(n > 1)
        def _():
            pltpu.make_async_copy(sums.at[pl.ds(k, 1), :], out_hbm.at[pl.ds(sid[p], 1), :], sum_sem).start()

        return p + n, k + (n > 1).astype(jnp.int32)

    lax.while_loop(lambda c: c[0] < hi, two, (lo, 0))

    def wait(sem):
        def body(i, c):
            pltpu.make_async_copy(sums.at[pl.ds(0, 1), :], out_hbm.at[pl.ds(0, 1), :], sem).wait()
            return c

        return body

    lax.fori_loop(0, singles, wait(row_sem), 0)
    lax.fori_loop(0, multi, wait(sum_sem), 0)


def scatter_rows(order, sid, runs, bounds, grads, base, tokens):
    _, dim = grads.shape
    rows = base.shape[0]
    return pl.pallas_call(
        scatter_kernel,
        out_shape=jax.ShapeDtypeStruct((rows, dim), F32),
        grid_spec=pltpu.PrefetchScalarGridSpec(
            num_scalar_prefetch=4,
            grid=(),
            in_specs=[pl.BlockSpec(memory_space=pltpu.VMEM), pl.BlockSpec(memory_space=pl.ANY)],
            out_specs=pl.BlockSpec(memory_space=pl.ANY),
            scratch_shapes=[pltpu.VMEM((tokens // 2, dim), F32), pltpu.SemaphoreType.DMA, pltpu.SemaphoreType.DMA],
        ),
        input_output_aliases={5: 0},
        compiler_params=pltpu.CompilerParams(vmem_limit_bytes=40 * 1024 * 1024),
        name="scatter_rows",
    )(order, sid, runs, bounds, grads, base)


def solution(mesh):
    cp_count = mesh.shape["cp"]
    tp_count = mesh.shape["tp"]
    both = ("cp", "tp")
    x_swap = [(i, i ^ 2) for i in range(cp_count)]
    core_swap = [(i, i ^ 1) for i in range(cp_count)]

    def compute(tokens, pos, doc_id, dy, table, w_q, w_k, w_v, w_o, w_gate, w_up, w_down, gain_one, gain_two, inv_freq):
        span = tokens.shape[0]
        total = span * cp_count
        part = span // tp_count
        rows, dim = table.shape
        head_dim = 2 * inv_freq.shape[0]
        heads = w_q.shape[1] // head_dim
        width = heads * head_dim
        tp_rank = lax.axis_index("tp")
        cp_rank = lax.axis_index("cp")
        core = cp_rank % 2
        gain_a = gain_one.astype(F32)
        gain_b = gain_two.astype(F32)

        barrier = lax.optimization_barrier
        swap = lambda arr, pairs, axis="cp": lax.ppermute(arr, axis, pairs)
        local_ids = tokens - tp_rank * rows
        owned = (local_ids >= 0) & (local_ids < rows)
        safe_ids = jnp.where(owned, local_ids, 0)
        picked = jnp.where(owned[:, None], jnp.take(table, safe_ids, axis=0), jnp.zeros((), BF16))
        half = dim // 2
        near = 256
        wo_half = lax.dynamic_slice_in_dim(w_o, core * half, half, 1)
        wo_near = lax.all_gather(wo_half[:, :near], "tp", axis=0, tiled=True)
        picked, wo_near = barrier((picked, wo_near))
        x_slice = lax.psum_scatter(picked, "tp", scatter_dimension=0, tiled=True)

        ints = lax.all_gather(jnp.stack([tokens, pos, doc_id]), "cp", axis=1, tiled=True)
        tok_all, pos_all, doc_all = ints[0], ints[1], ints[2]
        slot_ids = jnp.arange(total, dtype=jnp.int32)
        before = (tok_all[None, :] < tok_all[:, None]) | ((tok_all[None, :] == tok_all[:, None]) & (slot_ids[None, :] < slot_ids[:, None]))
        rank = jnp.sum(before.astype(jnp.int32), axis=1)
        count = jnp.sum((tok_all[None, :] == tok_all[:, None]).astype(jnp.int32), axis=1)
        at_rank = rank[None, :] == slot_ids[:, None]
        runs = jnp.sum(jnp.where(at_rank, count[None, :], 0), axis=1)
        order = jnp.sum(jnp.where(at_rank, slot_ids[None, :], 0), axis=1)
        sid = jnp.sum(jnp.where(at_rank, tok_all[None, :], 0), axis=1) - tp_rank * rows
        order = order + 8 * (order // part)
        bounds = jnp.stack([jnp.sum((tok_all < tp_rank * rows).astype(jnp.int32)), jnp.sum((tok_all < (tp_rank + 1) * rows).astype(jnp.int32))])
        base = zero_rows(bounds, rows, dim)
        x_slice, base, order, sid, runs, bounds, ints = barrier((x_slice, base, order, sid, runs, bounds, ints))
        pos_all, doc_all = ints[1], ints[2]
        x_all = lax.all_gather(x_slice, both, axis=0, tiled=True)

        wo_far = barrier((wo_half[:, near:], x_all))[0]
        wo_rest = lax.all_gather(wo_far, "tp", axis=0, tiled=True)
        wo_pieces = (wo_near, wo_rest, swap(wo_near, core_swap), swap(wo_rest, core_swap))

        angle = pos_all.astype(F32)[:, None] * inv_freq[None, :]
        cos = jnp.cos(angle)
        sin = jnp.sin(angle)
        cos = jnp.concatenate([cos, cos], axis=1)
        sin = jnp.concatenate([-sin, sin], axis=1)
        dy_x = swap(barrier((dy, x_all))[0], x_swap)
        act_a, query, key, value = project_qkv(x_all, gain_a[None, :], w_q, w_k, w_v, cos, sin)

        blk = span // 2
        blocks = total // blk
        doc_col = doc_all[:, None]
        doc_row = doc_all.reshape(blocks, 1, blk)
        seq_block = jnp.concatenate([jnp.arange(0, blocks, 2), jnp.arange(blocks - 1, 0, -2)])
        doc_seq = doc_all.reshape(blocks, blk)[seq_block]
        first_doc, last_doc = doc_seq[:, 0], doc_seq[:, -1]
        b_own = jnp.stack([cp_rank, blocks - 1 - cp_rank])
        first_own, last_own = first_doc[b_own], last_doc[b_own]
        jmin = jnp.sum((last_doc[None, :] < first_own[:, None]).astype(jnp.int32), axis=1)
        imax = jnp.sum((first_doc[None, :] <= last_own[:, None]).astype(jnp.int32), axis=1) - 1
        info = jnp.concatenate([b_own, jmin, imax, cp_rank[None], core[None]]).astype(jnp.int32)
        attended, lse = attend(info, query, key, value, doc_col, doc_row, head_dim, blk)

        att_parts = lax.all_gather(attended, "tp", axis=0, tiled=False)
        lse_all = lax.all_gather(lse, "cp", axis=0, tiled=True)
        d_hidden = dot(dy, w_down, 1, 1).astype(BF16)
        att_parts, lse_all, d_hidden = barrier((att_parts, lse_all, d_hidden))
        gain_row = gain_b[None, :]
        residual, act_b = out_proj(info, 0, x_all, att_parts, wo_pieces, gain_row)
        att_x = swap(att_parts, x_swap)

        wg, wu = w_gate.T, w_up.T
        ffn = wg.shape[0]
        hidden, d_gate, d_up, d_act_b = mlp_block(act_b, d_hidden, wg, wu, True)
        d_act_b = lax.psum_scatter(d_act_b, "tp", scatter_dimension=0, tiled=True)
        dhid_x = dot(dy_x, w_down, 1, 1).astype(BF16)
        act_x = out_proj(info, 2, x_all, att_x, wo_pieces, gain_row)[1]
        hidden_x, d_gate_x, d_up_x = mlp_block(act_x, dhid_x, wg, wu, False)
        d_act_b, hidden_x, d_gate_x, d_up_x = barrier((d_act_b, hidden_x, d_gate_x, d_up_x))
        d_act_b = to_bf16(d_act_b)
        acts, dys, hiddens, d_gates, d_ups = [(a, swap(a, core_swap), b, swap(b, core_swap)) for a, b in (
            (act_b, act_x), (dy, dy_x), (hidden, hidden_x), (d_gate, d_gate_x), (d_up, d_up_x))]
        heads_x = lax.dynamic_index_in_dim(att_x, tp_rank, 0, keepdims=False)
        head_parts = (attended, swap(attended, core_swap), heads_x, swap(heads_x, core_swap))
        att_heads = jnp.zeros((total, width), BF16)
        for k, piece in enumerate(head_parts):
            att_heads = lax.dynamic_update_slice_in_dim(att_heads, piece, (cp_rank ^ k) * span, 0)
        grad_down = weight_grad(info, hiddens, dys, rows=ffn)
        grad_gate = weight_grad(info, d_gates, acts, rows=ffn)
        grad_up = weight_grad(info, d_ups, acts, rows=ffn)

        def mine(arr):
            return lax.dynamic_slice_in_dim(arr, tp_rank * part, part, 0)

        res_part = mine(residual)
        normed_b, inv_b = rms_stats(res_part)
        grad_gain_b = jnp.sum(d_act_b * normed_b, axis=0)
        d_resid = mine(dy).astype(F32) + rms_back(d_act_b * gain_b, normed_b, inv_b)
        d_resid_all = lax.all_gather(d_resid.astype(BF16), both, axis=0, tiled=True)
        out_part = dot(hidden[:, :ffn], w_down, 1, 0)
        d_resid_all, grad_down, grad_gate, att_heads, out_part = barrier((d_resid_all, grad_down, grad_gate, att_heads, out_part))
        out_slice = lax.psum_scatter(out_part, "tp", scatter_dimension=0, tiled=True)
        out_slice = (res_part + out_slice).astype(BF16)

        d_att = dot(d_resid_all, w_o, 1, 1)
        d_att_b = d_att.astype(BF16)
        head_of = (jnp.arange(width)[None, :] // head_dim == jnp.arange(8)[:, None]).astype(F32)
        prod = att_heads.astype(F32) * d_att_b.astype(F32)
        delta = lax.dot_general(head_of, prod, (((1,), (1,)), ((), ())), precision=lax.Precision.HIGHEST, preferred_element_type=F32)

        def by_block(arr):
            return jnp.transpose(arr.reshape(8, blocks, blk), (1, 0, 2))

        dqkv = attend_back(info, query, key, value, d_att_b, doc_col, doc_row, lse_all, by_block(lse_all.T), delta.T, by_block(delta), cos, sin, blk)
        d_q_pre, d_k_pre, d_v_pre = (dqkv[:, i * width:(i + 1) * width] for i in range(3))
        d_act_a = dot(d_q_pre, w_q, 1, 1) + dot(d_k_pre, w_k, 1, 1) + dot(d_v_pre, w_v, 1, 1)
        d_act_a, out_slice = barrier((d_act_a, out_slice))
        d_act_a = lax.psum_scatter(d_act_a, "tp", scatter_dimension=0, tiled=True)
        dqkv_x = swap(dqkv, x_swap)
        dqkvs = (dqkv, swap(dqkv, core_swap), dqkv_x, swap(dqkv_x, core_swap))
        grad_out = weight_grad(info, head_parts, [d_resid_all.reshape(cp_count, span, dim)] * 4)
        d_act_a, dqkv_x, grad_out, grad_up = barrier((d_act_a, dqkv_x, grad_out, grad_up))
        d_act_a = to_bf16(d_act_a)
        normed_a, inv_a = rms_stats(x_slice.astype(F32))
        grad_gain_a = jnp.sum(d_act_a * normed_a, axis=0)
        d_embed = d_resid + rms_back(d_act_a * gain_a, normed_a, inv_a)
        payload = jnp.concatenate([d_embed, grad_gain_a[None], grad_gain_b[None], jnp.zeros((6, dim), F32)], axis=0)
        gathered = lax.all_gather(payload, both, axis=0, tiled=True)
        grad_qkv = weight_grad(info, [act_a.reshape(cp_count, span, dim)] * 4, dqkvs, splits=3)
        gathered, grad_qkv = barrier((gathered, grad_qkv))
        out_slice = barrier((out_slice, gathered))[0]
        layer_out = lax.all_gather(out_slice, "tp", axis=0, tiled=True)
        gain_grads = jnp.sum(gathered.reshape(cp_count * tp_count, part + 8, dim)[:, part:part + 2], axis=0)
        grad_table = scatter_rows(order, sid, runs, bounds, gathered, base, total)
        return (layer_out, grad_table, *grad_qkv, grad_out, grad_gate.T, grad_up.T, grad_down, gain_grads[0], gain_grads[1])

    col_spec = P(None, "tp")
    row_spec = P("tp", None)
    tok_spec = P("cp")
    rep_spec = P(None)
    in_specs = (tok_spec, tok_spec, tok_spec, P("cp", None), row_spec, col_spec, col_spec, col_spec, row_spec, col_spec, col_spec, row_spec, rep_spec, rep_spec, rep_spec)
    out_specs = (P("cp", None), row_spec, col_spec, col_spec, col_spec, row_spec, col_spec, col_spec, row_spec, rep_spec, rep_spec)
    return jax.shard_map(compute, mesh=mesh, in_specs=in_specs, out_specs=out_specs, check_vma=False)
```

```python
import functools
import jax
import jax.numpy as jnp
from jax import lax
from jax.experimental import pallas as pl
from jax.experimental.pallas import tpu as pltpu
from jax.sharding import PartitionSpec as P

NORM_EPS = 1e-5
NEG_BIG = -1e30
MIB = 2 ** 20
F32 = jnp.float32
BF16 = jnp.bfloat16
I32 = jnp.int32


def rms_stats(feats):
    inv_rms = lax.rsqrt(mean_row(feats * feats) + NORM_EPS)
    return feats * inv_rms, inv_rms


def rms_back(d_normed, normed, inv_rms):
    return inv_rms * (d_normed - normed * mean_row(d_normed * normed))


def to_bf16(feats):
    return feats.astype(BF16).astype(F32)


def contract(a, b, ca, cb):
    return lax.dot_general(a, b, (((ca,), (cb,)), ((), ())), preferred_element_type=F32)


def row_sum(t):
    return jnp.sum(t, axis=1, keepdims=True)


def mean_row(t):
    return jnp.mean(t, axis=-1, keepdims=True)


def whole(a):
    return pl.BlockSpec(a.shape, lambda *i: (0,) * a.ndim)


def cost(flops, moved):
    return pl.CostEstimate(flops=flops, bytes_accessed=moved, transcendentals=0)


def nn(a, b):
    return contract(a, b, 1, 0)


def nt(a, b):
    return contract(a, b, 1, 1)


def tn(a, b):
    return contract(a, b, 0, 0)


DIMS = ("x", "y", "z")


class Place:
    def __init__(self):
        tp = lax.axis_index("tp")
        cp = lax.axis_index("cp")
        self.at = {"x": cp // 2, "core": cp % 2, "z": tp // 2, "y": tp % 2}

    def coord(self, dim, flip):
        return 1 - self.at[dim] if dim in flip else self.at[dim]

    def tp(self, flip=()):
        return self.coord("z", flip) * 2 + self.coord("y", flip)

    def cp(self, flip=()):
        return self.coord("x", flip) * 2 + self.coord("core", flip)

    def device(self, flip):
        return {"tp": self.tp(flip), "cp": self.cp(flip)}

    def slot(self, flip=()):
        return self.cp(flip) * 4 + self.tp(flip)

    def meet(self, dims):
        barrier = pltpu.get_barrier_semaphore()
        for d in dims:
            pl.semaphore_signal(barrier, inc=1, device_id=self.device((d,)), device_id_type=MESH)
        pl.semaphore_wait(barrier, len(dims))


MESH = pl.DeviceIdType.MESH
ORDERS = (("x", "y", "z"), ("y", "z", "x"), ("z", "x", "y"))
FLIPS = tuple(tuple(d for i, d in enumerate(DIMS) if n >> i & 1) for n in range(8))


def flip_code(flip):
    return sum(1 << DIMS.index(d) for d in flip)


def column_parts(width, count):
    tiles = width // 128
    sizes = [(tiles // count + (i < tiles % count)) * 128 for i in range(count)]
    return [(sum(sizes[:i]), n) for i, n in enumerate(sizes)]


class Gather:
    def __init__(self, place, buf, send, recv, core_send, core_recv):
        self.place, self.buf, self.send, self.recv, self.core_send, self.core_recv = place, buf, send, recv, core_send, core_recv
        self.parts = column_parts(buf.shape[2], 3)
        self.started = []

    def view(self, part, flip):
        start, size = self.parts[part]
        return self.buf.at[self.place.slot(flip), :, pl.ds(start, size)]

    def hop(self, part, flip, dim):
        there = tuple(d for d in DIMS if (d in flip) != (d == dim))
        index = part * 7 + flip_code(there) - 1
        ref = self.view(part, flip)
        return pltpu.make_async_remote_copy(src_ref=ref, dst_ref=ref, send_sem=self.send.at[index], recv_sem=self.recv.at[index], device_id=self.place.device((dim,)), device_id_type=MESH)

    def core_hop(self, part, flip):
        index = part * 8 + flip_code(flip)
        ref = self.view(part, flip)
        return pltpu.make_async_remote_copy(src_ref=ref, dst_ref=ref, send_sem=self.core_send.at[index], recv_sem=self.core_recv.at[index], device_id=self.place.device(("core",)), device_id_type=MESH)

    def go(self, copy):
        copy.start()
        self.started.append(copy)

    def wait(self, part, flip):
        order = ORDERS[part]
        last = max(order.index(d) for d in flip)
        came = tuple(d for d in flip if d != order[last])
        self.hop(part, came, order[last]).wait_recv()
        for dim in order[last + 1:]:
            self.go(self.hop(part, flip, dim))
        self.go(self.core_hop(part, flip))

    def run(self):
        for step in range(3):
            for part, order in enumerate(ORDERS):
                self.go(self.hop(part, (), order[step]))
        for part in range(3):
            self.go(self.core_hop(part, ()))
        for step in range(3):
            for flip in FLIPS[1:]:
                for part, order in enumerate(ORDERS):
                    if max(order.index(d) for d in flip) == step and len(flip) == 1:
                        self.wait(part, flip)
            for flip in FLIPS[1:]:
                for part, order in enumerate(ORDERS):
                    if max(order.index(d) for d in flip) == step and len(flip) > 1:
                        self.wait(part, flip)

    def finish(self, out, out_sem):
        rows = self.buf.shape[1]
        copies = []

        def store(flip):
            slot = self.place.slot(flip)
            c = pltpu.make_async_copy(self.buf.at[slot], out.at[pl.ds(slot * rows, rows), :], out_sem.at[len(copies)])
            c.start()
            copies.append(c)

        for flip in FLIPS:
            store(flip)
        for flip in FLIPS:
            other = flip + ("core",)
            for part in range(3):
                start, size = self.parts[part]
                ref = self.buf.at[self.place.slot(other), :, pl.ds(start, size)]
                index = part * 8 + flip_code(flip)
                pltpu.make_async_remote_copy(src_ref=ref, dst_ref=ref, send_sem=self.core_send.at[index], recv_sem=self.core_recv.at[index], device_id=self.place.device(("core",)), device_id_type=MESH).wait_recv()
            store(other)
        for c in self.started:
            c.wait_send()
        for c in copies:
            c.wait()


def embed_kernel(picked, side_f, side_i, out, slice_out, all_f, all_i, buf, r1, r2, tmp, send, recv, core_send, core_recv, out_sem, rs_send, rs_recv, side_send, side_recv, slice_sem):
    place = Place()
    place.meet(("x", "y", "z", "core"))
    half = buf.shape[2] // 2
    near = ("y", "z")

    sides = ((side_f, all_f), (side_i, all_i))
    started = []

    def side_hop(i, step):
        src, dst = sides[i]
        if step == 0:
            src_ref, slot, dim = src, place.cp(), "x"
        elif step == 1:
            src_ref, slot, dim = src, place.cp(), "core"
        else:
            src_ref, slot, dim = dst.at[place.cp(("x",))], place.cp(("x",)), "core"
        return pltpu.make_async_remote_copy(src_ref=src_ref, dst_ref=dst.at[slot], send_sem=side_send.at[i, step], recv_sem=side_recv.at[i, step], device_id=place.device((dim,)), device_id_type=MESH)

    def first(h, k):
        a, b = near[h], near[1 - h]
        target = place.tp((a,)) if k == 0 else place.tp((a, b))
        cols = pl.ds(h * half, half)
        return pltpu.make_async_remote_copy(src_ref=picked.at[target, :, cols], dst_ref=r1.at[h, k], send_sem=rs_send.at[h, k], recv_sem=rs_recv.at[h, k], device_id=place.device((a,)), device_id_type=MESH)

    def second(h):
        return pltpu.make_async_remote_copy(src_ref=tmp.at[h], dst_ref=r2.at[h], send_sem=rs_send.at[h, 2], recv_sem=rs_recv.at[h, 2], device_id=place.device((near[1 - h],)), device_id_type=MESH)

    def go(copy):
        copy.start()
        started.append(copy)

    for k in (1, 0):
        for h in range(2):
            go(first(h, k))
    for i in range(2):
        go(side_hop(i, 0))
        go(side_hop(i, 1))
        all_i_or_f = sides[i][1]
        all_i_or_f[place.cp()] = sides[i][0][...]
    for h in range(2):
        cols = slice(h * half, (h + 1) * half)
        first(h, 1).wait_recv()
        tmp[h] = picked[place.tp((near[1 - h],)), :, cols] + r1[h, 1]
        go(second(h))
    for i in range(2):
        side_hop(i, 0).wait_recv()
        go(side_hop(i, 2))
    mine = place.slot()
    for h in range(2):
        cols = slice(h * half, (h + 1) * half)
        first(h, 0).wait_recv()
        part = picked[place.tp(), :, cols] + r1[h, 0]
        second(h).wait_recv()
        buf[mine, :, cols] = part + r2[h]
    gather = Gather(place, buf, send, recv, core_send, core_recv)
    gather.run()
    keep = pltpu.make_async_copy(buf.at[mine], slice_out, slice_sem)
    keep.start()
    gather.finish(out, out_sem)
    keep.wait()
    for i in range(2):
        side_hop(i, 1).wait_recv()
        side_hop(i, 2).wait_recv()
    for c in started:
        c.wait_send()


def embed_gather(picked, side_f, side_i):
    _, rows, dim = picked.shape
    half = dim // 2
    dma = pltpu.SemaphoreType.DMA
    vmem = pl.BlockSpec(memory_space=pltpu.VMEM)
    hbm = pl.BlockSpec(memory_space=pl.ANY)
    return pl.pallas_call(
        embed_kernel,
        out_shape=[
            jax.ShapeDtypeStruct((16 * rows, dim), BF16),
            jax.ShapeDtypeStruct((rows, dim), BF16),
            jax.ShapeDtypeStruct((4,) + side_f.shape, F32),
            jax.ShapeDtypeStruct((4,) + side_i.shape, I32),
        ],
        in_specs=[vmem, vmem, vmem],
        out_specs=[hbm, hbm, vmem, vmem],
        scratch_shapes=[
            pltpu.VMEM((16, rows, dim), BF16),
            pltpu.VMEM((2, 2, rows, half), BF16),
            pltpu.VMEM((2, rows, half), BF16),
            pltpu.VMEM((2, rows, half), BF16),
            dma((21,)), dma((21,)), dma((24,)), dma((24,)), dma((16,)),
            dma((2, 3)), dma((2, 3)), dma((2, 3)), dma((2, 3)), dma,
        ],
        compiler_params=pltpu.CompilerParams(collective_id=0, has_side_effects=True, vmem_limit_bytes=40 * MIB),
        name="embed_gather",
    )(picked, side_f, side_i)


def slot_block(j):
    return jnp.where(j < 4, 2 * j, 15 - 2 * j)


def unpack_angles(packed):
    turned = pltpu.roll(packed, packed.shape[1] // 2, 1)
    low = lax.broadcasted_iota(I32, packed.shape, 1) < packed.shape[1] // 2
    return jnp.where(low, packed, turned), jnp.where(low, -turned, packed)


def qkv_kernel(x, gain, wq, wk, wv, angles, act, q, k, v, wide, *, head_dim):
    width = wq.shape[1]

    @pl.when(pl.program_id(0) == 0)
    def _():
        for i, w in enumerate((wq, wk, wv)):
            wide[:, i * width:(i + 1) * width] = w[...]

    feats = x[...].astype(F32)
    inv = lax.rsqrt(mean_row(feats * feats) + NORM_EPS)
    a = (feats * inv * gain[...]).astype(BF16)
    act[...] = a
    t = nn(a, wide[...])
    cos, sin = unpack_angles(angles[...])
    for i, out in enumerate((q, k, v)):
        for h in range(width // head_dim):
            th = t[:, i * width + h * head_dim:i * width + (h + 1) * head_dim]
            if i < 2:
                th = th * cos + pltpu.roll(th, head_dim // 2, 1) * sin
            out[:, h * head_dim:(h + 1) * head_dim] = th.astype(BF16)


def project_qkv(x_all, gain, wq, wk, wv, angles, block=512):
    total, dim = x_all.shape
    width = wq.shape[1]
    head_dim = angles.shape[1]
    rows = lambda n: pl.BlockSpec((block, n), lambda i: (i, 0))
    whole = lambda a: pl.BlockSpec(a.shape, lambda i: (0, 0), pipeline_mode=pl.Buffered(1))
    return pl.pallas_call(
        functools.partial(qkv_kernel, head_dim=head_dim),
        out_shape=[jax.ShapeDtypeStruct((total, n), BF16) for n in (dim, width, width, width)] + [jax.ShapeDtypeStruct((dim, 3 * width), BF16)],
        grid=(total // block,),
        in_specs=[rows(dim), whole(gain), whole(wq), whole(wk), whole(wv), rows(head_dim)],
        out_specs=[rows(dim), rows(width), rows(width), rows(width), pl.BlockSpec((dim, 3 * width), lambda i: (0, 0), pipeline_mode=pl.Buffered(1))],
        compiler_params=pltpu.CompilerParams(vmem_limit_bytes=60 * MIB),
        cost_estimate=cost(6 * total * dim * width, 4 * total * dim + 6 * dim * width + 6 * total * width),
        name="project_qkv",
    )(x_all, gain, wq, wk, wv, angles)


def block_range(info, i, blocks):
    r = info[0]
    b = jnp.where(i == 0, r, blocks - 1 - r)
    mine = 2 + 2 * (2 * r + i)
    jmin = 0
    imax = -1
    for j in range(blocks):
        there = 2 + 2 * (2 * j if j < blocks // 2 else 2 * blocks - 1 - 2 * j)
        jmin = jmin + (info[there + 1] < info[mine]).astype(I32)
        imax = imax + (info[there] <= info[mine + 1]).astype(I32)
    return b, jmin, imax


def attend_kernel(info, q, k, v, doc_col, doc_row, out, lse, sc, *, heads, head_dim, scale):
    blk = q.shape[0]
    b, jmin, _ = block_range(info, pl.program_id(0), doc_row.shape[0])
    row_n = lax.broadcasted_iota(I32, (blk, blk), 0) + b * blk
    col_n = lax.broadcasted_iota(I32, (blk, blk), 1)

    def score(j, peaks):
        sb = slot_block(j)
        off = pl.multiple_of(sb * blk, blk)
        allowed = (doc_col[...] == doc_row[sb]) & (col_n + j * blk <= row_n)
        new = []
        for h in range(heads):
            cols = slice(h * head_dim, (h + 1) * head_dim)
            s = nt(q[:, cols], k[pl.ds(off, blk), cols]) * scale
            s = jnp.where(allowed, s, NEG_BIG)
            sc[j, h] = s
            new.append(jnp.maximum(peaks[h], jnp.max(s, axis=1, keepdims=True)))
        return tuple(new)

    peaks = lax.fori_loop(jmin, b + 1, score, tuple(jnp.full((blk, 1), NEG_BIG, F32) for _ in range(heads)))

    def weigh(j, sums):
        new = []
        for h in range(heads):
            p = jnp.exp(sc[j, h] - peaks[h])
            sc[j, h] = p
            new.append(sums[h] + row_sum(p))
        return tuple(new)

    sums = lax.fori_loop(jmin, b + 1, weigh, tuple(jnp.zeros((blk, 1), F32) for _ in range(heads)))
    inv = tuple(1.0 / t for t in sums)
    for h in range(heads):
        lse[:, h:h + 1] = peaks[h] + jnp.log(sums[h])

    def mix(j, acc):
        off = pl.multiple_of(slot_block(j) * blk, blk)
        new = []
        for h in range(heads):
            cols = slice(h * head_dim, (h + 1) * head_dim)
            new.append(acc[h] + nn((sc[j, h] * inv[h]).astype(BF16), v[pl.ds(off, blk), cols]))
        return tuple(new)

    acc = lax.fori_loop(jmin, b + 1, mix, tuple(jnp.zeros((blk, head_dim), F32) for _ in range(heads)))
    for h in range(heads):
        out[:, h * head_dim:(h + 1) * head_dim] = acc[h].astype(BF16)


def attend(info, q, k, v, doc_col, doc_row, head_dim, blk):
    total, width = k.shape
    heads = width // head_dim
    mine = lambda n: pl.BlockSpec((blk, n), lambda i, info: (2 * info[0] + i, 0))
    return pl.pallas_call(
        functools.partial(attend_kernel, heads=heads, head_dim=head_dim, scale=head_dim ** -0.5),
        out_shape=[jax.ShapeDtypeStruct((2 * blk, width), BF16), jax.ShapeDtypeStruct((2 * blk, 8), F32)],
        grid_spec=pltpu.PrefetchScalarGridSpec(
            num_scalar_prefetch=1,
            grid=(2,),
            in_specs=[mine(width), whole(k), whole(v), mine(1), whole(doc_row)],
            out_specs=[pl.BlockSpec((blk, width), lambda i, info: (i, 0)), pl.BlockSpec((blk, 8), lambda i, info: (i, 0))],
            scratch_shapes=[pltpu.VMEM((total // blk, heads, blk, blk), F32)],
        ),
        compiler_params=pltpu.CompilerParams(vmem_limit_bytes=40 * MIB),
        cost_estimate=cost(4 * 2 * blk * total * width, 8 * total * width),
        name="attend",
    )(info, q, k, v, doc_col, doc_row)


def attend_back_kernel(info, q, k, v, do, doc_col, doc_row, lse_col, lse_row, del_col, del_row, angles, out, acc, *, heads, head_dim, scale):
    blk = angles.shape[0]
    width = heads * head_dim
    i = pl.program_id(0)
    b, jmin, imax = block_range(info, i, doc_row.shape[0])
    me = pl.multiple_of((2 * info[0] + i) * blk, blk)
    mine = pl.ds(me, blk)
    iota_r = lax.broadcasted_iota(I32, (blk, blk), 0)
    iota_c = lax.broadcasted_iota(I32, (blk, blk), 1)
    acc[...] = jnp.zeros_like(acc)
    spans = [slice(h * head_dim, (h + 1) * head_dim) for h in range(heads)]

    def for_query(j, c):
        sb = slot_block(j)
        there = pl.ds(pl.multiple_of(sb * blk, blk), blk)
        allowed = (doc_col[mine, :] == doc_row[sb]) & (iota_c + j * blk <= iota_r + b * blk)
        for h, cols in enumerate(spans):
            s = jnp.where(allowed, nt(q[mine, cols], k[there, cols]) * scale, NEG_BIG)
            p = jnp.exp(s - lse_col[mine, h:h + 1])
            dp = to_bf16(nt(do[mine, cols], v[there, cols]))
            ds = (p * (dp - del_col[mine, h:h + 1]) * scale).astype(BF16)
            acc[0, :, cols] += nn(ds, k[there, cols])
        return c

    lax.fori_loop(jmin, b + 1, for_query, 0)

    def for_key(j, c):
        sb = slot_block(j)
        there = pl.ds(pl.multiple_of(sb * blk, blk), blk)
        allowed = (doc_col[mine, :] == doc_row[sb]) & (iota_r + b * blk <= iota_c + j * blk)
        for h, cols in enumerate(spans):
            s = jnp.where(allowed, nt(k[mine, cols], q[there, cols]) * scale, NEG_BIG)
            p = jnp.exp(s - lse_row[sb, h:h + 1, :])
            dp = to_bf16(nt(v[mine, cols], do[there, cols]))
            ds = (p * (dp - del_row[sb, h:h + 1, :]) * scale).astype(BF16)
            acc[2, :, cols] += nn(p.astype(BF16), do[there, cols])
            acc[1, :, cols] += nn(ds, q[there, cols])
        return c

    lax.fori_loop(b, imax + 1, for_key, 0)
    cos, sin = unpack_angles(angles[...])
    for part in range(3):
        for h, cols in enumerate(spans):
            t = acc[part, :, cols]
            if part < 2:
                t = to_bf16(t)
                t = t * cos - pltpu.roll(t, head_dim // 2, 1) * sin
            out[:, part * width + h * head_dim:part * width + (h + 1) * head_dim] = t.astype(BF16)


def attend_back(info, q, k, v, do, doc_col, doc_row, lse_col, lse_row, del_col, del_row, angles, blk):
    total, width = k.shape
    head_dim = angles.shape[1]
    heads = width // head_dim
    mine = lambda n: pl.BlockSpec((blk, n), lambda i, info: (2 * info[0] + i, 0))
    arrays = (q, k, v, do, doc_col, doc_row, lse_col, lse_row, del_col, del_row)
    return pl.pallas_call(
        functools.partial(attend_back_kernel, heads=heads, head_dim=head_dim, scale=head_dim ** -0.5),
        out_shape=jax.ShapeDtypeStruct((2 * blk, 3 * width), BF16),
        grid_spec=pltpu.PrefetchScalarGridSpec(
            num_scalar_prefetch=1,
            grid=(2,),
            in_specs=[whole(a) for a in arrays] + [mine(head_dim)],
            out_specs=pl.BlockSpec((blk, 3 * width), lambda i, info: (i, 0)),
            scratch_shapes=[pltpu.VMEM((3, blk, width), F32)],
        ),
        compiler_params=pltpu.CompilerParams(vmem_limit_bytes=48 * MIB),
        cost_estimate=cost(14 * 2 * blk * total * width // 2, 12 * total * width),
        name="attend_back",
    )(info, *arrays, angles)


def out_proj_kernel(info, x, att, a0, b0, a1, b1, gain, res, act, wide, abuf, bbuf, sems):
    tp, _, width = att.shape
    na, nb = a0.shape[1], b0.shape[1]
    sets = ((a0, b0), (a1, b1))

    def copies(i):
        return (pltpu.make_async_copy(sets[i][0], abuf.at[i], sems.at[i, 0]), pltpu.make_async_copy(sets[i][1], bbuf.at[i], sems.at[i, 1]))

    for i in range(2):
        for c in copies(i):
            c.start()
    for t in range(tp):
        wide[:, t * width:(t + 1) * width] = att[t]
    for i in range(2):
        start = (info[1] ^ i) * (na + nb)
        first, second = copies(i)
        first.wait()
        cols = pl.ds(pl.multiple_of(start, 128), na)
        res[:, cols] = x[:, cols].astype(F32) + nn(wide[...], abuf[i])
        second.wait()
        cols = pl.ds(pl.multiple_of(start + na, 128), nb)
        res[:, cols] = x[:, cols].astype(F32) + nn(wide[...], bbuf[i])
    h = res[...]
    inv = lax.rsqrt(mean_row(h * h) + NORM_EPS)
    act[...] = (h * inv * gain[...]).astype(BF16)


def out_proj(info, flip, x_all, att, pieces, gain):
    _, rows, _ = att.shape
    dim = x_all.shape[1]
    full = pl.BlockSpec((rows, dim), lambda i, info: (0, 0))
    return pl.pallas_call(
        out_proj_kernel,
        out_shape=[jax.ShapeDtypeStruct((rows, dim), F32), jax.ShapeDtypeStruct((rows, dim), BF16)],
        grid_spec=pltpu.PrefetchScalarGridSpec(
            num_scalar_prefetch=1,
            grid=(1,),
            in_specs=[pl.BlockSpec((rows, dim), lambda i, info: (info[0] ^ flip, 0)), whole(att)] + [pl.BlockSpec(memory_space=pl.ANY)] * 4 + [whole(gain)],
            out_specs=[full, full],
            scratch_shapes=[pltpu.VMEM((rows, dim), BF16), pltpu.VMEM((2,) + pieces[0].shape, BF16), pltpu.VMEM((2,) + pieces[1].shape, BF16), pltpu.SemaphoreType.DMA((2, 2))],
        ),
        compiler_params=pltpu.CompilerParams(vmem_limit_bytes=56 * MIB),
        cost_estimate=cost(2 * rows * dim * dim, 2 * dim * dim + 10 * rows * dim),
        name="out_proj",
    )(info, x_all, att, *pieces, gain)


def weight_grad_kernel(info, *refs, pieces, splits):
    lhs = refs[:pieces]
    rhs = refs[pieces:2 * pieces]
    outs = refs[2 * pieces:]
    t = tn(lhs[0][...], rhs[0][...])
    for a, b in zip(lhs[1:], rhs[1:]):
        t += tn(a[...], b[...])
    width = t.shape[1] // splits
    for i, out in enumerate(outs):
        out[...] = t[:, i * width:(i + 1) * width]


def weight_grad(info, lhs, rhs, block=256, splits=1, rows=None):
    def spec(arr, p, cols, moving):
        if arr.ndim == 3:
            return pl.BlockSpec((None, arr.shape[1], cols), lambda i, info: (info[0] ^ p, 0, i if moving else 0))
        return pl.BlockSpec((arr.shape[0], cols), lambda i, info: (0, i if moving else 0))

    tokens = lhs[0].shape[-2]
    rows, dim = rows or lhs[0].shape[-1], rhs[0].shape[-1]
    n = len(lhs)
    width = dim // splits
    outs = pl.pallas_call(
        functools.partial(weight_grad_kernel, pieces=n, splits=splits),
        out_shape=[jax.ShapeDtypeStruct((rows, width), F32)] * splits,
        grid_spec=pltpu.PrefetchScalarGridSpec(
            num_scalar_prefetch=1,
            grid=(pl.cdiv(rows, block),),
            in_specs=[spec(a, p, block, True) for p, a in enumerate(lhs)] + [spec(b, p, dim, False) for p, b in enumerate(rhs)],
            out_specs=[pl.BlockSpec((block, width), lambda i, info: (i, 0))] * splits,
        ),
        compiler_params=pltpu.CompilerParams(vmem_limit_bytes=56 * MIB),
        cost_estimate=cost(2 * n * tokens * rows * dim, 4 * rows * dim + 2 * n * tokens * (rows + dim)),
        name="weight_grad",
    )(info, *lhs, *rhs)
    return outs if splits > 1 else outs[0]


def mlp_kernel(act, dhid, wg, wu, hidden, d_gate, d_up, *grad, limit):
    i = pl.program_id(0)
    block = wg.shape[0]
    left = limit - i * block
    row_ok = lax.broadcasted_iota(I32, (block, 1), 0) < left
    col_ok = lax.broadcasted_iota(I32, (1, block), 1) < left
    wgt = jnp.where(row_ok, wg[...], 0).astype(BF16)
    wut = jnp.where(row_ok, wu[...], 0).astype(BF16)
    gate = nt(act[...], wgt)
    up = nt(act[...], wut)
    dh = jnp.where(col_ok, dhid[...].astype(F32), 0.0)
    sig = jax.nn.sigmoid(gate)
    hidden[...] = (gate * sig * up).astype(BF16)
    dg = (dh * up * sig * (1.0 + gate * (1.0 - sig))).astype(BF16)
    du = (dh * gate * sig).astype(BF16)
    d_gate[...] = dg
    d_up[...] = du
    if grad:
        t = nn(dg, wgt) + nn(du, wut)

        @pl.when(i == 0)
        def _():
            grad[0][...] = t

        @pl.when(i > 0)
        def _():
            grad[0][...] += t


def mlp_block(act, dhid, wg, wu, with_grad, block=256):
    rows, dim = act.shape
    limit = wg.shape[0]
    cols = pl.BlockSpec((rows, block), lambda i: (0, i))
    tile = pl.BlockSpec((block, dim), lambda i: (i, 0))
    whole = pl.BlockSpec((rows, dim), lambda i: (0, 0))
    return pl.pallas_call(
        functools.partial(mlp_kernel, limit=limit),
        out_shape=[jax.ShapeDtypeStruct((rows, pl.cdiv(limit, block) * block), BF16)] * 3 + [jax.ShapeDtypeStruct((rows, dim), F32)] * with_grad,
        grid=(pl.cdiv(limit, block),),
        in_specs=[whole, cols, tile, tile],
        out_specs=[cols] * 3 + [whole] * with_grad,
        compiler_params=pltpu.CompilerParams(vmem_limit_bytes=48 * MIB),
        cost_estimate=cost((4 + 4 * with_grad) * rows * dim * limit, 4 * dim * limit + 6 * rows * limit + 10 * rows * dim),
        name="mlp_block",
    )(act, dhid, wg, wu)


def zero_kernel(after, out, zeros, sem):
    zeros[...] = jnp.zeros_like(zeros)
    step = zeros.shape[0]
    count = out.shape[0] // step

    def send(i, c):
        pltpu.make_async_copy(zeros, out.at[pl.ds(pl.multiple_of(i * step, step), step), :], sem).start()
        return c

    def wait(i, c):
        pltpu.make_async_copy(zeros, out.at[pl.ds(0, step), :], sem).wait()
        return c

    lax.fori_loop(0, count, send, 0)
    lax.fori_loop(0, count, wait, 0)


def zero_rows(after, rows, dim, step=200):
    return pl.pallas_call(
        zero_kernel,
        out_shape=jax.ShapeDtypeStruct((rows, dim), F32),
        in_specs=[pl.BlockSpec(memory_space=pltpu.SMEM)],
        out_specs=pl.BlockSpec(memory_space=pl.ANY),
        scratch_shapes=[pltpu.VMEM((step, dim), F32), pltpu.SemaphoreType.DMA],
        compiler_params=pltpu.CompilerParams(vmem_limit_bytes=8 * MIB),
        cost_estimate=cost(rows * dim, 4 * rows * dim),
        name="zero_rows",
    )(after)


def scatter_kernel(order, sid, runs, bounds, rows, base_hbm, out_hbm, sums, row_sem, sum_sem):
    lo = bounds[0]
    hi = bounds[1]

    def one(c):
        p, singles, multi = c
        n = runs[p]
        t = order[p]
        single = n == 1

        @pl.when(single)
        def _():
            pltpu.make_async_copy(rows.at[pl.ds(t, 1), :], out_hbm.at[pl.ds(sid[p], 1), :], row_sem).start()

        @pl.when(jnp.logical_not(single))
        def _():
            def add(j, acc):
                return acc + rows[pl.ds(order[p + j], 1), :]

            sums[pl.ds(multi, 1), :] = lax.fori_loop(1, n, add, rows[pl.ds(t, 1), :])

        return p + n, singles + single.astype(I32), multi + 1 - single.astype(I32)

    _, singles, multi = lax.while_loop(lambda c: c[0] < hi, one, (lo, 0, 0))

    def two(c):
        p, k = c
        n = runs[p]

        @pl.when(n > 1)
        def _():
            pltpu.make_async_copy(sums.at[pl.ds(k, 1), :], out_hbm.at[pl.ds(sid[p], 1), :], sum_sem).start()

        return p + n, k + (n > 1).astype(I32)

    lax.while_loop(lambda c: c[0] < hi, two, (lo, 0))

    def wait(sem):
        def body(i, c):
            pltpu.make_async_copy(sums.at[pl.ds(0, 1), :], out_hbm.at[pl.ds(0, 1), :], sem).wait()
            return c

        return body

    lax.fori_loop(0, singles, wait(row_sem), 0)
    lax.fori_loop(0, multi, wait(sum_sem), 0)


def scatter_rows(order, sid, runs, bounds, grads, base, tokens):
    _, dim = grads.shape
    rows = base.shape[0]
    return pl.pallas_call(
        scatter_kernel,
        out_shape=jax.ShapeDtypeStruct((rows, dim), F32),
        grid_spec=pltpu.PrefetchScalarGridSpec(
            num_scalar_prefetch=4,
            grid=(),
            in_specs=[pl.BlockSpec(memory_space=pltpu.VMEM), pl.BlockSpec(memory_space=pl.ANY)],
            out_specs=pl.BlockSpec(memory_space=pl.ANY),
            scratch_shapes=[pltpu.VMEM((tokens // 2, dim), F32), pltpu.SemaphoreType.DMA, pltpu.SemaphoreType.DMA],
        ),
        input_output_aliases={5: 0},
        compiler_params=pltpu.CompilerParams(vmem_limit_bytes=40 * MIB),
        name="scatter_rows",
    )(order, sid, runs, bounds, grads, base)


def solution(mesh):
    cp_count = mesh.shape["cp"]
    tp_count = mesh.shape["tp"]
    both = ("cp", "tp")
    x_swap = [(i, i ^ 2) for i in range(cp_count)]
    core_swap = [(i, i ^ 1) for i in range(cp_count)]

    def compute(tokens, pos, doc_id, dy, table, w_q, w_k, w_v, w_o, w_gate, w_up, w_down, gain_one, gain_two, inv_freq):
        span = tokens.shape[0]
        total = span * cp_count
        part = span // tp_count
        rows, dim = table.shape
        head_dim = 2 * inv_freq.shape[0]
        heads = w_q.shape[1] // head_dim
        width = heads * head_dim
        tp_rank = lax.axis_index("tp")
        cp_rank = lax.axis_index("cp")
        core = cp_rank % 2
        gain_a = gain_one.astype(F32)
        gain_b = gain_two.astype(F32)

        barrier = lax.optimization_barrier
        join = lambda arr, axis: lax.all_gather(arr, axis, axis=0, tiled=True)
        add_up = lambda arr: lax.psum_scatter(arr, "tp", scatter_dimension=0, tiled=True)
        swap = lambda arr, pairs, axis="cp": lax.ppermute(arr, axis, pairs)
        local_ids = tokens - tp_rank * rows
        owned = (local_ids >= 0) & (local_ids < rows)
        safe_ids = jnp.where(owned, local_ids, 0)
        picked = jnp.where(owned[:, None], jnp.take(table, safe_ids, axis=0), 0).astype(BF16)
        half = dim // 2
        near = 512
        wo_half = lax.dynamic_slice_in_dim(w_o, core * half, half, 1)
        wo_near = join(wo_half[:, :near], "tp")
        angle = pos.astype(F32)[:, None] * inv_freq[None, :]
        side_f = jnp.concatenate([jnp.cos(angle), jnp.sin(angle)], axis=1)
        side_i = jnp.concatenate([tokens[None], doc_id[None], jnp.zeros((6, span), I32)], axis=0)
        x_all, x_slice, angles, ints = embed_gather(picked.reshape(tp_count, part, dim), side_f, side_i)
        angles = angles.reshape(total, head_dim)
        tok_all = ints[:, 0, :].reshape(total)
        doc_all = ints[:, 1, :].reshape(total)
        wo_far = barrier((wo_half[:, near:], x_all))[0]
        wo_rest = join(wo_far, "tp")
        wo_pieces = (wo_near, wo_rest, swap(wo_near, core_swap), swap(wo_rest, core_swap))

        dy_x = swap(barrier((dy, x_all))[0], x_swap)
        act_a, query, key, value, w_qkv = project_qkv(x_all, gain_a[None, :], w_q, w_k, w_v, angles)

        blk = span // 2
        blocks = total // blk
        doc_col = doc_all[:, None]
        doc_row = doc_all.reshape(blocks, 1, blk)
        docs = doc_all.reshape(blocks, blk)
        docs = jnp.stack([docs[:, 0], docs[:, -1]], axis=1).reshape(2 * blocks)
        info = jnp.concatenate([cp_rank[None], core[None], docs]).astype(I32)
        attended, lse = attend(info, query, key, value, doc_col, doc_row, head_dim, blk)

        att_parts = lax.all_gather(attended, "tp", axis=0, tiled=False)
        lse_all = join(lse, "cp")
        d_hidden = nt(dy, w_down).astype(BF16)
        slot_ids = jnp.arange(total, dtype=I32)
        before = (tok_all[None, :] < tok_all[:, None]) | ((tok_all[None, :] == tok_all[:, None]) & (slot_ids[None, :] < slot_ids[:, None]))
        rank = jnp.sum(before.astype(I32), axis=1)
        count = jnp.sum((tok_all[None, :] == tok_all[:, None]).astype(I32), axis=1)
        at_rank = rank[None, :] == slot_ids[:, None]
        runs = jnp.sum(jnp.where(at_rank, count[None, :], 0), axis=1)
        order = jnp.sum(jnp.where(at_rank, slot_ids[None, :], 0), axis=1)
        sid = jnp.sum(jnp.where(at_rank, tok_all[None, :], 0), axis=1) - tp_rank * rows
        order = order + 8 * (order // part)
        bounds = jnp.stack([jnp.sum((tok_all < tp_rank * rows).astype(I32)), jnp.sum((tok_all < (tp_rank + 1) * rows).astype(I32))])
        att_parts, lse_all, d_hidden, runs, order, sid, bounds = barrier((att_parts, lse_all, d_hidden, runs, order, sid, bounds))
        gain_row = gain_b[None, :]
        residual, act_b = out_proj(info, 0, x_all, att_parts, wo_pieces, gain_row)
        att_x = swap(att_parts, x_swap)

        wg, wu = w_gate.T, w_up.T
        ffn = wg.shape[0]
        hidden, d_gate, d_up, d_act_b = mlp_block(act_b, d_hidden, wg, wu, True)
        d_act_b = add_up(d_act_b)
        dhid_x = nt(dy_x, w_down).astype(BF16)
        act_x = out_proj(info, 2, x_all, att_x, wo_pieces, gain_row)[1]
        hidden_x, d_gate_x, d_up_x = mlp_block(act_x, dhid_x, wg, wu, False)
        d_act_b, hidden_x, d_gate_x, d_up_x = barrier((d_act_b, hidden_x, d_gate_x, d_up_x))
        d_act_b = to_bf16(d_act_b)
        acts, dys, hiddens, d_gates, d_ups = [(a, swap(a, core_swap), b, swap(b, core_swap)) for a, b in (
            (act_b, act_x), (dy, dy_x), (hidden, hidden_x), (d_gate, d_gate_x), (d_up, d_up_x))]
        heads_x = lax.dynamic_index_in_dim(att_x, tp_rank, 0, keepdims=False)
        head_parts = (attended, swap(attended, core_swap), heads_x, swap(heads_x, core_swap))
        att_heads = jnp.zeros((total, width), BF16)
        for k, piece in enumerate(head_parts):
            att_heads = lax.dynamic_update_slice_in_dim(att_heads, piece, (cp_rank ^ k) * span, 0)
        grad_down = weight_grad(info, hiddens, dys, rows=ffn)
        grad_gate = weight_grad(info, d_gates, acts, rows=ffn)
        grad_up = weight_grad(info, d_ups, acts, rows=ffn)

        def mine(arr):
            return lax.dynamic_slice_in_dim(arr, tp_rank * part, part, 0)

        res_part = mine(residual)
        normed_b, inv_b = rms_stats(res_part)
        grad_gain_b = jnp.sum(d_act_b * normed_b, axis=0)
        d_resid = mine(dy).astype(F32) + rms_back(d_act_b * gain_b, normed_b, inv_b)
        d_resid_all = join(d_resid.astype(BF16), both)
        out_part = nn(hidden[:, :ffn], w_down)
        d_resid_all, grad_down, att_heads, out_part = barrier((d_resid_all, grad_down, att_heads, out_part))
        out_slice = add_up(out_part)
        out_slice = (res_part + out_slice).astype(BF16)

        d_att = nt(d_resid_all, w_o)
        d_att_b = d_att.astype(BF16)
        head_of = (jnp.arange(width)[None, :] // head_dim == jnp.arange(8)[:, None]).astype(F32)
        prod = att_heads.astype(F32) * d_att_b.astype(F32)
        delta = lax.dot_general(head_of, prod, (((1,), (1,)), ((), ())), precision=lax.Precision.HIGHEST, preferred_element_type=F32)

        def by_block(arr):
            return jnp.transpose(arr.reshape(8, blocks, blk), (1, 0, 2))

        dqkv = attend_back(info, query, key, value, d_att_b, doc_col, doc_row, lse_all, by_block(lse_all.T), delta.T, by_block(delta), angles, blk)
        d_act_a = nt(dqkv, w_qkv)
        d_act_a, out_slice = barrier((d_act_a, out_slice))
        d_act_a = add_up(d_act_a)
        dqkv_x = swap(dqkv, x_swap)
        dqkvs = (dqkv, swap(dqkv, core_swap), dqkv_x, swap(dqkv_x, core_swap))
        grad_out = weight_grad(info, head_parts, [d_resid_all.reshape(cp_count, span, dim)] * 4)
        d_act_a, dqkv_x, grad_out, grad_up = barrier((d_act_a, dqkv_x, grad_out, grad_up))
        d_act_a = to_bf16(d_act_a)
        normed_a, inv_a = rms_stats(x_slice.astype(F32))
        grad_gain_a = jnp.sum(d_act_a * normed_a, axis=0)
        d_embed = d_resid + rms_back(d_act_a * gain_a, normed_a, inv_a)
        payload = jnp.concatenate([d_embed, grad_gain_a[None], grad_gain_b[None], jnp.zeros((6, dim), F32)], axis=0)
        gathered = join(payload, both)
        grad_qkv = weight_grad(info, [act_a.reshape(cp_count, span, dim)] * 4, dqkvs, splits=3)
        base = zero_rows(barrier((bounds, d_act_a))[0], rows, dim)
        gathered, grad_qkv, grad_gate, base = barrier((gathered, grad_qkv, grad_gate, base))
        out_slice = barrier((out_slice, gathered))[0]
        layer_out = join(out_slice, "tp")
        gain_grads = jnp.sum(gathered.reshape(cp_count * tp_count, part + 8, dim)[:, part:part + 2], axis=0)
        grad_table = scatter_rows(order, sid, runs, bounds, gathered, base, total)
        return (layer_out, grad_table, *grad_qkv, grad_out, grad_gate.T, grad_up.T, grad_down, gain_grads[0], gain_grads[1])

    col_spec = P(None, "tp")
    row_spec = P("tp", None)
    tok_spec = P("cp")
    rep_spec = P(None)
    in_specs = (tok_spec, tok_spec, tok_spec, P("cp", None), row_spec, col_spec, col_spec, col_spec, row_spec, col_spec, col_spec, row_spec, rep_spec, rep_spec, rep_spec)
    out_specs = (P("cp", None), row_spec, col_spec, col_spec, col_spec, row_spec, col_spec, col_spec, row_spec, rep_spec, rep_spec)
    return jax.shard_map(compute, mesh=mesh, in_specs=in_specs, out_specs=out_specs, check_vma=False)
```

```python
import functools
import jax
import jax.numpy as jnp
from jax import lax
from jax.experimental import pallas as pl
from jax.experimental.pallas import tpu as pltpu
from jax.sharding import PartitionSpec as P

NORM_EPS = 1e-5
NEG_BIG = -1e30
MIB = 2 ** 20
F32 = jnp.float32
BF16 = jnp.bfloat16
I32 = jnp.int32


def rms_stats(feats):
    inv_rms = lax.rsqrt(mean_row(feats * feats) + NORM_EPS)
    return feats * inv_rms, inv_rms


def rms_back(d_normed, normed, inv_rms):
    return inv_rms * (d_normed - normed * mean_row(d_normed * normed))


def to_bf16(feats):
    return feats.astype(BF16).astype(F32)


def contract(a, b, ca, cb):
    return lax.dot_general(a, b, (((ca,), (cb,)), ((), ())), preferred_element_type=F32)


def row_sum(t):
    return jnp.sum(t, axis=1, keepdims=True)


def mean_row(t):
    return jnp.mean(t, axis=-1, keepdims=True)


def whole(a):
    return pl.BlockSpec(a.shape, lambda *i: (0,) * a.ndim)


def cost(flops, moved):
    return pl.CostEstimate(flops=flops, bytes_accessed=moved, transcendentals=0)


def nn(a, b):
    return contract(a, b, 1, 0)


def nt(a, b):
    return contract(a, b, 1, 1)


def tn(a, b):
    return contract(a, b, 0, 0)


DIMS = ("x", "y", "z")


class Place:
    def __init__(self):
        tp = lax.axis_index("tp")
        cp = lax.axis_index("cp")
        self.at = {"x": cp // 2, "core": cp % 2, "z": tp // 2, "y": tp % 2}

    def coord(self, dim, flip):
        return 1 - self.at[dim] if dim in flip else self.at[dim]

    def tp(self, flip=()):
        return self.coord("z", flip) * 2 + self.coord("y", flip)

    def cp(self, flip=()):
        return self.coord("x", flip) * 2 + self.coord("core", flip)

    def device(self, flip):
        return {"tp": self.tp(flip), "cp": self.cp(flip)}

    def slot(self, flip=()):
        return self.cp(flip) * 4 + self.tp(flip)

    def meet(self, dims):
        barrier = pltpu.get_barrier_semaphore()
        for d in dims:
            pl.semaphore_signal(barrier, inc=1, device_id=self.device((d,)), device_id_type=MESH)
        pl.semaphore_wait(barrier, len(dims))


MESH = pl.DeviceIdType.MESH
ORDERS = (("x", "y", "z"), ("y", "z", "x"), ("z", "x", "y"))
FLIPS = tuple(tuple(d for i, d in enumerate(DIMS) if n >> i & 1) for n in range(8))


def flip_code(flip):
    return sum(1 << DIMS.index(d) for d in flip)


def column_parts(width, count):
    tiles = width // 128
    sizes = [(tiles // count + (i < tiles % count)) * 128 for i in range(count)]
    return [(sum(sizes[:i]), n) for i, n in enumerate(sizes)]


class Gather:
    def __init__(self, place, buf, send, recv, core_send, core_recv):
        self.place, self.buf, self.send, self.recv, self.core_send, self.core_recv = place, buf, send, recv, core_send, core_recv
        self.parts = column_parts(buf.shape[2], 3)
        self.started = []

    def view(self, part, flip):
        start, size = self.parts[part]
        return self.buf.at[self.place.slot(flip), :, pl.ds(start, size)]

    def hop(self, part, flip, dim):
        there = tuple(d for d in DIMS if (d in flip) != (d == dim))
        index = part * 7 + flip_code(there) - 1
        ref = self.view(part, flip)
        return pltpu.make_async_remote_copy(src_ref=ref, dst_ref=ref, send_sem=self.send.at[index], recv_sem=self.recv.at[index], device_id=self.place.device((dim,)), device_id_type=MESH)

    def core_hop(self, part, flip):
        index = part * 8 + flip_code(flip)
        ref = self.view(part, flip)
        return pltpu.make_async_remote_copy(src_ref=ref, dst_ref=ref, send_sem=self.core_send.at[index], recv_sem=self.core_recv.at[index], device_id=self.place.device(("core",)), device_id_type=MESH)

    def go(self, copy):
        copy.start()
        self.started.append(copy)

    def wait(self, part, flip):
        order = ORDERS[part]
        last = max(order.index(d) for d in flip)
        came = tuple(d for d in flip if d != order[last])
        self.hop(part, came, order[last]).wait_recv()
        for dim in order[last + 1:]:
            self.go(self.hop(part, flip, dim))
        self.go(self.core_hop(part, flip))

    def run(self):
        for step in range(3):
            for part, order in enumerate(ORDERS):
                self.go(self.hop(part, (), order[step]))
        for part in range(3):
            self.go(self.core_hop(part, ()))
        for step in range(3):
            for flip in FLIPS[1:]:
                for part, order in enumerate(ORDERS):
                    if max(order.index(d) for d in flip) == step and len(flip) == 1:
                        self.wait(part, flip)
            for flip in FLIPS[1:]:
                for part, order in enumerate(ORDERS):
                    if max(order.index(d) for d in flip) == step and len(flip) > 1:
                        self.wait(part, flip)

    def finish(self, out, out_sem):
        rows = self.buf.shape[1]
        copies = []

        def store(flip):
            slot = self.place.slot(flip)
            c = pltpu.make_async_copy(self.buf.at[slot], out.at[pl.ds(slot * rows, rows), :], out_sem.at[len(copies)])
            c.start()
            copies.append(c)

        for flip in FLIPS:
            store(flip)
        for flip in FLIPS:
            other = flip + ("core",)
            for part in range(3):
                start, size = self.parts[part]
                ref = self.buf.at[self.place.slot(other), :, pl.ds(start, size)]
                index = part * 8 + flip_code(flip)
                pltpu.make_async_remote_copy(src_ref=ref, dst_ref=ref, send_sem=self.core_send.at[index], recv_sem=self.core_recv.at[index], device_id=self.place.device(("core",)), device_id_type=MESH).wait_recv()
            store(other)
        for c in self.started:
            c.wait_send()
        for c in copies:
            c.wait()


def embed_kernel(picked, side_f, side_i, out, slice_out, all_f, all_i, base, zeros, zero_sem, buf, r1, r2, tmp, send, recv, core_send, core_recv, out_sem, rs_send, rs_recv, side_send, side_recv, slice_sem):
    place = Place()
    zeros[:] = jnp.zeros_like(zeros)
    step = zeros.shape[0]

    def blank(i):
        return pltpu.make_async_copy(zeros, base.at[pl.ds(i * step, step), :], zero_sem.at[i])

    place.meet(("x", "y", "z", "core"))
    half = buf.shape[2] // 2
    near = ("y", "z")

    sides = ((side_f, all_f), (side_i, all_i))
    started = []

    def side_hop(i, step):
        src, dst = sides[i]
        if step == 0:
            src_ref, slot, dim = src, place.cp(), "x"
        elif step == 1:
            src_ref, slot, dim = src, place.cp(), "core"
        else:
            src_ref, slot, dim = dst.at[place.cp(("x",))], place.cp(("x",)), "core"
        return pltpu.make_async_remote_copy(src_ref=src_ref, dst_ref=dst.at[slot], send_sem=side_send.at[i, step], recv_sem=side_recv.at[i, step], device_id=place.device((dim,)), device_id_type=MESH)

    def first(h, k):
        a, b = near[h], near[1 - h]
        target = place.tp((a,)) if k == 0 else place.tp((a, b))
        cols = pl.ds(h * half, half)
        return pltpu.make_async_remote_copy(src_ref=picked.at[target, :, cols], dst_ref=r1.at[h, k], send_sem=rs_send.at[h, k], recv_sem=rs_recv.at[h, k], device_id=place.device((a,)), device_id_type=MESH)

    def second(h):
        return pltpu.make_async_remote_copy(src_ref=tmp.at[h], dst_ref=r2.at[h], send_sem=rs_send.at[h, 2], recv_sem=rs_recv.at[h, 2], device_id=place.device((near[1 - h],)), device_id_type=MESH)

    def go(copy):
        copy.start()
        started.append(copy)

    for k in (1, 0):
        for h in range(2):
            go(first(h, k))
    for i in range(2):
        go(side_hop(i, 0))
        go(side_hop(i, 1))
        all_i_or_f = sides[i][1]
        all_i_or_f[place.cp()] = sides[i][0][:]
    for i in range(base.shape[0] // step):
        blank(i).start()
    for h in range(2):
        cols = slice(h * half, (h + 1) * half)
        first(h, 1).wait_recv()
        tmp[h] = picked[place.tp((near[1 - h],)), :, cols] + r1[h, 1]
        go(second(h))
    for i in range(2):
        side_hop(i, 0).wait_recv()
        go(side_hop(i, 2))
    mine = place.slot()
    for h in range(2):
        cols = slice(h * half, (h + 1) * half)
        first(h, 0).wait_recv()
        part = picked[place.tp(), :, cols] + r1[h, 0]
        second(h).wait_recv()
        buf[mine, :, cols] = part + r2[h]
    gather = Gather(place, buf, send, recv, core_send, core_recv)
    gather.run()
    keep = pltpu.make_async_copy(buf.at[mine], slice_out, slice_sem)
    keep.start()
    gather.finish(out, out_sem)
    keep.wait()
    for i in range(2):
        side_hop(i, 1).wait_recv()
        side_hop(i, 2).wait_recv()
    for i in range(base.shape[0] // step):
        blank(i).wait()
    for c in started:
        c.wait_send()


def embed_gather(picked, side_f, side_i, blank_rows, step=400):
    _, rows, dim = picked.shape
    half = dim // 2
    dma = pltpu.SemaphoreType.DMA
    vmem = pl.BlockSpec(memory_space=pltpu.VMEM)
    hbm = pl.BlockSpec(memory_space=pl.ANY)
    return pl.pallas_call(
        embed_kernel,
        out_shape=[
            jax.ShapeDtypeStruct((16 * rows, dim), BF16),
            jax.ShapeDtypeStruct((rows, dim), BF16),
            jax.ShapeDtypeStruct((4,) + side_f.shape, F32),
            jax.ShapeDtypeStruct((4,) + side_i.shape, I32),
            jax.ShapeDtypeStruct((blank_rows, dim), F32),
        ],
        in_specs=[vmem, vmem, vmem],
        out_specs=[hbm, hbm, vmem, vmem, hbm],
        scratch_shapes=[
            pltpu.VMEM((step, dim), F32),
            dma((blank_rows // step,)),
            pltpu.VMEM((16, rows, dim), BF16),
            pltpu.VMEM((2, 2, rows, half), BF16),
            pltpu.VMEM((2, rows, half), BF16),
            pltpu.VMEM((2, rows, half), BF16),
            dma((21,)), dma((21,)), dma((24,)), dma((24,)), dma((16,)),
            *[dma((2, 3))] * 4, dma,
        ],
        compiler_params=pltpu.CompilerParams(collective_id=0, has_side_effects=True, vmem_limit_bytes=40 * MIB),
        name="embed_gather",
    )(picked, side_f, side_i)


def slot_block(j):
    return jnp.where(j < 4, 2 * j, 15 - 2 * j)


def unpack_angles(packed):
    turned = pltpu.roll(packed, packed.shape[1] // 2, 1)
    low = lax.broadcasted_iota(I32, packed.shape, 1) < packed.shape[1] // 2
    return jnp.where(low, packed, turned), jnp.where(low, -turned, packed)


def qkv_kernel(x, gain, wq, wk, wv, angles, act, q, k, v, wide, *, head_dim):
    width = wq.shape[1]

    @pl.when(pl.program_id(0) == 0)
    def _():
        for i, w in enumerate((wq, wk, wv)):
            wide[:, i * width:(i + 1) * width] = w[:]

    feats = x[:].astype(F32)
    inv = lax.rsqrt(mean_row(feats * feats) + NORM_EPS)
    a = (feats * inv * gain[:]).astype(BF16)
    act[:] = a
    t = nn(a, wide[:])
    cos, sin = unpack_angles(angles[:])
    for i, out in enumerate((q, k, v)):
        for h in range(width // head_dim):
            th = t[:, i * width + h * head_dim:i * width + (h + 1) * head_dim]
            if i < 2:
                th = th * cos + pltpu.roll(th, head_dim // 2, 1) * sin
            out[:, h * head_dim:(h + 1) * head_dim] = th.astype(BF16)


def project_qkv(x_all, gain, wq, wk, wv, angles, block=512):
    total, dim = x_all.shape
    width = wq.shape[1]
    head_dim = angles.shape[1]
    rows = lambda n: pl.BlockSpec((block, n), lambda i: (i, 0))
    whole = lambda a: pl.BlockSpec(a.shape, lambda i: (0, 0), pipeline_mode=pl.Buffered(1))
    return pl.pallas_call(
        functools.partial(qkv_kernel, head_dim=head_dim),
        out_shape=[jax.ShapeDtypeStruct((total, n), BF16) for n in (dim, width, width, width)] + [jax.ShapeDtypeStruct((dim, 3 * width), BF16)],
        grid=(total // block,),
        in_specs=[rows(dim), whole(gain), whole(wq), whole(wk), whole(wv), rows(head_dim)],
        out_specs=[rows(dim), rows(width), rows(width), rows(width), pl.BlockSpec((dim, 3 * width), lambda i: (0, 0), pipeline_mode=pl.Buffered(1))],
        compiler_params=pltpu.CompilerParams(vmem_limit_bytes=60 * MIB),
        cost_estimate=cost(6 * total * dim * width, 4 * total * dim + 6 * dim * width + 6 * total * width),
        name="project_qkv",
    )(x_all, gain, wq, wk, wv, angles)


def block_range(info, i, blocks):
    r = info[0]
    b = jnp.where(i == 0, r, blocks - 1 - r)
    mine = 2 + 2 * (2 * r + i)
    jmin = 0
    imax = -1
    for j in range(blocks):
        there = 2 + 2 * (2 * j if j < blocks // 2 else 2 * blocks - 1 - 2 * j)
        jmin = jmin + (info[there + 1] < info[mine]).astype(I32)
        imax = imax + (info[there] <= info[mine + 1]).astype(I32)
    return b, jmin, imax


def attend_kernel(info, q, k, v, doc_col, doc_row, out, lse, sc, *, heads, head_dim, scale):
    blk = q.shape[0]
    b, jmin, _ = block_range(info, pl.program_id(0), doc_row.shape[0])
    row_n = lax.broadcasted_iota(I32, (blk, blk), 0) + b * blk
    col_n = lax.broadcasted_iota(I32, (blk, blk), 1)

    def score(j, peaks):
        sb = slot_block(j)
        off = pl.multiple_of(sb * blk, blk)
        allowed = (doc_col[:] == doc_row[sb]) & (col_n + j * blk <= row_n)
        new = []
        for h in range(heads):
            cols = slice(h * head_dim, (h + 1) * head_dim)
            s = nt(q[:, cols], k[pl.ds(off, blk), cols]) * scale
            s = jnp.where(allowed, s, NEG_BIG)
            sc[j, h] = s
            new.append(jnp.maximum(peaks[h], jnp.max(s, axis=1, keepdims=True)))
        return tuple(new)

    peaks = lax.fori_loop(jmin, b + 1, score, tuple(jnp.full((blk, 1), NEG_BIG, F32) for _ in range(heads)))

    def weigh(j, sums):
        new = []
        for h in range(heads):
            p = jnp.exp(sc[j, h] - peaks[h])
            sc[j, h] = p
            new.append(sums[h] + row_sum(p))
        return tuple(new)

    sums = lax.fori_loop(jmin, b + 1, weigh, tuple(jnp.zeros((blk, 1), F32) for _ in range(heads)))
    inv = tuple(1.0 / t for t in sums)
    for h in range(heads):
        lse[:, h:h + 1] = peaks[h] + jnp.log(sums[h])

    def mix(j, acc):
        off = pl.multiple_of(slot_block(j) * blk, blk)
        new = []
        for h in range(heads):
            cols = slice(h * head_dim, (h + 1) * head_dim)
            new.append(acc[h] + nn((sc[j, h] * inv[h]).astype(BF16), v[pl.ds(off, blk), cols]))
        return tuple(new)

    acc = lax.fori_loop(jmin, b + 1, mix, tuple(jnp.zeros((blk, head_dim), F32) for _ in range(heads)))
    for h in range(heads):
        out[:, h * head_dim:(h + 1) * head_dim] = acc[h].astype(BF16)


def attend(info, q, k, v, doc_col, doc_row, head_dim, blk):
    total, width = k.shape
    heads = width // head_dim
    mine = lambda n: pl.BlockSpec((blk, n), lambda i, info: (2 * info[0] + i, 0))
    return pl.pallas_call(
        functools.partial(attend_kernel, heads=heads, head_dim=head_dim, scale=head_dim ** -0.5),
        out_shape=[jax.ShapeDtypeStruct((2 * blk, width), BF16), jax.ShapeDtypeStruct((2 * blk, 8), F32)],
        grid_spec=pltpu.PrefetchScalarGridSpec(
            num_scalar_prefetch=1,
            grid=(2,),
            in_specs=[mine(width), whole(k), whole(v), mine(1), whole(doc_row)],
            out_specs=[pl.BlockSpec((blk, width), lambda i, info: (i, 0)), pl.BlockSpec((blk, 8), lambda i, info: (i, 0))],
            scratch_shapes=[pltpu.VMEM((total // blk, heads, blk, blk), F32)],
        ),
        compiler_params=pltpu.CompilerParams(vmem_limit_bytes=40 * MIB),
        cost_estimate=cost(4 * 2 * blk * total * width, 8 * total * width),
        name="attend",
    )(info, q, k, v, doc_col, doc_row)


def attend_back_kernel(info, q, k, v, do, doc_col, doc_row, lse_col, lse_row, del_col, del_row, angles, out, acc, *, heads, head_dim, scale):
    blk = angles.shape[0]
    width = heads * head_dim
    i = pl.program_id(0)
    b, jmin, imax = block_range(info, i, doc_row.shape[0])
    me = pl.multiple_of((2 * info[0] + i) * blk, blk)
    mine = pl.ds(me, blk)
    iota_r = lax.broadcasted_iota(I32, (blk, blk), 0)
    iota_c = lax.broadcasted_iota(I32, (blk, blk), 1)
    acc[:] = jnp.zeros_like(acc)
    spans = [slice(h * head_dim, (h + 1) * head_dim) for h in range(heads)]

    def for_query(j, c):
        sb = slot_block(j)
        there = pl.ds(pl.multiple_of(sb * blk, blk), blk)
        allowed = (doc_col[mine, :] == doc_row[sb]) & (iota_c + j * blk <= iota_r + b * blk)
        for h, cols in enumerate(spans):
            s = jnp.where(allowed, nt(q[mine, cols], k[there, cols]) * scale, NEG_BIG)
            p = jnp.exp(s - lse_col[mine, h:h + 1])
            dp = to_bf16(nt(do[mine, cols], v[there, cols]))
            ds = (p * (dp - del_col[mine, h:h + 1]) * scale).astype(BF16)
            acc[0, :, cols] += nn(ds, k[there, cols])
        return c

    lax.fori_loop(jmin, b + 1, for_query, 0)

    def for_key(j, c):
        sb = slot_block(j)
        there = pl.ds(pl.multiple_of(sb * blk, blk), blk)
        allowed = (doc_col[mine, :] == doc_row[sb]) & (iota_r + b * blk <= iota_c + j * blk)
        for h, cols in enumerate(spans):
            s = jnp.where(allowed, nt(k[mine, cols], q[there, cols]) * scale, NEG_BIG)
            p = jnp.exp(s - lse_row[sb, h:h + 1, :])
            dp = to_bf16(nt(v[mine, cols], do[there, cols]))
            ds = (p * (dp - del_row[sb, h:h + 1, :]) * scale).astype(BF16)
            acc[2, :, cols] += nn(p.astype(BF16), do[there, cols])
            acc[1, :, cols] += nn(ds, q[there, cols])
        return c

    lax.fori_loop(b, imax + 1, for_key, 0)
    cos, sin = unpack_angles(angles[:])
    for part in range(3):
        for h, cols in enumerate(spans):
            t = acc[part, :, cols]
            if part < 2:
                t = to_bf16(t)
                t = t * cos - pltpu.roll(t, head_dim // 2, 1) * sin
            out[:, part * width + h * head_dim:part * width + (h + 1) * head_dim] = t.astype(BF16)


def attend_back(info, q, k, v, do, doc_col, doc_row, lse_col, lse_row, del_col, del_row, angles, blk):
    total, width = k.shape
    head_dim = angles.shape[1]
    heads = width // head_dim
    mine = lambda n: pl.BlockSpec((blk, n), lambda i, info: (2 * info[0] + i, 0))
    arrays = (q, k, v, do, doc_col, doc_row, lse_col, lse_row, del_col, del_row)
    return pl.pallas_call(
        functools.partial(attend_back_kernel, heads=heads, head_dim=head_dim, scale=head_dim ** -0.5),
        out_shape=jax.ShapeDtypeStruct((2 * blk, 3 * width), BF16),
        grid_spec=pltpu.PrefetchScalarGridSpec(
            num_scalar_prefetch=1,
            grid=(2,),
            in_specs=[whole(a) for a in arrays] + [mine(head_dim)],
            out_specs=pl.BlockSpec((blk, 3 * width), lambda i, info: (i, 0)),
            scratch_shapes=[pltpu.VMEM((3, blk, width), F32)],
        ),
        compiler_params=pltpu.CompilerParams(vmem_limit_bytes=48 * MIB),
        cost_estimate=cost(14 * 2 * blk * total * width // 2, 12 * total * width),
        name="attend_back",
    )(info, *arrays, angles)


def out_proj_kernel(info, x, att, a0, b0, a1, b1, gain, res, act, wide, abuf, bbuf, sems):
    tp, _, width = att.shape
    na, nb = a0.shape[1], b0.shape[1]
    sets = ((a0, b0), (a1, b1))

    def copies(i):
        return (pltpu.make_async_copy(sets[i][0], abuf.at[i], sems.at[i, 0]), pltpu.make_async_copy(sets[i][1], bbuf.at[i], sems.at[i, 1]))

    for i in range(2):
        for c in copies(i):
            c.start()
    for t in range(tp):
        wide[:, t * width:(t + 1) * width] = att[t]
    for i in range(2):
        start = (info[1] ^ i) * (na + nb)
        first, second = copies(i)
        first.wait()
        cols = pl.ds(pl.multiple_of(start, 128), na)
        res[:, cols] = x[:, cols].astype(F32) + nn(wide[:], abuf[i])
        second.wait()
        cols = pl.ds(pl.multiple_of(start + na, 128), nb)
        res[:, cols] = x[:, cols].astype(F32) + nn(wide[:], bbuf[i])
    h = res[:]
    inv = lax.rsqrt(mean_row(h * h) + NORM_EPS)
    act[:] = (h * inv * gain[:]).astype(BF16)


def out_proj(info, flip, x_all, att, pieces, gain):
    _, rows, _ = att.shape
    dim = x_all.shape[1]
    full = pl.BlockSpec((rows, dim), lambda i, info: (0, 0))
    return pl.pallas_call(
        out_proj_kernel,
        out_shape=[jax.ShapeDtypeStruct((rows, dim), F32), jax.ShapeDtypeStruct((rows, dim), BF16)],
        grid_spec=pltpu.PrefetchScalarGridSpec(
            num_scalar_prefetch=1,
            grid=(1,),
            in_specs=[pl.BlockSpec((rows, dim), lambda i, info: (info[0] ^ flip, 0)), whole(att)] + [pl.BlockSpec(memory_space=pl.ANY)] * 4 + [whole(gain)],
            out_specs=[full, full],
            scratch_shapes=[pltpu.VMEM((rows, dim), BF16), pltpu.VMEM((2,) + pieces[0].shape, BF16), pltpu.VMEM((2,) + pieces[1].shape, BF16), pltpu.SemaphoreType.DMA((2, 2))],
        ),
        compiler_params=pltpu.CompilerParams(vmem_limit_bytes=56 * MIB),
        cost_estimate=cost(2 * rows * dim * dim, 2 * dim * dim + 10 * rows * dim),
        name="out_proj",
    )(info, x_all, att, *pieces, gain)


def att_kernel(att, lse, x_all, a0, b0, a1, b1, gain, parts, lse_out, res, act, x, abuf, bbuf, send, recv, lse_send, lse_recv, load):
    place = Place()
    rows, width = att.shape
    na, nb = a0.shape[1], b0.shape[1]
    mine = place.cp()
    loads = [pltpu.make_async_copy(x_all.at[pl.ds(mine * rows, rows), :], x, load.at[4])]
    for i, (src, dst) in enumerate(((a0, abuf.at[0]), (b0, bbuf.at[0]), (a1, abuf.at[1]), (b1, bbuf.at[1]))):
        loads.append(pltpu.make_async_copy(src, dst, load.at[i]))
    for c in loads:
        c.start()
    place.meet(("y", "z", "x", "core"))
    started = []
    near = ("y", "z")
    spans = column_parts(width, 2)

    def hop(p, flip, dim):
        there = tuple(d for d in near if (d in flip) != (d == dim))
        index = p * 3 + (there == ("y",)) + 2 * (there == ("z",))
        start, size = spans[p]
        cols = pl.ds(start, size)
        slot = place.tp(flip)
        src = parts.at[slot, :, cols] if flip else att.at[:, cols]
        return pltpu.make_async_remote_copy(src_ref=src, dst_ref=parts.at[slot, :, cols], send_sem=send.at[index], recv_sem=recv.at[index], device_id=place.device((dim,)), device_id_type=MESH)

    def lse_hop(step):
        src, slot, dim = ((lse, mine, "x"), (lse, mine, "core"), (lse_out.at[place.cp(("x",))], place.cp(("x",)), "core"))[step]
        return pltpu.make_async_remote_copy(src_ref=src, dst_ref=lse_out.at[slot], send_sem=lse_send.at[step], recv_sem=lse_recv.at[step], device_id=place.device((dim,)), device_id_type=MESH)

    def go(copy):
        copy.start()
        started.append(copy)

    for step in range(2):
        for p in range(2):
            go(hop(p, (), near[(p + step) % 2]))
    go(lse_hop(0))
    go(lse_hop(1))
    lse_out[mine] = lse[:]
    parts[place.tp()] = att[:]
    for c in loads:
        c.wait()

    def add(slot, first=False):
        for i in range(2):
            start = place.coord("core", ("core",) if i else ()) * (na + nb)
            k = pl.ds(pl.multiple_of(slot * width, width), width)
            for buf, at, n in ((abuf, 0, na), (bbuf, na, nb)):
                cols = pl.ds(pl.multiple_of(start + at, 128), n)
                t = nn(parts[slot], buf[i, k, :])
                res[:, cols] = t + (x[:, cols].astype(F32) if first else res[:, cols])

    add(place.tp(), True)
    for p in range(2):
        hop(p, (), near[p]).wait_recv()
        go(hop(p, (near[p],), near[1 - p]))
    lse_hop(0).wait_recv()
    go(lse_hop(2))
    for p in (1, 0):
        hop(p, (), near[1 - p]).wait_recv()
        add(place.tp((near[1 - p],)))
    for p in range(2):
        hop(p, (near[p],), near[1 - p]).wait_recv()
    add(place.tp(near))
    h = res[:]
    act[:] = (h * lax.rsqrt(mean_row(h * h) + NORM_EPS) * gain[:]).astype(BF16)
    lse_hop(1).wait_recv()
    lse_hop(2).wait_recv()
    for c in started:
        c.wait_send()


def att_project(att, lse, x_all, pieces, gain):
    rows, width = att.shape
    dim = x_all.shape[1]
    dma = pltpu.SemaphoreType.DMA
    vmem = pl.BlockSpec(memory_space=pltpu.VMEM)
    hbm = pl.BlockSpec(memory_space=pl.ANY)
    return pl.pallas_call(
        att_kernel,
        out_shape=[jax.ShapeDtypeStruct((4, rows, width), BF16), jax.ShapeDtypeStruct((4,) + lse.shape, F32), jax.ShapeDtypeStruct((rows, dim), F32), jax.ShapeDtypeStruct((rows, dim), BF16)],
        in_specs=[vmem, vmem] + [hbm] * 5 + [vmem],
        out_specs=[vmem] * 4,
        scratch_shapes=[
            pltpu.VMEM((rows, dim), BF16), pltpu.VMEM((2,) + pieces[0].shape, BF16), pltpu.VMEM((2,) + pieces[1].shape, BF16),
            *[dma((n,)) for n in (6, 6, 3, 3, 5)],
        ],
        compiler_params=pltpu.CompilerParams(collective_id=1, has_side_effects=True, vmem_limit_bytes=48 * MIB),
        name="att_project",
    )(att, lse, x_all, *pieces, gain)


def weight_grad_kernel(info, *refs, pieces, splits):
    lhs = refs[:pieces]
    rhs = refs[pieces:2 * pieces]
    outs = refs[2 * pieces:]
    t = tn(lhs[0][:], rhs[0][:])
    for a, b in zip(lhs[1:], rhs[1:]):
        t += tn(a[:], b[:])
    width = t.shape[1] // splits
    for i, out in enumerate(outs):
        out[:] = t[:, i * width:(i + 1) * width]


def weight_grad(info, lhs, rhs, block=256, splits=1, rows=None):
    def spec(arr, p, cols, moving):
        if arr.ndim == 3:
            return pl.BlockSpec((None, arr.shape[1], cols), lambda i, info: (info[0] ^ p, 0, i if moving else 0))
        return pl.BlockSpec((arr.shape[0], cols), lambda i, info: (0, i if moving else 0))

    tokens = lhs[0].shape[-2]
    rows, dim = rows or lhs[0].shape[-1], rhs[0].shape[-1]
    n = len(lhs)
    width = dim // splits
    outs = pl.pallas_call(
        functools.partial(weight_grad_kernel, pieces=n, splits=splits),
        out_shape=[jax.ShapeDtypeStruct((rows, width), F32)] * splits,
        grid_spec=pltpu.PrefetchScalarGridSpec(
            num_scalar_prefetch=1,
            grid=(pl.cdiv(rows, block),),
            in_specs=[spec(a, p, block, True) for p, a in enumerate(lhs)] + [spec(b, p, dim, False) for p, b in enumerate(rhs)],
            out_specs=[pl.BlockSpec((block, width), lambda i, info: (i, 0))] * splits,
        ),
        compiler_params=pltpu.CompilerParams(vmem_limit_bytes=56 * MIB),
        cost_estimate=cost(2 * n * tokens * rows * dim, 4 * rows * dim + 2 * n * tokens * (rows + dim)),
        name="weight_grad",
    )(info, *lhs, *rhs)
    return outs if splits > 1 else outs[0]


def mlp_kernel(act, dy, wg, wu, wd, hidden, d_gate, d_up, *grad, limit):
    i = pl.program_id(0)
    block = wg.shape[0]
    left = limit - i * block
    row_ok = lax.broadcasted_iota(I32, (block, 1), 0) < left
    col_ok = lax.broadcasted_iota(I32, (1, block), 1) < left
    wgt = jnp.where(row_ok, wg[:], 0).astype(BF16)
    wut = jnp.where(row_ok, wu[:], 0).astype(BF16)
    gate = nt(act[:], wgt)
    up = nt(act[:], wut)
    dh = jnp.where(col_ok, to_bf16(nt(dy[:], wd[:])), 0)
    sig = jax.nn.sigmoid(gate)
    hidden[:] = (gate * sig * up).astype(BF16)
    dg = (dh * up * sig * (1.0 + gate * (1.0 - sig))).astype(BF16)
    du = (dh * gate * sig).astype(BF16)
    d_gate[:] = dg
    d_up[:] = du
    if grad:
        t = nn(dg, wgt) + nn(du, wut)

        @pl.when(i == 0)
        def _():
            grad[0][:] = t

        @pl.when(i > 0)
        def _():
            grad[0][:] += t


def mlp_block(act, dy, wg, wu, wd, with_grad, block=256):
    rows, dim = act.shape
    limit = wg.shape[0]
    cols = pl.BlockSpec((rows, block), lambda i: (0, i))
    tile = pl.BlockSpec((block, dim), lambda i: (i, 0))
    whole = pl.BlockSpec((rows, dim), lambda i: (0, 0))
    return pl.pallas_call(
        functools.partial(mlp_kernel, limit=limit),
        out_shape=[jax.ShapeDtypeStruct((rows, pl.cdiv(limit, block) * block), BF16)] * 3 + [jax.ShapeDtypeStruct((rows, dim), F32)] * with_grad,
        grid=(pl.cdiv(limit, block),),
        in_specs=[whole, whole, tile, tile, tile],
        out_specs=[cols] * 3 + [whole] * with_grad,
        compiler_params=pltpu.CompilerParams(vmem_limit_bytes=48 * MIB),
        cost_estimate=cost((6 + 4 * with_grad) * rows * dim * limit, 4 * dim * limit + 6 * rows * limit + 10 * rows * dim),
        name="mlp_block",
    )(act, dy, wg, wu, wd)


def scatter_kernel(order, sid, runs, bounds, rows, base_hbm, out_hbm, sums, row_sem, sum_sem):
    lo = bounds[0]
    hi = bounds[1]

    def one(c):
        p, singles, multi = c
        n = runs[p]
        t = order[p]
        single = n == 1

        @pl.when(single)
        def _():
            pltpu.make_async_copy(rows.at[pl.ds(t, 1), :], out_hbm.at[pl.ds(sid[p], 1), :], row_sem).start()

        @pl.when(jnp.logical_not(single))
        def _():
            def add(j, acc):
                return acc + rows[pl.ds(order[p + j], 1), :]

            sums[pl.ds(multi, 1), :] = lax.fori_loop(1, n, add, rows[pl.ds(t, 1), :])

        return p + n, singles + single.astype(I32), multi + 1 - single.astype(I32)

    _, singles, multi = lax.while_loop(lambda c: c[0] < hi, one, (lo, 0, 0))

    def two(c):
        p, k = c
        n = runs[p]

        @pl.when(n > 1)
        def _():
            pltpu.make_async_copy(sums.at[pl.ds(k, 1), :], out_hbm.at[pl.ds(sid[p], 1), :], sum_sem).start()

        return p + n, k + (n > 1).astype(I32)

    lax.while_loop(lambda c: c[0] < hi, two, (lo, 0))

    def wait(sem):
        def body(i, c):
            pltpu.make_async_copy(sums.at[pl.ds(0, 1), :], out_hbm.at[pl.ds(0, 1), :], sem).wait()
            return c

        return body

    lax.fori_loop(0, singles, wait(row_sem), 0)
    lax.fori_loop(0, multi, wait(sum_sem), 0)


def scatter_rows(order, sid, runs, bounds, grads, base, tokens):
    _, dim = grads.shape
    rows = base.shape[0]
    return pl.pallas_call(
        scatter_kernel,
        out_shape=jax.ShapeDtypeStruct((rows, dim), F32),
        grid_spec=pltpu.PrefetchScalarGridSpec(
            num_scalar_prefetch=4,
            grid=(),
            in_specs=[pl.BlockSpec(memory_space=pltpu.VMEM), pl.BlockSpec(memory_space=pl.ANY)],
            out_specs=pl.BlockSpec(memory_space=pl.ANY),
            scratch_shapes=[pltpu.VMEM((tokens // 2, dim), F32), pltpu.SemaphoreType.DMA, pltpu.SemaphoreType.DMA],
        ),
        input_output_aliases={5: 0},
        compiler_params=pltpu.CompilerParams(vmem_limit_bytes=40 * MIB),
        name="scatter_rows",
    )(order, sid, runs, bounds, grads, base)


def solution(mesh):
    cp_count = mesh.shape["cp"]
    tp_count = mesh.shape["tp"]
    both = ("cp", "tp")
    x_swap = [(i, i ^ 2) for i in range(cp_count)]
    core_swap = [(i, i ^ 1) for i in range(cp_count)]

    def compute(tokens, pos, doc_id, dy, table, w_q, w_k, w_v, w_o, w_gate, w_up, w_down, gain_one, gain_two, inv_freq):
        span = tokens.shape[0]
        total = span * cp_count
        part = span // tp_count
        rows, dim = table.shape
        head_dim = 2 * inv_freq.shape[0]
        heads = w_q.shape[1] // head_dim
        width = heads * head_dim
        tp_rank = lax.axis_index("tp")
        cp_rank = lax.axis_index("cp")
        core = cp_rank % 2
        gain_a = gain_one.astype(F32)
        gain_b = gain_two.astype(F32)

        barrier = lax.optimization_barrier
        join = lambda arr, axis: lax.all_gather(arr, axis, axis=0, tiled=True)
        add_up = lambda arr: lax.psum_scatter(arr, "tp", scatter_dimension=0, tiled=True)
        swap = lambda arr, pairs, axis="cp": lax.ppermute(arr, axis, pairs)
        local_ids = tokens - tp_rank * rows
        owned = (local_ids >= 0) & (local_ids < rows)
        safe_ids = jnp.where(owned, local_ids, jnp.arange(span) * (rows // span))
        picked = jnp.where(owned[:, None], jnp.take(table, safe_ids, axis=0), 0).astype(BF16)
        half = dim // 2
        near = 512
        wo_half = lax.dynamic_slice_in_dim(w_o, core * half, half, 1)
        wo_near = join(wo_half[:, :near], "tp")
        angle = pos.astype(F32)[:, None] * inv_freq[None, :]
        side_f = jnp.concatenate([jnp.cos(angle), jnp.sin(angle)], axis=1)
        side_i = jnp.concatenate([tokens[None], doc_id[None], jnp.zeros((6, span), I32)], axis=0)
        x_all, x_slice, angles, ints, base = embed_gather(picked.reshape(tp_count, part, dim), side_f, side_i, rows)
        angles = angles.reshape(total, head_dim)
        tok_all = ints[:, 0, :].reshape(total)
        doc_all = ints[:, 1, :].reshape(total)
        wo_far = barrier((wo_half[:, near:], x_all))[0]
        wo_rest = join(wo_far, "tp")
        wo_pieces = (wo_near, wo_rest, swap(wo_near, core_swap), swap(wo_rest, core_swap))

        dy_x = swap(barrier((dy, x_all))[0], x_swap)
        act_a, query, key, value, w_qkv = project_qkv(x_all, gain_a[None, :], w_q, w_k, w_v, angles)

        blk = span // 2
        blocks = total // blk
        doc_col = doc_all[:, None]
        doc_row = doc_all.reshape(blocks, 1, blk)
        docs = doc_all.reshape(blocks, blk)
        docs = jnp.stack([docs[:, 0], docs[:, -1]], axis=1).reshape(2 * blocks)
        info = jnp.concatenate([cp_rank[None], core[None], docs]).astype(I32)
        attended, lse = attend(info, query, key, value, doc_col, doc_row, head_dim, blk)

        gain_row = gain_b[None, :]
        att_parts, lse_all, residual, act_b = att_project(attended, lse, x_all, wo_pieces, gain_row)
        lse_all = lse_all.reshape(total, 8)
        att_x = swap(att_parts, x_swap)

        wg, wu = w_gate.T, w_up.T
        ffn = wg.shape[0]
        hidden, d_gate, d_up, d_act_b = mlp_block(act_b, dy, wg, wu, w_down, True)
        d_act_b = add_up(d_act_b)
        act_x = out_proj(info, 2, x_all, att_x, wo_pieces, gain_row)[1]
        hidden_x, d_gate_x, d_up_x = mlp_block(act_x, dy_x, wg, wu, w_down, False)
        d_act_b, hidden_x, d_gate_x, d_up_x = barrier((d_act_b, hidden_x, d_gate_x, d_up_x))
        d_act_b = to_bf16(d_act_b)
        acts, dys, hiddens, d_gates, d_ups = [(a, swap(a, core_swap), b, swap(b, core_swap)) for a, b in (
            (act_b, act_x), (dy, dy_x), (hidden, hidden_x), (d_gate, d_gate_x), (d_up, d_up_x))]
        heads_x = lax.dynamic_index_in_dim(att_x, tp_rank, 0, keepdims=False)
        head_parts = (attended, swap(attended, core_swap), heads_x, swap(heads_x, core_swap))
        att_heads = jnp.zeros((total, width), BF16)
        for k, piece in enumerate(head_parts):
            att_heads = lax.dynamic_update_slice_in_dim(att_heads, piece, (cp_rank ^ k) * span, 0)
        grad_down = weight_grad(info, hiddens, dys, rows=ffn)
        grad_gate = weight_grad(info, d_gates, acts, rows=ffn)
        grad_up = weight_grad(info, d_ups, acts, rows=ffn)

        def mine(arr):
            return lax.dynamic_slice_in_dim(arr, tp_rank * part, part, 0)

        res_part = mine(residual)
        normed_b, inv_b = rms_stats(res_part)
        grad_gain_b = jnp.sum(d_act_b * normed_b, axis=0)
        d_resid = mine(dy).astype(F32) + rms_back(d_act_b * gain_b, normed_b, inv_b)
        d_resid_all = join(d_resid.astype(BF16), both)
        out_part = nn(hidden[:, :ffn], w_down)
        d_resid_all, grad_down, att_heads, out_part = barrier((d_resid_all, grad_down, att_heads, out_part))
        out_slice = add_up(out_part)
        out_slice = (res_part + out_slice).astype(BF16)

        d_att = nt(d_resid_all, w_o)
        d_att_b = d_att.astype(BF16)
        head_of = (jnp.arange(width)[None, :] // head_dim == jnp.arange(8)[:, None]).astype(F32)
        prod = att_heads.astype(F32) * d_att_b.astype(F32)
        delta = lax.dot_general(head_of, prod, (((1,), (1,)), ((), ())), precision=lax.Precision.HIGHEST, preferred_element_type=F32)

        def by_block(arr):
            return jnp.transpose(arr.reshape(8, blocks, blk), (1, 0, 2))

        dqkv = attend_back(info, query, key, value, d_att_b, doc_col, doc_row, lse_all, by_block(lse_all.T), delta.T, by_block(delta), angles, blk)
        d_act_a = nt(dqkv, w_qkv)
        d_act_a, out_slice = barrier((d_act_a, out_slice))
        d_act_a = add_up(d_act_a)
        dqkv_x = swap(dqkv, x_swap)
        dqkvs = (dqkv, swap(dqkv, core_swap), dqkv_x, swap(dqkv_x, core_swap))
        grad_out = weight_grad(info, head_parts, [d_resid_all.reshape(cp_count, span, dim)] * 4)
        d_act_a, dqkv_x, grad_out, grad_up = barrier((d_act_a, dqkv_x, grad_out, grad_up))
        d_act_a = to_bf16(d_act_a)
        normed_a, inv_a = rms_stats(x_slice.astype(F32))
        grad_gain_a = jnp.sum(d_act_a * normed_a, axis=0)
        d_embed = d_resid + rms_back(d_act_a * gain_a, normed_a, inv_a)
        payload = jnp.concatenate([d_embed, grad_gain_a[None], grad_gain_b[None], jnp.zeros((6, dim), F32)], axis=0)
        gathered = join(payload, both)
        grad_qkv = weight_grad(info, [act_a.reshape(cp_count, span, dim)] * 4, dqkvs, splits=3)
        slot_ids = jnp.arange(total, dtype=I32)
        before = (tok_all[None, :] < tok_all[:, None]) | ((tok_all[None, :] == tok_all[:, None]) & (slot_ids[None, :] < slot_ids[:, None]))
        rank = jnp.sum(before.astype(I32), axis=1)
        count = jnp.sum((tok_all[None, :] == tok_all[:, None]).astype(I32), axis=1)
        at_rank = rank[None, :] == slot_ids[:, None]
        runs = jnp.sum(jnp.where(at_rank, count[None, :], 0), axis=1)
        order = jnp.sum(jnp.where(at_rank, slot_ids[None, :], 0), axis=1)
        sid = jnp.sum(jnp.where(at_rank, tok_all[None, :], 0), axis=1) - tp_rank * rows
        order = order + 8 * (order // part)
        bounds = jnp.stack([jnp.sum((tok_all < tp_rank * rows).astype(I32)), jnp.sum((tok_all < (tp_rank + 1) * rows).astype(I32))])
        gathered, grad_qkv, grad_gate, runs, order, sid, bounds = barrier((gathered, grad_qkv, grad_gate, runs, order, sid, bounds))
        out_slice = barrier((out_slice, gathered))[0]
        layer_out = join(out_slice, "tp")
        gain_grads = jnp.sum(gathered.reshape(cp_count * tp_count, part + 8, dim)[:, part:part + 2], axis=0)
        grad_table = scatter_rows(order, sid, runs, bounds, gathered, base, total)
        return (layer_out, grad_table, *grad_qkv, grad_out, grad_gate.T, grad_up.T, grad_down, gain_grads[0], gain_grads[1])

    col_spec = P(None, "tp")
    row_spec = P("tp")
    tok_spec = P("cp")
    rep_spec = P()
    in_specs = (tok_spec, tok_spec, tok_spec, P("cp"), row_spec, col_spec, col_spec, col_spec, row_spec, col_spec, col_spec, row_spec, rep_spec, rep_spec, rep_spec)
    out_specs = (P("cp"), row_spec, col_spec, col_spec, col_spec, row_spec, col_spec, col_spec, row_spec, rep_spec, rep_spec)
    return jax.shard_map(compute, mesh=mesh, in_specs=in_specs, out_specs=out_specs, check_vma=False)
```

```python
import functools
import jax
import jax.numpy as jnp
from jax import lax
from jax.experimental import pallas as pl
from jax.experimental.pallas import tpu as pltpu
from jax.sharding import PartitionSpec as P

NORM_EPS = 1e-5
NEG_BIG = -1e30
MIB = 2 ** 20
F32 = jnp.float32
BF16 = jnp.bfloat16
I32 = jnp.int32


def rms_stats(feats):
    inv_rms = lax.rsqrt(mean_row(feats * feats) + NORM_EPS)
    return feats * inv_rms, inv_rms


def rms_back(d_normed, normed, inv_rms):
    return inv_rms * (d_normed - normed * mean_row(d_normed * normed))


def to_bf16(feats):
    return feats.astype(BF16).astype(F32)


def contract(a, b, ca, cb):
    return lax.dot_general(a, b, (((ca,), (cb,)), ((), ())), preferred_element_type=F32)


def row_sum(t):
    return jnp.sum(t, axis=1, keepdims=True)


def mean_row(t):
    return row_sum(t) / t.shape[1]


def whole(a):
    return pl.BlockSpec(a.shape, lambda *i: (0,) * a.ndim)


def cost(flops, moved):
    return pl.CostEstimate(flops=flops, bytes_accessed=moved, transcendentals=0)


def nn(a, b):
    return contract(a, b, 1, 0)


def nt(a, b):
    return contract(a, b, 1, 1)


def tn(a, b):
    return contract(a, b, 0, 0)


DIMS = ("x", "y", "z")


class Place:
    def __init__(self):
        tp = lax.axis_index("tp")
        cp = lax.axis_index("cp")
        self.at = {"x": cp // 2, "core": cp % 2, "z": tp // 2, "y": tp % 2}

    def coord(self, dim, flip):
        return 1 - self.at[dim] if dim in flip else self.at[dim]

    def tp(self, flip=()):
        return self.coord("z", flip) * 2 + self.coord("y", flip)

    def cp(self, flip=()):
        return self.coord("x", flip) * 2 + self.coord("core", flip)

    def device(self, flip):
        return {"tp": self.tp(flip), "cp": self.cp(flip)}

    def slot(self, flip=()):
        return self.cp(flip) * 4 + self.tp(flip)

    def meet(self, dims):
        barrier = pltpu.get_barrier_semaphore()
        for d in dims:
            pl.semaphore_signal(barrier, inc=1, device_id=self.device((d,)), device_id_type=MESH)
        pl.semaphore_wait(barrier, len(dims))


MESH = pl.DeviceIdType.MESH
ORDERS = (("x", "y", "z"), ("y", "z", "x"), ("z", "x", "y"))
FLIPS = tuple(tuple(d for i, d in enumerate(DIMS) if n >> i & 1) for n in range(8))


def flip_code(flip):
    return sum(1 << DIMS.index(d) for d in flip)


def column_parts(width, count):
    tiles = width // 128
    sizes = [(tiles // count + (i < tiles % count)) * 128 for i in range(count)]
    return [(sum(sizes[:i]), n) for i, n in enumerate(sizes)]


class Gather:
    def __init__(self, place, buf, send, recv, core_send, core_recv):
        self.place, self.buf, self.send, self.recv, self.core_send, self.core_recv = place, buf, send, recv, core_send, core_recv
        self.parts = column_parts(buf.shape[2], 3)
        self.started = []

    def view(self, part, flip):
        start, size = self.parts[part]
        return self.buf.at[self.place.slot(flip), :, pl.ds(start, size)]

    def hop(self, part, flip, dim):
        there = tuple(d for d in DIMS if (d in flip) != (d == dim))
        index = part * 7 + flip_code(there) - 1
        ref = self.view(part, flip)
        return pltpu.make_async_remote_copy(src_ref=ref, dst_ref=ref, send_sem=self.send.at[index], recv_sem=self.recv.at[index], device_id=self.place.device((dim,)), device_id_type=MESH)

    def core_hop(self, part, flip):
        index = part * 8 + flip_code(flip)
        ref = self.view(part, flip)
        return pltpu.make_async_remote_copy(src_ref=ref, dst_ref=ref, send_sem=self.core_send.at[index], recv_sem=self.core_recv.at[index], device_id=self.place.device(("core",)), device_id_type=MESH)

    def go(self, copy):
        copy.start()
        self.started.append(copy)

    def wait(self, part, flip):
        order = ORDERS[part]
        last = max(order.index(d) for d in flip)
        came = tuple(d for d in flip if d != order[last])
        self.hop(part, came, order[last]).wait_recv()
        for dim in order[last + 1:]:
            self.go(self.hop(part, flip, dim))
        self.go(self.core_hop(part, flip))

    def run(self):
        for step in range(3):
            for part, order in enumerate(ORDERS):
                self.go(self.hop(part, (), order[step]))
        for part in range(3):
            self.go(self.core_hop(part, ()))
        for step in range(3):
            for flip in FLIPS[1:]:
                for part, order in enumerate(ORDERS):
                    if max(order.index(d) for d in flip) == step and len(flip) == 1:
                        self.wait(part, flip)
            for flip in FLIPS[1:]:
                for part, order in enumerate(ORDERS):
                    if max(order.index(d) for d in flip) == step and len(flip) > 1:
                        self.wait(part, flip)

    def finish(self, out, out_sem):
        rows = self.buf.shape[1]
        copies = []

        def store(flip):
            slot = self.place.slot(flip)
            c = pltpu.make_async_copy(self.buf.at[slot], out.at[pl.ds(slot * rows, rows), :], out_sem.at[len(copies)])
            c.start()
            copies.append(c)

        for flip in FLIPS:
            store(flip)
        for flip in FLIPS:
            other = flip + ("core",)
            for part in range(3):
                start, size = self.parts[part]
                ref = self.buf.at[self.place.slot(other), :, pl.ds(start, size)]
                index = part * 8 + flip_code(flip)
                pltpu.make_async_remote_copy(src_ref=ref, dst_ref=ref, send_sem=self.core_send.at[index], recv_sem=self.core_recv.at[index], device_id=self.place.device(("core",)), device_id_type=MESH).wait_recv()
            store(other)
        for c in self.started:
            c.wait_send()
        for c in copies:
            c.wait()


def embed_kernel(picked, side_f, side_i, out, slice_out, all_f, all_i, buf, r1, r2, tmp, send, recv, core_send, core_recv, out_sem, rs_send, rs_recv, side_send, side_recv, slice_sem):
    place = Place()
    place.meet(("x", "y", "z", "core"))
    half = buf.shape[2] // 2
    near = ("y", "z")

    sides = ((side_f, all_f), (side_i, all_i))
    started = []

    def side_hop(i, step):
        src, dst = sides[i]
        if step == 0:
            src_ref, slot, dim = src, place.cp(), "x"
        elif step == 1:
            src_ref, slot, dim = src, place.cp(), "core"
        else:
            src_ref, slot, dim = dst.at[place.cp(("x",))], place.cp(("x",)), "core"
        return pltpu.make_async_remote_copy(src_ref=src_ref, dst_ref=dst.at[slot], send_sem=side_send.at[i, step], recv_sem=side_recv.at[i, step], device_id=place.device((dim,)), device_id_type=MESH)

    def first(h, k):
        a, b = near[h], near[1 - h]
        target = place.tp((a,)) if k == 0 else place.tp((a, b))
        cols = pl.ds(h * half, half)
        return pltpu.make_async_remote_copy(src_ref=picked.at[target, :, cols], dst_ref=r1.at[h, k], send_sem=rs_send.at[h, k], recv_sem=rs_recv.at[h, k], device_id=place.device((a,)), device_id_type=MESH)

    def second(h):
        return pltpu.make_async_remote_copy(src_ref=tmp.at[h], dst_ref=r2.at[h], send_sem=rs_send.at[h, 2], recv_sem=rs_recv.at[h, 2], device_id=place.device((near[1 - h],)), device_id_type=MESH)

    def go(copy):
        copy.start()
        started.append(copy)

    for k in (1, 0):
        for h in range(2):
            go(first(h, k))
    for i in range(2):
        go(side_hop(i, 0))
        go(side_hop(i, 1))
        all_i_or_f = sides[i][1]
        all_i_or_f[place.cp()] = sides[i][0][:]
    for h in range(2):
        cols = slice(h * half, (h + 1) * half)
        first(h, 1).wait_recv()
        tmp[h] = picked[place.tp((near[1 - h],)), :, cols] + r1[h, 1]
        go(second(h))
    for i in range(2):
        side_hop(i, 0).wait_recv()
        go(side_hop(i, 2))
    mine = place.slot()
    for h in range(2):
        cols = slice(h * half, (h + 1) * half)
        first(h, 0).wait_recv()
        part = picked[place.tp(), :, cols] + r1[h, 0]
        second(h).wait_recv()
        buf[mine, :, cols] = part + r2[h]
    gather = Gather(place, buf, send, recv, core_send, core_recv)
    gather.run()
    keep = pltpu.make_async_copy(buf.at[mine], slice_out, slice_sem)
    keep.start()
    gather.finish(out, out_sem)
    keep.wait()
    for i in range(2):
        side_hop(i, 1).wait_recv()
        side_hop(i, 2).wait_recv()
    for c in started:
        c.wait_send()


def embed_gather(picked, side_f, side_i):
    _, rows, dim = picked.shape
    half = dim // 2
    dma = pltpu.SemaphoreType.DMA
    vmem = pl.BlockSpec(memory_space=pltpu.VMEM)
    hbm = pl.BlockSpec(memory_space=pl.ANY)
    return pl.pallas_call(
        embed_kernel,
        out_shape=[
            jax.ShapeDtypeStruct((16 * rows, dim), BF16),
            jax.ShapeDtypeStruct((rows, dim), BF16),
            jax.ShapeDtypeStruct((4,) + side_f.shape, F32),
            jax.ShapeDtypeStruct((4,) + side_i.shape, I32),
        ],
        in_specs=[vmem, vmem, vmem],
        out_specs=[hbm, hbm, vmem, vmem],
        scratch_shapes=[
            pltpu.VMEM((16, rows, dim), BF16),
            pltpu.VMEM((2, 2, rows, half), BF16),
            pltpu.VMEM((2, rows, half), BF16),
            pltpu.VMEM((2, rows, half), BF16),
            dma((21,)), dma((21,)), dma((24,)), dma((24,)), dma((16,)),
            *[dma((2, 3))] * 4, dma,
        ],
        compiler_params=pltpu.CompilerParams(collective_id=0, has_side_effects=True, vmem_limit_bytes=40 * MIB),
        name="embed_gather",
    )(picked, side_f, side_i)


def slot_block(j):
    return jnp.where(j < 4, 2 * j, 15 - 2 * j)


def unpack_angles(packed):
    turned = pltpu.roll(packed, packed.shape[1] // 2, 1)
    low = lax.broadcasted_iota(I32, packed.shape, 1) < packed.shape[1] // 2
    return jnp.where(low, packed, turned), jnp.where(low, -turned, packed)


def qkv_kernel(x, gain, wq, wk, wv, angles, act, q, k, v, wide, *, head_dim):
    width = wq.shape[1]

    @pl.when(pl.program_id(0) == 0)
    def _():
        for i, w in enumerate((wq, wk, wv)):
            wide[:, i * width:(i + 1) * width] = w[:]

    feats = x[:].astype(F32)
    inv = lax.rsqrt(mean_row(feats * feats) + NORM_EPS)
    a = (feats * inv * gain[:]).astype(BF16)
    act[:] = a
    t = nn(a, wide[:])
    cos, sin = unpack_angles(angles[:])
    for i, out in enumerate((q, k, v)):
        for h in range(width // head_dim):
            th = t[:, i * width + h * head_dim:i * width + (h + 1) * head_dim]
            if i < 2:
                th = th * cos + pltpu.roll(th, head_dim // 2, 1) * sin
            out[:, h * head_dim:(h + 1) * head_dim] = th.astype(BF16)


def project_qkv(x_all, gain, wq, wk, wv, angles, block=512):
    total, dim = x_all.shape
    width = wq.shape[1]
    head_dim = angles.shape[1]
    rows = lambda n: pl.BlockSpec((block, n), lambda i: (i, 0))
    whole = lambda a: pl.BlockSpec(a.shape, lambda i: (0, 0), pipeline_mode=pl.Buffered(1))
    return pl.pallas_call(
        functools.partial(qkv_kernel, head_dim=head_dim),
        out_shape=[jax.ShapeDtypeStruct((total, n), BF16) for n in (dim, width, width, width)] + [jax.ShapeDtypeStruct((dim, 3 * width), BF16)],
        grid=(total // block,),
        in_specs=[rows(dim), whole(gain), whole(wq), whole(wk), whole(wv), rows(head_dim)],
        out_specs=[rows(dim), rows(width), rows(width), rows(width), pl.BlockSpec((dim, 3 * width), lambda i: (0, 0), pipeline_mode=pl.Buffered(1))],
        compiler_params=pltpu.CompilerParams(vmem_limit_bytes=60 * MIB),
        cost_estimate=cost(6 * total * dim * width, 4 * total * dim + 6 * dim * width + 6 * total * width),
        name="project_qkv",
    )(x_all, gain, wq, wk, wv, angles)


def block_range(info, i, blocks):
    r = info[0]
    b = jnp.where(i == 0, r, blocks - 1 - r)
    mine = 2 + 2 * (2 * r + i)
    jmin = 0
    imax = -1
    for j in range(blocks):
        there = 2 + 2 * (2 * j if j < blocks // 2 else 2 * blocks - 1 - 2 * j)
        jmin = jmin + (info[there + 1] < info[mine]).astype(I32)
        imax = imax + (info[there] <= info[mine + 1]).astype(I32)
    return b, jmin, imax


def attend_kernel(info, q, k, v, doc_col, doc_row, out, lse, sc, *, heads, head_dim, scale):
    blk = q.shape[0]
    b, jmin, _ = block_range(info, pl.program_id(0), doc_row.shape[0])
    row_n = lax.broadcasted_iota(I32, (blk, blk), 0) + b * blk
    col_n = lax.broadcasted_iota(I32, (blk, blk), 1)

    def score(j, peaks):
        sb = slot_block(j)
        off = pl.multiple_of(sb * blk, blk)
        allowed = (doc_col[:] == doc_row[sb]) & (col_n + j * blk <= row_n)
        new = []
        for h in range(heads):
            cols = slice(h * head_dim, (h + 1) * head_dim)
            s = nt(q[:, cols], k[pl.ds(off, blk), cols]) * scale
            s = jnp.where(allowed, s, NEG_BIG)
            sc[j, h] = s
            new.append(jnp.maximum(peaks[h], jnp.max(s, axis=1, keepdims=True)))
        return tuple(new)

    peaks = lax.fori_loop(jmin, b + 1, score, tuple(jnp.full((blk, 1), NEG_BIG, F32) for _ in range(heads)))

    def weigh(j, sums):
        new = []
        for h in range(heads):
            p = jnp.exp(sc[j, h] - peaks[h])
            sc[j, h] = p
            new.append(sums[h] + row_sum(p))
        return tuple(new)

    sums = lax.fori_loop(jmin, b + 1, weigh, tuple(jnp.zeros((blk, 1), F32) for _ in range(heads)))
    inv = tuple(1.0 / t for t in sums)
    for h in range(heads):
        lse[:, h:h + 1] = peaks[h] + jnp.log(sums[h])

    def mix(j, acc):
        off = pl.multiple_of(slot_block(j) * blk, blk)
        new = []
        for h in range(heads):
            cols = slice(h * head_dim, (h + 1) * head_dim)
            new.append(acc[h] + nn((sc[j, h] * inv[h]).astype(BF16), v[pl.ds(off, blk), cols]))
        return tuple(new)

    acc = lax.fori_loop(jmin, b + 1, mix, tuple(jnp.zeros((blk, head_dim), F32) for _ in range(heads)))
    for h in range(heads):
        out[:, h * head_dim:(h + 1) * head_dim] = acc[h].astype(BF16)


def attend(info, q, k, v, doc_col, doc_row, head_dim, blk):
    total, width = k.shape
    heads = width // head_dim
    mine = lambda n: pl.BlockSpec((blk, n), lambda i, info: (2 * info[0] + i, 0))
    return pl.pallas_call(
        functools.partial(attend_kernel, heads=heads, head_dim=head_dim, scale=head_dim ** -0.5),
        out_shape=[jax.ShapeDtypeStruct((2 * blk, width), BF16), jax.ShapeDtypeStruct((2 * blk, 8), F32)],
        grid_spec=pltpu.PrefetchScalarGridSpec(
            num_scalar_prefetch=1,
            grid=(2,),
            in_specs=[mine(width), whole(k), whole(v), mine(1), whole(doc_row)],
            out_specs=[pl.BlockSpec((blk, width), lambda i, info: (i, 0)), pl.BlockSpec((blk, 8), lambda i, info: (i, 0))],
            scratch_shapes=[pltpu.VMEM((total // blk, heads, blk, blk), F32)],
        ),
        compiler_params=pltpu.CompilerParams(vmem_limit_bytes=40 * MIB),
        cost_estimate=cost(4 * 2 * blk * total * width, 8 * total * width),
        name="attend",
    )(info, q, k, v, doc_col, doc_row)


def attend_back_kernel(info, q, k, v, do, doc_col, doc_row, lse_col, lse_row, del_col, del_row, angles, out, acc, *, heads, head_dim, scale):
    blk = angles.shape[0]
    width = heads * head_dim
    i = pl.program_id(0)
    b, jmin, imax = block_range(info, i, doc_row.shape[0])
    me = pl.multiple_of((2 * info[0] + i) * blk, blk)
    mine = pl.ds(me, blk)
    iota_r = lax.broadcasted_iota(I32, (blk, blk), 0)
    iota_c = lax.broadcasted_iota(I32, (blk, blk), 1)
    acc[:] = jnp.zeros_like(acc)
    spans = [slice(h * head_dim, (h + 1) * head_dim) for h in range(heads)]

    def for_query(j, c):
        sb = slot_block(j)
        there = pl.ds(pl.multiple_of(sb * blk, blk), blk)
        allowed = (doc_col[mine, :] == doc_row[sb]) & (iota_c + j * blk <= iota_r + b * blk)
        for h, cols in enumerate(spans):
            s = jnp.where(allowed, nt(q[mine, cols], k[there, cols]) * scale, NEG_BIG)
            p = jnp.exp(s - lse_col[mine, h:h + 1])
            dp = to_bf16(nt(do[mine, cols], v[there, cols]))
            ds = (p * (dp - del_col[mine, h:h + 1]) * scale).astype(BF16)
            acc[0, :, cols] += nn(ds, k[there, cols])
        return c

    lax.fori_loop(jmin, b + 1, for_query, 0)

    def for_key(j, c):
        sb = slot_block(j)
        there = pl.ds(pl.multiple_of(sb * blk, blk), blk)
        allowed = (doc_col[mine, :] == doc_row[sb]) & (iota_r + b * blk <= iota_c + j * blk)
        for h, cols in enumerate(spans):
            s = jnp.where(allowed, nt(k[mine, cols], q[there, cols]) * scale, NEG_BIG)
            p = jnp.exp(s - lse_row[sb, h:h + 1, :])
            dp = to_bf16(nt(v[mine, cols], do[there, cols]))
            ds = (p * (dp - del_row[sb, h:h + 1, :]) * scale).astype(BF16)
            acc[2, :, cols] += nn(p.astype(BF16), do[there, cols])
            acc[1, :, cols] += nn(ds, q[there, cols])
        return c

    lax.fori_loop(b, imax + 1, for_key, 0)
    cos, sin = unpack_angles(angles[:])
    for part in range(3):
        for h, cols in enumerate(spans):
            t = acc[part, :, cols]
            if part < 2:
                t = to_bf16(t)
                t = t * cos - pltpu.roll(t, head_dim // 2, 1) * sin
            out[:, part * width + h * head_dim:part * width + (h + 1) * head_dim] = t.astype(BF16)


def attend_back(info, q, k, v, do, doc_col, doc_row, lse_col, lse_row, del_col, del_row, angles, blk):
    total, width = k.shape
    head_dim = angles.shape[1]
    heads = width // head_dim
    mine = lambda n: pl.BlockSpec((blk, n), lambda i, info: (2 * info[0] + i, 0))
    arrays = (q, k, v, do, doc_col, doc_row, lse_col, lse_row, del_col, del_row)
    return pl.pallas_call(
        functools.partial(attend_back_kernel, heads=heads, head_dim=head_dim, scale=head_dim ** -0.5),
        out_shape=jax.ShapeDtypeStruct((2 * blk, 3 * width), BF16),
        grid_spec=pltpu.PrefetchScalarGridSpec(
            num_scalar_prefetch=1,
            grid=(2,),
            in_specs=[whole(a) for a in arrays] + [mine(head_dim)],
            out_specs=pl.BlockSpec((blk, 3 * width), lambda i, info: (i, 0)),
            scratch_shapes=[pltpu.VMEM((3, blk, width), F32)],
        ),
        compiler_params=pltpu.CompilerParams(vmem_limit_bytes=48 * MIB),
        cost_estimate=cost(14 * 2 * blk * total * width // 2, 12 * total * width),
        name="attend_back",
    )(info, *arrays, angles)


def out_proj_kernel(info, x, att, a0, b0, a1, b1, gain, res, act, wide, abuf, bbuf, sems):
    tp, _, width = att.shape
    na, nb = a0.shape[1], b0.shape[1]
    sets = ((a0, b0), (a1, b1))

    def copies(i):
        return (pltpu.make_async_copy(sets[i][0], abuf.at[i], sems.at[i, 0]), pltpu.make_async_copy(sets[i][1], bbuf.at[i], sems.at[i, 1]))

    for i in range(2):
        for c in copies(i):
            c.start()
    for t in range(tp):
        wide[:, t * width:(t + 1) * width] = att[t]
    for i in range(2):
        start = (info[1] ^ i) * (na + nb)
        first, second = copies(i)
        first.wait()
        cols = pl.ds(pl.multiple_of(start, 128), na)
        res[:, cols] = x[:, cols].astype(F32) + nn(wide[:], abuf[i])
        second.wait()
        cols = pl.ds(pl.multiple_of(start + na, 128), nb)
        res[:, cols] = x[:, cols].astype(F32) + nn(wide[:], bbuf[i])
    h = res[:]
    inv = lax.rsqrt(mean_row(h * h) + NORM_EPS)
    act[:] = (h * inv * gain[:]).astype(BF16)


def out_proj(info, flip, x_all, att, pieces, gain):
    _, rows, _ = att.shape
    dim = x_all.shape[1]
    full = pl.BlockSpec((rows, dim), lambda i, info: (0, 0))
    return pl.pallas_call(
        out_proj_kernel,
        out_shape=[jax.ShapeDtypeStruct((rows, dim), F32), jax.ShapeDtypeStruct((rows, dim), BF16)],
        grid_spec=pltpu.PrefetchScalarGridSpec(
            num_scalar_prefetch=1,
            grid=(1,),
            in_specs=[pl.BlockSpec((rows, dim), lambda i, info: (info[0] ^ flip, 0)), whole(att)] + [pl.BlockSpec(memory_space=pl.ANY)] * 4 + [whole(gain)],
            out_specs=[full, full],
            scratch_shapes=[pltpu.VMEM((rows, dim), BF16), pltpu.VMEM((2,) + pieces[0].shape, BF16), pltpu.VMEM((2,) + pieces[1].shape, BF16), pltpu.SemaphoreType.DMA((2, 2))],
        ),
        compiler_params=pltpu.CompilerParams(vmem_limit_bytes=56 * MIB),
        cost_estimate=cost(2 * rows * dim * dim, 2 * dim * dim + 10 * rows * dim),
        name="out_proj",
    )(info, x_all, att, *pieces, gain)


def att_kernel(att, lse, x_all, a0, b0, a1, b1, gain, parts, lse_out, res, act, x, abuf, bbuf, send, recv, lse_send, lse_recv, load):
    place = Place()
    rows, width = att.shape
    na, nb = a0.shape[1], b0.shape[1]
    mine = place.cp()
    loads = [pltpu.make_async_copy(x_all.at[pl.ds(mine * rows, rows), :], x, load.at[4])]
    for i, (src, dst) in enumerate(((a0, abuf.at[0]), (b0, bbuf.at[0]), (a1, abuf.at[1]), (b1, bbuf.at[1]))):
        loads.append(pltpu.make_async_copy(src, dst, load.at[i]))
    for c in loads:
        c.start()
    place.meet(("y", "z", "x", "core"))
    started = []
    near = ("y", "z")
    spans = column_parts(width, 2)

    def hop(p, flip, dim):
        there = tuple(d for d in near if (d in flip) != (d == dim))
        index = p * 3 + (there == ("y",)) + 2 * (there == ("z",))
        start, size = spans[p]
        cols = pl.ds(start, size)
        slot = place.tp(flip)
        src = parts.at[slot, :, cols] if flip else att.at[:, cols]
        return pltpu.make_async_remote_copy(src_ref=src, dst_ref=parts.at[slot, :, cols], send_sem=send.at[index], recv_sem=recv.at[index], device_id=place.device((dim,)), device_id_type=MESH)

    def lse_hop(step):
        src, slot, dim = ((lse, mine, "x"), (lse, mine, "core"), (lse_out.at[place.cp(("x",))], place.cp(("x",)), "core"))[step]
        return pltpu.make_async_remote_copy(src_ref=src, dst_ref=lse_out.at[slot], send_sem=lse_send.at[step], recv_sem=lse_recv.at[step], device_id=place.device((dim,)), device_id_type=MESH)

    def go(copy):
        copy.start()
        started.append(copy)

    for step in range(2):
        for p in range(2):
            go(hop(p, (), near[(p + step) % 2]))
    go(lse_hop(0))
    go(lse_hop(1))
    lse_out[mine] = lse[:]
    parts[place.tp()] = att[:]
    for c in loads:
        c.wait()

    def add(slot, first=False):
        for i in range(2):
            start = place.coord("core", ("core",) if i else ()) * (na + nb)
            k = pl.ds(pl.multiple_of(slot * width, width), width)
            for buf, at, n in ((abuf, 0, na), (bbuf, na, nb)):
                cols = pl.ds(pl.multiple_of(start + at, 128), n)
                t = nn(parts[slot], buf[i, k, :])
                res[:, cols] = t + (x[:, cols].astype(F32) if first else res[:, cols])

    add(place.tp(), True)
    for p in range(2):
        hop(p, (), near[p]).wait_recv()
        go(hop(p, (near[p],), near[1 - p]))
    lse_hop(0).wait_recv()
    go(lse_hop(2))
    for p in (1, 0):
        hop(p, (), near[1 - p]).wait_recv()
        add(place.tp((near[1 - p],)))
    for p in range(2):
        hop(p, (near[p],), near[1 - p]).wait_recv()
    add(place.tp(near))
    h = res[:]
    act[:] = (h * lax.rsqrt(mean_row(h * h) + NORM_EPS) * gain[:]).astype(BF16)
    lse_hop(1).wait_recv()
    lse_hop(2).wait_recv()
    for c in started:
        c.wait_send()


def att_project(att, lse, x_all, pieces, gain):
    rows, width = att.shape
    dim = x_all.shape[1]
    dma = pltpu.SemaphoreType.DMA
    vmem = pl.BlockSpec(memory_space=pltpu.VMEM)
    hbm = pl.BlockSpec(memory_space=pl.ANY)
    return pl.pallas_call(
        att_kernel,
        out_shape=[jax.ShapeDtypeStruct((4, rows, width), BF16), jax.ShapeDtypeStruct((4,) + lse.shape, F32), jax.ShapeDtypeStruct((rows, dim), F32), jax.ShapeDtypeStruct((rows, dim), BF16)],
        in_specs=[vmem, vmem] + [hbm] * 5 + [vmem],
        out_specs=[vmem] * 4,
        scratch_shapes=[
            pltpu.VMEM((rows, dim), BF16), pltpu.VMEM((2,) + pieces[0].shape, BF16), pltpu.VMEM((2,) + pieces[1].shape, BF16),
            *[dma((n,)) for n in (6, 6, 3, 3, 5)],
        ],
        compiler_params=pltpu.CompilerParams(collective_id=1, has_side_effects=True, vmem_limit_bytes=48 * MIB),
        name="att_project",
    )(att, lse, x_all, *pieces, gain)


def weight_grad_kernel(info, *refs, pieces, splits):
    lhs = refs[:pieces]
    rhs = refs[pieces:2 * pieces]
    outs = refs[2 * pieces:]
    t = tn(lhs[0][:], rhs[0][:])
    for a, b in zip(lhs[1:], rhs[1:]):
        t += tn(a[:], b[:])
    width = t.shape[1] // splits
    for i, out in enumerate(outs):
        out[:] = t[:, i * width:(i + 1) * width]


def weight_grad(info, lhs, rhs, block=256, splits=1, rows=None):
    def spec(arr, p, cols, moving):
        if arr.ndim == 3:
            return pl.BlockSpec((None, arr.shape[1], cols), lambda i, info: (info[0] ^ p, 0, i if moving else 0))
        return pl.BlockSpec((arr.shape[0], cols), lambda i, info: (0, i if moving else 0))

    tokens = lhs[0].shape[-2]
    rows, dim = rows or lhs[0].shape[-1], rhs[0].shape[-1]
    n = len(lhs)
    width = dim // splits
    outs = pl.pallas_call(
        functools.partial(weight_grad_kernel, pieces=n, splits=splits),
        out_shape=[jax.ShapeDtypeStruct((rows, width), F32)] * splits,
        grid_spec=pltpu.PrefetchScalarGridSpec(
            num_scalar_prefetch=1,
            grid=(pl.cdiv(rows, block),),
            in_specs=[spec(a, p, block, True) for p, a in enumerate(lhs)] + [spec(b, p, dim, False) for p, b in enumerate(rhs)],
            out_specs=[pl.BlockSpec((block, width), lambda i, info: (i, 0))] * splits,
        ),
        compiler_params=pltpu.CompilerParams(vmem_limit_bytes=56 * MIB),
        cost_estimate=cost(2 * n * tokens * rows * dim, 4 * rows * dim + 2 * n * tokens * (rows + dim)),
        name="weight_grad",
    )(info, *lhs, *rhs)
    return outs if splits > 1 else outs[0]


def mlp_kernel(act, dy, wg, wu, wd, hidden, d_gate, d_up, *rest, limit):
    i = pl.program_id(0)
    block = wg.shape[0]
    left = limit - i * block
    row_ok = lax.broadcasted_iota(I32, (block, 1), 0) < left
    col_ok = lax.broadcasted_iota(I32, (1, block), 1) < left
    both = rest[-1]
    both[:block] = jnp.where(row_ok, wg[:], 0).astype(BF16)
    both[block:] = jnp.where(row_ok, wu[:], 0).astype(BF16)
    t = nt(act[:], both[:])
    gate, up = t[:, :block], t[:, block:]
    dh = jnp.where(col_ok, to_bf16(nt(dy[:], wd[:])), 0)
    sig = jax.nn.sigmoid(gate)
    hidden[:] = (gate * sig * up).astype(BF16)
    dg = (dh * up * sig * (1.0 + gate * (1.0 - sig))).astype(BF16)
    du = (dh * gate * sig).astype(BF16)
    d_gate[:] = dg
    d_up[:] = du
    if len(rest) > 1:
        grad, grads = rest[:2]
        grads[:, :block] = dg
        grads[:, block:] = du
        t = nn(grads[:], both[:])

        @pl.when(i == 0)
        def _():
            grad[:] = t

        @pl.when(i > 0)
        def _():
            grad[:] += t


def mlp_block(act, dy, wg, wu, wd, with_grad, block=256):
    rows, dim = act.shape
    limit = wg.shape[0]
    cols = pl.BlockSpec((rows, block), lambda i: (0, i))
    tile = pl.BlockSpec((block, dim), lambda i: (i, 0))
    whole = pl.BlockSpec((rows, dim), lambda i: (0, 0))
    return pl.pallas_call(
        functools.partial(mlp_kernel, limit=limit),
        out_shape=[jax.ShapeDtypeStruct((rows, pl.cdiv(limit, block) * block), BF16)] * 3 + [jax.ShapeDtypeStruct((rows, dim), F32)] * with_grad,
        grid=(pl.cdiv(limit, block),),
        in_specs=[whole, whole, tile, tile, tile],
        out_specs=[cols] * 3 + [whole] * with_grad,
        scratch_shapes=[pltpu.VMEM((rows, 2 * block), BF16)] * with_grad + [pltpu.VMEM((2 * block, dim), BF16)],
        compiler_params=pltpu.CompilerParams(vmem_limit_bytes=48 * MIB),
        cost_estimate=cost((6 + 4 * with_grad) * rows * dim * limit, 4 * dim * limit + 6 * rows * limit + 10 * rows * dim),
        name="mlp_block",
    )(act, dy, wg, wu, wd)


def zero_kernel(after, out, zeros, sem):
    zeros[:] = jnp.zeros_like(zeros)
    step = zeros.shape[0]
    count = out.shape[0] // step

    def send(i, c):
        pltpu.make_async_copy(zeros, out.at[pl.ds(pl.multiple_of(i * step, step), step), :], sem).start()
        return c

    def wait(i, c):
        pltpu.make_async_copy(zeros, out.at[pl.ds(0, step), :], sem).wait()
        return c

    lax.fori_loop(0, count, send, 0)
    lax.fori_loop(0, count, wait, 0)


def zero_rows(after, rows, dim, step=200):
    return pl.pallas_call(
        zero_kernel,
        out_shape=jax.ShapeDtypeStruct((rows, dim), F32),
        in_specs=[pl.BlockSpec(memory_space=pltpu.SMEM)],
        out_specs=pl.BlockSpec(memory_space=pl.ANY),
        scratch_shapes=[pltpu.VMEM((step, dim), F32), pltpu.SemaphoreType.DMA],
        compiler_params=pltpu.CompilerParams(vmem_limit_bytes=8 * MIB),
        cost_estimate=cost(rows * dim, 4 * rows * dim),
        name="zero_rows",
    )(after)


def scatter_kernel(order, sid, runs, bounds, rows, base_hbm, out_hbm, sums, row_sem, sum_sem):
    lo = bounds[0]
    hi = bounds[1]

    def one(c):
        p, singles, multi = c
        n = runs[p]
        t = order[p]
        single = n == 1

        @pl.when(single)
        def _():
            pltpu.make_async_copy(rows.at[pl.ds(t, 1), :], out_hbm.at[pl.ds(sid[p], 1), :], row_sem).start()

        @pl.when(jnp.logical_not(single))
        def _():
            def add(j, acc):
                return acc + rows[pl.ds(order[p + j], 1), :]

            sums[pl.ds(multi, 1), :] = lax.fori_loop(1, n, add, rows[pl.ds(t, 1), :])

        return p + n, singles + single.astype(I32), multi + 1 - single.astype(I32)

    _, singles, multi = lax.while_loop(lambda c: c[0] < hi, one, (lo, 0, 0))

    def two(c):
        p, k = c
        n = runs[p]

        @pl.when(n > 1)
        def _():
            pltpu.make_async_copy(sums.at[pl.ds(k, 1), :], out_hbm.at[pl.ds(sid[p], 1), :], sum_sem).start()

        return p + n, k + (n > 1).astype(I32)

    lax.while_loop(lambda c: c[0] < hi, two, (lo, 0))

    def wait(sem):
        def body(i, c):
            pltpu.make_async_copy(sums.at[pl.ds(0, 1), :], out_hbm.at[pl.ds(0, 1), :], sem).wait()
            return c

        return body

    lax.fori_loop(0, singles, wait(row_sem), 0)
    lax.fori_loop(0, multi, wait(sum_sem), 0)


def scatter_rows(order, sid, runs, bounds, grads, base, tokens):
    _, dim = grads.shape
    rows = base.shape[0]
    return pl.pallas_call(
        scatter_kernel,
        out_shape=jax.ShapeDtypeStruct((rows, dim), F32),
        grid_spec=pltpu.PrefetchScalarGridSpec(
            num_scalar_prefetch=4,
            grid=(),
            in_specs=[pl.BlockSpec(memory_space=pltpu.VMEM), pl.BlockSpec(memory_space=pl.ANY)],
            out_specs=pl.BlockSpec(memory_space=pl.ANY),
            scratch_shapes=[pltpu.VMEM((tokens // 2, dim), F32), pltpu.SemaphoreType.DMA, pltpu.SemaphoreType.DMA],
        ),
        input_output_aliases={5: 0},
        compiler_params=pltpu.CompilerParams(vmem_limit_bytes=40 * MIB),
        name="scatter_rows",
    )(order, sid, runs, bounds, grads, base)


def solution(mesh):
    cp_count = mesh.shape["cp"]
    tp_count = mesh.shape["tp"]
    both = ("cp", "tp")
    x_swap = [(i, i ^ 2) for i in range(cp_count)]
    core_swap = [(i, i ^ 1) for i in range(cp_count)]

    def compute(tokens, pos, doc_id, dy, table, w_q, w_k, w_v, w_o, w_gate, w_up, w_down, gain_one, gain_two, inv_freq):
        span = tokens.shape[0]
        total = span * cp_count
        part = span // tp_count
        rows, dim = table.shape
        head_dim = 2 * inv_freq.shape[0]
        heads = w_q.shape[1] // head_dim
        width = heads * head_dim
        tp_rank = lax.axis_index("tp")
        cp_rank = lax.axis_index("cp")
        core = cp_rank % 2
        gain_a = gain_one.astype(F32)
        gain_b = gain_two.astype(F32)

        barrier = lax.optimization_barrier
        join = lambda arr, axis: lax.all_gather(arr, axis, axis=0, tiled=True)
        add_up = lambda arr: lax.psum_scatter(arr, "tp", scatter_dimension=0, tiled=True)
        swap = lambda arr, pairs, axis="cp": lax.ppermute(arr, axis, pairs)
        local_ids = tokens - tp_rank * rows
        owned = (local_ids >= 0) & (local_ids < rows)
        safe_ids = jnp.where(owned, local_ids, jnp.arange(span) * (rows // span))
        picked = jnp.where(owned[:, None], jnp.take(table, safe_ids, axis=0), 0).astype(BF16)
        half = dim // 2
        near = 256
        wo_half = lax.dynamic_slice_in_dim(w_o, core * half, half, 1)
        wo_near = join(wo_half[:, :near], "tp")
        angle = pos.astype(F32)[:, None] * inv_freq[None, :]
        side_f = jnp.concatenate([jnp.cos(angle), jnp.sin(angle)], axis=1)
        side_i = jnp.stack([tokens, doc_id] * 4)
        x_all, x_slice, angles, ints = embed_gather(picked.reshape(tp_count, part, dim), side_f, side_i)
        angles = angles.reshape(total, head_dim)
        tok_all = ints[:, 0, :].reshape(total)
        doc_all = ints[:, 1, :].reshape(total)
        wo_far = barrier((wo_half[:, near:], x_all))[0]
        wo_rest = join(wo_far, "tp")
        wo_pieces = (wo_near, wo_rest, swap(wo_near, core_swap), swap(wo_rest, core_swap))

        dy_x = swap(barrier((dy, x_all))[0], x_swap)
        act_a, query, key, value, w_qkv = project_qkv(x_all, gain_a[None, :], w_q, w_k, w_v, angles)

        blk = span // 2
        blocks = total // blk
        doc_col = doc_all[:, None]
        doc_row = doc_all.reshape(blocks, 1, blk)
        docs = doc_all.reshape(blocks, blk)
        docs = jnp.stack([docs[:, 0], docs[:, -1]], axis=1).reshape(2 * blocks)
        info = jnp.concatenate([jnp.stack([cp_rank, core]), docs]).astype(I32)
        attended, lse = attend(info, query, key, value, doc_col, doc_row, head_dim, blk)

        gain_row = gain_b[None, :]
        att_parts, lse_all, residual, act_b = att_project(attended, lse, x_all, wo_pieces, gain_row)
        lse_all = lse_all.reshape(total, 8)
        att_x = swap(att_parts, x_swap)

        wg, wu = w_gate.T, w_up.T
        ffn = wg.shape[0]
        hidden, d_gate, d_up, d_act_b = mlp_block(act_b, dy, wg, wu, w_down, True)
        d_act_b = add_up(d_act_b)
        act_x = out_proj(info, 2, x_all, att_x, wo_pieces, gain_row)[1]
        hidden_x, d_gate_x, d_up_x = mlp_block(act_x, dy_x, wg, wu, w_down, False)
        d_act_b, hidden_x, d_gate_x, d_up_x = barrier((d_act_b, hidden_x, d_gate_x, d_up_x))
        d_act_b = to_bf16(d_act_b)
        acts, dys, hiddens, d_gates, d_ups = [(a, swap(a, core_swap), b, swap(b, core_swap)) for a, b in (
            (act_b, act_x), (dy, dy_x), (hidden, hidden_x), (d_gate, d_gate_x), (d_up, d_up_x))]
        heads_x = lax.dynamic_index_in_dim(att_x, tp_rank, 0, keepdims=False)
        head_parts = (attended, swap(attended, core_swap), heads_x, swap(heads_x, core_swap))
        att_heads = jnp.zeros((total, width), BF16)
        for k, piece in enumerate(head_parts):
            att_heads = lax.dynamic_update_slice_in_dim(att_heads, piece, (cp_rank ^ k) * span, 0)
        grad_down = weight_grad(info, hiddens, dys, rows=ffn)
        grad_gate = weight_grad(info, d_gates, acts, rows=ffn)
        grad_up = weight_grad(info, d_ups, acts, rows=ffn)

        def mine(arr):
            return lax.dynamic_slice_in_dim(arr, tp_rank * part, part, 0)

        res_part = mine(residual)
        normed_b, inv_b = rms_stats(res_part)
        grad_gain_b = jnp.sum(d_act_b * normed_b, axis=0)
        d_resid = mine(dy).astype(F32) + rms_back(d_act_b * gain_b, normed_b, inv_b)
        d_resid_all = join(d_resid.astype(BF16), both)
        out_part = nn(hidden[:, :ffn], w_down)
        d_resid_all, grad_down, att_heads, out_part = barrier((d_resid_all, grad_down, att_heads, out_part))
        out_slice = add_up(out_part)
        out_slice = (res_part + out_slice).astype(BF16)

        d_att = nt(d_resid_all, w_o)
        d_att_b = d_att.astype(BF16)
        head_of = (jnp.arange(width)[None, :] // head_dim == jnp.arange(8)[:, None]).astype(F32)
        prod = att_heads.astype(F32) * d_att_b.astype(F32)
        delta = lax.dot_general(head_of, prod, (((1,), (1,)), ((), ())), precision=lax.Precision.HIGHEST, preferred_element_type=F32)

        def by_block(arr):
            return jnp.transpose(arr.reshape(8, blocks, blk), (1, 0, 2))

        dqkv = attend_back(info, query, key, value, d_att_b, doc_col, doc_row, lse_all, by_block(lse_all.T), delta.T, by_block(delta), angles, blk)
        d_act_a = nt(dqkv, w_qkv)
        d_act_a, out_slice = barrier((d_act_a, out_slice))
        d_act_a = add_up(d_act_a)
        dqkv_x = swap(dqkv, x_swap)
        dqkvs = (dqkv, swap(dqkv, core_swap), dqkv_x, swap(dqkv_x, core_swap))
        grad_out = weight_grad(info, head_parts, [d_resid_all.reshape(cp_count, span, dim)] * 4)
        d_act_a, dqkv_x, grad_out, grad_up = barrier((d_act_a, dqkv_x, grad_out, grad_up))
        d_act_a = to_bf16(d_act_a)
        normed_a, inv_a = rms_stats(x_slice.astype(F32))
        grad_gain_a = jnp.sum(d_act_a * normed_a, axis=0)
        d_embed = d_resid + rms_back(d_act_a * gain_a, normed_a, inv_a)
        payload = jnp.concatenate([d_embed, jnp.stack([grad_gain_a, grad_gain_b] * 4)])
        gathered = join(payload, both)
        grad_qkv = weight_grad(info, [act_a.reshape(cp_count, span, dim)] * 4, dqkvs, splits=3)
        slot_ids = jnp.arange(total, dtype=I32)
        before = (tok_all[None, :] < tok_all[:, None]) | ((tok_all[None, :] == tok_all[:, None]) & (slot_ids[None, :] < slot_ids[:, None]))
        rank = jnp.sum(before.astype(I32), axis=1)
        count = jnp.sum((tok_all[None, :] == tok_all[:, None]).astype(I32), axis=1)
        at_rank = rank[None, :] == slot_ids[:, None]
        runs = jnp.sum(jnp.where(at_rank, count[None, :], 0), axis=1)
        order = jnp.sum(jnp.where(at_rank, slot_ids[None, :], 0), axis=1)
        sid = jnp.sum(jnp.where(at_rank, tok_all[None, :], 0), axis=1) - tp_rank * rows
        order = order + 8 * (order // part)
        bounds = jnp.stack([jnp.sum((tok_all < tp_rank * rows).astype(I32)), jnp.sum((tok_all < (tp_rank + 1) * rows).astype(I32))])
        base = zero_rows(barrier((bounds, d_act_a))[0], rows, dim)
        gathered, grad_qkv, grad_gate, runs, order, sid, bounds, base = barrier((gathered, grad_qkv, grad_gate, runs, order, sid, bounds, base))
        out_slice = barrier((out_slice, gathered))[0]
        layer_out = join(out_slice, "tp")
        gain_grads = jnp.sum(gathered.reshape(cp_count * tp_count, part + 8, dim)[:, part:part + 2], axis=0)
        grad_table = scatter_rows(order, sid, runs, bounds, gathered, base, total)
        return (layer_out, grad_table, *grad_qkv, grad_out, grad_gate.T, grad_up.T, grad_down, gain_grads[0], gain_grads[1])

    col_spec = P(None, "tp")
    row_spec = P("tp")
    tok_spec = P("cp")
    rep_spec = P()
    in_specs = (tok_spec, tok_spec, tok_spec, P("cp"), row_spec, col_spec, col_spec, col_spec, row_spec, col_spec, col_spec, row_spec, rep_spec, rep_spec, rep_spec)
    out_specs = (P("cp"), row_spec, col_spec, col_spec, col_spec, row_spec, col_spec, col_spec, row_spec, rep_spec, rep_spec)
    return jax.shard_map(compute, mesh=mesh, in_specs=in_specs, out_specs=out_specs, check_vma=False)
```

```python
import functools
import jax
import jax.numpy as jnp
from jax import lax
from jax.experimental import pallas as pl
from jax.experimental.pallas import tpu as pltpu
from jax.sharding import PartitionSpec as P

NORM_EPS = 1e-5
NEG_BIG = -1e30
MIB = 2 ** 20
F32 = jnp.float32
BF16 = jnp.bfloat16
I32 = jnp.int32


def rms_stats(feats):
    inv_rms = lax.rsqrt(mean_row(feats * feats) + NORM_EPS)
    return feats * inv_rms, inv_rms


def rms_back(d_normed, normed, inv_rms):
    return inv_rms * (d_normed - normed * mean_row(d_normed * normed))


def to_bf16(feats):
    return feats.astype(BF16).astype(F32)


def contract(a, b, ca, cb):
    return lax.dot_general(a, b, (((ca,), (cb,)), ((), ())), preferred_element_type=F32)


def row_sum(t):
    return jnp.sum(t, axis=1, keepdims=True)


def mean_row(t):
    return row_sum(t) / t.shape[1]


def whole(a):
    return pl.BlockSpec(a.shape, lambda *i: (0,) * a.ndim)


def cost(flops, moved):
    return pl.CostEstimate(flops=flops, bytes_accessed=moved, transcendentals=0)


def nn(a, b):
    return contract(a, b, 1, 0)


def nt(a, b):
    return contract(a, b, 1, 1)


def tn(a, b):
    return contract(a, b, 0, 0)


DIMS = ("x", "y", "z")


class Place:
    def __init__(self):
        tp = lax.axis_index("tp")
        cp = lax.axis_index("cp")
        self.at = {"x": cp // 2, "core": cp % 2, "z": tp // 2, "y": tp % 2}

    def coord(self, dim, flip):
        return 1 - self.at[dim] if dim in flip else self.at[dim]

    def tp(self, flip=()):
        return self.coord("z", flip) * 2 + self.coord("y", flip)

    def cp(self, flip=()):
        return self.coord("x", flip) * 2 + self.coord("core", flip)

    def device(self, flip):
        return {"tp": self.tp(flip), "cp": self.cp(flip)}

    def slot(self, flip=()):
        return self.cp(flip) * 4 + self.tp(flip)

    def meet(self, dims):
        barrier = pltpu.get_barrier_semaphore()
        for d in dims:
            pl.semaphore_signal(barrier, inc=1, device_id=self.device((d,)), device_id_type=MESH)
        pl.semaphore_wait(barrier, len(dims))


MESH = pl.DeviceIdType.MESH
ORDERS = (("x", "y", "z"), ("y", "z", "x"), ("z", "x", "y"))
FLIPS = tuple(tuple(d for i, d in enumerate(DIMS) if n >> i & 1) for n in range(8))


def flip_code(flip):
    return sum(1 << DIMS.index(d) for d in flip)


def column_parts(width, count):
    tiles = width // 128
    sizes = [(tiles // count + (i < tiles % count)) * 128 for i in range(count)]
    return [(sum(sizes[:i]), n) for i, n in enumerate(sizes)]


class Gather:
    def __init__(self, place, buf, send, recv, core_send, core_recv):
        self.place, self.buf, self.send, self.recv, self.core_send, self.core_recv = place, buf, send, recv, core_send, core_recv
        self.parts = column_parts(buf.shape[2], 3)
        self.started = []

    def view(self, part, flip):
        start, size = self.parts[part]
        return self.buf.at[self.place.slot(flip), :, pl.ds(start, size)]

    def hop(self, part, flip, dim):
        there = tuple(d for d in DIMS if (d in flip) != (d == dim))
        index = part * 7 + flip_code(there) - 1
        ref = self.view(part, flip)
        return pltpu.make_async_remote_copy(src_ref=ref, dst_ref=ref, send_sem=self.send.at[index], recv_sem=self.recv.at[index], device_id=self.place.device((dim,)), device_id_type=MESH)

    def core_hop(self, part, flip):
        index = part * 8 + flip_code(flip)
        ref = self.view(part, flip)
        return pltpu.make_async_remote_copy(src_ref=ref, dst_ref=ref, send_sem=self.core_send.at[index], recv_sem=self.core_recv.at[index], device_id=self.place.device(("core",)), device_id_type=MESH)

    def go(self, copy):
        copy.start()
        self.started.append(copy)

    def wait(self, part, flip):
        order = ORDERS[part]
        last = max(order.index(d) for d in flip)
        came = tuple(d for d in flip if d != order[last])
        self.hop(part, came, order[last]).wait_recv()
        for dim in order[last + 1:]:
            self.go(self.hop(part, flip, dim))
        self.go(self.core_hop(part, flip))

    def run(self):
        for step in range(3):
            for part, order in enumerate(ORDERS):
                self.go(self.hop(part, (), order[step]))
        for part in range(3):
            self.go(self.core_hop(part, ()))
        for step in range(3):
            for flip in FLIPS[1:]:
                for part, order in enumerate(ORDERS):
                    if max(order.index(d) for d in flip) == step and len(flip) == 1:
                        self.wait(part, flip)
            for flip in FLIPS[1:]:
                for part, order in enumerate(ORDERS):
                    if max(order.index(d) for d in flip) == step and len(flip) > 1:
                        self.wait(part, flip)

    def finish(self, out, out_sem):
        rows = self.buf.shape[1]
        copies = []

        def store(flip):
            slot = self.place.slot(flip)
            c = pltpu.make_async_copy(self.buf.at[slot], out.at[pl.ds(slot * rows, rows), :], out_sem.at[len(copies)])
            c.start()
            copies.append(c)

        for flip in FLIPS:
            store(flip)
        for flip in FLIPS:
            other = flip + ("core",)
            for part in range(3):
                start, size = self.parts[part]
                ref = self.buf.at[self.place.slot(other), :, pl.ds(start, size)]
                index = part * 8 + flip_code(flip)
                pltpu.make_async_remote_copy(src_ref=ref, dst_ref=ref, send_sem=self.core_send.at[index], recv_sem=self.core_recv.at[index], device_id=self.place.device(("core",)), device_id_type=MESH).wait_recv()
            store(other)
        for c in self.started:
            c.wait_send()
        for c in copies:
            c.wait()


def embed_kernel(picked, side_f, side_i, out, slice_out, all_f, all_i, buf, r1, r2, tmp, send, recv, core_send, core_recv, out_sem, rs_send, rs_recv, side_send, side_recv, slice_sem):
    place = Place()
    place.meet(("x", "y", "z", "core"))
    half = buf.shape[2] // 2
    near = ("y", "z")

    sides = ((side_f, all_f), (side_i, all_i))
    started = []

    def side_hop(i, step):
        src, dst = sides[i]
        if step == 0:
            src_ref, slot, dim = src, place.cp(), "x"
        elif step == 1:
            src_ref, slot, dim = src, place.cp(), "core"
        else:
            src_ref, slot, dim = dst.at[place.cp(("x",))], place.cp(("x",)), "core"
        return pltpu.make_async_remote_copy(src_ref=src_ref, dst_ref=dst.at[slot], send_sem=side_send.at[i, step], recv_sem=side_recv.at[i, step], device_id=place.device((dim,)), device_id_type=MESH)

    def first(h, k):
        a, b = near[h], near[1 - h]
        target = place.tp((a,)) if k == 0 else place.tp((a, b))
        cols = pl.ds(h * half, half)
        return pltpu.make_async_remote_copy(src_ref=picked.at[target, :, cols], dst_ref=r1.at[h, k], send_sem=rs_send.at[h, k], recv_sem=rs_recv.at[h, k], device_id=place.device((a,)), device_id_type=MESH)

    def second(h):
        return pltpu.make_async_remote_copy(src_ref=tmp.at[h], dst_ref=r2.at[h], send_sem=rs_send.at[h, 2], recv_sem=rs_recv.at[h, 2], device_id=place.device((near[1 - h],)), device_id_type=MESH)

    def go(copy):
        copy.start()
        started.append(copy)

    for k in (1, 0):
        for h in range(2):
            go(first(h, k))
    for i in range(2):
        go(side_hop(i, 0))
        go(side_hop(i, 1))
        all_i_or_f = sides[i][1]
        all_i_or_f[place.cp()] = sides[i][0][:]
    for h in range(2):
        cols = slice(h * half, (h + 1) * half)
        first(h, 1).wait_recv()
        tmp[h] = picked[place.tp((near[1 - h],)), :, cols] + r1[h, 1]
        go(second(h))
    for i in range(2):
        side_hop(i, 0).wait_recv()
        go(side_hop(i, 2))
    mine = place.slot()
    for h in range(2):
        cols = slice(h * half, (h + 1) * half)
        first(h, 0).wait_recv()
        part = picked[place.tp(), :, cols] + r1[h, 0]
        second(h).wait_recv()
        buf[mine, :, cols] = part + r2[h]
    gather = Gather(place, buf, send, recv, core_send, core_recv)
    gather.run()
    keep = pltpu.make_async_copy(buf.at[mine], slice_out, slice_sem)
    keep.start()
    gather.finish(out, out_sem)
    keep.wait()
    for i in range(2):
        side_hop(i, 1).wait_recv()
        side_hop(i, 2).wait_recv()
    for c in started:
        c.wait_send()


def embed_gather(picked, side_f, side_i):
    _, rows, dim = picked.shape
    half = dim // 2
    dma = pltpu.SemaphoreType.DMA
    vmem = pl.BlockSpec(memory_space=pltpu.VMEM)
    hbm = pl.BlockSpec(memory_space=pl.ANY)
    return pl.pallas_call(
        embed_kernel,
        out_shape=[
            jax.ShapeDtypeStruct((16 * rows, dim), BF16),
            jax.ShapeDtypeStruct((rows, dim), BF16),
            jax.ShapeDtypeStruct((4,) + side_f.shape, F32),
            jax.ShapeDtypeStruct((4,) + side_i.shape, I32),
        ],
        in_specs=[vmem, vmem, vmem],
        out_specs=[hbm, hbm, vmem, vmem],
        scratch_shapes=[
            pltpu.VMEM((16, rows, dim), BF16),
            pltpu.VMEM((2, 2, rows, half), BF16),
            pltpu.VMEM((2, rows, half), BF16),
            pltpu.VMEM((2, rows, half), BF16),
            dma((21,)), dma((21,)), dma((24,)), dma((24,)), dma((16,)),
            *[dma((2, 3))] * 4, dma,
        ],
        compiler_params=pltpu.CompilerParams(collective_id=0, has_side_effects=True, vmem_limit_bytes=40 * MIB),
        name="embed_gather",
    )(picked, side_f, side_i)


def slot_block(j):
    return jnp.where(j < 4, 2 * j, 15 - 2 * j)


def unpack_angles(packed):
    turned = pltpu.roll(packed, packed.shape[1] // 2, 1)
    low = lax.broadcasted_iota(I32, packed.shape, 1) < packed.shape[1] // 2
    return jnp.where(low, packed, turned), jnp.where(low, -turned, packed)


def qkv_kernel(x, gain, wq, wk, wv, angles, act, q, k, v, wide, *, head_dim):
    width = wq.shape[1]

    @pl.when(pl.program_id(0) == 0)
    def _():
        for i, w in enumerate((wq, wk, wv)):
            wide[:, i * width:(i + 1) * width] = w[:]

    feats = x[:].astype(F32)
    inv = lax.rsqrt(mean_row(feats * feats) + NORM_EPS)
    a = (feats * inv * gain[:]).astype(BF16)
    act[:] = a
    t = nn(a, wide[:])
    cos, sin = unpack_angles(angles[:])
    for i, out in enumerate((q, k, v)):
        for h in range(width // head_dim):
            th = t[:, i * width + h * head_dim:i * width + (h + 1) * head_dim]
            if i < 2:
                th = th * cos + pltpu.roll(th, head_dim // 2, 1) * sin
            out[:, h * head_dim:(h + 1) * head_dim] = th.astype(BF16)


def project_qkv(x_all, gain, wq, wk, wv, angles, block=512):
    total, dim = x_all.shape
    width = wq.shape[1]
    head_dim = angles.shape[1]
    rows = lambda n: pl.BlockSpec((block, n), lambda i: (i, 0))
    whole = lambda a: pl.BlockSpec(a.shape, lambda i: (0, 0), pipeline_mode=pl.Buffered(1))
    return pl.pallas_call(
        functools.partial(qkv_kernel, head_dim=head_dim),
        out_shape=[jax.ShapeDtypeStruct((total, n), BF16) for n in (dim, width, width, width)] + [jax.ShapeDtypeStruct((dim, 3 * width), BF16)],
        grid=(total // block,),
        in_specs=[rows(dim), whole(gain), whole(wq), whole(wk), whole(wv), rows(head_dim)],
        out_specs=[rows(dim), rows(width), rows(width), rows(width), pl.BlockSpec((dim, 3 * width), lambda i: (0, 0), pipeline_mode=pl.Buffered(1))],
        compiler_params=pltpu.CompilerParams(vmem_limit_bytes=60 * MIB),
        cost_estimate=cost(6 * total * dim * width, 4 * total * dim + 6 * dim * width + 6 * total * width),
        name="project_qkv",
    )(x_all, gain, wq, wk, wv, angles)


def block_range(info, ids, i, blocks):
    r = info[0]
    blk = ids.shape[2] // 2
    b = jnp.where(i == 0, r, blocks - 1 - r)

    def docs(shard, half):
        return ids[shard, 1, half * blk], ids[shard, 1, half * blk + blk - 1]

    first, last = docs(r, i)
    jmin, imax = 0, -1
    for j in range(blocks):
        begin, end = docs(min(j, blocks - 1 - j), int(j >= blocks // 2))
        jmin = jmin + (end < first).astype(I32)
        imax = imax + (begin <= last).astype(I32)
    return b, jmin, imax


def attend_kernel(info, ids, q, k, v, doc_col, doc_row, out, lse, sc, *, heads, head_dim, scale):
    blk = q.shape[0]
    b, jmin, _ = block_range(info, ids, pl.program_id(0), doc_row.shape[0])
    row_n = lax.broadcasted_iota(I32, (blk, blk), 0) + b * blk
    col_n = lax.broadcasted_iota(I32, (blk, blk), 1)

    def score(j, peaks):
        sb = slot_block(j)
        off = pl.multiple_of(sb * blk, blk)
        allowed = (doc_col[:] == doc_row[sb]) & (col_n + j * blk <= row_n)
        new = []
        for h in range(heads):
            cols = slice(h * head_dim, (h + 1) * head_dim)
            s = nt(q[:, cols], k[pl.ds(off, blk), cols]) * scale
            s = jnp.where(allowed, s, NEG_BIG)
            sc[j, h] = s
            new.append(jnp.maximum(peaks[h], jnp.max(s, axis=1, keepdims=True)))
        return tuple(new)

    peaks = lax.fori_loop(jmin, b + 1, score, tuple(jnp.full((blk, 1), NEG_BIG, F32) for _ in range(heads)))

    def weigh(j, sums):
        new = []
        for h in range(heads):
            p = jnp.exp(sc[j, h] - peaks[h])
            sc[j, h] = p
            new.append(sums[h] + row_sum(p))
        return tuple(new)

    sums = lax.fori_loop(jmin, b + 1, weigh, tuple(jnp.zeros((blk, 1), F32) for _ in range(heads)))
    inv = tuple(1.0 / t for t in sums)
    for h in range(heads):
        lse[:, h:h + 1] = peaks[h] + jnp.log(sums[h])

    def mix(j, acc):
        off = pl.multiple_of(slot_block(j) * blk, blk)
        new = []
        for h in range(heads):
            cols = slice(h * head_dim, (h + 1) * head_dim)
            new.append(acc[h] + nn((sc[j, h] * inv[h]).astype(BF16), v[pl.ds(off, blk), cols]))
        return tuple(new)

    acc = lax.fori_loop(jmin, b + 1, mix, tuple(jnp.zeros((blk, head_dim), F32) for _ in range(heads)))
    for h in range(heads):
        out[:, h * head_dim:(h + 1) * head_dim] = acc[h].astype(BF16)


def attend(info, ids, q, k, v, doc_col, doc_row, head_dim, blk):
    total, width = k.shape
    heads = width // head_dim
    mine = lambda n: pl.BlockSpec((blk, n), lambda i, info, ids: (2 * info[0] + i, 0))
    return pl.pallas_call(
        functools.partial(attend_kernel, heads=heads, head_dim=head_dim, scale=head_dim ** -0.5),
        out_shape=[jax.ShapeDtypeStruct((2 * blk, width), BF16), jax.ShapeDtypeStruct((2 * blk, 8), F32)],
        grid_spec=pltpu.PrefetchScalarGridSpec(
            num_scalar_prefetch=2,
            grid=(2,),
            in_specs=[mine(width), whole(k), whole(v), mine(1), whole(doc_row)],
            out_specs=[pl.BlockSpec((blk, width), lambda i, info, ids: (i, 0)), pl.BlockSpec((blk, 8), lambda i, info, ids: (i, 0))],
            scratch_shapes=[pltpu.VMEM((total // blk, heads, blk, blk), F32)],
        ),
        compiler_params=pltpu.CompilerParams(vmem_limit_bytes=40 * MIB),
        cost_estimate=cost(4 * 2 * blk * total * width, 8 * total * width),
        name="attend",
    )(info, ids, q, k, v, doc_col, doc_row)


def attend_back_kernel(info, ids, q, k, v, do, doc_col, doc_row, lse_col, lse_row, del_col, del_row, angles, out, acc, *, heads, head_dim, scale):
    blk = angles.shape[0]
    width = heads * head_dim
    i = pl.program_id(0)
    b, jmin, imax = block_range(info, ids, i, doc_row.shape[0])
    me = pl.multiple_of((2 * info[0] + i) * blk, blk)
    mine = pl.ds(me, blk)
    iota_r = lax.broadcasted_iota(I32, (blk, blk), 0)
    iota_c = lax.broadcasted_iota(I32, (blk, blk), 1)
    acc[:] = jnp.zeros_like(acc)
    spans = [slice(h * head_dim, (h + 1) * head_dim) for h in range(heads)]

    def for_query(j, c):
        sb = slot_block(j)
        there = pl.ds(pl.multiple_of(sb * blk, blk), blk)
        allowed = (doc_col[mine, :] == doc_row[sb]) & (iota_c + j * blk <= iota_r + b * blk)
        for h, cols in enumerate(spans):
            s = jnp.where(allowed, nt(q[mine, cols], k[there, cols]) * scale, NEG_BIG)
            p = jnp.exp(s - lse_col[mine, h:h + 1])
            dp = to_bf16(nt(do[mine, cols], v[there, cols]))
            ds = (p * (dp - del_col[mine, h:h + 1]) * scale).astype(BF16)
            acc[0, :, cols] += nn(ds, k[there, cols])
        return c

    lax.fori_loop(jmin, b + 1, for_query, 0)

    def for_key(j, c):
        sb = slot_block(j)
        there = pl.ds(pl.multiple_of(sb * blk, blk), blk)
        allowed = (doc_col[mine, :] == doc_row[sb]) & (iota_r + b * blk <= iota_c + j * blk)
        for h, cols in enumerate(spans):
            s = jnp.where(allowed, nt(k[mine, cols], q[there, cols]) * scale, NEG_BIG)
            p = jnp.exp(s - lse_row[sb, h:h + 1, :])
            dp = to_bf16(nt(v[mine, cols], do[there, cols]))
            ds = (p * (dp - del_row[sb, h:h + 1, :]) * scale).astype(BF16)
            acc[2, :, cols] += nn(p.astype(BF16), do[there, cols])
            acc[1, :, cols] += nn(ds, q[there, cols])
        return c

    lax.fori_loop(b, imax + 1, for_key, 0)
    cos, sin = unpack_angles(angles[:])
    for part in range(3):
        for h, cols in enumerate(spans):
            t = acc[part, :, cols]
            if part < 2:
                t = to_bf16(t)
                t = t * cos - pltpu.roll(t, head_dim // 2, 1) * sin
            out[:, part * width + h * head_dim:part * width + (h + 1) * head_dim] = t.astype(BF16)


def attend_back(info, ids, q, k, v, do, doc_col, doc_row, lse_col, lse_row, del_col, del_row, angles, blk):
    total, width = k.shape
    head_dim = angles.shape[1]
    heads = width // head_dim
    mine = lambda n: pl.BlockSpec((blk, n), lambda i, info, ids: (2 * info[0] + i, 0))
    arrays = (q, k, v, do, doc_col, doc_row, lse_col, lse_row, del_col, del_row)
    return pl.pallas_call(
        functools.partial(attend_back_kernel, heads=heads, head_dim=head_dim, scale=head_dim ** -0.5),
        out_shape=jax.ShapeDtypeStruct((2 * blk, 3 * width), BF16),
        grid_spec=pltpu.PrefetchScalarGridSpec(
            num_scalar_prefetch=2,
            grid=(2,),
            in_specs=[whole(a) for a in arrays] + [mine(head_dim)],
            out_specs=pl.BlockSpec((blk, 3 * width), lambda i, info, ids: (i, 0)),
            scratch_shapes=[pltpu.VMEM((3, blk, width), F32)],
        ),
        compiler_params=pltpu.CompilerParams(vmem_limit_bytes=48 * MIB),
        cost_estimate=cost(14 * 2 * blk * total * width // 2, 12 * total * width),
        name="attend_back",
    )(info, ids, *arrays, angles)


def out_proj_kernel(info, x, att, a0, b0, a1, b1, gain, res, act, wide, abuf, bbuf, sems):
    tp, _, width = att.shape
    na, nb = a0.shape[1], b0.shape[1]
    sets = ((a0, b0), (a1, b1))

    def copies(i):
        return (pltpu.make_async_copy(sets[i][0], abuf.at[i], sems.at[i, 0]), pltpu.make_async_copy(sets[i][1], bbuf.at[i], sems.at[i, 1]))

    for i in range(2):
        for c in copies(i):
            c.start()
    for t in range(tp):
        wide[:, t * width:(t + 1) * width] = att[t]
    for i in range(2):
        start = (info[1] ^ i) * (na + nb)
        first, second = copies(i)
        first.wait()
        cols = pl.ds(pl.multiple_of(start, 128), na)
        res[:, cols] = x[:, cols].astype(F32) + nn(wide[:], abuf[i])
        second.wait()
        cols = pl.ds(pl.multiple_of(start + na, 128), nb)
        res[:, cols] = x[:, cols].astype(F32) + nn(wide[:], bbuf[i])
    h = res[:]
    inv = lax.rsqrt(mean_row(h * h) + NORM_EPS)
    act[:] = (h * inv * gain[:]).astype(BF16)


def out_proj(info, flip, x_all, att, pieces, gain):
    _, rows, _ = att.shape
    dim = x_all.shape[1]
    full = pl.BlockSpec((rows, dim), lambda i, info: (0, 0))
    return pl.pallas_call(
        out_proj_kernel,
        out_shape=[jax.ShapeDtypeStruct((rows, dim), F32), jax.ShapeDtypeStruct((rows, dim), BF16)],
        grid_spec=pltpu.PrefetchScalarGridSpec(
            num_scalar_prefetch=1,
            grid=(1,),
            in_specs=[pl.BlockSpec((rows, dim), lambda i, info: (info[0] ^ flip, 0)), whole(att)] + [pl.BlockSpec(memory_space=pl.ANY)] * 4 + [whole(gain)],
            out_specs=[full, full],
            scratch_shapes=[pltpu.VMEM((rows, dim), BF16), pltpu.VMEM((2,) + pieces[0].shape, BF16), pltpu.VMEM((2,) + pieces[1].shape, BF16), pltpu.SemaphoreType.DMA((2, 2))],
        ),
        compiler_params=pltpu.CompilerParams(vmem_limit_bytes=56 * MIB),
        cost_estimate=cost(2 * rows * dim * dim, 2 * dim * dim + 10 * rows * dim),
        name="out_proj",
    )(info, x_all, att, *pieces, gain)


def att_kernel(att, lse, x_all, a0, b0, gain, parts, lse_out, res, act, a1, b1, x, abuf, bbuf, send, recv, lse_send, lse_recv, load, swap_send, swap_recv):
    place = Place()
    rows, width = att.shape
    na, nb = a0.shape[1], b0.shape[1]
    mine = place.cp()
    loads = [pltpu.make_async_copy(x_all.at[pl.ds(mine * rows, rows), :], x, load.at[4])]
    for i, (src, dst) in enumerate(((a0, abuf.at[0]), (b0, bbuf.at[0]), (a1, abuf.at[1]), (b1, bbuf.at[1]))):
        loads.append(pltpu.make_async_copy(src, dst, load.at[i]))
    early, late = loads[:3], loads[3:]
    for c in early:
        c.start()
    place.meet(("y", "z", "x", "core"))
    started = []
    near = ("y", "z")
    spans = column_parts(width, 2)

    def hop(p, flip, dim):
        there = tuple(d for d in near if (d in flip) != (d == dim))
        index = p * 3 + (there == ("y",)) + 2 * (there == ("z",))
        start, size = spans[p]
        cols = pl.ds(start, size)
        slot = place.tp(flip)
        src = parts.at[slot, :, cols] if flip else att.at[:, cols]
        return pltpu.make_async_remote_copy(src_ref=src, dst_ref=parts.at[slot, :, cols], send_sem=send.at[index], recv_sem=recv.at[index], device_id=place.device((dim,)), device_id_type=MESH)

    def lse_hop(step):
        src, slot, dim = ((lse, mine, "x"), (lse, mine, "core"), (lse_out.at[place.cp(("x",))], place.cp(("x",)), "core"))[step]
        return pltpu.make_async_remote_copy(src_ref=src, dst_ref=lse_out.at[slot], send_sem=lse_send.at[step], recv_sem=lse_recv.at[step], device_id=place.device((dim,)), device_id_type=MESH)

    def go(copy):
        copy.start()
        started.append(copy)

    swaps = [pltpu.make_async_remote_copy(src_ref=src, dst_ref=dst, send_sem=swap_send.at[i], recv_sem=swap_recv.at[i], device_id=place.device(("core",)), device_id_type=MESH) for i, (src, dst) in enumerate(((a0, a1), (b0, b1)))]
    for step in range(2):
        for p in range(2):
            go(hop(p, (), near[(p + step) % 2]))
    for c in swaps:
        go(c)
    go(lse_hop(0))
    go(lse_hop(1))
    lse_out[mine] = lse[:]
    parts[place.tp()] = att[:]
    for c in early:
        c.wait()

    def add(slot, halves=(0, 1), first=False):
        for i in halves:
            start = place.coord("core", ("core",) if i else ()) * (na + nb)
            k = pl.ds(pl.multiple_of(slot * width, width), width)
            for buf, at, n in ((abuf, 0, na), (bbuf, na, nb)):
                cols = pl.ds(pl.multiple_of(start + at, 128), n)
                t = nn(parts[slot], buf[i, k, :])
                res[:, cols] = t + (x[:, cols].astype(F32) if first else res[:, cols])

    add(place.tp(), (0,), True)
    for c in swaps:
        c.wait_recv()
    for c in late:
        c.start()
    for p in range(2):
        hop(p, (), near[p]).wait_recv()
        go(hop(p, (near[p],), near[1 - p]))
    lse_hop(0).wait_recv()
    go(lse_hop(2))
    for c in late:
        c.wait()
    add(place.tp(), (1,), True)
    for p in (1, 0):
        hop(p, (), near[1 - p]).wait_recv()
        add(place.tp((near[1 - p],)))
    for p in range(2):
        hop(p, (near[p],), near[1 - p]).wait_recv()
    add(place.tp(near))
    h = res[:]
    act[:] = (h * lax.rsqrt(mean_row(h * h) + NORM_EPS) * gain[:]).astype(BF16)
    lse_hop(1).wait_recv()
    lse_hop(2).wait_recv()
    for c in started:
        c.wait_send()


def att_project(att, lse, x_all, pieces, gain):
    rows, width = att.shape
    dim = x_all.shape[1]
    dma = pltpu.SemaphoreType.DMA
    vmem = pl.BlockSpec(memory_space=pltpu.VMEM)
    hbm = pl.BlockSpec(memory_space=pl.ANY)
    return pl.pallas_call(
        att_kernel,
        out_shape=[jax.ShapeDtypeStruct((4, rows, width), BF16), jax.ShapeDtypeStruct((4,) + lse.shape, F32), jax.ShapeDtypeStruct((rows, dim), F32), jax.ShapeDtypeStruct((rows, dim), BF16)] + [jax.ShapeDtypeStruct(p.shape, BF16) for p in pieces],
        in_specs=[vmem, vmem] + [hbm] * 3 + [vmem],
        out_specs=[vmem] * 4 + [hbm, hbm],
        scratch_shapes=[
            pltpu.VMEM((rows, dim), BF16), pltpu.VMEM((2,) + pieces[0].shape, BF16), pltpu.VMEM((2,) + pieces[1].shape, BF16),
            *[dma((n,)) for n in (6, 6, 3, 3, 5, 2, 2)],
        ],
        compiler_params=pltpu.CompilerParams(collective_id=1, has_side_effects=True, vmem_limit_bytes=48 * MIB),
        name="att_project",
    )(att, lse, x_all, *pieces, gain)


def weight_grad_kernel(info, *refs, pieces, splits, blank):
    lhs = refs[:pieces]
    rhs = refs[pieces:2 * pieces]
    outs = refs[2 * pieces:2 * pieces + splits]
    if blank:
        base, zeros, sem = refs[-3:]
        step = zeros.shape[0]
        i = pl.program_id(0)

        def fill(n):
            return pltpu.make_async_copy(zeros, base.at[pl.ds(pl.multiple_of(n * step, step), step), :], sem)

        @pl.when(i == 0)
        def _():
            zeros[:] = jnp.zeros_like(zeros)

        each = base.shape[0] // step // pl.num_programs(0)
        for n in range(each):
            fill(i * each + n).start()
    t = tn(lhs[0][:], rhs[0][:])
    for a, b in zip(lhs[1:], rhs[1:]):
        t += tn(a[:], b[:])
    width = t.shape[1] // splits
    for i, out in enumerate(outs):
        out[:] = t[:, i * width:(i + 1) * width]
    if blank:
        for n in range(each):
            fill(n).wait()


def weight_grad(info, lhs, rhs, block=256, splits=1, rows=None, blank=()):
    def spec(arr, p, cols, moving):
        if arr.ndim == 3:
            return pl.BlockSpec((None, arr.shape[1], cols), lambda i, info: (info[0] ^ p, 0, i if moving else 0))
        return pl.BlockSpec((arr.shape[0], cols), lambda i, info: (0, i if moving else 0))

    tokens = lhs[0].shape[-2]
    rows, dim = rows or lhs[0].shape[-1], rhs[0].shape[-1]
    n = len(lhs)
    width = dim // splits
    outs = pl.pallas_call(
        functools.partial(weight_grad_kernel, pieces=n, splits=splits, blank=blank),
        out_shape=[jax.ShapeDtypeStruct((rows, width), F32)] * splits + [jax.ShapeDtypeStruct(b, F32) for b in blank],
        grid_spec=pltpu.PrefetchScalarGridSpec(
            num_scalar_prefetch=1,
            grid=(pl.cdiv(rows, block),),
            in_specs=[spec(a, p, block, True) for p, a in enumerate(lhs)] + [spec(b, p, dim, False) for p, b in enumerate(rhs)],
            out_specs=[pl.BlockSpec((block, width), lambda i, info: (i, 0))] * splits + [pl.BlockSpec(memory_space=pl.ANY)] * len(blank),
            scratch_shapes=[s for b in blank for s in (pltpu.VMEM((200, b[1]), F32), pltpu.SemaphoreType.DMA)],
        ),
        compiler_params=pltpu.CompilerParams(vmem_limit_bytes=56 * MIB),
        cost_estimate=cost(2 * n * tokens * rows * dim, 4 * rows * dim + 2 * n * tokens * (rows + dim)),
        name="weight_grad",
    )(info, *lhs, *rhs)
    return outs if splits > 1 else outs[0]


def mlp_kernel(act, dy, wg, wu, wd, hidden, d_gate, d_up, *rest, limit):
    i = pl.program_id(0)
    block = wg.shape[0]
    left = limit - i * block
    row_ok = lax.broadcasted_iota(I32, (block, 1), 0) < left
    col_ok = lax.broadcasted_iota(I32, (1, block), 1) < left
    both = rest[-1]
    both[:block] = jnp.where(row_ok, wg[:], 0).astype(BF16)
    both[block:] = jnp.where(row_ok, wu[:], 0).astype(BF16)
    t = nt(act[:], both[:])
    gate, up = t[:, :block], t[:, block:]
    dh = jnp.where(col_ok, to_bf16(nt(dy[:], wd[:])), 0)
    sig = jax.nn.sigmoid(gate)
    hidden[:] = (gate * sig * up).astype(BF16)
    dg = (dh * up * sig * (1.0 + gate * (1.0 - sig))).astype(BF16)
    du = (dh * gate * sig).astype(BF16)
    d_gate[:] = dg
    d_up[:] = du
    if len(rest) > 1:
        grad, grads = rest[:2]
        grads[:, :block] = dg
        grads[:, block:] = du
        t = nn(grads[:], both[:])

        @pl.when(i == 0)
        def _():
            grad[:] = t

        @pl.when(i > 0)
        def _():
            grad[:] += t


def mlp_block(act, dy, wg, wu, wd, with_grad, block=256):
    rows, dim = act.shape
    limit = wg.shape[0]
    cols = pl.BlockSpec((rows, block), lambda i: (0, i))
    tile = pl.BlockSpec((block, dim), lambda i: (i, 0))
    whole = pl.BlockSpec((rows, dim), lambda i: (0, 0))
    return pl.pallas_call(
        functools.partial(mlp_kernel, limit=limit),
        out_shape=[jax.ShapeDtypeStruct((rows, pl.cdiv(limit, block) * block), BF16)] * 3 + [jax.ShapeDtypeStruct((rows, dim), F32)] * with_grad,
        grid=(pl.cdiv(limit, block),),
        in_specs=[whole, whole, tile, tile, tile],
        out_specs=[cols] * 3 + [whole] * with_grad,
        scratch_shapes=[pltpu.VMEM((rows, 2 * block), BF16)] * with_grad + [pltpu.VMEM((2 * block, dim), BF16)],
        compiler_params=pltpu.CompilerParams(vmem_limit_bytes=48 * MIB),
        cost_estimate=cost((6 + 4 * with_grad) * rows * dim * limit, 4 * dim * limit + 6 * rows * limit + 10 * rows * dim),
        name="mlp_block",
    )(act, dy, wg, wu, wd)


def scatter_kernel(order, sid, runs, bounds, rows, base_hbm, out_hbm, sums, row_sem, sum_sem):
    lo = bounds[0]
    hi = bounds[1]

    def one(c):
        p, singles, multi = c
        n = runs[p]
        t = order[p]
        single = n == 1

        @pl.when(single)
        def _():
            pltpu.make_async_copy(rows.at[pl.ds(t, 1), :], out_hbm.at[pl.ds(sid[p], 1), :], row_sem).start()

        @pl.when(jnp.logical_not(single))
        def _():
            def add(j, acc):
                return acc + rows[pl.ds(order[p + j], 1), :]

            sums[pl.ds(multi, 1), :] = lax.fori_loop(1, n, add, rows[pl.ds(t, 1), :])

        return p + n, singles + single.astype(I32), multi + 1 - single.astype(I32)

    _, singles, multi = lax.while_loop(lambda c: c[0] < hi, one, (lo, 0, 0))

    def two(c):
        p, k = c
        n = runs[p]

        @pl.when(n > 1)
        def _():
            pltpu.make_async_copy(sums.at[pl.ds(k, 1), :], out_hbm.at[pl.ds(sid[p], 1), :], sum_sem).start()

        return p + n, k + (n > 1).astype(I32)

    lax.while_loop(lambda c: c[0] < hi, two, (lo, 0))

    def wait(sem):
        def body(i, c):
            pltpu.make_async_copy(sums.at[pl.ds(0, 1), :], out_hbm.at[pl.ds(0, 1), :], sem).wait()
            return c

        return body

    lax.fori_loop(0, singles, wait(row_sem), 0)
    lax.fori_loop(0, multi, wait(sum_sem), 0)


def scatter_rows(order, sid, runs, bounds, grads, base, tokens):
    _, dim = grads.shape
    rows = base.shape[0]
    return pl.pallas_call(
        scatter_kernel,
        out_shape=jax.ShapeDtypeStruct((rows, dim), F32),
        grid_spec=pltpu.PrefetchScalarGridSpec(
            num_scalar_prefetch=4,
            grid=(),
            in_specs=[pl.BlockSpec(memory_space=pltpu.VMEM), pl.BlockSpec(memory_space=pl.ANY)],
            out_specs=pl.BlockSpec(memory_space=pl.ANY),
            scratch_shapes=[pltpu.VMEM((tokens // 2, dim), F32), pltpu.SemaphoreType.DMA, pltpu.SemaphoreType.DMA],
        ),
        input_output_aliases={5: 0},
        compiler_params=pltpu.CompilerParams(vmem_limit_bytes=40 * MIB),
        name="scatter_rows",
    )(order, sid, runs, bounds, grads, base)


def solution(mesh):
    cp_count = mesh.shape["cp"]
    tp_count = mesh.shape["tp"]
    both = ("cp", "tp")
    x_swap = [(i, i ^ 2) for i in range(cp_count)]
    core_swap = [(i, i ^ 1) for i in range(cp_count)]

    def compute(tokens, pos, doc_id, dy, table, w_q, w_k, w_v, w_o, w_gate, w_up, w_down, gain_one, gain_two, inv_freq):
        span = tokens.shape[0]
        total = span * cp_count
        part = span // tp_count
        rows, dim = table.shape
        head_dim = 2 * inv_freq.shape[0]
        heads = w_q.shape[1] // head_dim
        width = heads * head_dim
        tp_rank = lax.axis_index("tp")
        cp_rank = lax.axis_index("cp")
        core = cp_rank % 2
        gain_a = gain_one.astype(F32)
        gain_b = gain_two.astype(F32)

        barrier = lax.optimization_barrier
        join = lambda arr, axis: lax.all_gather(arr, axis, axis=0, tiled=True)
        add_up = lambda arr: lax.psum_scatter(arr, "tp", scatter_dimension=0, tiled=True)
        swap = lambda arr, pairs, axis="cp": lax.ppermute(arr, axis, pairs)
        local_ids = tokens - tp_rank * rows
        owned = (local_ids >= 0) & (local_ids < rows)
        safe_ids = jnp.where(owned, local_ids, jnp.arange(span) * (rows // span))
        picked = jnp.where(owned[:, None], jnp.take(table, safe_ids, axis=0), 0).astype(BF16)
        info = jnp.stack([cp_rank, core]).astype(I32)
        half = dim // 2
        near = 256
        wo_half = lax.dynamic_slice_in_dim(w_o, core * half, half, 1)
        wo_near = join(wo_half[:, :near], "tp")
        angle = pos.astype(F32)[:, None] * inv_freq[None, :]
        side_f = jnp.concatenate([jnp.cos(angle), jnp.sin(angle)], axis=1)
        side_i = jnp.stack([tokens, doc_id] * 4)
        x_all, x_slice, angles, ints = embed_gather(picked.reshape(tp_count, part, dim), side_f, side_i)
        angles = angles.reshape(total, head_dim)
        tok_all = ints[:, 0, :].reshape(total)
        doc_all = ints[:, 1, :].reshape(total)
        wo_far = barrier((wo_half[:, near:], x_all))[0]
        wo_rest = join(wo_far, "tp")

        dy_x = swap(barrier((dy, x_all))[0], x_swap)
        act_a, query, key, value, w_qkv = project_qkv(x_all, gain_a[None, :], w_q, w_k, w_v, angles)

        blk = span // 2
        blocks = total // blk
        doc_col = doc_all[:, None]
        doc_row = doc_all.reshape(blocks, 1, blk)
        attended, lse = attend(info, ints, query, key, value, doc_col, doc_row, head_dim, blk)

        gain_row = gain_b[None, :]
        att_parts, lse_all, residual, act_b, *wo_other = att_project(attended, lse, x_all, (wo_near, wo_rest), gain_row)
        lse_all = lse_all.reshape(total, 8)
        att_x = swap(att_parts, x_swap)

        wg, wu = w_gate.T, w_up.T
        ffn = wg.shape[0]
        hidden, d_gate, d_up, d_act_b = mlp_block(act_b, dy, wg, wu, w_down, True)
        d_act_b = add_up(d_act_b)
        act_x = out_proj(info, 2, x_all, att_x, (wo_near, wo_rest, *wo_other), gain_row)[1]
        hidden_x, d_gate_x, d_up_x = mlp_block(act_x, dy_x, wg, wu, w_down, False)
        d_act_b, hidden_x, d_gate_x, d_up_x = barrier((d_act_b, hidden_x, d_gate_x, d_up_x))
        d_act_b = to_bf16(d_act_b)
        acts, dys, hiddens, d_gates, d_ups = [(a, swap(a, core_swap), b, swap(b, core_swap)) for a, b in (
            (act_b, act_x), (dy, dy_x), (hidden, hidden_x), (d_gate, d_gate_x), (d_up, d_up_x))]
        heads_x = lax.dynamic_index_in_dim(att_x, tp_rank, 0, keepdims=False)
        head_parts = (attended, swap(attended, core_swap), heads_x, swap(heads_x, core_swap))
        att_heads = jnp.zeros((total, width), BF16)
        for k, piece in enumerate(head_parts):
            att_heads = lax.dynamic_update_slice_in_dim(att_heads, piece, (cp_rank ^ k) * span, 0)
        grad_down = weight_grad(info, hiddens, dys, rows=ffn)
        grad_gate = weight_grad(info, d_gates, acts, rows=ffn)
        grad_up = weight_grad(info, d_ups, acts, rows=ffn)

        def mine(arr):
            return lax.dynamic_slice_in_dim(arr, tp_rank * part, part, 0)

        res_part = mine(residual)
        normed_b, inv_b = rms_stats(res_part)
        grad_gain_b = jnp.sum(d_act_b * normed_b, axis=0)
        d_resid = mine(dy).astype(F32) + rms_back(d_act_b * gain_b, normed_b, inv_b)
        d_resid_all = join(d_resid.astype(BF16), both)
        out_part = nn(hidden[:, :ffn], w_down)
        d_resid_all, grad_down, att_heads, out_part = barrier((d_resid_all, grad_down, att_heads, out_part))
        tp_swap = lambda arr, k: swap(arr, [(i, i ^ k) for i in range(tp_count)], "tp")
        tp_part = lambda arr, k: lax.dynamic_slice_in_dim(arr, (tp_rank ^ k) * part, part, 0)
        others = range(1, tp_count)
        arrived = [tp_swap(tp_part(out_part, k), k) for k in others]
        out_slice = res_part + tp_part(out_part, 0)
        for piece in arrived:
            out_slice = out_slice + piece
        out_slice = out_slice.astype(BF16)

        d_att = nt(d_resid_all, w_o)
        d_att_b = d_att.astype(BF16)
        head_of = (jnp.arange(width)[None, :] // head_dim == jnp.arange(8)[:, None]).astype(F32)
        prod = att_heads.astype(F32) * d_att_b.astype(F32)
        delta = lax.dot_general(head_of, prod, (((1,), (1,)), ((), ())), precision=lax.Precision.HIGHEST, preferred_element_type=F32)

        def by_block(arr):
            return jnp.transpose(arr.reshape(8, blocks, blk), (1, 0, 2))

        dqkv = attend_back(info, ints, query, key, value, d_att_b, doc_col, doc_row, lse_all, by_block(lse_all.T), delta.T, by_block(delta), angles, blk)
        d_act_a = nt(dqkv, w_qkv)
        d_act_a = add_up(d_act_a)
        dqkv_x = swap(dqkv, x_swap)
        dqkvs = (dqkv, swap(dqkv, core_swap), dqkv_x, swap(dqkv_x, core_swap))
        grad_out = weight_grad(info, head_parts, [d_resid_all.reshape(cp_count, span, dim)] * 4)
        d_act_a, dqkv_x, grad_out, grad_up = barrier((d_act_a, dqkv_x, grad_out, grad_up))
        d_act_a, out_slice = barrier((d_act_a, out_slice))
        d_act_a = to_bf16(d_act_a)
        y_parts = [tp_swap(out_slice, k) for k in others]
        normed_a, inv_a = rms_stats(x_slice.astype(F32))
        grad_gain_a = jnp.sum(d_act_a * normed_a, axis=0)
        d_embed = d_resid + rms_back(d_act_a * gain_a, normed_a, inv_a)
        payload = jnp.concatenate([d_embed, jnp.stack([grad_gain_a, grad_gain_b] * 4)])
        gathered = join(payload, both)
        *grad_qkv, base = weight_grad(info, [act_a.reshape(cp_count, span, dim)] * 4, dqkvs, splits=3, blank=((rows, dim),))
        slot_ids = jnp.arange(total, dtype=I32)
        before = (tok_all[None, :] < tok_all[:, None]) | ((tok_all[None, :] == tok_all[:, None]) & (slot_ids[None, :] < slot_ids[:, None]))
        rank = jnp.sum(before.astype(I32), axis=1)
        count = jnp.sum((tok_all[None, :] == tok_all[:, None]).astype(I32), axis=1)
        at_rank = rank[None, :] == slot_ids[:, None]
        runs = jnp.sum(jnp.where(at_rank, count[None, :], 0), axis=1)
        order = jnp.sum(jnp.where(at_rank, slot_ids[None, :], 0), axis=1)
        sid = jnp.sum(jnp.where(at_rank, tok_all[None, :], 0), axis=1) - tp_rank * rows
        order = order + 8 * (order // part)
        bounds = jnp.stack([jnp.sum((tok_all < tp_rank * rows).astype(I32)), jnp.sum((tok_all < (tp_rank + 1) * rows).astype(I32))])
        gathered, grad_qkv, grad_gate, runs, order, sid, bounds, base = barrier((gathered, grad_qkv, grad_gate, runs, order, sid, bounds, base))
        layer_out = jnp.concatenate([out_slice] * tp_count)
        for k, piece in zip(others, y_parts):
            layer_out = lax.dynamic_update_slice_in_dim(layer_out, piece, (tp_rank ^ k) * part, 0)
        gain_grads = jnp.sum(gathered.reshape(cp_count * tp_count, part + 8, dim)[:, part:part + 2], axis=0)
        grad_table = scatter_rows(order, sid, runs, bounds, gathered, base, total)
        return (layer_out, grad_table, *grad_qkv, grad_out, grad_gate.T, grad_up.T, grad_down, gain_grads[0], gain_grads[1])

    col_spec = P(None, "tp")
    row_spec = P("tp")
    tok_spec = P("cp")
    rep_spec = P()
    in_specs = (tok_spec, tok_spec, tok_spec, P("cp"), row_spec, col_spec, col_spec, col_spec, row_spec, col_spec, col_spec, row_spec, rep_spec, rep_spec, rep_spec)
    out_specs = (P("cp"), row_spec, col_spec, col_spec, col_spec, row_spec, col_spec, col_spec, row_spec, rep_spec, rep_spec)
    return jax.shard_map(compute, mesh=mesh, in_specs=in_specs, out_specs=out_specs, check_vma=False)
```

```python
import functools
import jax
import jax.numpy as jnp
from jax import lax
from jax.experimental import pallas as pl
from jax.experimental.pallas import tpu as pltpu
from jax.sharding import PartitionSpec as P

NORM_EPS = 1e-5
NEG_BIG = -1e30
MIB = 2 ** 20
FULL = 62 * MIB
F32 = jnp.float32
BF16 = jnp.bfloat16
I32 = jnp.int32


def rms_stats(feats):
    inv_rms = lax.rsqrt(mean_row(feats * feats) + NORM_EPS)
    return feats * inv_rms, inv_rms


def rms_back(d_normed, normed, inv_rms):
    return inv_rms * (d_normed - normed * mean_row(d_normed * normed))


def to_bf16(feats):
    return feats.astype(BF16).astype(F32)


def contract(a, b, ca, cb):
    return lax.dot_general(a, b, (((ca,), (cb,)), ((), ())), preferred_element_type=F32)


def row_sum(t):
    return jnp.sum(t, 1, keepdims=True)


def mean_row(t):
    return row_sum(t) / t.shape[1]


def whole(a):
    return pl.BlockSpec(a.shape, lambda *i: (0,) * a.ndim)


def cost(flops):
    return pl.CostEstimate(flops=flops, bytes_accessed=flops // 512, transcendentals=0)


def nn(a, b):
    return contract(a, b, 1, 0)


def nt(a, b):
    return contract(a, b, 1, 1)


def tn(a, b):
    return contract(a, b, 0, 0)


DIMS = ("x", "y", "z")


class Place:
    def __init__(self):
        tp = lax.axis_index("tp")
        cp = lax.axis_index("cp")
        self.at = {"x": cp // 2, "core": cp % 2, "z": tp // 2, "y": tp % 2}

    def coord(self, dim, flip):
        return 1 - self.at[dim] if dim in flip else self.at[dim]

    def tp(self, flip=()):
        return self.coord("z", flip) * 2 + self.coord("y", flip)

    def cp(self, flip=()):
        return self.coord("x", flip) * 2 + self.coord("core", flip)

    def device(self, flip):
        return {"tp": self.tp(flip), "cp": self.cp(flip)}

    def slot(self, flip=()):
        return self.cp(flip) * 4 + self.tp(flip)

    def meet(self, dims):
        barrier = pltpu.get_barrier_semaphore()
        for d in dims:
            pl.semaphore_signal(barrier, inc=1, device_id=self.device((d,)), device_id_type=MESH)
        pl.semaphore_wait(barrier, len(dims))


MESH = pl.DeviceIdType.MESH
ORDERS = (("x", "y", "z"), ("y", "z", "x"), ("z", "x", "y"))
FLIPS = tuple(tuple(d for i, d in enumerate(DIMS) if n >> i & 1) for n in range(8))


def flip_code(flip):
    return sum(1 << DIMS.index(d) for d in flip)


def column_parts(width, count):
    tiles = width // 128
    sizes = [(tiles // count + (i < tiles % count)) * 128 for i in range(count)]
    return [(sum(sizes[:i]), n) for i, n in enumerate(sizes)]


class Gather:
    def __init__(self, place, buf, send, recv, core_send, core_recv):
        self.place, self.buf, self.send, self.recv, self.core_send, self.core_recv = place, buf, send, recv, core_send, core_recv
        self.parts = column_parts(buf.shape[2], 3)
        self.started = []

    def view(self, part, flip):
        start, size = self.parts[part]
        return self.buf.at[self.place.slot(flip), :, pl.ds(start, size)]

    def hop(self, part, flip, dim):
        there = tuple(d for d in DIMS if (d in flip) != (d == dim))
        index = part * 7 + flip_code(there) - 1
        ref = self.view(part, flip)
        return pltpu.make_async_remote_copy(src_ref=ref, dst_ref=ref, send_sem=self.send.at[index], recv_sem=self.recv.at[index], device_id=self.place.device((dim,)), device_id_type=MESH)

    def core_hop(self, part, flip):
        index = part * 8 + flip_code(flip)
        ref = self.view(part, flip)
        return pltpu.make_async_remote_copy(src_ref=ref, dst_ref=ref, send_sem=self.core_send.at[index], recv_sem=self.core_recv.at[index], device_id=self.place.device(("core",)), device_id_type=MESH)

    def go(self, copy):
        copy.start()
        self.started.append(copy)

    def wait(self, part, flip):
        order = ORDERS[part]
        last = max(order.index(d) for d in flip)
        came = tuple(d for d in flip if d != order[last])
        self.hop(part, came, order[last]).wait_recv()
        for dim in order[last + 1:]:
            self.go(self.hop(part, flip, dim))
        self.go(self.core_hop(part, flip))

    def run(self):
        for step in range(3):
            for part, order in enumerate(ORDERS):
                self.go(self.hop(part, (), order[step]))
        for part in range(3):
            self.go(self.core_hop(part, ()))
        for step in range(3):
            for flip in FLIPS[1:]:
                for part, order in enumerate(ORDERS):
                    if max(order.index(d) for d in flip) == step and len(flip) == 1:
                        self.wait(part, flip)
            for flip in FLIPS[1:]:
                for part, order in enumerate(ORDERS):
                    if max(order.index(d) for d in flip) == step and len(flip) > 1:
                        self.wait(part, flip)

    def finish(self, out, out_sem):
        rows = self.buf.shape[1]
        copies = []

        def store(flip):
            slot = self.place.slot(flip)
            c = pltpu.make_async_copy(self.buf.at[slot], out.at[pl.ds(slot * rows, rows), :], out_sem.at[len(copies)])
            c.start()
            copies.append(c)

        for flip in FLIPS:
            store(flip)
        for flip in FLIPS:
            other = flip + ("core",)
            for part in range(3):
                start, size = self.parts[part]
                ref = self.buf.at[self.place.slot(other), :, pl.ds(start, size)]
                index = part * 8 + flip_code(flip)
                pltpu.make_async_remote_copy(src_ref=ref, dst_ref=ref, send_sem=self.core_send.at[index], recv_sem=self.core_recv.at[index], device_id=self.place.device(("core",)), device_id_type=MESH).wait_recv()
            store(other)
        for c in self.started:
            c.wait_send()
        for c in copies:
            c.wait()


def embed_kernel(picked, side_f, side_i, out, slice_out, all_f, all_i, buf, r1, r2, tmp, send, recv, core_send, core_recv, out_sem, rs_send, rs_recv, side_send, side_recv, slice_sem):
    place = Place()
    place.meet(("x", "y", "z", "core"))
    half = buf.shape[2] // 2
    near = ("y", "z")

    sides = ((side_f, all_f), (side_i, all_i))
    started, keeps = [], []

    def side_hop(i, step):
        src, dst = sides[i]
        if step == 0:
            src_ref, slot, dim = src, place.cp(), "x"
        elif step == 1:
            src_ref, slot, dim = src, place.cp(), "core"
        else:
            src_ref, slot, dim = dst.at[place.cp(("x",))], place.cp(("x",)), "core"
        return pltpu.make_async_remote_copy(src_ref=src_ref, dst_ref=dst.at[slot], send_sem=side_send.at[i, step], recv_sem=side_recv.at[i, step], device_id=place.device((dim,)), device_id_type=MESH)

    def first(h, k):
        a, b = near[h], near[1 - h]
        target = place.tp((a,)) if k == 0 else place.tp((a, b))
        cols = pl.ds(h * half, half)
        return pltpu.make_async_remote_copy(src_ref=picked.at[target, :, cols], dst_ref=r1.at[h, k], send_sem=rs_send.at[h, k], recv_sem=rs_recv.at[h, k], device_id=place.device((a,)), device_id_type=MESH)

    def second(h):
        return pltpu.make_async_remote_copy(src_ref=tmp.at[h], dst_ref=r2.at[h], send_sem=rs_send.at[h, 2], recv_sem=rs_recv.at[h, 2], device_id=place.device((near[1 - h],)), device_id_type=MESH)

    def go(copy):
        copy.start()
        started.append(copy)

    for k in (1, 0):
        for h in range(2):
            go(first(h, k))
    for i in range(2):
        go(side_hop(i, 0))
        go(side_hop(i, 1))
        keeps.append(pltpu.make_async_copy(sides[i][0], sides[i][1].at[place.cp()], slice_sem.at[i]))
        keeps[i].start()
    for h in range(2):
        cols = slice(h * half, (h + 1) * half)
        first(h, 1).wait_recv()
        tmp[h] = picked[place.tp((near[1 - h],)), :, cols] + r1[h, 1]
        go(second(h))
    for i in range(2):
        side_hop(i, 0).wait_recv()
        go(side_hop(i, 2))
    mine = place.slot()
    for h in range(2):
        cols = slice(h * half, (h + 1) * half)
        first(h, 0).wait_recv()
        part = picked[place.tp(), :, cols] + r1[h, 0]
        second(h).wait_recv()
        buf[mine, :, cols] = part + r2[h]
    gather = Gather(place, buf, send, recv, core_send, core_recv)
    gather.run()
    keeps.append(pltpu.make_async_copy(buf.at[mine], slice_out, slice_sem.at[2]))
    keeps[-1].start()
    gather.finish(out, out_sem)
    for c in keeps:
        c.wait()
    for i in range(2):
        side_hop(i, 1).wait_recv()
        side_hop(i, 2).wait_recv()
    for c in started:
        c.wait_send()


def embed_gather(picked, side_f, side_i):
    _, rows, dim = picked.shape
    half = dim // 2
    dma = pltpu.SemaphoreType.DMA
    vmem = pl.BlockSpec(memory_space=pltpu.VMEM)
    hbm = pl.BlockSpec(memory_space=pl.ANY)
    return pl.pallas_call(
        embed_kernel,
        out_shape=[
            jax.ShapeDtypeStruct((16 * rows, dim), BF16),
            jax.ShapeDtypeStruct((rows, dim), BF16),
            jax.ShapeDtypeStruct((4,) + side_f.shape, F32),
            jax.ShapeDtypeStruct((4,) + side_i.shape, I32),
        ],
        in_specs=[vmem, vmem, vmem],
        out_specs=[pl.BlockSpec(memory_space=pltpu.HBM)] * 4,
        scratch_shapes=[
            pltpu.VMEM((16, rows, dim), BF16),
            pltpu.VMEM((2, 2, rows, half), BF16),
            pltpu.VMEM((2, rows, half), BF16),
            pltpu.VMEM((2, rows, half), BF16),
            dma((21,)), dma((21,)), dma((24,)), dma((24,)), dma((16,)),
            *[dma((2, 3))] * 4, dma((3,)),
        ],
        compiler_params=pltpu.CompilerParams(collective_id=0, has_side_effects=True, vmem_limit_bytes=FULL),
        name="embed_gather",
    )(picked, side_f, side_i)


def slot_block(j):
    return jnp.where(j < 4, 2 * j, 15 - 2 * j)


def unpack_angles(packed):
    turned = pltpu.roll(packed, packed.shape[1] // 2, 1)
    low = lax.broadcasted_iota(I32, packed.shape, 1) < packed.shape[1] // 2
    return jnp.where(low, packed, turned), jnp.where(low, -turned, packed)


def qkv_kernel(x, gain, wq, wk, wv, angles, act, q, k, v, wide, *, head_dim):
    width = wq.shape[1]

    @pl.when(pl.program_id(0) == 0)
    def _():
        for i, w in enumerate((wq, wk, wv)):
            wide[:, i * width:(i + 1) * width] = w[:]

    feats = x[:].astype(F32)
    inv = lax.rsqrt(mean_row(feats * feats) + NORM_EPS)
    a = (feats * inv * gain[:]).astype(BF16)
    act[:] = a
    t = nn(a, wide[:])
    cos, sin = unpack_angles(angles[:])
    for i, out in enumerate((q, k, v)):
        for h in range(width // head_dim):
            th = t[:, i * width + h * head_dim:i * width + (h + 1) * head_dim]
            if i < 2:
                th = th * cos + pltpu.roll(th, head_dim // 2, 1) * sin
            out[:, h * head_dim:(h + 1) * head_dim] = th.astype(BF16)


def project_qkv(x_all, gain, wq, wk, wv, angles, block=512):
    total, dim = x_all.shape
    width = wq.shape[1]
    head_dim = angles.shape[1]
    rows = lambda n: pl.BlockSpec((block, n), lambda i: (i, 0))
    whole = lambda a: pl.BlockSpec(a.shape, lambda i: (0, 0), pipeline_mode=pl.Buffered(1))
    return pl.pallas_call(
        functools.partial(qkv_kernel, head_dim=head_dim),
        out_shape=[jax.ShapeDtypeStruct((total, n), BF16) for n in (dim, width, width, width)],
        grid=(total // block,),
        in_specs=[rows(dim), whole(gain), whole(wq), whole(wk), whole(wv), rows(head_dim)],
        out_specs=[rows(dim), rows(width), rows(width), rows(width)],
        scratch_shapes=[pltpu.VMEM((dim, 3 * width), BF16)],
        compiler_params=pltpu.CompilerParams(vmem_limit_bytes=FULL),
        cost_estimate=cost(6 * total * dim * width),
        name="project_qkv",
    )(x_all, gain, wq, wk, wv, angles)


def block_range(info, ids, i, blocks):
    r = info[0]
    blk = ids.shape[2] // 2
    b = jnp.where(i == 0, r, blocks - 1 - r)

    def docs(shard, half):
        return ids[shard, 1, half * blk], ids[shard, 1, half * blk + blk - 1]

    first, last = docs(r, i)
    jmin, imax = 0, -1
    for j in range(blocks):
        begin, end = docs(min(j, blocks - 1 - j), int(j >= blocks // 2))
        jmin = jmin + (end < first).astype(I32)
        imax = imax + (begin <= last).astype(I32)
    return b, jmin, imax


def attend_kernel(info, ids, q, k, v, doc_col, doc_row, out, lse, sc, *, heads, head_dim, scale):
    blk = q.shape[0]
    b, jmin, _ = block_range(info, ids, pl.program_id(0), doc_row.shape[0])
    row_n = lax.broadcasted_iota(I32, (blk, blk), 0) + b * blk
    col_n = lax.broadcasted_iota(I32, (blk, blk), 1)

    def score(j, peaks):
        sb = slot_block(j)
        off = pl.multiple_of(sb * blk, blk)
        allowed = (doc_col[:] == doc_row[sb]) & (col_n + j * blk <= row_n)
        new = []
        for h in range(heads):
            cols = slice(h * head_dim, (h + 1) * head_dim)
            s = nt(q[:, cols], k[pl.ds(off, blk), cols]) * scale
            s = jnp.where(allowed, s, NEG_BIG)
            sc[j, h] = s
            new.append(jnp.maximum(peaks[h], jnp.max(s, axis=1, keepdims=True)))
        return tuple(new)

    peaks = lax.fori_loop(jmin, b + 1, score, tuple(jnp.full((blk, 1), NEG_BIG, F32) for _ in range(heads)))

    def weigh(j, sums):
        new = []
        for h in range(heads):
            p = jnp.exp(sc[j, h] - peaks[h])
            sc[j, h] = p
            new.append(sums[h] + row_sum(p))
        return tuple(new)

    sums = lax.fori_loop(jmin, b + 1, weigh, tuple(jnp.zeros((blk, 1), F32) for _ in range(heads)))
    inv = tuple(1.0 / t for t in sums)
    for h in range(heads):
        lse[:, h:h + 1] = peaks[h] + jnp.log(sums[h])

    def mix(j, acc):
        off = pl.multiple_of(slot_block(j) * blk, blk)
        new = []
        for h in range(heads):
            cols = slice(h * head_dim, (h + 1) * head_dim)
            new.append(acc[h] + nn((sc[j, h] * inv[h]).astype(BF16), v[pl.ds(off, blk), cols]))
        return tuple(new)

    acc = lax.fori_loop(jmin, b + 1, mix, tuple(jnp.zeros((blk, head_dim), F32) for _ in range(heads)))
    for h in range(heads):
        out[:, h * head_dim:(h + 1) * head_dim] = acc[h].astype(BF16)


def attend(info, ids, q, k, v, doc_col, doc_row, head_dim, blk):
    total, width = k.shape
    heads = width // head_dim
    mine = lambda n: pl.BlockSpec((blk, n), lambda i, info, ids: (2 * info[0] + i, 0))
    return pl.pallas_call(
        functools.partial(attend_kernel, heads=heads, head_dim=head_dim, scale=head_dim ** -0.5),
        out_shape=[jax.ShapeDtypeStruct((2 * blk, width), BF16), jax.ShapeDtypeStruct((2 * blk, 8), F32)],
        grid_spec=pltpu.PrefetchScalarGridSpec(
            num_scalar_prefetch=2,
            grid=(2,),
            in_specs=[mine(width), whole(k), whole(v), mine(1), whole(doc_row)],
            out_specs=[pl.BlockSpec((blk, width), lambda i, info, ids: (i, 0)), pl.BlockSpec((blk, 8), lambda i, info, ids: (i, 0))],
            scratch_shapes=[pltpu.VMEM((total // blk, heads, blk, blk), F32)],
        ),
        compiler_params=pltpu.CompilerParams(vmem_limit_bytes=FULL),
        cost_estimate=cost(4 * 2 * blk * total * width),
        name="attend",
    )(info, ids, q, k, v, doc_col, doc_row)


def attend_back_kernel(info, ids, q, k, v, do, doc_col, doc_row, lse_col, lse_row, del_col, del_row, angles, out, acc, *, heads, head_dim, scale):
    blk = angles.shape[0]
    width = heads * head_dim
    i = pl.program_id(0)
    b, jmin, imax = block_range(info, ids, i, doc_row.shape[0])
    me = pl.multiple_of((2 * info[0] + i) * blk, blk)
    mine = pl.ds(me, blk)
    iota_r = lax.broadcasted_iota(I32, (blk, blk), 0)
    iota_c = lax.broadcasted_iota(I32, (blk, blk), 1)
    acc[:] = jnp.zeros_like(acc)
    spans = [slice(h * head_dim, (h + 1) * head_dim) for h in range(heads)]

    def for_query(j, c):
        sb = slot_block(j)
        there = pl.ds(pl.multiple_of(sb * blk, blk), blk)
        allowed = (doc_col[mine, :] == doc_row[sb]) & (iota_c + j * blk <= iota_r + b * blk)
        for h, cols in enumerate(spans):
            s = jnp.where(allowed, nt(q[mine, cols], k[there, cols]) * scale, NEG_BIG)
            p = jnp.exp(s - lse_col[mine, h:h + 1])
            dp = to_bf16(nt(do[mine, cols], v[there, cols]))
            ds = (p * (dp - del_col[mine, h:h + 1]) * scale).astype(BF16)
            acc[0, :, cols] += nn(ds, k[there, cols])
        return c

    lax.fori_loop(jmin, b + 1, for_query, 0)

    def for_key(j, c):
        sb = slot_block(j)
        there = pl.ds(pl.multiple_of(sb * blk, blk), blk)
        allowed = (doc_col[mine, :] == doc_row[sb]) & (iota_r + b * blk <= iota_c + j * blk)
        for h, cols in enumerate(spans):
            s = jnp.where(allowed, nt(k[mine, cols], q[there, cols]) * scale, NEG_BIG)
            p = jnp.exp(s - lse_row[sb, h:h + 1, :])
            dp = to_bf16(nt(v[mine, cols], do[there, cols]))
            ds = (p * (dp - del_row[sb, h:h + 1, :]) * scale).astype(BF16)
            acc[2, :, cols] += nn(p.astype(BF16), do[there, cols])
            acc[1, :, cols] += nn(ds, q[there, cols])
        return c

    lax.fori_loop(b, imax + 1, for_key, 0)
    cos, sin = unpack_angles(angles[:])
    for part in range(3):
        for h, cols in enumerate(spans):
            t = acc[part, :, cols]
            if part < 2:
                t = to_bf16(t)
                t = t * cos - pltpu.roll(t, head_dim // 2, 1) * sin
            out[:, part * width + h * head_dim:part * width + (h + 1) * head_dim] = t.astype(BF16)


def attend_back(info, ids, q, k, v, do, doc_col, doc_row, lse_col, lse_row, del_col, del_row, angles, blk):
    total, width = k.shape
    head_dim = angles.shape[1]
    heads = width // head_dim
    mine = lambda n: pl.BlockSpec((blk, n), lambda i, info, ids: (2 * info[0] + i, 0))
    arrays = (q, k, v, do, doc_col, doc_row, lse_col, lse_row, del_col, del_row)
    return pl.pallas_call(
        functools.partial(attend_back_kernel, heads=heads, head_dim=head_dim, scale=head_dim ** -0.5),
        out_shape=jax.ShapeDtypeStruct((2 * blk, 3 * width), BF16),
        grid_spec=pltpu.PrefetchScalarGridSpec(
            num_scalar_prefetch=2,
            grid=(2,),
            in_specs=[whole(a) for a in arrays] + [mine(head_dim)],
            out_specs=pl.BlockSpec((blk, 3 * width), lambda i, info, ids: (i, 0)),
            scratch_shapes=[pltpu.VMEM((3, blk, width), F32)],
        ),
        compiler_params=pltpu.CompilerParams(vmem_limit_bytes=FULL),
        cost_estimate=cost(14 * 2 * blk * total * width // 2),
        name="attend_back",
    )(info, ids, *arrays, angles)


def out_proj_kernel(info, x, att, a0, b0, a1, b1, gain, res, act, wide, abuf, bbuf, sems):
    tp, _, width = att.shape
    na, nb = a0.shape[1], b0.shape[1]
    sets = ((a0, b0), (a1, b1))

    def copies(i):
        return (pltpu.make_async_copy(sets[i][0], abuf.at[i], sems.at[i, 0]), pltpu.make_async_copy(sets[i][1], bbuf.at[i], sems.at[i, 1]))

    for i in range(2):
        for c in copies(i):
            c.start()
    for t in range(tp):
        wide[:, t * width:(t + 1) * width] = att[t]
    for i in range(2):
        start = (info[1] ^ i) * (na + nb)
        first, second = copies(i)
        first.wait()
        cols = pl.ds(pl.multiple_of(start, 128), na)
        res[:, cols] = x[:, cols].astype(F32) + nn(wide[:], abuf[i])
        second.wait()
        cols = pl.ds(pl.multiple_of(start + na, 128), nb)
        res[:, cols] = x[:, cols].astype(F32) + nn(wide[:], bbuf[i])
    h = res[:]
    inv = lax.rsqrt(mean_row(h * h) + NORM_EPS)
    act[:] = (h * inv * gain[:]).astype(BF16)


def out_proj(info, flip, x_all, att, pieces, gain):
    _, rows, _ = att.shape
    dim = x_all.shape[1]
    full = pl.BlockSpec((rows, dim), lambda i, info: (0, 0))
    return pl.pallas_call(
        out_proj_kernel,
        out_shape=[jax.ShapeDtypeStruct((rows, dim), F32), jax.ShapeDtypeStruct((rows, dim), BF16)],
        grid_spec=pltpu.PrefetchScalarGridSpec(
            num_scalar_prefetch=1,
            grid=(1,),
            in_specs=[pl.BlockSpec((rows, dim), lambda i, info: (info[0] ^ flip, 0)), whole(att)] + [pl.BlockSpec(memory_space=pl.ANY)] * 4 + [whole(gain)],
            out_specs=[full, full],
            scratch_shapes=[pltpu.VMEM((rows, dim), BF16), pltpu.VMEM((2,) + pieces[0].shape, BF16), pltpu.VMEM((2,) + pieces[1].shape, BF16), pltpu.SemaphoreType.DMA((2, 2))],
        ),
        compiler_params=pltpu.CompilerParams(vmem_limit_bytes=FULL),
        cost_estimate=cost(2 * rows * dim * dim),
        name="out_proj",
    )(info, x_all, att, *pieces, gain)


def att_kernel(att, lse, x_all, a0, b0, gain, parts, lse_out, res, act, a1, b1, x, abuf, bbuf, send, recv, lse_send, lse_recv, load, swap_send, swap_recv):
    place = Place()
    rows, width = att.shape
    na, nb = a0.shape[1], b0.shape[1]
    mine = place.cp()
    loads = [pltpu.make_async_copy(x_all.at[pl.ds(mine * rows, rows), :], x, load.at[4])]
    for i, (src, dst) in enumerate(((a0, abuf.at[0]), (b0, bbuf.at[0]), (a1, abuf.at[1]), (b1, bbuf.at[1]))):
        loads.append(pltpu.make_async_copy(src, dst, load.at[i]))
    early, late = loads[:3], loads[3:]
    for c in early:
        c.start()
    place.meet(("y", "z", "x", "core"))
    started = []
    near = ("y", "z")
    spans = column_parts(width, 2)

    def hop(p, flip, dim):
        there = tuple(d for d in near if (d in flip) != (d == dim))
        index = p * 3 + (there == ("y",)) + 2 * (there == ("z",))
        start, size = spans[p]
        cols = pl.ds(start, size)
        slot = place.tp(flip)
        src = parts.at[slot, :, cols] if flip else att.at[:, cols]
        return pltpu.make_async_remote_copy(src_ref=src, dst_ref=parts.at[slot, :, cols], send_sem=send.at[index], recv_sem=recv.at[index], device_id=place.device((dim,)), device_id_type=MESH)

    def lse_hop(step):
        src, slot, dim = ((lse, mine, "x"), (lse, mine, "core"), (lse_out.at[place.cp(("x",))], place.cp(("x",)), "core"))[step]
        return pltpu.make_async_remote_copy(src_ref=src, dst_ref=lse_out.at[slot], send_sem=lse_send.at[step], recv_sem=lse_recv.at[step], device_id=place.device((dim,)), device_id_type=MESH)

    def go(copy):
        copy.start()
        started.append(copy)

    swaps = [pltpu.make_async_remote_copy(src_ref=src, dst_ref=dst, send_sem=swap_send.at[i], recv_sem=swap_recv.at[i], device_id=place.device(("core",)), device_id_type=MESH) for i, (src, dst) in enumerate(((a0, a1), (b0, b1)))]
    for step in range(2):
        for p in range(2):
            go(hop(p, (), near[(p + step) % 2]))
    for c in swaps:
        go(c)
    go(lse_hop(0))
    go(lse_hop(1))
    lse_out[mine] = lse[:]
    parts[place.tp()] = att[:]
    for c in early:
        c.wait()

    def add(slot, halves=(0, 1), first=False):
        for i in halves:
            start = place.coord("core", ("core",) if i else ()) * (na + nb)
            k = pl.ds(pl.multiple_of(slot * width, width), width)
            for buf, at, n in ((abuf, 0, na), (bbuf, na, nb)):
                cols = pl.ds(pl.multiple_of(start + at, 128), n)
                t = nn(parts[slot], buf[i, k, :])
                res[:, cols] = t + (x[:, cols].astype(F32) if first else res[:, cols])

    add(place.tp(), (0,), True)
    for c in swaps:
        c.wait_recv()
    for c in late:
        c.start()
    for p in range(2):
        hop(p, (), near[p]).wait_recv()
        go(hop(p, (near[p],), near[1 - p]))
    lse_hop(0).wait_recv()
    go(lse_hop(2))
    for c in late:
        c.wait()
    add(place.tp(), (1,), True)
    for p in (1, 0):
        hop(p, (), near[1 - p]).wait_recv()
        add(place.tp((near[1 - p],)))
    for p in range(2):
        hop(p, (near[p],), near[1 - p]).wait_recv()
    add(place.tp(near))
    h = res[:]
    act[:] = (h * lax.rsqrt(mean_row(h * h) + NORM_EPS) * gain[:]).astype(BF16)
    lse_hop(1).wait_recv()
    lse_hop(2).wait_recv()
    for c in started:
        c.wait_send()


def att_project(att, lse, x_all, pieces, gain):
    rows, width = att.shape
    dim = x_all.shape[1]
    dma = pltpu.SemaphoreType.DMA
    vmem = pl.BlockSpec(memory_space=pltpu.VMEM)
    hbm = pl.BlockSpec(memory_space=pl.ANY)
    return pl.pallas_call(
        att_kernel,
        out_shape=[jax.ShapeDtypeStruct((4, rows, width), BF16), jax.ShapeDtypeStruct((4,) + lse.shape, F32), jax.ShapeDtypeStruct((rows, dim), F32), jax.ShapeDtypeStruct((rows, dim), BF16)] + [jax.ShapeDtypeStruct(p.shape, BF16) for p in pieces],
        in_specs=[vmem, vmem] + [hbm] * 3 + [vmem],
        out_specs=[vmem] * 4 + [hbm, hbm],
        scratch_shapes=[
            pltpu.VMEM((rows, dim), BF16), pltpu.VMEM((2,) + pieces[0].shape, BF16), pltpu.VMEM((2,) + pieces[1].shape, BF16),
            *[dma((n,)) for n in (6, 6, 3, 3, 5, 2, 2)],
        ],
        compiler_params=pltpu.CompilerParams(collective_id=1, has_side_effects=True, vmem_limit_bytes=FULL),
        name="att_project",
    )(att, lse, x_all, *pieces, gain)


def weight_grad_kernel(info, *refs, pieces, splits):
    lhs = refs[:pieces]
    rhs = refs[pieces:2 * pieces]
    outs = refs[2 * pieces:]
    t = tn(lhs[0][:], rhs[0][:])
    for a, b in zip(lhs[1:], rhs[1:]):
        t += tn(a[:], b[:])
    width = t.shape[1] // splits
    for i, out in enumerate(outs):
        out[:] = t[:, i * width:(i + 1) * width]


def weight_grad(info, lhs, rhs, block=256, splits=1, rows=None):
    def spec(arr, p, cols, moving):
        if arr.ndim == 3:
            return pl.BlockSpec((None, arr.shape[1], cols), lambda i, info: (info[0] ^ p, 0, i if moving else 0))
        return pl.BlockSpec((arr.shape[0], cols), lambda i, info: (0, i if moving else 0))

    tokens = lhs[0].shape[-2]
    rows, dim = rows or lhs[0].shape[-1], rhs[0].shape[-1]
    n = len(lhs)
    width = dim // splits
    outs = pl.pallas_call(
        functools.partial(weight_grad_kernel, pieces=n, splits=splits),
        out_shape=[jax.ShapeDtypeStruct((rows, width), F32)] * splits,
        grid_spec=pltpu.PrefetchScalarGridSpec(
            num_scalar_prefetch=1,
            grid=(pl.cdiv(rows, block),),
            in_specs=[spec(a, p, block, True) for p, a in enumerate(lhs)] + [spec(b, p, dim, False) for p, b in enumerate(rhs)],
            out_specs=[pl.BlockSpec((block, width), lambda i, info: (i, 0))] * splits,
        ),
        compiler_params=pltpu.CompilerParams(vmem_limit_bytes=56 * MIB),
        cost_estimate=cost(2 * n * tokens * rows * dim),
        name="weight_grad",
    )(info, *lhs, *rhs)
    return outs if splits > 1 else outs[0]


def mlp_kernel(act, dy, wg, wu, wd, hidden, d_gate, d_up, *rest, limit, tiles):
    i = pl.program_id(0)
    block = wg.shape[0]
    both = rest[-1]

    @pl.when(i < tiles)
    def _():
        left = limit - i * block
        row_ok = lax.broadcasted_iota(I32, (block, 1), 0) < left
        col_ok = lax.broadcasted_iota(I32, (1, block), 1) < left
        pair = pl.ds(pl.multiple_of(2 * i * block, block), 2 * block) if tiles < pl.num_programs(0) else slice(2 * block)
        both[pair] = jnp.concatenate([jnp.where(row_ok, w[:], 0).astype(BF16) for w in (wg, wu)])
        t = nt(act[:], both[pair])
        gate, up = t[:, :block], t[:, block:]
        dh = jnp.where(col_ok, to_bf16(nt(dy[:], wd[:])), 0)
        sig = jax.nn.sigmoid(gate)
        hidden[:] = (gate * sig * up).astype(BF16)
        dg = (dh * up * sig * (1.0 + gate * (1.0 - sig))).astype(BF16)
        du = (dh * gate * sig).astype(BF16)
        d_gate[:] = dg
        d_up[:] = du
        if len(rest) > 1:
            rest[1][:, pair] = jnp.concatenate([dg, du], axis=1)

    if len(rest) > 1:
        grad, grads = rest[:2]

        @pl.when(i >= tiles)
        def _():
            wide = grad.shape[1]
            grad[:] = nn(grads[:], both[:, pl.ds(pl.multiple_of((i - tiles) * wide, wide), wide)])


def mlp_block(act, dy, wg, wu, wd, with_grad, block=256, wide=512):
    rows, dim = act.shape
    limit = wg.shape[0]
    tiles = pl.cdiv(limit, block)
    steps = tiles + with_grad * dim // wide
    cols = pl.BlockSpec((rows, block), lambda i: (0, jnp.minimum(i, tiles - 1)))
    tile = pl.BlockSpec((block, dim), lambda i: (jnp.minimum(i, tiles - 1), 0))
    full = pl.BlockSpec((rows, dim), lambda i: (0, 0), pipeline_mode=pl.Buffered(1))
    deep = 2 * block * (tiles if with_grad else 1)
    return pl.pallas_call(
        functools.partial(mlp_kernel, limit=limit, tiles=tiles),
        out_shape=[jax.ShapeDtypeStruct((rows, tiles * block), BF16)] * 3 + [jax.ShapeDtypeStruct((rows, dim), F32)] * with_grad,
        grid=(steps,),
        in_specs=[full, full, tile, tile, tile],
        out_specs=[cols] * 3 + [pl.BlockSpec((rows, wide), lambda i: (0, jnp.maximum(i - tiles, 0)))] * with_grad,
        scratch_shapes=[pltpu.VMEM((rows, deep), BF16)] * with_grad + [pltpu.VMEM((deep, dim), BF16)],
        compiler_params=pltpu.CompilerParams(vmem_limit_bytes=FULL),
        cost_estimate=cost((6 + 4 * with_grad) * rows * dim * limit),
        name="mlp_block",
    )(act, dy, wg, wu, wd)


def zero_kernel(after, out, zeros, sem):
    zeros[:] = jnp.zeros_like(zeros)
    step = zeros.shape[0]
    count = out.shape[0] // step

    def send(i, c):
        pltpu.make_async_copy(zeros, out.at[pl.ds(pl.multiple_of(i * step, step), step), :], sem).start()
        return c

    def wait(i, c):
        pltpu.make_async_copy(zeros, out.at[pl.ds(0, step), :], sem).wait()
        return c

    lax.fori_loop(0, count, send, 0)
    lax.fori_loop(0, count, wait, 0)


def zero_rows(after, rows, dim, step=200):
    return pl.pallas_call(
        zero_kernel,
        out_shape=jax.ShapeDtypeStruct((rows, dim), F32),
        in_specs=[pl.BlockSpec(memory_space=pltpu.SMEM)],
        out_specs=pl.BlockSpec(memory_space=pl.ANY),
        scratch_shapes=[pltpu.VMEM((step, dim), F32), pltpu.SemaphoreType.DMA],
        compiler_params=pltpu.CompilerParams(vmem_limit_bytes=8 * MIB),
        cost_estimate=cost(rows * dim),
        name="zero_rows",
    )(after)


def scatter_kernel(order, sid, runs, bounds, rows, base_hbm, out_hbm, sums, row_sem, sum_sem):
    lo = bounds[0]
    hi = bounds[1]

    def one(c):
        p, singles, multi = c
        n = runs[p]
        t = order[p]
        single = n == 1

        @pl.when(single)
        def _():
            pltpu.make_async_copy(rows.at[pl.ds(t, 1), :], out_hbm.at[pl.ds(sid[p], 1), :], row_sem).start()

        @pl.when(jnp.logical_not(single))
        def _():
            def add(j, acc):
                return acc + rows[pl.ds(order[p + j], 1), :]

            sums[pl.ds(multi, 1), :] = lax.fori_loop(1, n, add, rows[pl.ds(t, 1), :])

        return p + n, singles + single.astype(I32), multi + 1 - single.astype(I32)

    _, singles, multi = lax.while_loop(lambda c: c[0] < hi, one, (lo, 0, 0))

    def two(c):
        p, k = c
        n = runs[p]

        @pl.when(n > 1)
        def _():
            pltpu.make_async_copy(sums.at[pl.ds(k, 1), :], out_hbm.at[pl.ds(sid[p], 1), :], sum_sem).start()

        return p + n, k + (n > 1).astype(I32)

    lax.while_loop(lambda c: c[0] < hi, two, (lo, 0))

    def wait(sem):
        def body(i, c):
            pltpu.make_async_copy(sums.at[pl.ds(0, 1), :], out_hbm.at[pl.ds(0, 1), :], sem).wait()
            return c

        return body

    lax.fori_loop(0, singles, wait(row_sem), 0)
    lax.fori_loop(0, multi, wait(sum_sem), 0)


def scatter_rows(order, sid, runs, bounds, grads, base, tokens):
    _, dim = grads.shape
    rows = base.shape[0]
    return pl.pallas_call(
        scatter_kernel,
        out_shape=jax.ShapeDtypeStruct((rows, dim), F32),
        grid_spec=pltpu.PrefetchScalarGridSpec(
            num_scalar_prefetch=4,
            grid=(),
            in_specs=[pl.BlockSpec(memory_space=pltpu.VMEM), pl.BlockSpec(memory_space=pl.ANY)],
            out_specs=pl.BlockSpec(memory_space=pl.ANY),
            scratch_shapes=[pltpu.VMEM((tokens // 2, dim), F32), pltpu.SemaphoreType.DMA, pltpu.SemaphoreType.DMA],
        ),
        input_output_aliases={5: 0},
        compiler_params=pltpu.CompilerParams(vmem_limit_bytes=FULL),
        name="scatter_rows",
    )(order, sid, runs, bounds, grads, base)


def solution(mesh):
    cp_count = mesh.shape["cp"]
    tp_count = mesh.shape["tp"]
    both = ("cp", "tp")
    x_swap = [(i, i ^ 2) for i in range(cp_count)]
    core_swap = [(i, i ^ 1) for i in range(cp_count)]

    def compute(tokens, pos, doc_id, dy, table, w_q, w_k, w_v, w_o, w_gate, w_up, w_down, gain_one, gain_two, inv_freq):
        span = tokens.shape[0]
        total = span * cp_count
        part = span // tp_count
        rows, dim = table.shape
        head_dim = 2 * inv_freq.shape[0]
        heads = w_q.shape[1] // head_dim
        width = heads * head_dim
        tp_rank = lax.axis_index("tp")
        cp_rank = lax.axis_index("cp")
        core = cp_rank % 2
        gain_a = gain_one.astype(F32)
        gain_b = gain_two.astype(F32)

        barrier = lax.optimization_barrier
        join = lambda arr, axis: lax.all_gather(arr, axis, axis=0, tiled=True)
        add_up = lambda arr: lax.psum_scatter(arr, "tp", scatter_dimension=0, tiled=True)
        swap = lambda arr, pairs, axis="cp": lax.ppermute(arr, axis, pairs)
        local_ids = tokens - tp_rank * rows
        owned = (local_ids >= 0) & (local_ids < rows)
        safe_ids = jnp.where(owned, local_ids, jnp.arange(span) * (rows // span))
        picked = jnp.where(owned[:, None], jnp.take(table, safe_ids, axis=0), 0).astype(BF16)
        info = jnp.stack([cp_rank, core]).astype(I32)
        half = dim // 2
        near = 256
        wo_half = lax.dynamic_slice_in_dim(w_o, core * half, half, 1)
        wo_near = join(wo_half[:, :near], "tp")
        angle = pos.astype(F32)[:, None] * inv_freq[None, :]
        side_f = jnp.concatenate([jnp.cos(angle), jnp.sin(angle)], axis=1)
        side_i = jnp.stack([tokens, doc_id] * 4)
        x_all, x_slice, angles, ints = embed_gather(picked.reshape(tp_count, part, dim), side_f, side_i)
        angles = angles.reshape(total, head_dim)
        tok_all = ints[:, 0, :].reshape(total)
        doc_all = ints[:, 1, :].reshape(total)
        wo_far = barrier((wo_half[:, near:], x_all))[0]
        wo_rest = join(wo_far, "tp")

        dy_x = swap(barrier((dy, x_all))[0], x_swap)
        act_a, query, key, value = project_qkv(x_all, gain_a[None, :], w_q, w_k, w_v, angles)

        blk = span // 2
        blocks = total // blk
        doc_col = doc_all[:, None]
        doc_row = doc_all.reshape(blocks, 1, blk)
        attended, lse = attend(info, ints, query, key, value, doc_col, doc_row, head_dim, blk)

        gain_row = gain_b[None, :]
        att_parts, lse_all, residual, act_b, *wo_other = att_project(attended, lse, x_all, (wo_near, wo_rest), gain_row)
        lse_all = lse_all.reshape(total, 8)
        att_x = swap(att_parts, x_swap)

        wg, wu = w_gate.T, w_up.T
        ffn = wg.shape[0]
        hidden, d_gate, d_up, d_act_b = mlp_block(act_b, dy, wg, wu, w_down, True)
        d_act_b = add_up(d_act_b)
        act_x = out_proj(info, 2, x_all, att_x, (wo_near, wo_rest, *wo_other), gain_row)[1]
        hidden_x, d_gate_x, d_up_x = mlp_block(act_x, dy_x, wg, wu, w_down, False)
        d_act_b, hidden_x, d_gate_x, d_up_x = barrier((d_act_b, hidden_x, d_gate_x, d_up_x))
        d_act_b = to_bf16(d_act_b)
        acts, dys, hiddens, d_gates, d_ups = [(a, swap(a, core_swap), b, swap(b, core_swap)) for a, b in (
            (act_b, act_x), (dy, dy_x), (hidden, hidden_x), (d_gate, d_gate_x), (d_up, d_up_x))]
        heads_x = lax.dynamic_index_in_dim(att_x, tp_rank, 0, keepdims=False)
        head_parts = (attended, swap(attended, core_swap), heads_x, swap(heads_x, core_swap))
        att_heads = jnp.zeros((total, width), BF16)
        for k, piece in enumerate(head_parts):
            att_heads = lax.dynamic_update_slice_in_dim(att_heads, piece, (cp_rank ^ k) * span, 0)
        grad_down = weight_grad(info, hiddens, dys, rows=ffn)
        grad_gate = weight_grad(info, d_gates, acts, rows=ffn)
        grad_up = weight_grad(info, d_ups, acts, rows=ffn)

        def mine(arr):
            return lax.dynamic_slice_in_dim(arr, tp_rank * part, part, 0)

        res_part = mine(residual)
        normed_b, inv_b = rms_stats(res_part)
        grad_gain_b = jnp.sum(d_act_b * normed_b, axis=0)
        d_resid = mine(dy).astype(F32) + rms_back(d_act_b * gain_b, normed_b, inv_b)
        d_resid_all = join(d_resid.astype(BF16), both)
        out_part = nn(hidden[:, :ffn], w_down)
        d_resid_all, grad_down, att_heads, out_part = barrier((d_resid_all, grad_down, att_heads, out_part))
        out_slice = add_up(out_part)
        out_slice = (res_part + out_slice).astype(BF16)

        d_att = nt(d_resid_all, w_o)
        d_att_b = d_att.astype(BF16)
        head_of = (jnp.arange(width)[None, :] // head_dim == jnp.arange(8)[:, None]).astype(F32)
        prod = att_heads.astype(F32) * d_att_b.astype(F32)
        delta = lax.dot_general(head_of, prod, (((1,), (1,)), ((), ())), precision=lax.Precision.HIGHEST, preferred_element_type=F32)

        def by_block(arr):
            return jnp.transpose(arr.reshape(8, blocks, blk), (1, 0, 2))

        dqkv = attend_back(info, ints, query, key, value, d_att_b, doc_col, doc_row, lse_all, by_block(lse_all.T), delta.T, by_block(delta), angles, blk)
        d_act_a = sum(nt(dqkv[:, i * width:(i + 1) * width], w) for i, w in enumerate((w_q, w_k, w_v)))
        d_act_a, out_slice = barrier((d_act_a, out_slice))
        d_act_a = add_up(d_act_a)
        dqkv_x = swap(dqkv, x_swap)
        dqkvs = (dqkv, swap(dqkv, core_swap), dqkv_x, swap(dqkv_x, core_swap))
        grad_out = weight_grad(info, head_parts, [d_resid_all.reshape(cp_count, span, dim)] * 4)
        d_act_a, dqkv_x, grad_out, grad_up = barrier((d_act_a, dqkv_x, grad_out, grad_up))
        d_act_a = to_bf16(d_act_a)
        normed_a, inv_a = rms_stats(x_slice.astype(F32))
        grad_gain_a = jnp.sum(d_act_a * normed_a, axis=0)
        d_embed = d_resid + rms_back(d_act_a * gain_a, normed_a, inv_a)
        payload = jnp.concatenate([d_embed, jnp.stack([grad_gain_a, grad_gain_b] * 4)])
        gathered = join(payload, both)
        grad_qkv = weight_grad(info, [act_a.reshape(cp_count, span, dim)] * 4, dqkvs, splits=3)
        tok_all = barrier((tok_all, d_act_a))[0]
        slot_ids = jnp.arange(total, dtype=I32)
        before = (tok_all[None, :] < tok_all[:, None]) | ((tok_all[None, :] == tok_all[:, None]) & (slot_ids[None, :] < slot_ids[:, None]))
        rank = jnp.sum(before.astype(I32), axis=1)
        count = jnp.sum((tok_all[None, :] == tok_all[:, None]).astype(I32), axis=1)
        at_rank = rank[None, :] == slot_ids[:, None]
        runs = jnp.sum(jnp.where(at_rank, count[None, :], 0), axis=1)
        order = jnp.sum(jnp.where(at_rank, slot_ids[None, :], 0), axis=1)
        sid = jnp.sum(jnp.where(at_rank, tok_all[None, :], 0), axis=1) - tp_rank * rows
        order = order + 8 * (order // part)
        bounds = jnp.stack([jnp.sum((tok_all < tp_rank * rows).astype(I32)), jnp.sum((tok_all < (tp_rank + 1) * rows).astype(I32))])
        base = zero_rows(barrier((bounds, d_act_a))[0], rows, dim)
        gathered, grad_qkv, grad_gate, runs, order, sid, bounds, base = barrier((gathered, grad_qkv, grad_gate, runs, order, sid, bounds, base))
        out_slice = barrier((out_slice, gathered))[0]
        layer_out = join(out_slice, "tp")
        gain_grads = jnp.sum(gathered.reshape(cp_count * tp_count, part + 8, dim)[:, part:part + 2], axis=0)
        grad_table = scatter_rows(order, sid, runs, bounds, gathered, base, total)
        return (layer_out, grad_table, *grad_qkv, grad_out, grad_gate.T, grad_up.T, grad_down, gain_grads[0], gain_grads[1])

    col_spec = P(None, "tp")
    row_spec = P("tp")
    tok_spec = P("cp")
    rep_spec = P()
    in_specs = (tok_spec, tok_spec, tok_spec, P("cp"), row_spec, col_spec, col_spec, col_spec, row_spec, col_spec, col_spec, row_spec, rep_spec, rep_spec, rep_spec)
    out_specs = (P("cp"), row_spec, col_spec, col_spec, col_spec, row_spec, col_spec, col_spec, row_spec, rep_spec, rep_spec)
    return jax.shard_map(compute, mesh=mesh, in_specs=in_specs, out_specs=out_specs, check_vma=False)
```

```python
import functools
import jax
import jax.numpy as jnp
from jax import lax
from jax.experimental import pallas as pl
from jax.experimental.pallas import tpu as pltpu
from jax.sharding import PartitionSpec as P

NORM_EPS = 1e-5
NEG_BIG = -1e30
MIB = 2 ** 20
FULL = 62 * MIB
F32 = jnp.float32
BF16 = jnp.bfloat16
I32 = jnp.int32


def rms_stats(feats):
    inv_rms = lax.rsqrt(mean_row(feats * feats) + NORM_EPS)
    return feats * inv_rms, inv_rms


def rms_back(d_normed, normed, inv_rms):
    return inv_rms * (d_normed - normed * mean_row(d_normed * normed))


def to_bf16(feats):
    return feats.astype(BF16).astype(F32)


def contract(a, b, ca, cb):
    return lax.dot_general(a, b, (((ca,), (cb,)), ((), ())), preferred_element_type=F32)


def row_sum(t):
    return jnp.sum(t, 1, keepdims=True)


def mean_row(t):
    return row_sum(t) / t.shape[1]


def whole(a):
    return pl.BlockSpec(a.shape, lambda *i: (0,) * a.ndim)


def cost(flops):
    return pl.CostEstimate(flops=flops, bytes_accessed=flops // 512, transcendentals=0)


def nn(a, b):
    return contract(a, b, 1, 0)


def nt(a, b):
    return contract(a, b, 1, 1)


def tn(a, b):
    return contract(a, b, 0, 0)


DIMS = ("x", "y", "z")


class Place:
    def __init__(self):
        tp = lax.axis_index("tp")
        cp = lax.axis_index("cp")
        self.at = {"x": cp // 2, "core": cp % 2, "z": tp // 2, "y": tp % 2}

    def coord(self, dim, flip):
        return 1 - self.at[dim] if dim in flip else self.at[dim]

    def tp(self, flip=()):
        return self.coord("z", flip) * 2 + self.coord("y", flip)

    def cp(self, flip=()):
        return self.coord("x", flip) * 2 + self.coord("core", flip)

    def device(self, flip):
        return {"tp": self.tp(flip), "cp": self.cp(flip)}

    def slot(self, flip=()):
        return self.cp(flip) * 4 + self.tp(flip)

    def meet(self, dims):
        barrier = pltpu.get_barrier_semaphore()
        for d in dims:
            pl.semaphore_signal(barrier, inc=1, device_id=self.device((d,)), device_id_type=MESH)
        pl.semaphore_wait(barrier, len(dims))


MESH = pl.DeviceIdType.MESH
ORDERS = (("x", "y", "z"), ("y", "z", "x"), ("z", "x", "y"))
FLIPS = tuple(tuple(d for i, d in enumerate(DIMS) if n >> i & 1) for n in range(8))


def flip_code(flip):
    return sum(1 << DIMS.index(d) for d in flip)


def column_parts(width, count):
    tiles = width // 128
    sizes = [(tiles // count + (i < tiles % count)) * 128 for i in range(count)]
    return [(sum(sizes[:i]), n) for i, n in enumerate(sizes)]


class Gather:
    def __init__(self, place, buf, send, recv, core_send, core_recv):
        self.place, self.buf, self.send, self.recv, self.core_send, self.core_recv = place, buf, send, recv, core_send, core_recv
        self.parts = column_parts(buf.shape[2], 3)
        self.started = []

    def view(self, part, flip):
        start, size = self.parts[part]
        return self.buf.at[self.place.slot(flip), :, pl.ds(start, size)]

    def hop(self, part, flip, dim):
        there = tuple(d for d in DIMS if (d in flip) != (d == dim))
        index = part * 7 + flip_code(there) - 1
        ref = self.view(part, flip)
        return pltpu.make_async_remote_copy(src_ref=ref, dst_ref=ref, send_sem=self.send.at[index], recv_sem=self.recv.at[index], device_id=self.place.device((dim,)), device_id_type=MESH)

    def core_hop(self, part, flip):
        index = part * 8 + flip_code(flip)
        ref = self.view(part, flip)
        return pltpu.make_async_remote_copy(src_ref=ref, dst_ref=ref, send_sem=self.core_send.at[index], recv_sem=self.core_recv.at[index], device_id=self.place.device(("core",)), device_id_type=MESH)

    def go(self, copy):
        copy.start()
        self.started.append(copy)

    def wait(self, part, flip):
        order = ORDERS[part]
        last = max(order.index(d) for d in flip)
        came = tuple(d for d in flip if d != order[last])
        self.hop(part, came, order[last]).wait_recv()
        for dim in order[last + 1:]:
            self.go(self.hop(part, flip, dim))
        self.go(self.core_hop(part, flip))

    def run(self):
        for step in range(3):
            for part, order in enumerate(ORDERS):
                self.go(self.hop(part, (), order[step]))
        for part in range(3):
            self.go(self.core_hop(part, ()))
        for step in range(3):
            for flip in FLIPS[1:]:
                for part, order in enumerate(ORDERS):
                    if max(order.index(d) for d in flip) == step and len(flip) == 1:
                        self.wait(part, flip)
            for flip in FLIPS[1:]:
                for part, order in enumerate(ORDERS):
                    if max(order.index(d) for d in flip) == step and len(flip) > 1:
                        self.wait(part, flip)

    def finish(self, out, out_sem):
        rows = self.buf.shape[1]
        copies = []

        def store(flip):
            slot = self.place.slot(flip)
            c = pltpu.make_async_copy(self.buf.at[slot], out.at[pl.ds(slot * rows, rows), :], out_sem.at[len(copies)])
            c.start()
            copies.append(c)

        for flip in FLIPS:
            store(flip)
        for flip in FLIPS:
            other = flip + ("core",)
            for part in range(3):
                start, size = self.parts[part]
                ref = self.buf.at[self.place.slot(other), :, pl.ds(start, size)]
                index = part * 8 + flip_code(flip)
                pltpu.make_async_remote_copy(src_ref=ref, dst_ref=ref, send_sem=self.core_send.at[index], recv_sem=self.core_recv.at[index], device_id=self.place.device(("core",)), device_id_type=MESH).wait_recv()
            store(other)
        for c in self.started:
            c.wait_send()
        for c in copies:
            c.wait()


def embed_kernel(picked, side_f, side_i, out, slice_out, all_f, all_i, buf, r1, r2, tmp, send, recv, core_send, core_recv, out_sem, rs_send, rs_recv, side_send, side_recv, slice_sem):
    place = Place()
    place.meet(("x", "y", "z", "core"))
    half = buf.shape[2] // 2
    near = ("y", "z")

    sides = ((side_f, all_f), (side_i, all_i))
    started, keeps = [], []

    def side_hop(i, step):
        src, dst = sides[i]
        if step == 0:
            src_ref, slot, dim = src, place.cp(), "x"
        elif step == 1:
            src_ref, slot, dim = src, place.cp(), "core"
        else:
            src_ref, slot, dim = dst.at[place.cp(("x",))], place.cp(("x",)), "core"
        return pltpu.make_async_remote_copy(src_ref=src_ref, dst_ref=dst.at[slot], send_sem=side_send.at[i, step], recv_sem=side_recv.at[i, step], device_id=place.device((dim,)), device_id_type=MESH)

    def first(h, k):
        a, b = near[h], near[1 - h]
        target = place.tp((a,)) if k == 0 else place.tp((a, b))
        cols = pl.ds(h * half, half)
        return pltpu.make_async_remote_copy(src_ref=picked.at[target, :, cols], dst_ref=r1.at[h, k], send_sem=rs_send.at[h, k], recv_sem=rs_recv.at[h, k], device_id=place.device((a,)), device_id_type=MESH)

    def second(h):
        return pltpu.make_async_remote_copy(src_ref=tmp.at[h], dst_ref=r2.at[h], send_sem=rs_send.at[h, 2], recv_sem=rs_recv.at[h, 2], device_id=place.device((near[1 - h],)), device_id_type=MESH)

    def go(copy):
        copy.start()
        started.append(copy)

    for k in (1, 0):
        for h in range(2):
            go(first(h, k))
    for i in range(2):
        go(side_hop(i, 0))
        go(side_hop(i, 1))
        keeps.append(pltpu.make_async_copy(sides[i][0], sides[i][1].at[place.cp()], slice_sem.at[i]))
        keeps[i].start()
    for h in range(2):
        cols = slice(h * half, (h + 1) * half)
        first(h, 1).wait_recv()
        tmp[h] = picked[place.tp((near[1 - h],)), :, cols] + r1[h, 1]
        go(second(h))
    for i in range(2):
        side_hop(i, 0).wait_recv()
        go(side_hop(i, 2))
    mine = place.slot()
    for h in range(2):
        cols = slice(h * half, (h + 1) * half)
        first(h, 0).wait_recv()
        part = picked[place.tp(), :, cols] + r1[h, 0]
        second(h).wait_recv()
        buf[mine, :, cols] = part + r2[h]
    gather = Gather(place, buf, send, recv, core_send, core_recv)
    gather.run()
    keeps.append(pltpu.make_async_copy(buf.at[mine], slice_out, slice_sem.at[2]))
    keeps[-1].start()
    gather.finish(out, out_sem)
    for c in keeps:
        c.wait()
    for i in range(2):
        side_hop(i, 1).wait_recv()
        side_hop(i, 2).wait_recv()
    for c in started:
        c.wait_send()


def embed_gather(picked, side_f, side_i):
    _, rows, dim = picked.shape
    half = dim // 2
    dma = pltpu.SemaphoreType.DMA
    vmem = pl.BlockSpec(memory_space=pltpu.VMEM)
    hbm = pl.BlockSpec(memory_space=pl.ANY)
    return pl.pallas_call(
        embed_kernel,
        out_shape=[
            jax.ShapeDtypeStruct((16 * rows, dim), BF16),
            jax.ShapeDtypeStruct((rows, dim), BF16),
            jax.ShapeDtypeStruct((4,) + side_f.shape, F32),
            jax.ShapeDtypeStruct((4,) + side_i.shape, I32),
        ],
        in_specs=[vmem, vmem, vmem],
        out_specs=[pl.BlockSpec(memory_space=pltpu.HBM)] * 4,
        scratch_shapes=[
            pltpu.VMEM((16, rows, dim), BF16),
            pltpu.VMEM((2, 2, rows, half), BF16),
            pltpu.VMEM((2, rows, half), BF16),
            pltpu.VMEM((2, rows, half), BF16),
            dma((21,)), dma((21,)), dma((24,)), dma((24,)), dma((16,)),
            *[dma((2, 3))] * 4, dma((3,)),
        ],
        compiler_params=pltpu.CompilerParams(collective_id=0, has_side_effects=True, vmem_limit_bytes=FULL),
        name="embed_gather",
    )(picked, side_f, side_i)


def slot_block(j):
    return jnp.where(j < 4, 2 * j, 15 - 2 * j)


def unpack_angles(packed):
    turned = pltpu.roll(packed, packed.shape[1] // 2, 1)
    low = lax.broadcasted_iota(I32, packed.shape, 1) < packed.shape[1] // 2
    return jnp.where(low, packed, turned), jnp.where(low, -turned, packed)


def qkv_kernel(x, gain, wq, wk, wv, angles, act, q, k, v, wide, *, head_dim):
    width = wq.shape[1]

    @pl.when(pl.program_id(0) == 0)
    def _():
        for i, w in enumerate((wq, wk, wv)):
            wide[:, i * width:(i + 1) * width] = w[:]

    feats = x[:].astype(F32)
    inv = lax.rsqrt(mean_row(feats * feats) + NORM_EPS)
    a = (feats * inv * gain[:]).astype(BF16)
    act[:] = a
    t = nn(a, wide[:])
    cos, sin = unpack_angles(angles[:])
    for i, out in enumerate((q, k, v)):
        for h in range(width // head_dim):
            th = t[:, i * width + h * head_dim:i * width + (h + 1) * head_dim]
            if i < 2:
                th = th * cos + pltpu.roll(th, head_dim // 2, 1) * sin
            out[:, h * head_dim:(h + 1) * head_dim] = th.astype(BF16)


def project_qkv(x_all, gain, wq, wk, wv, angles, block=512):
    total, dim = x_all.shape
    width = wq.shape[1]
    head_dim = angles.shape[1]
    rows = lambda n: pl.BlockSpec((block, n), lambda i: (i, 0))
    whole = lambda a: pl.BlockSpec(a.shape, lambda i: (0, 0), pipeline_mode=pl.Buffered(1))
    return pl.pallas_call(
        functools.partial(qkv_kernel, head_dim=head_dim),
        out_shape=[jax.ShapeDtypeStruct((total, n), BF16) for n in (dim, width, width, width)],
        grid=(total // block,),
        in_specs=[rows(dim), whole(gain), whole(wq), whole(wk), whole(wv), rows(head_dim)],
        out_specs=[rows(dim), rows(width), rows(width), rows(width)],
        scratch_shapes=[pltpu.VMEM((dim, 3 * width), BF16)],
        compiler_params=pltpu.CompilerParams(vmem_limit_bytes=FULL),
        cost_estimate=cost(6 * total * dim * width),
        name="project_qkv",
    )(x_all, gain, wq, wk, wv, angles)


def block_range(info, ids, i, blocks):
    r = info[0]
    blk = ids.shape[2] // 2
    b = jnp.where(i == 0, r, blocks - 1 - r)

    def docs(shard, half):
        return ids[shard, 1, half * blk], ids[shard, 1, half * blk + blk - 1]

    first, last = docs(r, i)
    jmin, imax = 0, -1
    for j in range(blocks):
        begin, end = docs(min(j, blocks - 1 - j), int(j >= blocks // 2))
        jmin = jmin + (end < first).astype(I32)
        imax = imax + (begin <= last).astype(I32)
    return b, jmin, imax


def attend_kernel(info, ids, q, k, v, doc_col, doc_row, out, lse, sc, *, heads, head_dim, scale):
    blk = q.shape[0]
    b, jmin, _ = block_range(info, ids, pl.program_id(0), doc_row.shape[0])
    row_n = lax.broadcasted_iota(I32, (blk, blk), 0) + b * blk
    col_n = lax.broadcasted_iota(I32, (blk, blk), 1)

    def score(j, peaks):
        sb = slot_block(j)
        off = pl.multiple_of(sb * blk, blk)
        allowed = (doc_col[:] == doc_row[sb]) & (col_n + j * blk <= row_n)
        new = []
        for h in range(heads):
            cols = slice(h * head_dim, (h + 1) * head_dim)
            s = nt(q[:, cols], k[pl.ds(off, blk), cols]) * scale
            s = jnp.where(allowed, s, NEG_BIG)
            sc[j, h] = s
            new.append(jnp.maximum(peaks[h], jnp.max(s, axis=1, keepdims=True)))
        return tuple(new)

    peaks = lax.fori_loop(jmin, b + 1, score, tuple(jnp.full((blk, 1), NEG_BIG, F32) for _ in range(heads)))

    def weigh(j, sums):
        new = []
        for h in range(heads):
            p = jnp.exp(sc[j, h] - peaks[h])
            sc[j, h] = p
            new.append(sums[h] + row_sum(p))
        return tuple(new)

    sums = lax.fori_loop(jmin, b + 1, weigh, tuple(jnp.zeros((blk, 1), F32) for _ in range(heads)))
    inv = tuple(1.0 / t for t in sums)
    for h in range(heads):
        lse[:, h:h + 1] = peaks[h] + jnp.log(sums[h])

    def mix(j, acc):
        off = pl.multiple_of(slot_block(j) * blk, blk)
        new = []
        for h in range(heads):
            cols = slice(h * head_dim, (h + 1) * head_dim)
            new.append(acc[h] + nn((sc[j, h] * inv[h]).astype(BF16), v[pl.ds(off, blk), cols]))
        return tuple(new)

    acc = lax.fori_loop(jmin, b + 1, mix, tuple(jnp.zeros((blk, head_dim), F32) for _ in range(heads)))
    for h in range(heads):
        out[:, h * head_dim:(h + 1) * head_dim] = acc[h].astype(BF16)


def attend(info, ids, q, k, v, doc_col, doc_row, head_dim, blk):
    total, width = k.shape
    heads = width // head_dim
    mine = lambda n: pl.BlockSpec((blk, n), lambda i, info, ids: (2 * info[0] + i, 0))
    return pl.pallas_call(
        functools.partial(attend_kernel, heads=heads, head_dim=head_dim, scale=head_dim ** -0.5),
        out_shape=[jax.ShapeDtypeStruct((2 * blk, width), BF16), jax.ShapeDtypeStruct((2 * blk, 8), F32)],
        grid_spec=pltpu.PrefetchScalarGridSpec(
            num_scalar_prefetch=2,
            grid=(2,),
            in_specs=[mine(width), whole(k), whole(v), mine(1), whole(doc_row)],
            out_specs=[pl.BlockSpec((blk, width), lambda i, info, ids: (i, 0)), pl.BlockSpec((blk, 8), lambda i, info, ids: (i, 0))],
            scratch_shapes=[pltpu.VMEM((total // blk, heads, blk, blk), F32)],
        ),
        compiler_params=pltpu.CompilerParams(vmem_limit_bytes=FULL),
        cost_estimate=cost(4 * 2 * blk * total * width),
        name="attend",
    )(info, ids, q, k, v, doc_col, doc_row)


def attend_back_kernel(info, ids, q, k, v, do, doc_col, doc_row, lse_col, lse_row, del_col, del_row, angles, out, acc, *, heads, head_dim, scale):
    blk = angles.shape[0]
    width = heads * head_dim
    i = pl.program_id(0)
    b, jmin, imax = block_range(info, ids, i, doc_row.shape[0])
    me = pl.multiple_of((2 * info[0] + i) * blk, blk)
    mine = pl.ds(me, blk)
    iota_r = lax.broadcasted_iota(I32, (blk, blk), 0)
    iota_c = lax.broadcasted_iota(I32, (blk, blk), 1)
    acc[:] = jnp.zeros_like(acc)
    spans = [slice(h * head_dim, (h + 1) * head_dim) for h in range(heads)]

    def for_query(j, c):
        sb = slot_block(j)
        there = pl.ds(pl.multiple_of(sb * blk, blk), blk)
        allowed = (doc_col[mine, :] == doc_row[sb]) & (iota_c + j * blk <= iota_r + b * blk)
        for h, cols in enumerate(spans):
            s = jnp.where(allowed, nt(q[mine, cols], k[there, cols]) * scale, NEG_BIG)
            p = jnp.exp(s - lse_col[mine, h:h + 1])
            dp = to_bf16(nt(do[mine, cols], v[there, cols]))
            ds = (p * (dp - del_col[mine, h:h + 1]) * scale).astype(BF16)
            acc[0, :, cols] += nn(ds, k[there, cols])
        return c

    lax.fori_loop(jmin, b + 1, for_query, 0)

    def for_key(j, c):
        sb = slot_block(j)
        there = pl.ds(pl.multiple_of(sb * blk, blk), blk)
        allowed = (doc_col[mine, :] == doc_row[sb]) & (iota_r + b * blk <= iota_c + j * blk)
        for h, cols in enumerate(spans):
            s = jnp.where(allowed, nt(k[mine, cols], q[there, cols]) * scale, NEG_BIG)
            p = jnp.exp(s - lse_row[sb, h:h + 1, :])
            dp = to_bf16(nt(v[mine, cols], do[there, cols]))
            ds = (p * (dp - del_row[sb, h:h + 1, :]) * scale).astype(BF16)
            acc[2, :, cols] += nn(p.astype(BF16), do[there, cols])
            acc[1, :, cols] += nn(ds, q[there, cols])
        return c

    lax.fori_loop(b, imax + 1, for_key, 0)
    cos, sin = unpack_angles(angles[:])
    for part in range(3):
        for h, cols in enumerate(spans):
            t = acc[part, :, cols]
            if part < 2:
                t = to_bf16(t)
                t = t * cos - pltpu.roll(t, head_dim // 2, 1) * sin
            out[:, part * width + h * head_dim:part * width + (h + 1) * head_dim] = t.astype(BF16)


def attend_back(info, ids, q, k, v, do, doc_col, doc_row, lse_col, lse_row, del_col, del_row, angles, blk):
    total, width = k.shape
    head_dim = angles.shape[1]
    heads = width // head_dim
    mine = lambda n: pl.BlockSpec((blk, n), lambda i, info, ids: (2 * info[0] + i, 0))
    arrays = (q, k, v, do, doc_col, doc_row, lse_col, lse_row, del_col, del_row)
    return pl.pallas_call(
        functools.partial(attend_back_kernel, heads=heads, head_dim=head_dim, scale=head_dim ** -0.5),
        out_shape=jax.ShapeDtypeStruct((2 * blk, 3 * width), BF16),
        grid_spec=pltpu.PrefetchScalarGridSpec(
            num_scalar_prefetch=2,
            grid=(2,),
            in_specs=[whole(a) for a in arrays] + [mine(head_dim)],
            out_specs=pl.BlockSpec((blk, 3 * width), lambda i, info, ids: (i, 0)),
            scratch_shapes=[pltpu.VMEM((3, blk, width), F32)],
        ),
        compiler_params=pltpu.CompilerParams(vmem_limit_bytes=FULL),
        cost_estimate=cost(14 * 2 * blk * total * width // 2),
        name="attend_back",
    )(info, ids, *arrays, angles)


def att_kernel(att, lse, x_all, w, gain, lse_out, res, act, parts, x, wide, send, recv, lse_send, lse_recv, load, swap_send, swap_recv):
    place = Place()
    rows, width = att.shape
    half = w.shape[1]
    mine = place.cp()
    loads = [pltpu.make_async_copy(src, dst, load.at[i]) for i, (src, dst) in enumerate(((x_all.at[pl.ds(mine * rows, rows), :], x), (w, wide.at[0])))]
    for c in loads:
        c.start()
    place.meet(("y", "z", "x", "core"))
    started = []
    near = ("y", "z")
    spans = column_parts(width, 2)

    def hop(p, flip, dim):
        there = tuple(d for d in near if (d in flip) != (d == dim))
        index = p * 3 + (there == ("y",)) + 2 * (there == ("z",))
        start, size = spans[p]
        cols = pl.ds(start, size)
        slot = place.tp(flip)
        src = parts.at[slot, :, cols] if flip else att.at[:, cols]
        return pltpu.make_async_remote_copy(src_ref=src, dst_ref=parts.at[slot, :, cols], send_sem=send.at[index], recv_sem=recv.at[index], device_id=place.device((dim,)), device_id_type=MESH)

    def lse_hop(step):
        src, slot, dim = ((lse, mine, "x"), (lse, mine, "core"), (lse_out.at[place.cp(("x",))], place.cp(("x",)), "core"))[step]
        return pltpu.make_async_remote_copy(src_ref=src, dst_ref=lse_out.at[slot], send_sem=lse_send.at[step], recv_sem=lse_recv.at[step], device_id=place.device((dim,)), device_id_type=MESH)

    def go(copy):
        copy.start()
        started.append(copy)

    other = pltpu.make_async_remote_copy(src_ref=w, dst_ref=wide.at[1], send_sem=swap_send, recv_sem=swap_recv, device_id=place.device(("core",)), device_id_type=MESH)
    for step in range(2):
        for p in range(2):
            go(hop(p, (), near[(p + step) % 2]))
    go(other)
    go(lse_hop(0))
    go(lse_hop(1))
    lse_out[mine] = lse[:]
    for c in loads:
        c.wait()

    def add(piece, slot, halves=(0, 1), first=False):
        for i in halves:
            cols = pl.ds(pl.multiple_of(place.coord("core", ("core",) if i else ()) * half, 128), half)
            t = nn(piece, wide[i, pl.ds(pl.multiple_of(slot * width, width), width), :])
            res[:, cols] = t + (x[:, cols].astype(F32) if first else res[:, cols])

    add(att[:], place.tp(), (0,), True)
    for p in range(2):
        hop(p, (), near[p]).wait_recv()
        go(hop(p, (near[p],), near[1 - p]))
    lse_hop(0).wait_recv()
    go(lse_hop(2))
    other.wait_recv()
    add(att[:], place.tp(), (1,), True)
    for p in (1, 0):
        hop(p, (), near[1 - p]).wait_recv()
        slot = place.tp((near[1 - p],))
        add(parts[slot], slot)
    for p in range(2):
        hop(p, (near[p],), near[1 - p]).wait_recv()
    slot = place.tp(near)
    add(parts[slot], slot)
    h = res[:]
    act[:] = (h * lax.rsqrt(mean_row(h * h) + NORM_EPS) * gain[:]).astype(BF16)
    lse_hop(1).wait_recv()
    lse_hop(2).wait_recv()
    for c in started:
        c.wait_send()


def att_project(att, lse, x_all, w, gain):
    rows, width = att.shape
    dim = x_all.shape[1]
    dma = pltpu.SemaphoreType.DMA
    vmem = pl.BlockSpec(memory_space=pltpu.VMEM)
    hbm = pl.BlockSpec(memory_space=pl.ANY)
    return pl.pallas_call(
        att_kernel,
        out_shape=[jax.ShapeDtypeStruct((4,) + lse.shape, F32), jax.ShapeDtypeStruct((rows, dim), F32), jax.ShapeDtypeStruct((rows, dim), BF16)],
        in_specs=[vmem, vmem, hbm, hbm, vmem],
        out_specs=[vmem] * 3,
        scratch_shapes=[
            pltpu.VMEM((4, rows, width), BF16), pltpu.VMEM((rows, dim), BF16), pltpu.VMEM((2,) + w.shape, BF16),
            *[dma((n,)) for n in (6, 6, 3, 3, 2)], dma, dma,
        ],
        compiler_params=pltpu.CompilerParams(collective_id=1, has_side_effects=True, vmem_limit_bytes=FULL),
        name="att_project",
    )(att, lse, x_all, w, gain)


def weight_grad_kernel(info, *refs, pieces, splits):
    lhs = refs[:pieces]
    rhs = refs[pieces:2 * pieces]
    outs = refs[2 * pieces:]
    t = tn(lhs[0][:], rhs[0][:])
    for a, b in zip(lhs[1:], rhs[1:]):
        t += tn(a[:], b[:])
    width = t.shape[1] // splits
    for i, out in enumerate(outs):
        out[:] = t[:, i * width:(i + 1) * width]


def weight_grad(info, lhs, rhs, block=256, splits=1, rows=None):
    def spec(arr, p, cols, moving):
        if arr.ndim == 3:
            return pl.BlockSpec((None, arr.shape[1], cols), lambda i, info: (info[0] ^ p, 0, i if moving else 0))
        return pl.BlockSpec((arr.shape[0], cols), lambda i, info: (0, i if moving else 0))

    tokens = lhs[0].shape[-2]
    rows, dim = rows or lhs[0].shape[-1], rhs[0].shape[-1]
    n = len(lhs)
    width = dim // splits
    outs = pl.pallas_call(
        functools.partial(weight_grad_kernel, pieces=n, splits=splits),
        out_shape=[jax.ShapeDtypeStruct((rows, width), F32)] * splits,
        grid_spec=pltpu.PrefetchScalarGridSpec(
            num_scalar_prefetch=1,
            grid=(pl.cdiv(rows, block),),
            in_specs=[spec(a, p, block, True) for p, a in enumerate(lhs)] + [spec(b, p, dim, False) for p, b in enumerate(rhs)],
            out_specs=[pl.BlockSpec((block, width), lambda i, info: (i, 0))] * splits,
        ),
        compiler_params=pltpu.CompilerParams(vmem_limit_bytes=56 * MIB),
        cost_estimate=cost(2 * n * tokens * rows * dim),
        name="weight_grad",
    )(info, *lhs, *rhs)
    return outs if splits > 1 else outs[0]


def mlp_kernel(act, dy, wg, wu, wd, hidden, d_gate, d_up, *rest, limit, tiles):
    i = pl.program_id(0)
    block = wg.shape[0]
    both = rest[-1]

    @pl.when(i < tiles)
    def _():
        left = limit - i * block
        row_ok = lax.broadcasted_iota(I32, (block, 1), 0) < left
        col_ok = lax.broadcasted_iota(I32, (1, block), 1) < left
        pair = pl.ds(pl.multiple_of(2 * i * block, block), 2 * block) if tiles < pl.num_programs(0) else slice(2 * block)
        both[pair] = jnp.concatenate([jnp.where(row_ok, w[:], 0).astype(BF16) for w in (wg, wu)])
        t = nt(act[:], both[pair])
        gate, up = t[:, :block], t[:, block:]
        dh = jnp.where(col_ok, to_bf16(nt(dy[:], wd[:])), 0)
        sig = jax.nn.sigmoid(gate)
        hidden[:] = (gate * sig * up).astype(BF16)
        dg = (dh * up * sig * (1.0 + gate * (1.0 - sig))).astype(BF16)
        du = (dh * gate * sig).astype(BF16)
        d_gate[:] = dg
        d_up[:] = du
        if len(rest) > 1:
            rest[1][:, pair] = jnp.concatenate([dg, du], axis=1)

    if len(rest) > 1:
        grad, grads = rest[:2]

        @pl.when(i >= tiles)
        def _():
            wide = grad.shape[1]
            grad[:] = nn(grads[:], both[:, pl.ds(pl.multiple_of((i - tiles) * wide, wide), wide)])


def mlp_block(act, dy, wg, wu, wd, with_grad, block=256, wide=512):
    rows, dim = act.shape
    limit = wg.shape[0]
    tiles = pl.cdiv(limit, block)
    steps = tiles + with_grad * dim // wide
    cols = pl.BlockSpec((rows, block), lambda i: (0, jnp.minimum(i, tiles - 1)))
    tile = pl.BlockSpec((block, dim), lambda i: (jnp.minimum(i, tiles - 1), 0))
    full = pl.BlockSpec((rows, dim), lambda i: (0, 0), pipeline_mode=pl.Buffered(1))
    deep = 2 * block * (tiles if with_grad else 1)
    return pl.pallas_call(
        functools.partial(mlp_kernel, limit=limit, tiles=tiles),
        out_shape=[jax.ShapeDtypeStruct((rows, tiles * block), BF16)] * 3 + [jax.ShapeDtypeStruct((rows, dim), F32)] * with_grad,
        grid=(steps,),
        in_specs=[full, full, tile, tile, tile],
        out_specs=[cols] * 3 + [pl.BlockSpec((rows, wide), lambda i: (0, jnp.maximum(i - tiles, 0)))] * with_grad,
        scratch_shapes=[pltpu.VMEM((rows, deep), BF16)] * with_grad + [pltpu.VMEM((deep, dim), BF16)],
        compiler_params=pltpu.CompilerParams(vmem_limit_bytes=FULL),
        cost_estimate=cost((6 + 4 * with_grad) * rows * dim * limit),
        name="mlp_block",
    )(act, dy, wg, wu, wd)


def zero_kernel(after, out, zeros, sem):
    zeros[:] = jnp.zeros_like(zeros)
    step = zeros.shape[0]
    count = out.shape[0] // step

    def send(i, c):
        pltpu.make_async_copy(zeros, out.at[pl.ds(pl.multiple_of(i * step, step), step), :], sem).start()
        return c

    def wait(i, c):
        pltpu.make_async_copy(zeros, out.at[pl.ds(0, step), :], sem).wait()
        return c

    lax.fori_loop(0, count, send, 0)
    lax.fori_loop(0, count, wait, 0)


def zero_rows(after, rows, dim, step=200):
    return pl.pallas_call(
        zero_kernel,
        out_shape=jax.ShapeDtypeStruct((rows, dim), F32),
        in_specs=[pl.BlockSpec(memory_space=pltpu.SMEM)],
        out_specs=pl.BlockSpec(memory_space=pl.ANY),
        scratch_shapes=[pltpu.VMEM((step, dim), F32), pltpu.SemaphoreType.DMA],
        compiler_params=pltpu.CompilerParams(vmem_limit_bytes=8 * MIB),
        cost_estimate=cost(rows * dim),
        name="zero_rows",
    )(after)


def scatter_kernel(order, sid, runs, bounds, rows, base_hbm, out_hbm, sums, row_sem, sum_sem):
    lo = bounds[0]
    hi = bounds[1]

    def one(c):
        p, singles, multi = c
        n = runs[p]
        t = order[p]
        single = n == 1

        @pl.when(single)
        def _():
            pltpu.make_async_copy(rows.at[pl.ds(t, 1), :], out_hbm.at[pl.ds(sid[p], 1), :], row_sem).start()

        @pl.when(jnp.logical_not(single))
        def _():
            def add(j, acc):
                return acc + rows[pl.ds(order[p + j], 1), :]

            sums[pl.ds(multi, 1), :] = lax.fori_loop(1, n, add, rows[pl.ds(t, 1), :])

        return p + n, singles + single.astype(I32), multi + 1 - single.astype(I32)

    _, singles, multi = lax.while_loop(lambda c: c[0] < hi, one, (lo, 0, 0))

    def two(c):
        p, k = c
        n = runs[p]

        @pl.when(n > 1)
        def _():
            pltpu.make_async_copy(sums.at[pl.ds(k, 1), :], out_hbm.at[pl.ds(sid[p], 1), :], sum_sem).start()

        return p + n, k + (n > 1).astype(I32)

    lax.while_loop(lambda c: c[0] < hi, two, (lo, 0))

    def wait(sem):
        def body(i, c):
            pltpu.make_async_copy(sums.at[pl.ds(0, 1), :], out_hbm.at[pl.ds(0, 1), :], sem).wait()
            return c

        return body

    lax.fori_loop(0, singles, wait(row_sem), 0)
    lax.fori_loop(0, multi, wait(sum_sem), 0)


def scatter_rows(order, sid, runs, bounds, grads, base, tokens):
    _, dim = grads.shape
    rows = base.shape[0]
    return pl.pallas_call(
        scatter_kernel,
        out_shape=jax.ShapeDtypeStruct((rows, dim), F32),
        grid_spec=pltpu.PrefetchScalarGridSpec(
            num_scalar_prefetch=4,
            grid=(),
            in_specs=[pl.BlockSpec(memory_space=pltpu.VMEM), pl.BlockSpec(memory_space=pl.ANY)],
            out_specs=pl.BlockSpec(memory_space=pl.ANY),
            scratch_shapes=[pltpu.VMEM((tokens // 2, dim), F32), pltpu.SemaphoreType.DMA, pltpu.SemaphoreType.DMA],
        ),
        input_output_aliases={5: 0},
        compiler_params=pltpu.CompilerParams(vmem_limit_bytes=FULL),
        name="scatter_rows",
    )(order, sid, runs, bounds, grads, base)


def solution(mesh):
    cp_count = mesh.shape["cp"]
    tp_count = mesh.shape["tp"]
    both = ("cp", "tp")
    x_swap = [(i, i ^ 2) for i in range(cp_count)]
    core_swap = [(i, i ^ 1) for i in range(cp_count)]

    def compute(tokens, pos, doc_id, dy, table, w_q, w_k, w_v, w_o, w_gate, w_up, w_down, gain_one, gain_two, inv_freq):
        span = tokens.shape[0]
        total = span * cp_count
        part = span // tp_count
        rows, dim = table.shape
        head_dim = 2 * inv_freq.shape[0]
        heads = w_q.shape[1] // head_dim
        width = heads * head_dim
        tp_rank = lax.axis_index("tp")
        cp_rank = lax.axis_index("cp")
        core = cp_rank % 2
        gain_a = gain_one.astype(F32)
        gain_b = gain_two.astype(F32)

        barrier = lax.optimization_barrier
        join = lambda arr, axis: lax.all_gather(arr, axis, axis=0, tiled=True)
        add_up = lambda arr: lax.psum_scatter(arr, "tp", scatter_dimension=0, tiled=True)
        swap = lambda arr, pairs, axis="cp": lax.ppermute(arr, axis, pairs)
        local_ids = tokens - tp_rank * rows
        owned = (local_ids >= 0) & (local_ids < rows)
        safe_ids = jnp.where(owned, local_ids, jnp.arange(span) * (rows // span))
        picked = jnp.where(owned[:, None], jnp.take(table, safe_ids, axis=0), 0).astype(BF16)
        info = jnp.stack([cp_rank, core]).astype(I32)
        half = dim // 2
        angle = pos.astype(F32)[:, None] * inv_freq[None, :]
        side_f = jnp.concatenate([jnp.cos(angle), jnp.sin(angle)], axis=1)
        side_i = jnp.stack([tokens, doc_id] * 4)
        x_all, x_slice, angles, ints = embed_gather(picked.reshape(tp_count, part, dim), side_f, side_i)
        angles = angles.reshape(total, head_dim)
        tok_all = ints[:, 0, :].reshape(total)
        doc_all = ints[:, 1, :].reshape(total)
        wo_half = barrier((lax.dynamic_slice_in_dim(w_o, core * half, half, 1), x_all))[0]
        wo_half = join(wo_half, "tp")

        dy_x = swap(barrier((dy, x_all))[0], x_swap)
        act_a, query, key, value = project_qkv(x_all, gain_a[None, :], w_q, w_k, w_v, angles)

        blk = span // 2
        blocks = total // blk
        doc_col = doc_all[:, None]
        doc_row = doc_all.reshape(blocks, 1, blk)
        attended, lse = attend(info, ints, query, key, value, doc_col, doc_row, head_dim, blk)

        tok_all = barrier((tok_all, attended))[0]
        slot_ids = jnp.arange(total, dtype=I32)
        before = (tok_all[None, :] < tok_all[:, None]) | ((tok_all[None, :] == tok_all[:, None]) & (slot_ids[None, :] < slot_ids[:, None]))
        rank = jnp.sum(before.astype(I32), axis=1)
        count = jnp.sum((tok_all[None, :] == tok_all[:, None]).astype(I32), axis=1)
        at_rank = rank[None, :] == slot_ids[:, None]
        runs = jnp.sum(jnp.where(at_rank, count[None, :], 0), axis=1)
        order = jnp.sum(jnp.where(at_rank, slot_ids[None, :], 0), axis=1)
        sid = jnp.sum(jnp.where(at_rank, tok_all[None, :], 0), axis=1) - tp_rank * rows
        order = order + 8 * (order // part)
        bounds = jnp.stack([jnp.sum((tok_all < tp_rank * rows).astype(I32)), jnp.sum((tok_all < (tp_rank + 1) * rows).astype(I32))])
        wo_half, runs, order, sid, bounds = barrier((wo_half, runs, order, sid, bounds))
        heads_x = swap(attended, x_swap)
        lse_all, residual, act_b = att_project(attended, lse, x_all, wo_half, gain_b[None, :])
        lse_all = lse_all.reshape(total, 8)
        act_x = swap(act_b, x_swap)
        wg, wu = w_gate.T, w_up.T
        ffn = wg.shape[0]
        hidden, d_gate, d_up, d_act_b = mlp_block(act_b, dy, wg, wu, w_down, True)
        d_act_b = add_up(d_act_b)
        hidden_x, d_gate_x, d_up_x = mlp_block(act_x, dy_x, wg, wu, w_down, False)
        out_part = nn(hidden[:, :ffn], w_down)
        d_act_b, hidden_x, d_gate_x, d_up_x, out_part = barrier((d_act_b, hidden_x, d_gate_x, d_up_x, out_part))
        d_act_b = to_bf16(d_act_b)
        acts, dys, hiddens, d_gates, d_ups = [(a, swap(a, core_swap), b, swap(b, core_swap)) for a, b in (
            (act_b, act_x), (dy, dy_x), (hidden, hidden_x), (d_gate, d_gate_x), (d_up, d_up_x))]
        head_parts = (attended, swap(attended, core_swap), heads_x, swap(heads_x, core_swap))
        att_heads = jnp.zeros((total, width), BF16)
        for k, piece in enumerate(head_parts):
            att_heads = lax.dynamic_update_slice_in_dim(att_heads, piece, (cp_rank ^ k) * span, 0)
        grad_down = weight_grad(info, hiddens, dys, rows=ffn)
        grad_gate = weight_grad(info, d_gates, acts, rows=ffn)
        grad_up = weight_grad(info, d_ups, acts, rows=ffn)

        def mine(arr):
            return lax.dynamic_slice_in_dim(arr, tp_rank * part, part, 0)

        res_part = mine(residual)
        normed_b, inv_b = rms_stats(res_part)
        grad_gain_b = jnp.sum(d_act_b * normed_b, axis=0)
        d_resid = mine(dy).astype(F32) + rms_back(d_act_b * gain_b, normed_b, inv_b)
        d_resid_all = join(d_resid.astype(BF16), both)
        d_resid_all, grad_down, att_heads, out_part = barrier((d_resid_all, grad_down, att_heads, out_part))
        out_slice = add_up(out_part)
        out_slice = (res_part + out_slice).astype(BF16)

        d_att = nt(d_resid_all, w_o)
        d_att_b = d_att.astype(BF16)
        head_of = (jnp.arange(width)[None, :] // head_dim == jnp.arange(8)[:, None]).astype(F32)
        prod = att_heads.astype(F32) * d_att_b.astype(F32)
        delta = lax.dot_general(head_of, prod, (((1,), (1,)), ((), ())), precision=lax.Precision.HIGHEST, preferred_element_type=F32)

        def by_block(arr):
            return jnp.transpose(arr.reshape(8, blocks, blk), (1, 0, 2))

        dqkv = attend_back(info, ints, query, key, value, d_att_b, doc_col, doc_row, lse_all, by_block(lse_all.T), delta.T, by_block(delta), angles, blk)
        d_act_a = sum(nt(dqkv[:, i * width:(i + 1) * width], w) for i, w in enumerate((w_q, w_k, w_v)))
        d_act_a, out_slice = barrier((d_act_a, out_slice))
        d_act_a = add_up(d_act_a)
        dqkv_x = swap(dqkv, x_swap)
        dqkvs = (dqkv, swap(dqkv, core_swap), dqkv_x, swap(dqkv_x, core_swap))
        grad_out = weight_grad(info, head_parts, [d_resid_all.reshape(cp_count, span, dim)] * 4)
        d_act_a, dqkv_x, grad_out, grad_up = barrier((d_act_a, dqkv_x, grad_out, grad_up))
        d_act_a = to_bf16(d_act_a)
        normed_a, inv_a = rms_stats(x_slice.astype(F32))
        grad_gain_a = jnp.sum(d_act_a * normed_a, axis=0)
        d_embed = d_resid + rms_back(d_act_a * gain_a, normed_a, inv_a)
        payload = jnp.concatenate([d_embed, jnp.stack([grad_gain_a, grad_gain_b] * 4)])
        gathered = join(payload, both)
        grad_qkv = weight_grad(info, [act_a.reshape(cp_count, span, dim)] * 4, dqkvs, splits=3)
        base = zero_rows(barrier((bounds, d_act_a))[0], rows, dim)
        gathered, grad_qkv, grad_gate, base = barrier((gathered, grad_qkv, grad_gate, base))
        out_slice = barrier((out_slice, gathered))[0]
        layer_out = jnp.concatenate([out_slice] * tp_count)
        for k in range(1, tp_count):
            piece = swap(out_slice, [(i, i ^ k) for i in range(tp_count)], "tp")
            layer_out = lax.dynamic_update_slice_in_dim(layer_out, piece, (tp_rank ^ k) * part, 0)
        gain_grads = jnp.sum(gathered.reshape(cp_count * tp_count, part + 8, dim)[:, part:part + 2], axis=0)
        grad_table = scatter_rows(order, sid, runs, bounds, gathered, base, total)
        return (layer_out, grad_table, *grad_qkv, grad_out, grad_gate.T, grad_up.T, grad_down, gain_grads[0], gain_grads[1])

    col_spec = P(None, "tp")
    row_spec = P("tp")
    tok_spec = P("cp")
    rep_spec = P()
    in_specs = (tok_spec, tok_spec, tok_spec, P("cp"), row_spec, col_spec, col_spec, col_spec, row_spec, col_spec, col_spec, row_spec, rep_spec, rep_spec, rep_spec)
    out_specs = (P("cp"), row_spec, col_spec, col_spec, col_spec, row_spec, col_spec, col_spec, row_spec, rep_spec, rep_spec)
    return jax.shard_map(compute, mesh=mesh, in_specs=in_specs, out_specs=out_specs, check_vma=False)
```

```python
import functools
import jax
import jax.numpy as jnp
from jax import lax
from jax.experimental import pallas as pl
from jax.experimental.pallas import tpu as pltpu
from jax.sharding import PartitionSpec as P

NORM_EPS = 1e-5
NEG_BIG = -1e30
MIB = 2 ** 20
FULL = 62 * MIB
F32 = jnp.float32
BF16 = jnp.bfloat16
I32 = jnp.int32


def rms_stats(feats):
    inv_rms = lax.rsqrt(mean_row(feats * feats) + NORM_EPS)
    return feats * inv_rms, inv_rms


def rms_back(d_normed, normed, inv_rms):
    return inv_rms * (d_normed - normed * mean_row(d_normed * normed))


def to_bf16(feats):
    return feats.astype(BF16).astype(F32)


def contract(a, b, ca, cb):
    return lax.dot_general(a, b, (((ca,), (cb,)), ((), ())), preferred_element_type=F32)


def row_sum(t):
    return jnp.sum(t, 1, keepdims=True)


def mean_row(t):
    return row_sum(t) / t.shape[1]


def whole(a):
    return pl.BlockSpec(a.shape, lambda *i: (0,) * a.ndim)


def cost(flops):
    return pl.CostEstimate(flops=flops, bytes_accessed=flops // 512, transcendentals=0)


def nn(a, b):
    return contract(a, b, 1, 0)


def nt(a, b):
    return contract(a, b, 1, 1)


def tn(a, b):
    return contract(a, b, 0, 0)


DIMS = ("x", "y", "z")


class Place:
    def __init__(self):
        tp = lax.axis_index("tp")
        cp = lax.axis_index("cp")
        self.at = {"x": cp // 2, "core": cp % 2, "z": tp // 2, "y": tp % 2}

    def coord(self, dim, flip):
        return 1 - self.at[dim] if dim in flip else self.at[dim]

    def tp(self, flip=()):
        return self.coord("z", flip) * 2 + self.coord("y", flip)

    def cp(self, flip=()):
        return self.coord("x", flip) * 2 + self.coord("core", flip)

    def device(self, flip):
        return {"tp": self.tp(flip), "cp": self.cp(flip)}

    def slot(self, flip=()):
        return self.cp(flip) * 4 + self.tp(flip)

    def meet(self, dims):
        barrier = pltpu.get_barrier_semaphore()
        for d in dims:
            pl.semaphore_signal(barrier, inc=1, device_id=self.device((d,)), device_id_type=MESH)
        pl.semaphore_wait(barrier, len(dims))


MESH = pl.DeviceIdType.MESH
ORDERS = (("x", "y", "z"), ("y", "z", "x"), ("z", "x", "y"))
FLIPS = tuple(tuple(d for i, d in enumerate(DIMS) if n >> i & 1) for n in range(8))


def flip_code(flip):
    return sum(1 << DIMS.index(d) for d in flip)


def column_parts(width, count):
    tiles = width // 128
    sizes = [(tiles // count + (i < tiles % count)) * 128 for i in range(count)]
    return [(sum(sizes[:i]), n) for i, n in enumerate(sizes)]


class Gather:
    def __init__(self, place, buf, send, recv, core_send, core_recv):
        self.place, self.buf, self.send, self.recv, self.core_send, self.core_recv = place, buf, send, recv, core_send, core_recv
        self.parts = column_parts(buf.shape[2], 3)
        self.started = []

    def view(self, part, flip):
        start, size = self.parts[part]
        return self.buf.at[self.place.slot(flip), :, pl.ds(start, size)]

    def hop(self, part, flip, dim):
        there = tuple(d for d in DIMS if (d in flip) != (d == dim))
        index = part * 7 + flip_code(there) - 1
        ref = self.view(part, flip)
        return pltpu.make_async_remote_copy(src_ref=ref, dst_ref=ref, send_sem=self.send.at[index], recv_sem=self.recv.at[index], device_id=self.place.device((dim,)), device_id_type=MESH)

    def core_hop(self, part, flip):
        index = part * 8 + flip_code(flip)
        ref = self.view(part, flip)
        return pltpu.make_async_remote_copy(src_ref=ref, dst_ref=ref, send_sem=self.core_send.at[index], recv_sem=self.core_recv.at[index], device_id=self.place.device(("core",)), device_id_type=MESH)

    def go(self, copy):
        copy.start()
        self.started.append(copy)

    def wait(self, part, flip):
        order = ORDERS[part]
        last = max(order.index(d) for d in flip)
        came = tuple(d for d in flip if d != order[last])
        self.hop(part, came, order[last]).wait_recv()
        for dim in order[last + 1:]:
            self.go(self.hop(part, flip, dim))
        self.go(self.core_hop(part, flip))

    def run(self):
        for step in range(3):
            for part, order in enumerate(ORDERS):
                self.go(self.hop(part, (), order[step]))
        for part in range(3):
            self.go(self.core_hop(part, ()))
        for step in range(3):
            for flip in FLIPS[1:]:
                for part, order in enumerate(ORDERS):
                    if max(order.index(d) for d in flip) == step and len(flip) == 1:
                        self.wait(part, flip)
            for flip in FLIPS[1:]:
                for part, order in enumerate(ORDERS):
                    if max(order.index(d) for d in flip) == step and len(flip) > 1:
                        self.wait(part, flip)

    def finish(self, out, out_sem):
        rows = self.buf.shape[1]
        copies = []

        def store(flip):
            slot = self.place.slot(flip)
            c = pltpu.make_async_copy(self.buf.at[slot], out.at[pl.ds(slot * rows, rows), :], out_sem.at[len(copies)])
            c.start()
            copies.append(c)

        for flip in FLIPS:
            store(flip)
        for flip in FLIPS:
            other = flip + ("core",)
            for part in range(3):
                start, size = self.parts[part]
                ref = self.buf.at[self.place.slot(other), :, pl.ds(start, size)]
                index = part * 8 + flip_code(flip)
                pltpu.make_async_remote_copy(src_ref=ref, dst_ref=ref, send_sem=self.core_send.at[index], recv_sem=self.core_recv.at[index], device_id=self.place.device(("core",)), device_id_type=MESH).wait_recv()
            store(other)
        for c in self.started:
            c.wait_send()
        for c in copies:
            c.wait()


def embed_kernel(picked, side_f, side_i, out, slice_out, all_f, all_i, buf, r1, r2, tmp, send, recv, core_send, core_recv, out_sem, rs_send, rs_recv, side_send, side_recv, slice_sem):
    place = Place()
    place.meet(("x", "y", "z", "core"))
    half = buf.shape[2] // 2
    near = ("y", "z")

    sides = ((side_f, all_f), (side_i, all_i))
    started, keeps = [], []

    def side_hop(i, step):
        src, dst = sides[i]
        if step == 0:
            src_ref, slot, dim = src, place.cp(), "x"
        elif step == 1:
            src_ref, slot, dim = src, place.cp(), "core"
        else:
            src_ref, slot, dim = dst.at[place.cp(("x",))], place.cp(("x",)), "core"
        return pltpu.make_async_remote_copy(src_ref=src_ref, dst_ref=dst.at[slot], send_sem=side_send.at[i, step], recv_sem=side_recv.at[i, step], device_id=place.device((dim,)), device_id_type=MESH)

    def first(h, k):
        a, b = near[h], near[1 - h]
        target = place.tp((a,)) if k == 0 else place.tp((a, b))
        cols = pl.ds(h * half, half)
        return pltpu.make_async_remote_copy(src_ref=picked.at[target, :, cols], dst_ref=r1.at[h, k], send_sem=rs_send.at[h, k], recv_sem=rs_recv.at[h, k], device_id=place.device((a,)), device_id_type=MESH)

    def second(h):
        return pltpu.make_async_remote_copy(src_ref=tmp.at[h], dst_ref=r2.at[h], send_sem=rs_send.at[h, 2], recv_sem=rs_recv.at[h, 2], device_id=place.device((near[1 - h],)), device_id_type=MESH)

    def go(copy):
        copy.start()
        started.append(copy)

    for k in (1, 0):
        for h in range(2):
            go(first(h, k))
    for i in range(2):
        go(side_hop(i, 0))
        go(side_hop(i, 1))
        keeps.append(pltpu.make_async_copy(sides[i][0], sides[i][1].at[place.cp()], slice_sem.at[i]))
        keeps[i].start()
    for h in range(2):
        cols = slice(h * half, (h + 1) * half)
        first(h, 1).wait_recv()
        tmp[h] = picked[place.tp((near[1 - h],)), :, cols] + r1[h, 1]
        go(second(h))
    for i in range(2):
        side_hop(i, 0).wait_recv()
        go(side_hop(i, 2))
    mine = place.slot()
    for h in range(2):
        cols = slice(h * half, (h + 1) * half)
        first(h, 0).wait_recv()
        part = picked[place.tp(), :, cols] + r1[h, 0]
        second(h).wait_recv()
        buf[mine, :, cols] = part + r2[h]
    gather = Gather(place, buf, send, recv, core_send, core_recv)
    gather.run()
    keeps.append(pltpu.make_async_copy(buf.at[mine], slice_out, slice_sem.at[2]))
    keeps[-1].start()
    gather.finish(out, out_sem)
    for c in keeps:
        c.wait()
    for i in range(2):
        side_hop(i, 1).wait_recv()
        side_hop(i, 2).wait_recv()
    for c in started:
        c.wait_send()


def embed_gather(picked, side_f, side_i):
    _, rows, dim = picked.shape
    half = dim // 2
    dma = pltpu.SemaphoreType.DMA
    vmem = pl.BlockSpec(memory_space=pltpu.VMEM)
    hbm = pl.BlockSpec(memory_space=pl.ANY)
    return pl.pallas_call(
        embed_kernel,
        out_shape=[
            jax.ShapeDtypeStruct((16 * rows, dim), BF16),
            jax.ShapeDtypeStruct((rows, dim), BF16),
            jax.ShapeDtypeStruct((4,) + side_f.shape, F32),
            jax.ShapeDtypeStruct((4,) + side_i.shape, I32),
        ],
        in_specs=[vmem, vmem, vmem],
        out_specs=[pl.BlockSpec(memory_space=pltpu.HBM)] * 4,
        scratch_shapes=[
            pltpu.VMEM((16, rows, dim), BF16),
            pltpu.VMEM((2, 2, rows, half), BF16),
            pltpu.VMEM((2, rows, half), BF16),
            pltpu.VMEM((2, rows, half), BF16),
            dma((21,)), dma((21,)), dma((24,)), dma((24,)), dma((16,)),
            *[dma((2, 3))] * 4, dma((3,)),
        ],
        compiler_params=pltpu.CompilerParams(collective_id=0, has_side_effects=True, vmem_limit_bytes=FULL),
        name="embed_gather",
    )(picked, side_f, side_i)


def spread_kernel(piece, out, buf, send, recv, core_send, core_recv, out_sem, load):
    place = Place()
    first = pltpu.make_async_copy(piece, buf.at[place.slot()], load)
    first.start()
    place.meet(("x", "y", "z", "core"))
    first.wait()
    gather = Gather(place, buf, send, recv, core_send, core_recv)
    gather.run()
    gather.finish(out, out_sem)


def spread(piece):
    rows, dim = piece.shape
    dma = pltpu.SemaphoreType.DMA
    hbm = pl.BlockSpec(memory_space=pltpu.HBM)
    return pl.pallas_call(
        spread_kernel,
        out_shape=jax.ShapeDtypeStruct((16 * rows, dim), BF16),
        in_specs=[hbm],
        out_specs=hbm,
        scratch_shapes=[pltpu.VMEM((16, rows, dim), BF16), *[dma((n,)) for n in (21, 21, 24, 24, 16)], dma],
        compiler_params=pltpu.CompilerParams(collective_id=2, has_side_effects=True, vmem_limit_bytes=FULL),
        name="spread",
    )(piece)


def slot_block(j):
    return jnp.where(j < 4, 2 * j, 15 - 2 * j)


def unpack_angles(packed):
    turned = pltpu.roll(packed, packed.shape[1] // 2, 1)
    low = lax.broadcasted_iota(I32, packed.shape, 1) < packed.shape[1] // 2
    return jnp.where(low, packed, turned), jnp.where(low, -turned, packed)


def qkv_kernel(x, gain, wq, wk, wv, angles, act, q, k, v, wide, *, head_dim):
    width = wq.shape[1]

    @pl.when(pl.program_id(0) == 0)
    def _():
        for i, w in enumerate((wq, wk, wv)):
            wide[:, i * width:(i + 1) * width] = w[:]

    feats = x[:].astype(F32)
    inv = lax.rsqrt(mean_row(feats * feats) + NORM_EPS)
    a = (feats * inv * gain[:]).astype(BF16)
    act[:] = a
    t = nn(a, wide[:])
    cos, sin = unpack_angles(angles[:])
    for i, out in enumerate((q, k, v)):
        for h in range(width // head_dim):
            th = t[:, i * width + h * head_dim:i * width + (h + 1) * head_dim]
            if i < 2:
                th = th * cos + pltpu.roll(th, head_dim // 2, 1) * sin
            out[:, h * head_dim:(h + 1) * head_dim] = th.astype(BF16)


def project_qkv(x_all, gain, wq, wk, wv, angles, block=512):
    total, dim = x_all.shape
    width = wq.shape[1]
    head_dim = angles.shape[1]
    rows = lambda n: pl.BlockSpec((block, n), lambda i: (i, 0))
    whole = lambda a: pl.BlockSpec(a.shape, lambda i: (0, 0), pipeline_mode=pl.Buffered(1))
    return pl.pallas_call(
        functools.partial(qkv_kernel, head_dim=head_dim),
        out_shape=[jax.ShapeDtypeStruct((total, n), BF16) for n in (dim, width, width, width)],
        grid=(total // block,),
        in_specs=[rows(dim), whole(gain), whole(wq), whole(wk), whole(wv), rows(head_dim)],
        out_specs=[rows(dim), rows(width), rows(width), rows(width)],
        scratch_shapes=[pltpu.VMEM((dim, 3 * width), BF16)],
        compiler_params=pltpu.CompilerParams(vmem_limit_bytes=FULL),
        cost_estimate=cost(6 * total * dim * width),
        name="project_qkv",
    )(x_all, gain, wq, wk, wv, angles)


def block_range(info, ids, i, blocks):
    r = info[0]
    blk = ids.shape[2] // 2
    b = jnp.where(i == 0, r, blocks - 1 - r)

    def docs(shard, half):
        return ids[shard, 1, half * blk], ids[shard, 1, half * blk + blk - 1]

    first, last = docs(r, i)
    jmin, imax = 0, -1
    for j in range(blocks):
        begin, end = docs(min(j, blocks - 1 - j), int(j >= blocks // 2))
        jmin = jmin + (end < first).astype(I32)
        imax = imax + (begin <= last).astype(I32)
    return b, jmin, imax


def attend_kernel(info, ids, q, k, v, doc_col, doc_row, out, lse, sc, *, heads, head_dim, scale):
    blk = q.shape[0]
    b, jmin, _ = block_range(info, ids, pl.program_id(0), doc_row.shape[0])
    row_n = lax.broadcasted_iota(I32, (blk, blk), 0) + b * blk
    col_n = lax.broadcasted_iota(I32, (blk, blk), 1)

    def score(j, peaks):
        sb = slot_block(j)
        off = pl.multiple_of(sb * blk, blk)
        allowed = (doc_col[:] == doc_row[sb]) & (col_n + j * blk <= row_n)
        new = []
        for h in range(heads):
            cols = slice(h * head_dim, (h + 1) * head_dim)
            s = nt(q[:, cols], k[pl.ds(off, blk), cols]) * scale
            s = jnp.where(allowed, s, NEG_BIG)
            sc[j, h] = s
            new.append(jnp.maximum(peaks[h], jnp.max(s, axis=1, keepdims=True)))
        return tuple(new)

    peaks = lax.fori_loop(jmin, b + 1, score, tuple(jnp.full((blk, 1), NEG_BIG, F32) for _ in range(heads)))

    def weigh(j, sums):
        new = []
        for h in range(heads):
            p = jnp.exp(sc[j, h] - peaks[h])
            sc[j, h] = p
            new.append(sums[h] + row_sum(p))
        return tuple(new)

    sums = lax.fori_loop(jmin, b + 1, weigh, tuple(jnp.zeros((blk, 1), F32) for _ in range(heads)))
    inv = tuple(1.0 / t for t in sums)
    for h in range(heads):
        lse[:, h:h + 1] = peaks[h] + jnp.log(sums[h])

    def mix(j, acc):
        off = pl.multiple_of(slot_block(j) * blk, blk)
        new = []
        for h in range(heads):
            cols = slice(h * head_dim, (h + 1) * head_dim)
            new.append(acc[h] + nn((sc[j, h] * inv[h]).astype(BF16), v[pl.ds(off, blk), cols]))
        return tuple(new)

    acc = lax.fori_loop(jmin, b + 1, mix, tuple(jnp.zeros((blk, head_dim), F32) for _ in range(heads)))
    for h in range(heads):
        out[:, h * head_dim:(h + 1) * head_dim] = acc[h].astype(BF16)


def attend(info, ids, q, k, v, doc_col, doc_row, head_dim, blk):
    total, width = k.shape
    heads = width // head_dim
    mine = lambda n: pl.BlockSpec((blk, n), lambda i, info, ids: (2 * info[0] + i, 0))
    return pl.pallas_call(
        functools.partial(attend_kernel, heads=heads, head_dim=head_dim, scale=head_dim ** -0.5),
        out_shape=[jax.ShapeDtypeStruct((2 * blk, width), BF16), jax.ShapeDtypeStruct((2 * blk, 8), F32)],
        grid_spec=pltpu.PrefetchScalarGridSpec(
            num_scalar_prefetch=2,
            grid=(2,),
            in_specs=[mine(width), whole(k), whole(v), mine(1), whole(doc_row)],
            out_specs=[pl.BlockSpec((blk, width), lambda i, info, ids: (i, 0)), pl.BlockSpec((blk, 8), lambda i, info, ids: (i, 0))],
            scratch_shapes=[pltpu.VMEM((total // blk, heads, blk, blk), F32)],
        ),
        compiler_params=pltpu.CompilerParams(vmem_limit_bytes=FULL),
        cost_estimate=cost(4 * 2 * blk * total * width),
        name="attend",
    )(info, ids, q, k, v, doc_col, doc_row)


def attend_back_kernel(info, ids, q, k, v, do, doc_col, doc_row, lse_col, lse_row, del_col, del_row, angles, out, acc, *, heads, head_dim, scale):
    blk = angles.shape[0]
    width = heads * head_dim
    i = pl.program_id(0)
    b, jmin, imax = block_range(info, ids, i, doc_row.shape[0])
    me = pl.multiple_of((2 * info[0] + i) * blk, blk)
    mine = pl.ds(me, blk)
    iota_r = lax.broadcasted_iota(I32, (blk, blk), 0)
    iota_c = lax.broadcasted_iota(I32, (blk, blk), 1)
    acc[:] = jnp.zeros_like(acc)
    spans = [slice(h * head_dim, (h + 1) * head_dim) for h in range(heads)]

    def for_query(j, c):
        sb = slot_block(j)
        there = pl.ds(pl.multiple_of(sb * blk, blk), blk)
        allowed = (doc_col[mine, :] == doc_row[sb]) & (iota_c + j * blk <= iota_r + b * blk)
        for h, cols in enumerate(spans):
            s = jnp.where(allowed, nt(q[mine, cols], k[there, cols]) * scale, NEG_BIG)
            p = jnp.exp(s - lse_col[mine, h:h + 1])
            dp = to_bf16(nt(do[mine, cols], v[there, cols]))
            ds = (p * (dp - del_col[mine, h:h + 1]) * scale).astype(BF16)
            acc[0, :, cols] += nn(ds, k[there, cols])
        return c

    lax.fori_loop(jmin, b + 1, for_query, 0)

    def for_key(j, c):
        sb = slot_block(j)
        there = pl.ds(pl.multiple_of(sb * blk, blk), blk)
        allowed = (doc_col[mine, :] == doc_row[sb]) & (iota_r + b * blk <= iota_c + j * blk)
        for h, cols in enumerate(spans):
            s = jnp.where(allowed, nt(k[mine, cols], q[there, cols]) * scale, NEG_BIG)
            p = jnp.exp(s - lse_row[sb, h:h + 1, :])
            dp = to_bf16(nt(v[mine, cols], do[there, cols]))
            ds = (p * (dp - del_row[sb, h:h + 1, :]) * scale).astype(BF16)
            acc[2, :, cols] += nn(p.astype(BF16), do[there, cols])
            acc[1, :, cols] += nn(ds, q[there, cols])
        return c

    lax.fori_loop(b, imax + 1, for_key, 0)
    cos, sin = unpack_angles(angles[:])
    for part in range(3):
        for h, cols in enumerate(spans):
            t = acc[part, :, cols]
            if part < 2:
                t = to_bf16(t)
                t = t * cos - pltpu.roll(t, head_dim // 2, 1) * sin
            out[:, part * width + h * head_dim:part * width + (h + 1) * head_dim] = t.astype(BF16)


def attend_back(info, ids, q, k, v, do, doc_col, doc_row, lse_col, lse_row, del_col, del_row, angles, blk):
    total, width = k.shape
    head_dim = angles.shape[1]
    heads = width // head_dim
    mine = lambda n: pl.BlockSpec((blk, n), lambda i, info, ids: (2 * info[0] + i, 0))
    arrays = (q, k, v, do, doc_col, doc_row, lse_col, lse_row, del_col, del_row)
    return pl.pallas_call(
        functools.partial(attend_back_kernel, heads=heads, head_dim=head_dim, scale=head_dim ** -0.5),
        out_shape=jax.ShapeDtypeStruct((2 * blk, 3 * width), BF16),
        grid_spec=pltpu.PrefetchScalarGridSpec(
            num_scalar_prefetch=2,
            grid=(2,),
            in_specs=[whole(a) for a in arrays] + [mine(head_dim)],
            out_specs=pl.BlockSpec((blk, 3 * width), lambda i, info, ids: (i, 0)),
            scratch_shapes=[pltpu.VMEM((3, blk, width), F32)],
        ),
        compiler_params=pltpu.CompilerParams(vmem_limit_bytes=FULL),
        cost_estimate=cost(14 * 2 * blk * total * width // 2),
        name="attend_back",
    )(info, ids, *arrays, angles)


def att_kernel(att, lse, x_all, w, gain, lse_out, res, act, parts, x, wide, send, recv, lse_send, lse_recv, load, swap_send, swap_recv):
    place = Place()
    rows, width = att.shape
    half = w.shape[1]
    mine = place.cp()
    loads = [pltpu.make_async_copy(src, dst, load.at[i]) for i, (src, dst) in enumerate(((x_all.at[pl.ds(mine * rows, rows), :], x), (w, wide.at[0])))]
    for c in loads:
        c.start()
    place.meet(("y", "z", "x", "core"))
    started = []
    near = ("y", "z")
    spans = column_parts(width, 2)

    def hop(p, flip, dim):
        there = tuple(d for d in near if (d in flip) != (d == dim))
        index = p * 3 + (there == ("y",)) + 2 * (there == ("z",))
        start, size = spans[p]
        cols = pl.ds(start, size)
        slot = place.tp(flip)
        src = parts.at[slot, :, cols] if flip else att.at[:, cols]
        return pltpu.make_async_remote_copy(src_ref=src, dst_ref=parts.at[slot, :, cols], send_sem=send.at[index], recv_sem=recv.at[index], device_id=place.device((dim,)), device_id_type=MESH)

    def lse_hop(step):
        src, slot, dim = ((lse, mine, "x"), (lse, mine, "core"), (lse_out.at[place.cp(("x",))], place.cp(("x",)), "core"))[step]
        return pltpu.make_async_remote_copy(src_ref=src, dst_ref=lse_out.at[slot], send_sem=lse_send.at[step], recv_sem=lse_recv.at[step], device_id=place.device((dim,)), device_id_type=MESH)

    def go(copy):
        copy.start()
        started.append(copy)

    other = pltpu.make_async_remote_copy(src_ref=w, dst_ref=wide.at[1], send_sem=swap_send, recv_sem=swap_recv, device_id=place.device(("core",)), device_id_type=MESH)
    for step in range(2):
        for p in range(2):
            go(hop(p, (), near[(p + step) % 2]))
    go(other)
    go(lse_hop(0))
    go(lse_hop(1))
    lse_out[mine] = lse[:]
    for c in loads:
        c.wait()

    def add(piece, slot, halves=(0, 1), first=False):
        for i in halves:
            cols = pl.ds(pl.multiple_of(place.coord("core", ("core",) if i else ()) * half, 128), half)
            t = nn(piece, wide[i, pl.ds(pl.multiple_of(slot * width, width), width), :])
            res[:, cols] = t + (x[:, cols].astype(F32) if first else res[:, cols])

    add(att[:], place.tp(), (0,), True)
    for p in range(2):
        hop(p, (), near[p]).wait_recv()
        go(hop(p, (near[p],), near[1 - p]))
    lse_hop(0).wait_recv()
    go(lse_hop(2))
    other.wait_recv()
    add(att[:], place.tp(), (1,), True)
    for p in (1, 0):
        hop(p, (), near[1 - p]).wait_recv()
        slot = place.tp((near[1 - p],))
        add(parts[slot], slot)
    for p in range(2):
        hop(p, (near[p],), near[1 - p]).wait_recv()
    slot = place.tp(near)
    add(parts[slot], slot)
    h = res[:]
    act[:] = (h * lax.rsqrt(mean_row(h * h) + NORM_EPS) * gain[:]).astype(BF16)
    lse_hop(1).wait_recv()
    lse_hop(2).wait_recv()
    for c in started:
        c.wait_send()


def att_project(att, lse, x_all, w, gain):
    rows, width = att.shape
    dim = x_all.shape[1]
    dma = pltpu.SemaphoreType.DMA
    vmem = pl.BlockSpec(memory_space=pltpu.VMEM)
    hbm = pl.BlockSpec(memory_space=pl.ANY)
    return pl.pallas_call(
        att_kernel,
        out_shape=[jax.ShapeDtypeStruct((4,) + lse.shape, F32), jax.ShapeDtypeStruct((rows, dim), F32), jax.ShapeDtypeStruct((rows, dim), BF16)],
        in_specs=[vmem, vmem, hbm, hbm, vmem],
        out_specs=[vmem] * 3,
        scratch_shapes=[
            pltpu.VMEM((4, rows, width), BF16), pltpu.VMEM((rows, dim), BF16), pltpu.VMEM((2,) + w.shape, BF16),
            *[dma((n,)) for n in (6, 6, 3, 3, 2)], dma, dma,
        ],
        compiler_params=pltpu.CompilerParams(collective_id=1, has_side_effects=True, vmem_limit_bytes=FULL),
        name="att_project",
    )(att, lse, x_all, w, gain)


def weight_grad_kernel(info, *refs, pieces, splits):
    lhs = refs[:pieces]
    rhs = refs[pieces:2 * pieces]
    outs = refs[2 * pieces:]
    t = tn(lhs[0][:], rhs[0][:])
    for a, b in zip(lhs[1:], rhs[1:]):
        t += tn(a[:], b[:])
    width = t.shape[1] // splits
    for i, out in enumerate(outs):
        out[:] = t[:, i * width:(i + 1) * width]


def weight_grad(info, lhs, rhs, block=256, splits=1, rows=None):
    def spec(arr, p, cols, moving):
        if arr.ndim == 3:
            return pl.BlockSpec((None, arr.shape[1], cols), lambda i, info: (info[0] ^ p, 0, i if moving else 0))
        return pl.BlockSpec((arr.shape[0], cols), lambda i, info: (0, i if moving else 0))

    tokens = lhs[0].shape[-2]
    rows, dim = rows or lhs[0].shape[-1], rhs[0].shape[-1]
    n = len(lhs)
    width = dim // splits
    outs = pl.pallas_call(
        functools.partial(weight_grad_kernel, pieces=n, splits=splits),
        out_shape=[jax.ShapeDtypeStruct((rows, width), F32)] * splits,
        grid_spec=pltpu.PrefetchScalarGridSpec(
            num_scalar_prefetch=1,
            grid=(pl.cdiv(rows, block),),
            in_specs=[spec(a, p, block, True) for p, a in enumerate(lhs)] + [spec(b, p, dim, False) for p, b in enumerate(rhs)],
            out_specs=[pl.BlockSpec((block, width), lambda i, info: (i, 0))] * splits,
        ),
        compiler_params=pltpu.CompilerParams(vmem_limit_bytes=56 * MIB),
        cost_estimate=cost(2 * n * tokens * rows * dim),
        name="weight_grad",
    )(info, *lhs, *rhs)
    return outs if splits > 1 else outs[0]


def mlp_kernel(act, dy, wg, wu, wd, hidden, d_gate, d_up, *rest, limit, tiles):
    i = pl.program_id(0)
    block = wg.shape[0]
    both = rest[-1]

    @pl.when(i < tiles)
    def _():
        left = limit - i * block
        row_ok = lax.broadcasted_iota(I32, (block, 1), 0) < left
        col_ok = lax.broadcasted_iota(I32, (1, block), 1) < left
        pair = pl.ds(pl.multiple_of(2 * i * block, block), 2 * block) if tiles < pl.num_programs(0) else slice(2 * block)
        both[pair] = jnp.concatenate([jnp.where(row_ok, w[:], 0).astype(BF16) for w in (wg, wu)])
        t = nt(act[:], both[pair])
        gate, up = t[:, :block], t[:, block:]
        dh = jnp.where(col_ok, to_bf16(nt(dy[:], wd[:])), 0)
        sig = jax.nn.sigmoid(gate)
        hidden[:] = (gate * sig * up).astype(BF16)
        dg = (dh * up * sig * (1.0 + gate * (1.0 - sig))).astype(BF16)
        du = (dh * gate * sig).astype(BF16)
        d_gate[:] = dg
        d_up[:] = du
        if len(rest) > 1:
            rest[1][:, pair] = jnp.concatenate([dg, du], axis=1)

    if len(rest) > 1:
        grad, grads = rest[:2]

        @pl.when(i >= tiles)
        def _():
            wide = grad.shape[1]
            grad[:] = nn(grads[:], both[:, pl.ds(pl.multiple_of((i - tiles) * wide, wide), wide)])


def mlp_block(act, dy, wg, wu, wd, with_grad, block=256, wide=512):
    rows, dim = act.shape
    limit = wg.shape[0]
    tiles = pl.cdiv(limit, block)
    steps = tiles + with_grad * dim // wide
    cols = pl.BlockSpec((rows, block), lambda i: (0, jnp.minimum(i, tiles - 1)))
    tile = pl.BlockSpec((block, dim), lambda i: (jnp.minimum(i, tiles - 1), 0))
    full = pl.BlockSpec((rows, dim), lambda i: (0, 0), pipeline_mode=pl.Buffered(1))
    deep = 2 * block * (tiles if with_grad else 1)
    return pl.pallas_call(
        functools.partial(mlp_kernel, limit=limit, tiles=tiles),
        out_shape=[jax.ShapeDtypeStruct((rows, tiles * block), BF16)] * 3 + [jax.ShapeDtypeStruct((rows, dim), F32)] * with_grad,
        grid=(steps,),
        in_specs=[full, full, tile, tile, tile],
        out_specs=[cols] * 3 + [pl.BlockSpec((rows, wide), lambda i: (0, jnp.maximum(i - tiles, 0)))] * with_grad,
        scratch_shapes=[pltpu.VMEM((rows, deep), BF16)] * with_grad + [pltpu.VMEM((deep, dim), BF16)],
        compiler_params=pltpu.CompilerParams(vmem_limit_bytes=FULL),
        cost_estimate=cost((6 + 4 * with_grad) * rows * dim * limit),
        name="mlp_block",
    )(act, dy, wg, wu, wd)


def zero_kernel(after, out, zeros, sem):
    zeros[:] = jnp.zeros_like(zeros)
    step = zeros.shape[0]
    count = out.shape[0] // step

    def send(i, c):
        pltpu.make_async_copy(zeros, out.at[pl.ds(pl.multiple_of(i * step, step), step), :], sem).start()
        return c

    def wait(i, c):
        pltpu.make_async_copy(zeros, out.at[pl.ds(0, step), :], sem).wait()
        return c

    lax.fori_loop(0, count, send, 0)
    lax.fori_loop(0, count, wait, 0)


def zero_rows(after, rows, dim, step=200):
    return pl.pallas_call(
        zero_kernel,
        out_shape=jax.ShapeDtypeStruct((rows, dim), F32),
        in_specs=[pl.BlockSpec(memory_space=pltpu.SMEM)],
        out_specs=pl.BlockSpec(memory_space=pl.ANY),
        scratch_shapes=[pltpu.VMEM((step, dim), F32), pltpu.SemaphoreType.DMA],
        compiler_params=pltpu.CompilerParams(vmem_limit_bytes=8 * MIB),
        cost_estimate=cost(rows * dim),
        name="zero_rows",
    )(after)


def scatter_kernel(order, sid, runs, bounds, rows, base_hbm, out_hbm, sums, row_sem, sum_sem):
    lo = bounds[0]
    hi = bounds[1]

    def one(c):
        p, singles, multi = c
        n = runs[p]
        t = order[p]
        single = n == 1

        @pl.when(single)
        def _():
            pltpu.make_async_copy(rows.at[pl.ds(t, 1), :], out_hbm.at[pl.ds(sid[p], 1), :], row_sem).start()

        @pl.when(jnp.logical_not(single))
        def _():
            def add(j, acc):
                return acc + rows[pl.ds(order[p + j], 1), :]

            sums[pl.ds(multi, 1), :] = lax.fori_loop(1, n, add, rows[pl.ds(t, 1), :])

        return p + n, singles + single.astype(I32), multi + 1 - single.astype(I32)

    _, singles, multi = lax.while_loop(lambda c: c[0] < hi, one, (lo, 0, 0))

    def two(c):
        p, k = c
        n = runs[p]

        @pl.when(n > 1)
        def _():
            pltpu.make_async_copy(sums.at[pl.ds(k, 1), :], out_hbm.at[pl.ds(sid[p], 1), :], sum_sem).start()

        return p + n, k + (n > 1).astype(I32)

    lax.while_loop(lambda c: c[0] < hi, two, (lo, 0))

    def wait(sem):
        def body(i, c):
            pltpu.make_async_copy(sums.at[pl.ds(0, 1), :], out_hbm.at[pl.ds(0, 1), :], sem).wait()
            return c

        return body

    lax.fori_loop(0, singles, wait(row_sem), 0)
    lax.fori_loop(0, multi, wait(sum_sem), 0)


def scatter_rows(order, sid, runs, bounds, grads, base, tokens):
    _, dim = grads.shape
    rows = base.shape[0]
    return pl.pallas_call(
        scatter_kernel,
        out_shape=jax.ShapeDtypeStruct((rows, dim), F32),
        grid_spec=pltpu.PrefetchScalarGridSpec(
            num_scalar_prefetch=4,
            grid=(),
            in_specs=[pl.BlockSpec(memory_space=pltpu.VMEM), pl.BlockSpec(memory_space=pl.ANY)],
            out_specs=pl.BlockSpec(memory_space=pl.ANY),
            scratch_shapes=[pltpu.VMEM((tokens // 2, dim), F32), pltpu.SemaphoreType.DMA, pltpu.SemaphoreType.DMA],
        ),
        input_output_aliases={5: 0},
        compiler_params=pltpu.CompilerParams(vmem_limit_bytes=FULL),
        name="scatter_rows",
    )(order, sid, runs, bounds, grads, base)


def solution(mesh):
    cp_count = mesh.shape["cp"]
    tp_count = mesh.shape["tp"]
    both = ("cp", "tp")
    x_swap = [(i, i ^ 2) for i in range(cp_count)]
    core_swap = [(i, i ^ 1) for i in range(cp_count)]

    def compute(tokens, pos, doc_id, dy, table, w_q, w_k, w_v, w_o, w_gate, w_up, w_down, gain_one, gain_two, inv_freq):
        span = tokens.shape[0]
        total = span * cp_count
        part = span // tp_count
        rows, dim = table.shape
        head_dim = 2 * inv_freq.shape[0]
        heads = w_q.shape[1] // head_dim
        width = heads * head_dim
        tp_rank = lax.axis_index("tp")
        cp_rank = lax.axis_index("cp")
        core = cp_rank % 2
        gain_a = gain_one.astype(F32)
        gain_b = gain_two.astype(F32)

        barrier = lax.optimization_barrier
        join = lambda arr, axis: lax.all_gather(arr, axis, axis=0, tiled=True)
        add_up = lambda arr: lax.psum_scatter(arr, "tp", scatter_dimension=0, tiled=True)
        swap = lambda arr, pairs, axis="cp": lax.ppermute(arr, axis, pairs)
        local_ids = tokens - tp_rank * rows
        owned = (local_ids >= 0) & (local_ids < rows)
        safe_ids = jnp.where(owned, local_ids, jnp.arange(span) * (rows // span))
        picked = jnp.where(owned[:, None], jnp.take(table, safe_ids, axis=0), 0).astype(BF16)
        info = jnp.stack([cp_rank, core]).astype(I32)
        half = dim // 2
        angle = pos.astype(F32)[:, None] * inv_freq[None, :]
        side_f = jnp.concatenate([jnp.cos(angle), jnp.sin(angle)], axis=1)
        side_i = jnp.stack([tokens, doc_id] * 4)
        x_all, x_slice, angles, ints = embed_gather(picked.reshape(tp_count, part, dim), side_f, side_i)
        angles = angles.reshape(total, head_dim)
        tok_all = ints[:, 0, :].reshape(total)
        doc_all = ints[:, 1, :].reshape(total)
        wo_half = barrier((lax.dynamic_slice_in_dim(w_o, core * half, half, 1), x_all))[0]
        wo_half = join(wo_half, "tp")

        dy_x = swap(barrier((dy, x_all))[0], x_swap)
        act_a, query, key, value = project_qkv(x_all, gain_a[None, :], w_q, w_k, w_v, angles)

        blk = span // 2
        blocks = total // blk
        doc_col = doc_all[:, None]
        doc_row = doc_all.reshape(blocks, 1, blk)
        attended, lse = attend(info, ints, query, key, value, doc_col, doc_row, head_dim, blk)

        tok_all = barrier((tok_all, attended))[0]
        slot_ids = jnp.arange(total, dtype=I32)
        before = (tok_all[None, :] < tok_all[:, None]) | ((tok_all[None, :] == tok_all[:, None]) & (slot_ids[None, :] < slot_ids[:, None]))
        rank = jnp.sum(before.astype(I32), axis=1)
        count = jnp.sum((tok_all[None, :] == tok_all[:, None]).astype(I32), axis=1)
        at_rank = rank[None, :] == slot_ids[:, None]
        runs = jnp.sum(jnp.where(at_rank, count[None, :], 0), axis=1)
        order = jnp.sum(jnp.where(at_rank, slot_ids[None, :], 0), axis=1)
        sid = jnp.sum(jnp.where(at_rank, tok_all[None, :], 0), axis=1) - tp_rank * rows
        order = order + 8 * (order // part)
        bounds = jnp.stack([jnp.sum((tok_all < tp_rank * rows).astype(I32)), jnp.sum((tok_all < (tp_rank + 1) * rows).astype(I32))])
        wo_half, runs, order, sid, bounds = barrier((wo_half, runs, order, sid, bounds))
        heads_x = swap(attended, x_swap)
        lse_all, residual, act_b = att_project(attended, lse, x_all, wo_half, gain_b[None, :])
        lse_all = lse_all.reshape(total, 8)
        act_x = swap(act_b, x_swap)
        wg, wu = w_gate.T, w_up.T
        ffn = wg.shape[0]
        hidden, d_gate, d_up, d_act_b = mlp_block(act_b, dy, wg, wu, w_down, True)
        d_act_b = add_up(d_act_b)
        hidden_x, d_gate_x, d_up_x = mlp_block(act_x, dy_x, wg, wu, w_down, False)
        out_part = nn(hidden[:, :ffn], w_down)
        base = zero_rows(bounds, rows, dim)
        heads_x = barrier((heads_x, act_b))[0]
        head_parts = (attended, swap(attended, core_swap), heads_x, swap(heads_x, core_swap))
        att_heads = jnp.concatenate([attended] * cp_count)
        for k, piece in enumerate(head_parts):
            if k:
                att_heads = lax.dynamic_update_slice_in_dim(att_heads, piece, (cp_rank ^ k) * span, 0)
        d_act_b, hidden_x, d_gate_x, d_up_x, out_part, base, att_heads = barrier((d_act_b, hidden_x, d_gate_x, d_up_x, out_part, base, att_heads))
        d_act_b = to_bf16(d_act_b)
        acts, dys, hiddens, d_gates, d_ups = [(a, swap(a, core_swap), b, swap(b, core_swap)) for a, b in (
            (act_b, act_x), (dy, dy_x), (hidden, hidden_x), (d_gate, d_gate_x), (d_up, d_up_x))]
        grad_down = weight_grad(info, hiddens, dys, rows=ffn)
        grad_gate = weight_grad(info, d_gates, acts, rows=ffn)
        grad_up = weight_grad(info, d_ups, acts, rows=ffn)

        def mine(arr):
            return lax.dynamic_slice_in_dim(arr, tp_rank * part, part, 0)

        res_part = mine(residual)
        normed_b, inv_b = rms_stats(res_part)
        grad_gain_b = jnp.sum(d_act_b * normed_b, axis=0)
        d_resid = mine(dy).astype(F32) + rms_back(d_act_b * gain_b, normed_b, inv_b)
        d_resid_all, out_part = barrier((spread(d_resid.astype(BF16)), out_part))
        out_slice = add_up(out_part)
        out_slice = (res_part + out_slice).astype(BF16)

        d_att = nt(d_resid_all, w_o)
        d_att_b = d_att.astype(BF16)
        head_of = (jnp.arange(width)[None, :] // head_dim == jnp.arange(8)[:, None]).astype(F32)
        prod = att_heads.astype(F32) * d_att_b.astype(F32)
        delta = lax.dot_general(head_of, prod, (((1,), (1,)), ((), ())), precision=lax.Precision.HIGHEST, preferred_element_type=F32)

        def by_block(arr):
            return jnp.transpose(arr.reshape(8, blocks, blk), (1, 0, 2))

        dqkv = attend_back(info, ints, query, key, value, d_att_b, doc_col, doc_row, lse_all, by_block(lse_all.T), delta.T, by_block(delta), angles, blk)
        d_act_a = sum(nt(dqkv[:, i * width:(i + 1) * width], w) for i, w in enumerate((w_q, w_k, w_v)))
        d_act_a, out_slice = barrier((d_act_a, out_slice))
        d_act_a = add_up(d_act_a)
        dqkv_x = swap(dqkv, x_swap)
        dqkvs = (dqkv, swap(dqkv, core_swap), dqkv_x, swap(dqkv_x, core_swap))
        grad_out = weight_grad(info, head_parts, [d_resid_all.reshape(cp_count, span, dim)] * 4)
        d_act_a, dqkv_x, grad_out, grad_up = barrier((d_act_a, dqkv_x, grad_out, grad_up))
        d_act_a = to_bf16(d_act_a)
        normed_a, inv_a = rms_stats(x_slice.astype(F32))
        grad_gain_a = jnp.sum(d_act_a * normed_a, axis=0)
        d_embed = d_resid + rms_back(d_act_a * gain_a, normed_a, inv_a)
        payload = jnp.concatenate([d_embed, jnp.stack([grad_gain_a, grad_gain_b] * 4)])
        gathered = join(payload, both)
        grad_qkv = weight_grad(info, [act_a.reshape(cp_count, span, dim)] * 4, dqkvs, splits=3)
        gathered, grad_qkv, grad_gate, grad_down = barrier((gathered, grad_qkv, grad_gate, grad_down))
        out_slice = barrier((out_slice, grad_qkv))[0]
        layer_out = jnp.concatenate([out_slice] * tp_count)
        for k in range(1, tp_count):
            piece = swap(out_slice, [(i, i ^ k) for i in range(tp_count)], "tp")
            layer_out = lax.dynamic_update_slice_in_dim(layer_out, piece, (tp_rank ^ k) * part, 0)
        gain_grads = jnp.sum(gathered.reshape(cp_count * tp_count, part + 8, dim)[:, part:part + 2], axis=0)
        grad_table = scatter_rows(order, sid, runs, bounds, gathered, base, total)
        return (layer_out, grad_table, *grad_qkv, grad_out, grad_gate.T, grad_up.T, grad_down, gain_grads[0], gain_grads[1])

    col_spec = P(None, "tp")
    row_spec = P("tp")
    tok_spec = P("cp")
    rep_spec = P()
    in_specs = (tok_spec, tok_spec, tok_spec, P("cp"), row_spec, col_spec, col_spec, col_spec, row_spec, col_spec, col_spec, row_spec, rep_spec, rep_spec, rep_spec)
    out_specs = (P("cp"), row_spec, col_spec, col_spec, col_spec, row_spec, col_spec, col_spec, row_spec, rep_spec, rep_spec)
    return jax.shard_map(compute, mesh=mesh, in_specs=in_specs, out_specs=out_specs, check_vma=False)
```

```python
import functools
import jax
import jax.numpy as jnp
from jax import lax
from jax.experimental import pallas as pl
from jax.experimental.pallas import tpu as pltpu
from jax.sharding import PartitionSpec as P

NORM_EPS = 1e-5
NEG_BIG = -1e30
MIB = 2 ** 20
FULL = 62 * MIB
F32 = jnp.float32
BF16 = jnp.bfloat16
I32 = jnp.int32


def rms_stats(feats):
    inv_rms = lax.rsqrt(mean_row(feats * feats) + NORM_EPS)
    return feats * inv_rms, inv_rms


def rms_back(d_normed, normed, inv_rms):
    return inv_rms * (d_normed - normed * mean_row(d_normed * normed))


def to_bf16(feats):
    return feats.astype(BF16).astype(F32)


def contract(a, b, ca, cb):
    return lax.dot_general(a, b, (((ca,), (cb,)), ((), ())), preferred_element_type=F32)


def row_sum(t):
    return jnp.sum(t, 1, keepdims=True)


def mean_row(t):
    return row_sum(t) / t.shape[1]


def whole(a):
    return pl.BlockSpec(a.shape, lambda *i: (0,) * a.ndim)


def cost(flops):
    return pl.CostEstimate(flops=flops, bytes_accessed=flops // 512, transcendentals=0)


def nn(a, b):
    return contract(a, b, 1, 0)


def nt(a, b):
    return contract(a, b, 1, 1)


def tn(a, b):
    return contract(a, b, 0, 0)


DIMS = ("x", "y", "z")


class Place:
    def __init__(self):
        tp = lax.axis_index("tp")
        cp = lax.axis_index("cp")
        self.at = {"x": cp // 2, "core": cp % 2, "z": tp // 2, "y": tp % 2}

    def coord(self, dim, flip):
        return 1 - self.at[dim] if dim in flip else self.at[dim]

    def tp(self, flip=()):
        return self.coord("z", flip) * 2 + self.coord("y", flip)

    def cp(self, flip=()):
        return self.coord("x", flip) * 2 + self.coord("core", flip)

    def device(self, flip):
        return {"tp": self.tp(flip), "cp": self.cp(flip)}

    def slot(self, flip=()):
        return self.cp(flip) * 4 + self.tp(flip)

    def meet(self, dims):
        barrier = pltpu.get_barrier_semaphore()
        for d in dims:
            pl.semaphore_signal(barrier, inc=1, device_id=self.device((d,)), device_id_type=MESH)
        pl.semaphore_wait(barrier, len(dims))


MESH = pl.DeviceIdType.MESH
ORDERS = (("x", "y", "z"), ("y", "z", "x"), ("z", "x", "y"))
FLIPS = tuple(tuple(d for i, d in enumerate(DIMS) if n >> i & 1) for n in range(8))


def flip_code(flip):
    return sum(1 << DIMS.index(d) for d in flip)


def column_parts(width, count):
    tiles = width // 128
    sizes = [(tiles // count + (i < tiles % count)) * 128 for i in range(count)]
    return [(sum(sizes[:i]), n) for i, n in enumerate(sizes)]


class Gather:
    def __init__(self, place, buf, send, recv, core_send, core_recv):
        self.place, self.buf, self.send, self.recv, self.core_send, self.core_recv = place, buf, send, recv, core_send, core_recv
        self.parts = column_parts(buf.shape[2], 3)
        self.started = []

    def view(self, part, flip):
        start, size = self.parts[part]
        return self.buf.at[self.place.slot(flip), :, pl.ds(start, size)]

    def hop(self, part, flip, dim):
        there = tuple(d for d in DIMS if (d in flip) != (d == dim))
        index = part * 7 + flip_code(there) - 1
        ref = self.view(part, flip)
        return pltpu.make_async_remote_copy(src_ref=ref, dst_ref=ref, send_sem=self.send.at[index], recv_sem=self.recv.at[index], device_id=self.place.device((dim,)), device_id_type=MESH)

    def core_hop(self, part, flip):
        index = part * 8 + flip_code(flip)
        ref = self.view(part, flip)
        return pltpu.make_async_remote_copy(src_ref=ref, dst_ref=ref, send_sem=self.core_send.at[index], recv_sem=self.core_recv.at[index], device_id=self.place.device(("core",)), device_id_type=MESH)

    def go(self, copy):
        copy.start()
        self.started.append(copy)

    def wait(self, part, flip):
        order = ORDERS[part]
        last = max(order.index(d) for d in flip)
        came = tuple(d for d in flip if d != order[last])
        self.hop(part, came, order[last]).wait_recv()
        for dim in order[last + 1:]:
            self.go(self.hop(part, flip, dim))
        self.go(self.core_hop(part, flip))

    def run(self):
        for step in range(3):
            for part, order in enumerate(ORDERS):
                self.go(self.hop(part, (), order[step]))
        for part in range(3):
            self.go(self.core_hop(part, ()))
        for step in range(3):
            for flip in FLIPS[1:]:
                for part, order in enumerate(ORDERS):
                    if max(order.index(d) for d in flip) == step and len(flip) == 1:
                        self.wait(part, flip)
            for flip in FLIPS[1:]:
                for part, order in enumerate(ORDERS):
                    if max(order.index(d) for d in flip) == step and len(flip) > 1:
                        self.wait(part, flip)

    def finish(self, out, out_sem):
        rows = self.buf.shape[1]
        copies = []

        def store(flip):
            slot = self.place.slot(flip)
            c = pltpu.make_async_copy(self.buf.at[slot], out.at[pl.ds(slot * rows, rows), :], out_sem.at[len(copies)])
            c.start()
            copies.append(c)

        for flip in FLIPS:
            store(flip)
        for flip in FLIPS:
            other = flip + ("core",)
            for part in range(3):
                start, size = self.parts[part]
                ref = self.buf.at[self.place.slot(other), :, pl.ds(start, size)]
                index = part * 8 + flip_code(flip)
                pltpu.make_async_remote_copy(src_ref=ref, dst_ref=ref, send_sem=self.core_send.at[index], recv_sem=self.core_recv.at[index], device_id=self.place.device(("core",)), device_id_type=MESH).wait_recv()
            store(other)
        for c in self.started:
            c.wait_send()
        for c in copies:
            c.wait()


def embed_kernel(picked, side_f, side_i, out, slice_out, all_f, all_i, buf, r1, r2, tmp, send, recv, core_send, core_recv, out_sem, rs_send, rs_recv, side_send, side_recv, slice_sem):
    place = Place()
    place.meet(("x", "y", "z", "core"))
    half = buf.shape[2] // 2
    near = ("y", "z")

    sides = ((side_f, all_f), (side_i, all_i))
    started, keeps = [], []

    def side_hop(i, step):
        src, dst = sides[i]
        if step == 0:
            src_ref, slot, dim = src, place.cp(), "x"
        elif step == 1:
            src_ref, slot, dim = src, place.cp(), "core"
        else:
            src_ref, slot, dim = dst.at[place.cp(("x",))], place.cp(("x",)), "core"
        return pltpu.make_async_remote_copy(src_ref=src_ref, dst_ref=dst.at[slot], send_sem=side_send.at[i, step], recv_sem=side_recv.at[i, step], device_id=place.device((dim,)), device_id_type=MESH)

    def first(h, k):
        a, b = near[h], near[1 - h]
        target = place.tp((a,)) if k == 0 else place.tp((a, b))
        cols = pl.ds(h * half, half)
        return pltpu.make_async_remote_copy(src_ref=picked.at[target, :, cols], dst_ref=r1.at[h, k], send_sem=rs_send.at[h, k], recv_sem=rs_recv.at[h, k], device_id=place.device((a,)), device_id_type=MESH)

    def second(h):
        return pltpu.make_async_remote_copy(src_ref=tmp.at[h], dst_ref=r2.at[h], send_sem=rs_send.at[h, 2], recv_sem=rs_recv.at[h, 2], device_id=place.device((near[1 - h],)), device_id_type=MESH)

    def go(copy):
        copy.start()
        started.append(copy)

    for k in (1, 0):
        for h in range(2):
            go(first(h, k))
    for i in range(2):
        go(side_hop(i, 0))
        go(side_hop(i, 1))
        keeps.append(pltpu.make_async_copy(sides[i][0], sides[i][1].at[place.cp()], slice_sem.at[i]))
        keeps[i].start()
    for h in range(2):
        cols = slice(h * half, (h + 1) * half)
        first(h, 1).wait_recv()
        tmp[h] = picked[place.tp((near[1 - h],)), :, cols] + r1[h, 1]
        go(second(h))
    for i in range(2):
        side_hop(i, 0).wait_recv()
        go(side_hop(i, 2))
    mine = place.slot()
    for h in range(2):
        cols = slice(h * half, (h + 1) * half)
        first(h, 0).wait_recv()
        part = picked[place.tp(), :, cols] + r1[h, 0]
        second(h).wait_recv()
        buf[mine, :, cols] = part + r2[h]
    gather = Gather(place, buf, send, recv, core_send, core_recv)
    gather.run()
    keeps.append(pltpu.make_async_copy(buf.at[mine], slice_out, slice_sem.at[2]))
    keeps[-1].start()
    gather.finish(out, out_sem)
    for c in keeps:
        c.wait()
    for i in range(2):
        side_hop(i, 1).wait_recv()
        side_hop(i, 2).wait_recv()
    for c in started:
        c.wait_send()


def embed_gather(picked, side_f, side_i):
    _, rows, dim = picked.shape
    half = dim // 2
    dma = pltpu.SemaphoreType.DMA
    vmem = pl.BlockSpec(memory_space=pltpu.VMEM)
    hbm = pl.BlockSpec(memory_space=pl.ANY)
    return pl.pallas_call(
        embed_kernel,
        out_shape=[
            jax.ShapeDtypeStruct((16 * rows, dim), BF16),
            jax.ShapeDtypeStruct((rows, dim), BF16),
            jax.ShapeDtypeStruct((4,) + side_f.shape, F32),
            jax.ShapeDtypeStruct((4,) + side_i.shape, I32),
        ],
        in_specs=[vmem, vmem, vmem],
        out_specs=[pl.BlockSpec(memory_space=pltpu.HBM)] * 4,
        scratch_shapes=[
            pltpu.VMEM((16, rows, dim), BF16),
            pltpu.VMEM((2, 2, rows, half), BF16),
            pltpu.VMEM((2, rows, half), BF16),
            pltpu.VMEM((2, rows, half), BF16),
            dma((21,)), dma((21,)), dma((24,)), dma((24,)), dma((16,)),
            *[dma((2, 3))] * 4, dma((3,)),
        ],
        compiler_params=pltpu.CompilerParams(collective_id=0, has_side_effects=True, vmem_limit_bytes=FULL),
        name="embed_gather",
    )(picked, side_f, side_i)


def spread_kernel(piece, out, buf, send, recv, core_send, core_recv, out_sem, load):
    place = Place()
    first = pltpu.make_async_copy(piece, buf.at[place.slot()], load)
    first.start()
    place.meet(("x", "y", "z", "core"))
    first.wait()
    gather = Gather(place, buf, send, recv, core_send, core_recv)
    gather.run()
    gather.finish(out, out_sem)


def spread(piece):
    rows, dim = piece.shape
    dma = pltpu.SemaphoreType.DMA
    hbm = pl.BlockSpec(memory_space=pltpu.HBM)
    return pl.pallas_call(
        spread_kernel,
        out_shape=jax.ShapeDtypeStruct((16 * rows, dim), BF16),
        in_specs=[hbm],
        out_specs=hbm,
        scratch_shapes=[pltpu.VMEM((16, rows, dim), BF16), *[dma((n,)) for n in (21, 21, 24, 24, 16)], dma],
        compiler_params=pltpu.CompilerParams(collective_id=2, has_side_effects=True, vmem_limit_bytes=FULL),
        name="spread",
    )(piece)


def slot_block(j):
    return jnp.where(j < 4, 2 * j, 15 - 2 * j)


def unpack_angles(packed):
    turned = pltpu.roll(packed, packed.shape[1] // 2, 1)
    low = lax.broadcasted_iota(I32, packed.shape, 1) < packed.shape[1] // 2
    return jnp.where(low, packed, turned), jnp.where(low, -turned, packed)


def qkv_kernel(x, gain, wq, wk, wv, angles, act, q, k, v, wide, *, head_dim):
    width = wq.shape[1]

    @pl.when(pl.program_id(0) == 0)
    def _():
        for i, w in enumerate((wq, wk, wv)):
            wide[:, i * width:(i + 1) * width] = w[:]

    feats = x[:].astype(F32)
    inv = lax.rsqrt(mean_row(feats * feats) + NORM_EPS)
    a = (feats * inv * gain[:]).astype(BF16)
    act[:] = a
    t = nn(a, wide[:])
    cos, sin = unpack_angles(angles[:])
    for i, out in enumerate((q, k, v)):
        for h in range(width // head_dim):
            th = t[:, i * width + h * head_dim:i * width + (h + 1) * head_dim]
            if i < 2:
                th = th * cos + pltpu.roll(th, head_dim // 2, 1) * sin
            out[:, h * head_dim:(h + 1) * head_dim] = th.astype(BF16)


def project_qkv(x_all, gain, wq, wk, wv, angles, block=512):
    total, dim = x_all.shape
    width = wq.shape[1]
    head_dim = angles.shape[1]
    rows = lambda n: pl.BlockSpec((block, n), lambda i: (i, 0))
    whole = lambda a: pl.BlockSpec(a.shape, lambda i: (0, 0), pipeline_mode=pl.Buffered(1))
    return pl.pallas_call(
        functools.partial(qkv_kernel, head_dim=head_dim),
        out_shape=[jax.ShapeDtypeStruct((total, n), BF16) for n in (dim, width, width, width)],
        grid=(total // block,),
        in_specs=[rows(dim), whole(gain), whole(wq), whole(wk), whole(wv), rows(head_dim)],
        out_specs=[rows(dim), rows(width), rows(width), rows(width)],
        scratch_shapes=[pltpu.VMEM((dim, 3 * width), BF16)],
        compiler_params=pltpu.CompilerParams(vmem_limit_bytes=FULL),
        cost_estimate=cost(6 * total * dim * width),
        name="project_qkv",
    )(x_all, gain, wq, wk, wv, angles)


def block_range(info, ids, i, blocks):
    r = info[0]
    blk = ids.shape[2] // 2
    b = jnp.where(i == 0, r, blocks - 1 - r)

    def docs(shard, half):
        return ids[shard, 1, half * blk], ids[shard, 1, half * blk + blk - 1]

    first, last = docs(r, i)
    jmin, imax = 0, -1
    for j in range(blocks):
        begin, end = docs(min(j, blocks - 1 - j), int(j >= blocks // 2))
        jmin = jmin + (end < first).astype(I32)
        imax = imax + (begin <= last).astype(I32)
    return b, jmin, imax


def attend_kernel(info, ids, q, k, v, doc_col, doc_row, out, lse, sc, *, heads, head_dim, scale):
    blk = q.shape[0]
    b, jmin, _ = block_range(info, ids, pl.program_id(0), doc_row.shape[0])
    row_n = lax.broadcasted_iota(I32, (blk, blk), 0) + b * blk
    col_n = lax.broadcasted_iota(I32, (blk, blk), 1)

    def score(j, peaks):
        sb = slot_block(j)
        off = pl.multiple_of(sb * blk, blk)
        allowed = (doc_col[:] == doc_row[sb]) & (col_n + j * blk <= row_n)
        new = []
        for h in range(heads):
            cols = slice(h * head_dim, (h + 1) * head_dim)
            s = nt(q[:, cols], k[pl.ds(off, blk), cols]) * scale
            s = jnp.where(allowed, s, NEG_BIG)
            sc[j, h] = s
            new.append(jnp.maximum(peaks[h], jnp.max(s, axis=1, keepdims=True)))
        return tuple(new)

    peaks = lax.fori_loop(jmin, b + 1, score, tuple(jnp.full((blk, 1), NEG_BIG, F32) for _ in range(heads)))

    def weigh(j, sums):
        new = []
        for h in range(heads):
            p = jnp.exp(sc[j, h] - peaks[h])
            sc[j, h] = p
            new.append(sums[h] + row_sum(p))
        return tuple(new)

    sums = lax.fori_loop(jmin, b + 1, weigh, tuple(jnp.zeros((blk, 1), F32) for _ in range(heads)))
    inv = tuple(1.0 / t for t in sums)
    for h in range(heads):
        lse[:, h:h + 1] = peaks[h] + jnp.log(sums[h])

    def mix(j, acc):
        off = pl.multiple_of(slot_block(j) * blk, blk)
        new = []
        for h in range(heads):
            cols = slice(h * head_dim, (h + 1) * head_dim)
            new.append(acc[h] + nn((sc[j, h] * inv[h]).astype(BF16), v[pl.ds(off, blk), cols]))
        return tuple(new)

    acc = lax.fori_loop(jmin, b + 1, mix, tuple(jnp.zeros((blk, head_dim), F32) for _ in range(heads)))
    for h in range(heads):
        out[:, h * head_dim:(h + 1) * head_dim] = acc[h].astype(BF16)


def attend(info, ids, q, k, v, doc_col, doc_row, head_dim, blk):
    total, width = k.shape
    heads = width // head_dim
    mine = lambda n: pl.BlockSpec((blk, n), lambda i, info, ids: (2 * info[0] + i, 0))
    return pl.pallas_call(
        functools.partial(attend_kernel, heads=heads, head_dim=head_dim, scale=head_dim ** -0.5),
        out_shape=[jax.ShapeDtypeStruct((2 * blk, width), BF16), jax.ShapeDtypeStruct((2 * blk, 8), F32)],
        grid_spec=pltpu.PrefetchScalarGridSpec(
            num_scalar_prefetch=2,
            grid=(2,),
            in_specs=[mine(width), whole(k), whole(v), mine(1), whole(doc_row)],
            out_specs=[pl.BlockSpec((blk, width), lambda i, info, ids: (i, 0)), pl.BlockSpec((blk, 8), lambda i, info, ids: (i, 0))],
            scratch_shapes=[pltpu.VMEM((total // blk, heads, blk, blk), F32)],
        ),
        compiler_params=pltpu.CompilerParams(vmem_limit_bytes=FULL),
        cost_estimate=cost(4 * 2 * blk * total * width),
        name="attend",
    )(info, ids, q, k, v, doc_col, doc_row)


def attend_back_kernel(info, ids, q, k, v, do, doc_col, doc_row, lse_col, lse_row, del_col, del_row, angles, out, acc, *, heads, head_dim, scale):
    blk = angles.shape[0]
    width = heads * head_dim
    i = pl.program_id(0)
    b, jmin, imax = block_range(info, ids, i, doc_row.shape[0])
    me = pl.multiple_of((2 * info[0] + i) * blk, blk)
    mine = pl.ds(me, blk)
    iota_r = lax.broadcasted_iota(I32, (blk, blk), 0)
    iota_c = lax.broadcasted_iota(I32, (blk, blk), 1)
    acc[:] = jnp.zeros_like(acc)
    spans = [slice(h * head_dim, (h + 1) * head_dim) for h in range(heads)]

    def for_query(j, c):
        sb = slot_block(j)
        there = pl.ds(pl.multiple_of(sb * blk, blk), blk)
        allowed = (doc_col[mine, :] == doc_row[sb]) & (iota_c + j * blk <= iota_r + b * blk)
        for h, cols in enumerate(spans):
            s = jnp.where(allowed, nt(q[mine, cols], k[there, cols]) * scale, NEG_BIG)
            p = jnp.exp(s - lse_col[mine, h:h + 1])
            dp = to_bf16(nt(do[mine, cols], v[there, cols]))
            ds = (p * (dp - del_col[mine, h:h + 1]) * scale).astype(BF16)
            acc[0, :, cols] += nn(ds, k[there, cols])
        return c

    lax.fori_loop(jmin, b + 1, for_query, 0)

    def for_key(j, c):
        sb = slot_block(j)
        there = pl.ds(pl.multiple_of(sb * blk, blk), blk)
        allowed = (doc_col[mine, :] == doc_row[sb]) & (iota_r + b * blk <= iota_c + j * blk)
        for h, cols in enumerate(spans):
            s = jnp.where(allowed, nt(k[mine, cols], q[there, cols]) * scale, NEG_BIG)
            p = jnp.exp(s - lse_row[sb, h:h + 1, :])
            dp = to_bf16(nt(v[mine, cols], do[there, cols]))
            ds = (p * (dp - del_row[sb, h:h + 1, :]) * scale).astype(BF16)
            acc[2, :, cols] += nn(p.astype(BF16), do[there, cols])
            acc[1, :, cols] += nn(ds, q[there, cols])
        return c

    lax.fori_loop(b, imax + 1, for_key, 0)
    cos, sin = unpack_angles(angles[:])
    for part in range(3):
        for h, cols in enumerate(spans):
            t = acc[part, :, cols]
            if part < 2:
                t = to_bf16(t)
                t = t * cos - pltpu.roll(t, head_dim // 2, 1) * sin
            out[:, part * width + h * head_dim:part * width + (h + 1) * head_dim] = t.astype(BF16)


def attend_back(info, ids, q, k, v, do, doc_col, doc_row, lse_col, lse_row, del_col, del_row, angles, blk):
    total, width = k.shape
    head_dim = angles.shape[1]
    heads = width // head_dim
    mine = lambda n: pl.BlockSpec((blk, n), lambda i, info, ids: (2 * info[0] + i, 0))
    arrays = (q, k, v, do, doc_col, doc_row, lse_col, lse_row, del_col, del_row)
    return pl.pallas_call(
        functools.partial(attend_back_kernel, heads=heads, head_dim=head_dim, scale=head_dim ** -0.5),
        out_shape=jax.ShapeDtypeStruct((2 * blk, 3 * width), BF16),
        grid_spec=pltpu.PrefetchScalarGridSpec(
            num_scalar_prefetch=2,
            grid=(2,),
            in_specs=[whole(a) for a in arrays] + [mine(head_dim)],
            out_specs=pl.BlockSpec((blk, 3 * width), lambda i, info, ids: (i, 0)),
            scratch_shapes=[pltpu.VMEM((3, blk, width), F32)],
        ),
        compiler_params=pltpu.CompilerParams(vmem_limit_bytes=FULL),
        cost_estimate=cost(14 * 2 * blk * total * width // 2),
        name="attend_back",
    )(info, ids, *arrays, angles)


def att_kernel(att, lse, x_all, w, gain, lse_out, res, act, parts, x, wide, send, recv, lse_send, lse_recv, load, swap_send, swap_recv):
    place = Place()
    rows, width = att.shape
    half = w.shape[1]
    mine = place.cp()
    loads = [pltpu.make_async_copy(src, dst, load.at[i]) for i, (src, dst) in enumerate(((x_all.at[pl.ds(mine * rows, rows), :], x), (w, wide.at[0])))]
    for c in loads:
        c.start()
    place.meet(("y", "z", "x", "core"))
    started = []
    near = ("y", "z")
    spans = column_parts(width, 2)

    def hop(p, flip, dim):
        there = tuple(d for d in near if (d in flip) != (d == dim))
        index = p * 3 + (there == ("y",)) + 2 * (there == ("z",))
        start, size = spans[p]
        cols = pl.ds(start, size)
        slot = place.tp(flip)
        src = parts.at[slot, :, cols] if flip else att.at[:, cols]
        return pltpu.make_async_remote_copy(src_ref=src, dst_ref=parts.at[slot, :, cols], send_sem=send.at[index], recv_sem=recv.at[index], device_id=place.device((dim,)), device_id_type=MESH)

    def lse_hop(step):
        src, slot, dim = ((lse, mine, "x"), (lse, mine, "core"), (lse_out.at[place.cp(("x",))], place.cp(("x",)), "core"))[step]
        return pltpu.make_async_remote_copy(src_ref=src, dst_ref=lse_out.at[slot], send_sem=lse_send.at[step], recv_sem=lse_recv.at[step], device_id=place.device((dim,)), device_id_type=MESH)

    def go(copy):
        copy.start()
        started.append(copy)

    other = pltpu.make_async_remote_copy(src_ref=w, dst_ref=wide.at[1], send_sem=swap_send, recv_sem=swap_recv, device_id=place.device(("core",)), device_id_type=MESH)
    for step in range(2):
        for p in range(2):
            go(hop(p, (), near[(p + step) % 2]))
    go(other)
    go(lse_hop(0))
    go(lse_hop(1))
    lse_out[mine] = lse[:]
    for c in loads:
        c.wait()

    def add(piece, slot, halves=(0, 1), first=False):
        for i in halves:
            cols = pl.ds(pl.multiple_of(place.coord("core", ("core",) if i else ()) * half, 128), half)
            t = nn(piece, wide[i, pl.ds(pl.multiple_of(slot * width, width), width), :])
            res[:, cols] = t + (x[:, cols].astype(F32) if first else res[:, cols])

    add(att[:], place.tp(), (0,), True)
    for p in range(2):
        hop(p, (), near[p]).wait_recv()
        go(hop(p, (near[p],), near[1 - p]))
    lse_hop(0).wait_recv()
    go(lse_hop(2))
    other.wait_recv()
    add(att[:], place.tp(), (1,), True)
    for p in (1, 0):
        hop(p, (), near[1 - p]).wait_recv()
        slot = place.tp((near[1 - p],))
        add(parts[slot], slot)
    for p in range(2):
        hop(p, (near[p],), near[1 - p]).wait_recv()
    slot = place.tp(near)
    add(parts[slot], slot)
    h = res[:]
    act[:] = (h * lax.rsqrt(mean_row(h * h) + NORM_EPS) * gain[:]).astype(BF16)
    lse_hop(1).wait_recv()
    lse_hop(2).wait_recv()
    for c in started:
        c.wait_send()


def att_project(att, lse, x_all, w, gain):
    rows, width = att.shape
    dim = x_all.shape[1]
    dma = pltpu.SemaphoreType.DMA
    vmem = pl.BlockSpec(memory_space=pltpu.VMEM)
    hbm = pl.BlockSpec(memory_space=pl.ANY)
    return pl.pallas_call(
        att_kernel,
        out_shape=[jax.ShapeDtypeStruct((4,) + lse.shape, F32), jax.ShapeDtypeStruct((rows, dim), F32), jax.ShapeDtypeStruct((rows, dim), BF16)],
        in_specs=[vmem, vmem, hbm, hbm, vmem],
        out_specs=[vmem] * 3,
        scratch_shapes=[
            pltpu.VMEM((4, rows, width), BF16), pltpu.VMEM((rows, dim), BF16), pltpu.VMEM((2,) + w.shape, BF16),
            *[dma((n,)) for n in (6, 6, 3, 3, 2)], dma, dma,
        ],
        compiler_params=pltpu.CompilerParams(collective_id=1, has_side_effects=True, vmem_limit_bytes=FULL),
        name="att_project",
    )(att, lse, x_all, w, gain)


def weight_grad_kernel(info, *refs, pieces, splits):
    lhs = refs[:pieces]
    rhs = refs[pieces:2 * pieces]
    outs = refs[2 * pieces:]
    t = tn(lhs[0][:], rhs[0][:])
    for a, b in zip(lhs[1:], rhs[1:]):
        t += tn(a[:], b[:])
    width = t.shape[1] // splits
    for i, out in enumerate(outs):
        out[:] = t[:, i * width:(i + 1) * width]


def weight_grad(info, lhs, rhs, block=256, splits=1, rows=None):
    def spec(arr, p, cols, moving):
        if arr.ndim == 3:
            return pl.BlockSpec((None, arr.shape[1], cols), lambda i, info: (info[0] ^ p, 0, i if moving else 0))
        return pl.BlockSpec((arr.shape[0], cols), lambda i, info: (0, i if moving else 0))

    tokens = lhs[0].shape[-2]
    rows, dim = rows or lhs[0].shape[-1], rhs[0].shape[-1]
    n = len(lhs)
    width = dim // splits
    outs = pl.pallas_call(
        functools.partial(weight_grad_kernel, pieces=n, splits=splits),
        out_shape=[jax.ShapeDtypeStruct((rows, width), F32)] * splits,
        grid_spec=pltpu.PrefetchScalarGridSpec(
            num_scalar_prefetch=1,
            grid=(pl.cdiv(rows, block),),
            in_specs=[spec(a, p, block, True) for p, a in enumerate(lhs)] + [spec(b, p, dim, False) for p, b in enumerate(rhs)],
            out_specs=[pl.BlockSpec((block, width), lambda i, info: (i, 0))] * splits,
        ),
        compiler_params=pltpu.CompilerParams(vmem_limit_bytes=56 * MIB),
        cost_estimate=cost(2 * n * tokens * rows * dim),
        name="weight_grad",
    )(info, *lhs, *rhs)
    return outs if splits > 1 else outs[0]


def mlp_kernel(act, dy, wg, wu, wd, hidden, d_gate, d_up, *rest, limit, tiles):
    i = pl.program_id(0)
    block = wg.shape[0]
    both = rest[-1]

    @pl.when(i < tiles)
    def _():
        left = limit - i * block
        row_ok = lax.broadcasted_iota(I32, (block, 1), 0) < left
        col_ok = lax.broadcasted_iota(I32, (1, block), 1) < left
        pair = pl.ds(pl.multiple_of(2 * i * block, block), 2 * block) if tiles < pl.num_programs(0) else slice(2 * block)
        both[pair] = jnp.concatenate([jnp.where(row_ok, w[:], 0).astype(BF16) for w in (wg, wu)])
        t = nt(act[:], both[pair])
        gate, up = t[:, :block], t[:, block:]
        dh = jnp.where(col_ok, to_bf16(nt(dy[:], wd[:])), 0)
        sig = jax.nn.sigmoid(gate)
        hidden[:] = (gate * sig * up).astype(BF16)
        dg = (dh * up * sig * (1.0 + gate * (1.0 - sig))).astype(BF16)
        du = (dh * gate * sig).astype(BF16)
        d_gate[:] = dg
        d_up[:] = du
        if len(rest) > 1:
            rest[1][:, pair] = jnp.concatenate([dg, du], axis=1)

    if len(rest) > 1:
        grad, grads = rest[:2]

        @pl.when(i >= tiles)
        def _():
            wide = grad.shape[1]
            grad[:] = nn(grads[:], both[:, pl.ds(pl.multiple_of((i - tiles) * wide, wide), wide)])


def mlp_block(act, dy, wg, wu, wd, with_grad, block=256, wide=512):
    rows, dim = act.shape
    limit = wg.shape[0]
    tiles = pl.cdiv(limit, block)
    steps = tiles + with_grad * dim // wide
    cols = pl.BlockSpec((rows, block), lambda i: (0, jnp.minimum(i, tiles - 1)))
    tile = pl.BlockSpec((block, dim), lambda i: (jnp.minimum(i, tiles - 1), 0))
    full = pl.BlockSpec((rows, dim), lambda i: (0, 0), pipeline_mode=pl.Buffered(1))
    deep = 2 * block * (tiles if with_grad else 1)
    return pl.pallas_call(
        functools.partial(mlp_kernel, limit=limit, tiles=tiles),
        out_shape=[jax.ShapeDtypeStruct((rows, tiles * block), BF16)] * 3 + [jax.ShapeDtypeStruct((rows, dim), F32)] * with_grad,
        grid=(steps,),
        in_specs=[full, full, tile, tile, tile],
        out_specs=[cols] * 3 + [pl.BlockSpec((rows, wide), lambda i: (0, jnp.maximum(i - tiles, 0)))] * with_grad,
        scratch_shapes=[pltpu.VMEM((rows, deep), BF16)] * with_grad + [pltpu.VMEM((deep, dim), BF16)],
        compiler_params=pltpu.CompilerParams(vmem_limit_bytes=FULL),
        cost_estimate=cost((6 + 4 * with_grad) * rows * dim * limit),
        name="mlp_block",
    )(act, dy, wg, wu, wd)


def zero_kernel(after, *refs, begin, end):
    out, zeros, sem = refs[-3:]
    zeros[:] = jnp.zeros_like(zeros)
    step = zeros.shape[0]

    def send(i, c):
        pltpu.make_async_copy(zeros, out.at[pl.ds(pl.multiple_of(i * step, step), step), :], sem).start()
        return c

    def wait(i, c):
        pltpu.make_async_copy(zeros, out.at[pl.ds(0, step), :], sem).wait()
        return c

    lax.fori_loop(begin // step, end // step, send, 0)
    lax.fori_loop(begin // step, end // step, wait, 0)


def zero_rows(after, shape, begin, end, base=(), step=200):
    return pl.pallas_call(
        functools.partial(zero_kernel, begin=begin, end=end),
        out_shape=jax.ShapeDtypeStruct(shape, F32),
        in_specs=[pl.BlockSpec(memory_space=pltpu.SMEM)] + [pl.BlockSpec(memory_space=pl.ANY)] * len(base),
        out_specs=pl.BlockSpec(memory_space=pl.ANY),
        scratch_shapes=[pltpu.VMEM((step, shape[1]), F32), pltpu.SemaphoreType.DMA],
        input_output_aliases={1: 0} if base else {},
        compiler_params=pltpu.CompilerParams(vmem_limit_bytes=8 * MIB),
        cost_estimate=cost((end - begin) * shape[1]),
        name="zero_rows",
    )(after, *base)


def scatter_kernel(order, sid, runs, bounds, rows, base_hbm, out_hbm, sums, row_sem, sum_sem):
    lo = bounds[0]
    hi = bounds[1]

    def one(c):
        p, singles, multi = c
        n = runs[p]
        t = order[p]
        single = n == 1

        @pl.when(single)
        def _():
            pltpu.make_async_copy(rows.at[pl.ds(t, 1), :], out_hbm.at[pl.ds(sid[p], 1), :], row_sem).start()

        @pl.when(jnp.logical_not(single))
        def _():
            def add(j, acc):
                return acc + rows[pl.ds(order[p + j], 1), :]

            sums[pl.ds(multi, 1), :] = lax.fori_loop(1, n, add, rows[pl.ds(t, 1), :])

        return p + n, singles + single.astype(I32), multi + 1 - single.astype(I32)

    _, singles, multi = lax.while_loop(lambda c: c[0] < hi, one, (lo, 0, 0))

    def two(c):
        p, k = c
        n = runs[p]

        @pl.when(n > 1)
        def _():
            pltpu.make_async_copy(sums.at[pl.ds(k, 1), :], out_hbm.at[pl.ds(sid[p], 1), :], sum_sem).start()

        return p + n, k + (n > 1).astype(I32)

    lax.while_loop(lambda c: c[0] < hi, two, (lo, 0))

    def wait(sem):
        def body(i, c):
            pltpu.make_async_copy(sums.at[pl.ds(0, 1), :], out_hbm.at[pl.ds(0, 1), :], sem).wait()
            return c

        return body

    lax.fori_loop(0, singles, wait(row_sem), 0)
    lax.fori_loop(0, multi, wait(sum_sem), 0)


def scatter_rows(order, sid, runs, bounds, grads, base, tokens):
    _, dim = grads.shape
    rows = base.shape[0]
    return pl.pallas_call(
        scatter_kernel,
        out_shape=jax.ShapeDtypeStruct((rows, dim), F32),
        grid_spec=pltpu.PrefetchScalarGridSpec(
            num_scalar_prefetch=4,
            grid=(),
            in_specs=[pl.BlockSpec(memory_space=pltpu.VMEM), pl.BlockSpec(memory_space=pl.ANY)],
            out_specs=pl.BlockSpec(memory_space=pl.ANY),
            scratch_shapes=[pltpu.VMEM((tokens // 2, dim), F32), pltpu.SemaphoreType.DMA, pltpu.SemaphoreType.DMA],
        ),
        input_output_aliases={5: 0},
        compiler_params=pltpu.CompilerParams(vmem_limit_bytes=FULL),
        name="scatter_rows",
    )(order, sid, runs, bounds, grads, base)


def solution(mesh):
    cp_count = mesh.shape["cp"]
    tp_count = mesh.shape["tp"]
    both = ("cp", "tp")
    x_swap = [(i, i ^ 2) for i in range(cp_count)]
    core_swap = [(i, i ^ 1) for i in range(cp_count)]

    def compute(tokens, pos, doc_id, dy, table, w_q, w_k, w_v, w_o, w_gate, w_up, w_down, gain_one, gain_two, inv_freq):
        span = tokens.shape[0]
        total = span * cp_count
        part = span // tp_count
        rows, dim = table.shape
        head_dim = 2 * inv_freq.shape[0]
        heads = w_q.shape[1] // head_dim
        width = heads * head_dim
        tp_rank = lax.axis_index("tp")
        cp_rank = lax.axis_index("cp")
        core = cp_rank % 2
        gain_a = gain_one.astype(F32)
        gain_b = gain_two.astype(F32)

        barrier = lax.optimization_barrier
        join = lambda arr, axis: lax.all_gather(arr, axis, axis=0, tiled=True)
        add_up = lambda arr: lax.psum_scatter(arr, "tp", scatter_dimension=0, tiled=True)
        swap = lambda arr, pairs, axis="cp": lax.ppermute(arr, axis, pairs)
        local_ids = tokens - tp_rank * rows
        owned = (local_ids >= 0) & (local_ids < rows)
        safe_ids = jnp.where(owned, local_ids, jnp.arange(span) * (rows // span))
        picked = jnp.where(owned[:, None], jnp.take(table, safe_ids, axis=0), 0).astype(BF16)
        info = jnp.stack([cp_rank, core]).astype(I32)
        half = dim // 2
        angle = pos.astype(F32)[:, None] * inv_freq[None, :]
        side_f = jnp.concatenate([jnp.cos(angle), jnp.sin(angle)], axis=1)
        side_i = jnp.stack([tokens, doc_id] * 4)
        x_all, x_slice, angles, ints = embed_gather(picked.reshape(tp_count, part, dim), side_f, side_i)
        angles = angles.reshape(total, head_dim)
        tok_all = ints[:, 0, :].reshape(total)
        doc_all = ints[:, 1, :].reshape(total)
        wo_half = barrier((lax.dynamic_slice_in_dim(w_o, core * half, half, 1), x_all))[0]
        wo_half = join(wo_half, "tp")

        dy_x = swap(barrier((dy, x_all))[0], x_swap)
        act_a, query, key, value = project_qkv(x_all, gain_a[None, :], w_q, w_k, w_v, angles)

        blk = span // 2
        blocks = total // blk
        doc_col = doc_all[:, None]
        doc_row = doc_all.reshape(blocks, 1, blk)
        attended, lse = attend(info, ints, query, key, value, doc_col, doc_row, head_dim, blk)

        tok_all = barrier((tok_all, attended))[0]
        slot_ids = jnp.arange(total, dtype=I32)
        before = (tok_all[None, :] < tok_all[:, None]) | ((tok_all[None, :] == tok_all[:, None]) & (slot_ids[None, :] < slot_ids[:, None]))
        rank = jnp.sum(before.astype(I32), axis=1)
        count = jnp.sum((tok_all[None, :] == tok_all[:, None]).astype(I32), axis=1)
        at_rank = rank[None, :] == slot_ids[:, None]
        runs = jnp.sum(jnp.where(at_rank, count[None, :], 0), axis=1)
        order = jnp.sum(jnp.where(at_rank, slot_ids[None, :], 0), axis=1)
        sid = jnp.sum(jnp.where(at_rank, tok_all[None, :], 0), axis=1) - tp_rank * rows
        order = order + 8 * (order // part)
        bounds = jnp.stack([jnp.sum((tok_all < tp_rank * rows).astype(I32)), jnp.sum((tok_all < (tp_rank + 1) * rows).astype(I32))])
        wo_half, runs, order, sid, bounds = barrier((wo_half, runs, order, sid, bounds))
        heads_x = swap(attended, x_swap)
        lse_all, residual, act_b = att_project(attended, lse, x_all, wo_half, gain_b[None, :])
        lse_all = lse_all.reshape(total, 8)
        act_x = swap(act_b, x_swap)
        wg, wu = w_gate.T, w_up.T
        ffn = wg.shape[0]
        hidden, d_gate, d_up, d_act_b = mlp_block(act_b, dy, wg, wu, w_down, True)
        d_act_b = add_up(d_act_b)
        hidden_x, d_gate_x, d_up_x = mlp_block(act_x, dy_x, wg, wu, w_down, False)
        out_part = nn(hidden[:, :ffn], w_down)
        split = rows // 1000 * 600
        base = zero_rows(bounds, (rows, dim), 0, split)
        heads_x = barrier((heads_x, act_b))[0]
        head_parts = (attended, swap(attended, core_swap), heads_x, swap(heads_x, core_swap))
        att_heads = jnp.zeros((total, width), BF16)
        for k, piece in enumerate(head_parts):
            att_heads = lax.dynamic_update_slice_in_dim(att_heads, piece, (cp_rank ^ k) * span, 0)
        d_act_b, hidden_x, d_gate_x, d_up_x, out_part, base, att_heads = barrier((d_act_b, hidden_x, d_gate_x, d_up_x, out_part, base, att_heads))
        d_act_b = to_bf16(d_act_b)
        acts, dys, hiddens, d_gates, d_ups = [(a, swap(a, core_swap), b, swap(b, core_swap)) for a, b in (
            (act_b, act_x), (dy, dy_x), (hidden, hidden_x), (d_gate, d_gate_x), (d_up, d_up_x))]
        grad_down = weight_grad(info, hiddens, dys, rows=ffn)
        grad_gate = weight_grad(info, d_gates, acts, rows=ffn)
        grad_up = weight_grad(info, d_ups, acts, rows=ffn)

        def mine(arr):
            return lax.dynamic_slice_in_dim(arr, tp_rank * part, part, 0)

        res_part = mine(residual)
        normed_b, inv_b = rms_stats(res_part)
        grad_gain_b = jnp.sum(d_act_b * normed_b, axis=0)
        d_resid = mine(dy).astype(F32) + rms_back(d_act_b * gain_b, normed_b, inv_b)
        d_resid_all, out_part = barrier((spread(d_resid.astype(BF16)), out_part))
        out_slice = add_up(out_part)
        out_slice = (res_part + out_slice).astype(BF16)

        d_att = nt(d_resid_all, w_o)
        d_att_b = d_att.astype(BF16)
        head_of = (jnp.arange(width)[None, :] // head_dim == jnp.arange(8)[:, None]).astype(F32)
        prod = att_heads.astype(F32) * d_att_b.astype(F32)
        delta = lax.dot_general(head_of, prod, (((1,), (1,)), ((), ())), precision=lax.Precision.HIGHEST, preferred_element_type=F32)

        def by_block(arr):
            return jnp.transpose(arr.reshape(8, blocks, blk), (1, 0, 2))

        dqkv = attend_back(info, ints, query, key, value, d_att_b, doc_col, doc_row, lse_all, by_block(lse_all.T), delta.T, by_block(delta), angles, blk)
        d_act_a = sum(nt(dqkv[:, i * width:(i + 1) * width], w) for i, w in enumerate((w_q, w_k, w_v)))
        d_act_a, out_slice = barrier((d_act_a, out_slice))
        d_act_a = add_up(d_act_a)
        dqkv_x = swap(dqkv, x_swap)
        dqkvs = (dqkv, swap(dqkv, core_swap), dqkv_x, swap(dqkv_x, core_swap))
        grad_out = weight_grad(info, head_parts, [d_resid_all.reshape(cp_count, span, dim)] * 4)
        base = zero_rows(bounds, (rows, dim), split, rows, (barrier((base, dqkv))[0],))
        d_act_a, dqkv_x, grad_out, grad_up, base = barrier((d_act_a, dqkv_x, grad_out, grad_up, base))
        d_act_a = to_bf16(d_act_a)
        normed_a, inv_a = rms_stats(x_slice.astype(F32))
        grad_gain_a = jnp.sum(d_act_a * normed_a, axis=0)
        d_embed = d_resid + rms_back(d_act_a * gain_a, normed_a, inv_a)
        payload = jnp.concatenate([d_embed, jnp.stack([grad_gain_a, grad_gain_b] * 4)])
        gathered = join(payload, both)
        grad_qkv = weight_grad(info, [act_a.reshape(cp_count, span, dim)] * 4, dqkvs, splits=3)
        gathered, grad_qkv, grad_gate, grad_down = barrier((gathered, grad_qkv, grad_gate, grad_down))
        out_slice = barrier((out_slice, grad_qkv))[0]
        layer_out = jnp.concatenate([out_slice] * tp_count)
        for k in range(1, tp_count):
            piece = swap(out_slice, [(i, i ^ k) for i in range(tp_count)], "tp")
            layer_out = lax.dynamic_update_slice_in_dim(layer_out, piece, (tp_rank ^ k) * part, 0)
        gain_grads = jnp.sum(gathered.reshape(cp_count * tp_count, part + 8, dim)[:, part:part + 2], axis=0)
        grad_table = scatter_rows(order, sid, runs, bounds, gathered, base, total)
        return (layer_out, grad_table, *grad_qkv, grad_out, grad_gate.T, grad_up.T, grad_down, gain_grads[0], gain_grads[1])

    col_spec = P(None, "tp")
    row_spec = P("tp")
    tok_spec = P("cp")
    rep_spec = P()
    in_specs = (tok_spec, tok_spec, tok_spec, P("cp"), row_spec, col_spec, col_spec, col_spec, row_spec, col_spec, col_spec, row_spec, rep_spec, rep_spec, rep_spec)
    out_specs = (P("cp"), row_spec, col_spec, col_spec, col_spec, row_spec, col_spec, col_spec, row_spec, rep_spec, rep_spec)
    return jax.shard_map(compute, mesh=mesh, in_specs=in_specs, out_specs=out_specs, check_vma=False)
```

```python
import functools
import jax
import jax.numpy as jnp
from jax import lax
from jax.experimental import pallas as pl
from jax.experimental.pallas import tpu as pltpu
from jax.sharding import PartitionSpec as P

NORM_EPS = 1e-5
NEG_BIG = -1e30
MIB = 2 ** 20
FULL = 62 * MIB
F32 = jnp.float32
BF16 = jnp.bfloat16
I32 = jnp.int32


def rms_stats(feats):
    inv_rms = lax.rsqrt(mean_row(feats * feats) + NORM_EPS)
    return feats * inv_rms, inv_rms


def rms_back(d_normed, normed, inv_rms):
    return inv_rms * (d_normed - normed * mean_row(d_normed * normed))


def to_bf16(feats):
    return feats.astype(BF16).astype(F32)


def contract(a, b, ca, cb):
    return lax.dot_general(a, b, (((ca,), (cb,)), ((), ())), preferred_element_type=F32)


def row_sum(t):
    return jnp.sum(t, 1, keepdims=True)


def mean_row(t):
    return row_sum(t) / t.shape[1]


def whole(a):
    return pl.BlockSpec(a.shape, lambda *i: (0,) * a.ndim)


def cost(flops):
    return pl.CostEstimate(flops=flops, bytes_accessed=flops // 512, transcendentals=0)


def nn(a, b):
    return contract(a, b, 1, 0)


def nt(a, b):
    return contract(a, b, 1, 1)


def tn(a, b):
    return contract(a, b, 0, 0)


DIMS = ("x", "y", "z")


class Place:
    def __init__(self):
        tp = lax.axis_index("tp")
        cp = lax.axis_index("cp")
        self.at = {"x": cp // 2, "core": cp % 2, "z": tp // 2, "y": tp % 2}

    def coord(self, dim, flip):
        return 1 - self.at[dim] if dim in flip else self.at[dim]

    def tp(self, flip=()):
        return self.coord("z", flip) * 2 + self.coord("y", flip)

    def cp(self, flip=()):
        return self.coord("x", flip) * 2 + self.coord("core", flip)

    def device(self, flip):
        return {"tp": self.tp(flip), "cp": self.cp(flip)}

    def slot(self, flip=()):
        return self.cp(flip) * 4 + self.tp(flip)

    def meet(self, dims):
        barrier = pltpu.get_barrier_semaphore()
        for d in dims:
            pl.semaphore_signal(barrier, inc=1, device_id=self.device((d,)), device_id_type=MESH)
        pl.semaphore_wait(barrier, len(dims))


MESH = pl.DeviceIdType.MESH
ORDERS = (("x", "y", "z"), ("y", "z", "x"), ("z", "x", "y"))
COUNTS = (21, 21, 24, 24, 48)
FLIPS = tuple(tuple(d for i, d in enumerate(DIMS) if n >> i & 1) for n in range(8))


def flip_code(flip):
    return sum(1 << DIMS.index(d) for d in flip)


def column_parts(width, count):
    tiles = width // 128
    sizes = [(tiles // count + (i < tiles % count)) * 128 for i in range(count)]
    return [(sum(sizes[:i]), n) for i, n in enumerate(sizes)]


class Gather:
    def __init__(self, place, buf, out, send, recv, core_send, core_recv, out_sem):
        self.place, self.buf, self.out = place, buf, out
        self.send, self.recv, self.core_send, self.core_recv, self.out_sem = send, recv, core_send, core_recv, out_sem
        self.parts = column_parts(buf.shape[2], 3)
        self.started, self.stores = [], []

    def view(self, part, flip):
        start, size = self.parts[part]
        return self.buf.at[self.place.slot(flip), :, pl.ds(start, size)]

    def hop(self, part, flip, dim):
        there = tuple(d for d in DIMS if (d in flip) != (d == dim))
        index = part * 7 + flip_code(there) - 1
        ref = self.view(part, flip)
        return pltpu.make_async_remote_copy(src_ref=ref, dst_ref=ref, send_sem=self.send.at[index], recv_sem=self.recv.at[index], device_id=self.place.device((dim,)), device_id_type=MESH)

    def core_hop(self, part, flip):
        index = part * 8 + flip_code(flip)
        ref = self.view(part, flip)
        return pltpu.make_async_remote_copy(src_ref=ref, dst_ref=ref, send_sem=self.core_send.at[index], recv_sem=self.core_recv.at[index], device_id=self.place.device(("core",)), device_id_type=MESH)

    def go(self, copy):
        copy.start()
        self.started.append(copy)

    def wait(self, part, flip):
        order = ORDERS[part]
        last = max(order.index(d) for d in flip)
        came = tuple(d for d in flip if d != order[last])
        self.hop(part, came, order[last]).wait_recv()
        for dim in order[last + 1:]:
            self.go(self.hop(part, flip, dim))
        self.go(self.core_hop(part, flip))
        self.store(part, flip)

    def take(self, part, flip):
        index = part * 8 + flip_code(flip)
        there = flip + ("core",)
        ref = self.view(part, there)
        pltpu.make_async_remote_copy(src_ref=ref, dst_ref=ref, send_sem=self.core_send.at[index], recv_sem=self.core_recv.at[index], device_id=self.place.device(("core",)), device_id_type=MESH).wait_recv()
        self.store(part, there)

    def store(self, part, flip):
        start, size = self.parts[part]
        rows = self.buf.shape[1]
        dst = self.out.at[pl.ds(self.place.slot(flip) * rows, rows), pl.ds(start, size)]
        copy = pltpu.make_async_copy(self.view(part, flip), dst, self.out_sem.at[len(self.stores)])
        copy.start()
        self.stores.append(copy)

    def run(self):
        for step in range(3):
            for part, order in enumerate(ORDERS):
                self.go(self.hop(part, (), order[step]))
        pending = [(part, ()) for part in range(3)]
        for item in pending:
            self.go(self.core_hop(*item))
            self.store(*item)
        for step in range(3):
            batch = [(part, flip) for flip in sorted(FLIPS[1:], key=len) for part, order in enumerate(ORDERS) if max(order.index(d) for d in flip) == step]
            for item in batch:
                self.wait(*item)
            for item in pending:
                self.take(*item)
            pending = batch
        for item in pending:
            self.take(*item)
        for c in self.started:
            c.wait_send()
        for c in self.stores:
            c.wait()


def embed_kernel(picked, side_f, side_i, out, slice_out, all_f, all_i, buf, r1, r2, tmp, send, recv, core_send, core_recv, out_sem, rs_send, rs_recv, side_send, side_recv, slice_sem):
    place = Place()
    place.meet(("x", "y", "z", "core"))
    half = buf.shape[2] // 2
    near = ("y", "z")

    sides = ((side_f, all_f), (side_i, all_i))
    started, keeps = [], []

    def side_hop(i, step):
        src, dst = sides[i]
        if step == 0:
            src_ref, slot, dim = src, place.cp(), "x"
        elif step == 1:
            src_ref, slot, dim = src, place.cp(), "core"
        else:
            src_ref, slot, dim = dst.at[place.cp(("x",))], place.cp(("x",)), "core"
        return pltpu.make_async_remote_copy(src_ref=src_ref, dst_ref=dst.at[slot], send_sem=side_send.at[i, step], recv_sem=side_recv.at[i, step], device_id=place.device((dim,)), device_id_type=MESH)

    def first(h, k):
        a, b = near[h], near[1 - h]
        target = place.tp((a,)) if k == 0 else place.tp((a, b))
        cols = pl.ds(h * half, half)
        return pltpu.make_async_remote_copy(src_ref=picked.at[target, :, cols], dst_ref=r1.at[h, k], send_sem=rs_send.at[h, k], recv_sem=rs_recv.at[h, k], device_id=place.device((a,)), device_id_type=MESH)

    def second(h):
        return pltpu.make_async_remote_copy(src_ref=tmp.at[h], dst_ref=r2.at[h], send_sem=rs_send.at[h, 2], recv_sem=rs_recv.at[h, 2], device_id=place.device((near[1 - h],)), device_id_type=MESH)

    def go(copy):
        copy.start()
        started.append(copy)

    for k in (1, 0):
        for h in range(2):
            go(first(h, k))
    for i in range(2):
        go(side_hop(i, 0))
        go(side_hop(i, 1))
        keeps.append(pltpu.make_async_copy(sides[i][0], sides[i][1].at[place.cp()], slice_sem.at[i]))
        keeps[i].start()
    for h in range(2):
        cols = slice(h * half, (h + 1) * half)
        first(h, 1).wait_recv()
        tmp[h] = picked[place.tp((near[1 - h],)), :, cols] + r1[h, 1]
        go(second(h))
    for i in range(2):
        side_hop(i, 0).wait_recv()
        go(side_hop(i, 2))
    mine = place.slot()
    for h in range(2):
        cols = slice(h * half, (h + 1) * half)
        first(h, 0).wait_recv()
        part = picked[place.tp(), :, cols] + r1[h, 0]
        second(h).wait_recv()
        buf[mine, :, cols] = part + r2[h]
    keeps.append(pltpu.make_async_copy(buf.at[mine], slice_out, slice_sem.at[2]))
    keeps[-1].start()
    Gather(place, buf, out, send, recv, core_send, core_recv, out_sem).run()
    for c in keeps:
        c.wait()
    for i in range(2):
        side_hop(i, 1).wait_recv()
        side_hop(i, 2).wait_recv()
    for c in started:
        c.wait_send()


def embed_gather(picked, side_f, side_i):
    _, rows, dim = picked.shape
    half = dim // 2
    dma = pltpu.SemaphoreType.DMA
    vmem = pl.BlockSpec(memory_space=pltpu.VMEM)
    hbm = pl.BlockSpec(memory_space=pl.ANY)
    return pl.pallas_call(
        embed_kernel,
        out_shape=[
            jax.ShapeDtypeStruct((16 * rows, dim), BF16),
            jax.ShapeDtypeStruct((rows, dim), BF16),
            jax.ShapeDtypeStruct((4,) + side_f.shape, F32),
            jax.ShapeDtypeStruct((4,) + side_i.shape, I32),
        ],
        in_specs=[vmem, vmem, vmem],
        out_specs=[pl.BlockSpec(memory_space=pltpu.HBM)] * 4,
        scratch_shapes=[
            pltpu.VMEM((16, rows, dim), BF16),
            pltpu.VMEM((2, 2, rows, half), BF16),
            pltpu.VMEM((2, rows, half), BF16),
            pltpu.VMEM((2, rows, half), BF16),
            *[dma((n,)) for n in COUNTS],
            *[dma((2, 3))] * 4, dma((3,)),
        ],
        compiler_params=pltpu.CompilerParams(collective_id=0, has_side_effects=True, vmem_limit_bytes=FULL),
        name="embed_gather",
    )(picked, side_f, side_i)


def spread_kernel(d_act, res, dy, gain, out, d_resid, d_gain, buf, send, recv, core_send, core_recv, out_sem):
    place = Place()
    d = to_bf16(d_act[:])
    normed, inv = rms_stats(res[:])
    t = dy[:].astype(F32) + rms_back(d * gain[:], normed, inv)
    d_resid[:] = t
    d_gain[:] = jnp.sum(d * normed, 0, keepdims=True)
    buf[place.slot()] = t.astype(BF16)
    place.meet(("x", "y", "z", "core"))
    Gather(place, buf, out, send, recv, core_send, core_recv, out_sem).run()


def spread(d_act, res, dy, gain):
    rows, dim = res.shape
    dma = pltpu.SemaphoreType.DMA
    vmem = pl.BlockSpec(memory_space=pltpu.VMEM)
    return pl.pallas_call(
        spread_kernel,
        out_shape=[jax.ShapeDtypeStruct((16 * rows, dim), BF16), jax.ShapeDtypeStruct((rows, dim), F32), jax.ShapeDtypeStruct((1, dim), F32)],
        in_specs=[vmem] * 4,
        out_specs=[pl.BlockSpec(memory_space=pltpu.HBM), vmem, vmem],
        scratch_shapes=[pltpu.VMEM((16, rows, dim), BF16), *[dma((n,)) for n in COUNTS]],
        compiler_params=pltpu.CompilerParams(collective_id=2, has_side_effects=True, vmem_limit_bytes=FULL),
        name="spread",
    )(d_act, res, dy, gain)


def payload_kernel(d_act, x, d_resid, gain, d_gain_b, out):
    rows = x.shape[0]
    d = to_bf16(d_act[:])
    normed, inv = rms_stats(x[:].astype(F32))
    out[:rows] = d_resid[:] + rms_back(d * gain[:], normed, inv)
    d_gain_a = jnp.sum(d * normed, 0, keepdims=True)
    extra = (out.shape[0] - rows, out.shape[1])
    out[rows:] = jnp.where(lax.broadcasted_iota(I32, extra, 0) == 0, d_gain_a, d_gain_b[:])


def payload_rows(d_act, x, d_resid, gain, d_gain_b):
    rows, dim = x.shape
    return pl.pallas_call(
        payload_kernel,
        out_shape=jax.ShapeDtypeStruct((rows + 8, dim), F32),
        compiler_params=pltpu.CompilerParams(vmem_limit_bytes=FULL),
        name="payload_rows",
    )(d_act, x, d_resid, gain, d_gain_b)


def slot_block(j):
    return jnp.where(j < 4, 2 * j, 15 - 2 * j)


def unpack_angles(packed):
    turned = pltpu.roll(packed, packed.shape[1] // 2, 1)
    low = lax.broadcasted_iota(I32, packed.shape, 1) < packed.shape[1] // 2
    return jnp.where(low, packed, turned), jnp.where(low, -turned, packed)


def qkv_kernel(x, gain, wq, wk, wv, angles, act, q, k, v, wide, *, head_dim):
    width = wq.shape[1]

    @pl.when(pl.program_id(0) == 0)
    def _():
        for i, w in enumerate((wq, wk, wv)):
            wide[:, i * width:(i + 1) * width] = w[:]

    feats = x[:].astype(F32)
    inv = lax.rsqrt(mean_row(feats * feats) + NORM_EPS)
    a = (feats * inv * gain[:]).astype(BF16)
    act[:] = a
    t = nn(a, wide[:])
    cos, sin = unpack_angles(angles[:])
    for i, out in enumerate((q, k, v)):
        for h in range(width // head_dim):
            th = t[:, i * width + h * head_dim:i * width + (h + 1) * head_dim]
            if i < 2:
                th = th * cos + pltpu.roll(th, head_dim // 2, 1) * sin
            out[:, h * head_dim:(h + 1) * head_dim] = th.astype(BF16)


def project_qkv(x_all, gain, wq, wk, wv, angles, block=512):
    total, dim = x_all.shape
    width = wq.shape[1]
    head_dim = angles.shape[1]
    rows = lambda n: pl.BlockSpec((block, n), lambda i: (i, 0))
    whole = lambda a: pl.BlockSpec(a.shape, lambda i: (0, 0), pipeline_mode=pl.Buffered(1))
    return pl.pallas_call(
        functools.partial(qkv_kernel, head_dim=head_dim),
        out_shape=[jax.ShapeDtypeStruct((total, n), BF16) for n in (dim, width, width, width)],
        grid=(total // block,),
        in_specs=[rows(dim), whole(gain), whole(wq), whole(wk), whole(wv), rows(head_dim)],
        out_specs=[rows(dim), rows(width), rows(width), rows(width)],
        scratch_shapes=[pltpu.VMEM((dim, 3 * width), BF16)],
        compiler_params=pltpu.CompilerParams(vmem_limit_bytes=FULL),
        cost_estimate=cost(6 * total * dim * width),
        name="project_qkv",
    )(x_all, gain, wq, wk, wv, angles)


def block_range(info, ids, i, blocks):
    r = info[0]
    blk = ids.shape[2] // 2
    b = jnp.where(i == 0, r, blocks - 1 - r)

    def docs(shard, half):
        return ids[shard, 1, half * blk], ids[shard, 1, half * blk + blk - 1]

    first, last = docs(r, i)
    jmin, imax = 0, -1
    for j in range(blocks):
        begin, end = docs(min(j, blocks - 1 - j), int(j >= blocks // 2))
        jmin = jmin + (end < first).astype(I32)
        imax = imax + (begin <= last).astype(I32)
    return b, jmin, imax


def attend_kernel(info, ids, q, k, v, doc_col, doc_row, out, lse, sc, *, heads, head_dim, scale):
    blk = q.shape[0]
    b, jmin, _ = block_range(info, ids, pl.program_id(0), doc_row.shape[0])
    row_n = lax.broadcasted_iota(I32, (blk, blk), 0) + b * blk
    col_n = lax.broadcasted_iota(I32, (blk, blk), 1)

    def score(j, peaks):
        sb = slot_block(j)
        off = pl.multiple_of(sb * blk, blk)
        allowed = (doc_col[:] == doc_row[sb]) & (col_n + j * blk <= row_n)
        new = []
        for h in range(heads):
            cols = slice(h * head_dim, (h + 1) * head_dim)
            s = nt(q[:, cols], k[pl.ds(off, blk), cols]) * scale
            s = jnp.where(allowed, s, NEG_BIG)
            sc[j, h] = s
            new.append(jnp.maximum(peaks[h], jnp.max(s, axis=1, keepdims=True)))
        return tuple(new)

    peaks = lax.fori_loop(jmin, b + 1, score, tuple(jnp.full((blk, 1), NEG_BIG, F32) for _ in range(heads)))

    def weigh(j, sums):
        new = []
        for h in range(heads):
            p = jnp.exp(sc[j, h] - peaks[h])
            sc[j, h] = p
            new.append(sums[h] + row_sum(p))
        return tuple(new)

    sums = lax.fori_loop(jmin, b + 1, weigh, tuple(jnp.zeros((blk, 1), F32) for _ in range(heads)))
    inv = tuple(1.0 / t for t in sums)
    for h in range(heads):
        lse[:, h:h + 1] = peaks[h] + jnp.log(sums[h])

    def mix(j, acc):
        off = pl.multiple_of(slot_block(j) * blk, blk)
        new = []
        for h in range(heads):
            cols = slice(h * head_dim, (h + 1) * head_dim)
            new.append(acc[h] + nn((sc[j, h] * inv[h]).astype(BF16), v[pl.ds(off, blk), cols]))
        return tuple(new)

    acc = lax.fori_loop(jmin, b + 1, mix, tuple(jnp.zeros((blk, head_dim), F32) for _ in range(heads)))
    for h in range(heads):
        out[:, h * head_dim:(h + 1) * head_dim] = acc[h].astype(BF16)


def attend(info, ids, q, k, v, doc_col, doc_row, head_dim, blk):
    total, width = k.shape
    heads = width // head_dim
    mine = lambda n: pl.BlockSpec((blk, n), lambda i, info, ids: (2 * info[0] + i, 0))
    return pl.pallas_call(
        functools.partial(attend_kernel, heads=heads, head_dim=head_dim, scale=head_dim ** -0.5),
        out_shape=[jax.ShapeDtypeStruct((2 * blk, width), BF16), jax.ShapeDtypeStruct((2 * blk, 8), F32)],
        grid_spec=pltpu.PrefetchScalarGridSpec(
            num_scalar_prefetch=2,
            grid=(2,),
            in_specs=[mine(width), whole(k), whole(v), mine(1), whole(doc_row)],
            out_specs=[pl.BlockSpec((blk, width), lambda i, info, ids: (i, 0)), pl.BlockSpec((blk, 8), lambda i, info, ids: (i, 0))],
            scratch_shapes=[pltpu.VMEM((total // blk, heads, blk, blk), F32)],
        ),
        compiler_params=pltpu.CompilerParams(vmem_limit_bytes=FULL),
        cost_estimate=cost(4 * 2 * blk * total * width),
        name="attend",
    )(info, ids, q, k, v, doc_col, doc_row)


def attend_back_kernel(info, ids, q, k, v, do, doc_col, doc_row, lse_col, lse_row, del_col, del_row, angles, out, acc, *, heads, head_dim, scale):
    blk = angles.shape[0]
    width = heads * head_dim
    i = pl.program_id(0)
    b, jmin, imax = block_range(info, ids, i, doc_row.shape[0])
    me = pl.multiple_of((2 * info[0] + i) * blk, blk)
    mine = pl.ds(me, blk)
    iota_r = lax.broadcasted_iota(I32, (blk, blk), 0)
    iota_c = lax.broadcasted_iota(I32, (blk, blk), 1)
    acc[:] = jnp.zeros_like(acc)
    spans = [slice(h * head_dim, (h + 1) * head_dim) for h in range(heads)]

    def for_query(j, c):
        sb = slot_block(j)
        there = pl.ds(pl.multiple_of(sb * blk, blk), blk)
        allowed = (doc_col[mine, :] == doc_row[sb]) & (iota_c + j * blk <= iota_r + b * blk)
        for h, cols in enumerate(spans):
            s = jnp.where(allowed, nt(q[mine, cols], k[there, cols]) * scale, NEG_BIG)
            p = jnp.exp(s - lse_col[mine, h:h + 1])
            dp = to_bf16(nt(do[mine, cols], v[there, cols]))
            ds = (p * (dp - del_col[mine, h:h + 1]) * scale).astype(BF16)
            acc[0, :, cols] += nn(ds, k[there, cols])
        return c

    lax.fori_loop(jmin, b + 1, for_query, 0)

    def for_key(j, c):
        sb = slot_block(j)
        there = pl.ds(pl.multiple_of(sb * blk, blk), blk)
        allowed = (doc_col[mine, :] == doc_row[sb]) & (iota_r + b * blk <= iota_c + j * blk)
        for h, cols in enumerate(spans):
            s = jnp.where(allowed, nt(k[mine, cols], q[there, cols]) * scale, NEG_BIG)
            p = jnp.exp(s - lse_row[sb, h:h + 1, :])
            dp = to_bf16(nt(v[mine, cols], do[there, cols]))
            ds = (p * (dp - del_row[sb, h:h + 1, :]) * scale).astype(BF16)
            acc[2, :, cols] += nn(p.astype(BF16), do[there, cols])
            acc[1, :, cols] += nn(ds, q[there, cols])
        return c

    lax.fori_loop(b, imax + 1, for_key, 0)
    cos, sin = unpack_angles(angles[:])
    for part in range(3):
        for h, cols in enumerate(spans):
            t = acc[part, :, cols]
            if part < 2:
                t = to_bf16(t)
                t = t * cos - pltpu.roll(t, head_dim // 2, 1) * sin
            out[:, part * width + h * head_dim:part * width + (h + 1) * head_dim] = t.astype(BF16)


def attend_back(info, ids, q, k, v, do, doc_col, doc_row, lse_col, lse_row, del_col, del_row, angles, blk):
    total, width = k.shape
    head_dim = angles.shape[1]
    heads = width // head_dim
    mine = lambda n: pl.BlockSpec((blk, n), lambda i, info, ids: (2 * info[0] + i, 0))
    arrays = (q, k, v, do, doc_col, doc_row, lse_col, lse_row, del_col, del_row)
    return pl.pallas_call(
        functools.partial(attend_back_kernel, heads=heads, head_dim=head_dim, scale=head_dim ** -0.5),
        out_shape=jax.ShapeDtypeStruct((2 * blk, 3 * width), BF16),
        grid_spec=pltpu.PrefetchScalarGridSpec(
            num_scalar_prefetch=2,
            grid=(2,),
            in_specs=[whole(a) for a in arrays] + [mine(head_dim)],
            out_specs=pl.BlockSpec((blk, 3 * width), lambda i, info, ids: (i, 0)),
            scratch_shapes=[pltpu.VMEM((3, blk, width), F32)],
        ),
        compiler_params=pltpu.CompilerParams(vmem_limit_bytes=FULL),
        cost_estimate=cost(14 * 2 * blk * total * width // 2),
        name="attend_back",
    )(info, ids, *arrays, angles)


def att_kernel(att, lse, x_all, w, gain, lse_out, res, act, parts, x, wide, send, recv, lse_send, lse_recv, load, swap_send, swap_recv):
    place = Place()
    rows, width = att.shape
    half = w.shape[1]
    mine = place.cp()
    loads = [pltpu.make_async_copy(src, dst, load.at[i]) for i, (src, dst) in enumerate(((x_all.at[pl.ds(mine * rows, rows), :], x), (w, wide.at[0])))]
    for c in loads:
        c.start()
    place.meet(("y", "z", "x", "core"))
    started = []
    near = ("y", "z")
    spans = column_parts(width, 2)

    def hop(p, flip, dim):
        there = tuple(d for d in near if (d in flip) != (d == dim))
        index = p * 3 + (there == ("y",)) + 2 * (there == ("z",))
        start, size = spans[p]
        cols = pl.ds(start, size)
        slot = place.tp(flip)
        src = parts.at[slot, :, cols] if flip else att.at[:, cols]
        return pltpu.make_async_remote_copy(src_ref=src, dst_ref=parts.at[slot, :, cols], send_sem=send.at[index], recv_sem=recv.at[index], device_id=place.device((dim,)), device_id_type=MESH)

    def lse_hop(step):
        src, slot, dim = ((lse, mine, "x"), (lse, mine, "core"), (lse_out.at[place.cp(("x",))], place.cp(("x",)), "core"))[step]
        return pltpu.make_async_remote_copy(src_ref=src, dst_ref=lse_out.at[slot], send_sem=lse_send.at[step], recv_sem=lse_recv.at[step], device_id=place.device((dim,)), device_id_type=MESH)

    def go(copy):
        copy.start()
        started.append(copy)

    other = pltpu.make_async_remote_copy(src_ref=w, dst_ref=wide.at[1], send_sem=swap_send, recv_sem=swap_recv, device_id=place.device(("core",)), device_id_type=MESH)
    for step in range(2):
        for p in range(2):
            go(hop(p, (), near[(p + step) % 2]))
    go(other)
    go(lse_hop(0))
    go(lse_hop(1))
    lse_out[mine] = lse[:]
    for c in loads:
        c.wait()

    def add(piece, slot, halves=(0, 1), first=False):
        for i in halves:
            cols = pl.ds(pl.multiple_of(place.coord("core", ("core",) if i else ()) * half, 128), half)
            t = nn(piece, wide[i, pl.ds(pl.multiple_of(slot * width, width), width), :])
            res[:, cols] = t + (x[:, cols].astype(F32) if first else res[:, cols])

    add(att[:], place.tp(), (0,), True)
    for p in range(2):
        hop(p, (), near[p]).wait_recv()
        go(hop(p, (near[p],), near[1 - p]))
    lse_hop(0).wait_recv()
    go(lse_hop(2))
    other.wait_recv()
    add(att[:], place.tp(), (1,), True)
    for p in (1, 0):
        hop(p, (), near[1 - p]).wait_recv()
        slot = place.tp((near[1 - p],))
        add(parts[slot], slot)
    for p in range(2):
        hop(p, (near[p],), near[1 - p]).wait_recv()
    slot = place.tp(near)
    add(parts[slot], slot)
    h = res[:]
    act[:] = (h * lax.rsqrt(mean_row(h * h) + NORM_EPS) * gain[:]).astype(BF16)
    lse_hop(1).wait_recv()
    lse_hop(2).wait_recv()
    for c in started:
        c.wait_send()


def att_project(att, lse, x_all, w, gain):
    rows, width = att.shape
    dim = x_all.shape[1]
    dma = pltpu.SemaphoreType.DMA
    vmem = pl.BlockSpec(memory_space=pltpu.VMEM)
    hbm = pl.BlockSpec(memory_space=pl.ANY)
    return pl.pallas_call(
        att_kernel,
        out_shape=[jax.ShapeDtypeStruct((4,) + lse.shape, F32), jax.ShapeDtypeStruct((rows, dim), F32), jax.ShapeDtypeStruct((rows, dim), BF16)],
        in_specs=[vmem, vmem, hbm, hbm, vmem],
        out_specs=[vmem] * 3,
        scratch_shapes=[
            pltpu.VMEM((4, rows, width), BF16), pltpu.VMEM((rows, dim), BF16), pltpu.VMEM((2,) + w.shape, BF16),
            *[dma((n,)) for n in (6, 6, 3, 3, 2)], dma, dma,
        ],
        compiler_params=pltpu.CompilerParams(collective_id=1, has_side_effects=True, vmem_limit_bytes=FULL),
        name="att_project",
    )(att, lse, x_all, w, gain)


def weight_grad_kernel(info, *refs, pieces, splits):
    lhs = refs[:pieces]
    rhs = refs[pieces:2 * pieces]
    outs = refs[2 * pieces:]
    t = tn(lhs[0][:], rhs[0][:])
    for a, b in zip(lhs[1:], rhs[1:]):
        t += tn(a[:], b[:])
    width = t.shape[1] // splits
    for i, out in enumerate(outs):
        out[:] = t[:, i * width:(i + 1) * width]


def weight_grad(info, lhs, rhs, block=256, splits=1, rows=None):
    def spec(arr, p, cols, moving):
        if arr.ndim == 3:
            return pl.BlockSpec((None, arr.shape[1], cols), lambda i, info: (info[0] ^ p, 0, i if moving else 0))
        return pl.BlockSpec((arr.shape[0], cols), lambda i, info: (0, i if moving else 0))

    tokens = lhs[0].shape[-2]
    rows, dim = rows or lhs[0].shape[-1], rhs[0].shape[-1]
    n = len(lhs)
    width = dim // splits
    outs = pl.pallas_call(
        functools.partial(weight_grad_kernel, pieces=n, splits=splits),
        out_shape=[jax.ShapeDtypeStruct((rows, width), F32)] * splits,
        grid_spec=pltpu.PrefetchScalarGridSpec(
            num_scalar_prefetch=1,
            grid=(pl.cdiv(rows, block),),
            in_specs=[spec(a, p, block, True) for p, a in enumerate(lhs)] + [spec(b, p, dim, False) for p, b in enumerate(rhs)],
            out_specs=[pl.BlockSpec((block, width), lambda i, info: (i, 0))] * splits,
        ),
        compiler_params=pltpu.CompilerParams(vmem_limit_bytes=56 * MIB),
        cost_estimate=cost(2 * n * tokens * rows * dim),
        name="weight_grad",
    )(info, *lhs, *rhs)
    return outs if splits > 1 else outs[0]


def mlp_kernel(act, dy, wg, wu, wd, hidden, d_gate, d_up, *rest, limit, tiles):
    i = pl.program_id(0)
    block = wg.shape[0]
    both = rest[-1]

    @pl.when(i < tiles)
    def _():
        left = limit - i * block
        row_ok = lax.broadcasted_iota(I32, (block, 1), 0) < left
        col_ok = lax.broadcasted_iota(I32, (1, block), 1) < left
        pair = pl.ds(pl.multiple_of(2 * i * block, block), 2 * block) if tiles < pl.num_programs(0) else slice(2 * block)
        both[pair] = jnp.concatenate([jnp.where(row_ok, w[:], 0).astype(BF16) for w in (wg, wu)])
        t = nt(act[:], both[pair])
        gate, up = t[:, :block], t[:, block:]
        dh = jnp.where(col_ok, to_bf16(nt(dy[:], wd[:])), 0)
        sig = jax.nn.sigmoid(gate)
        hidden[:] = (gate * sig * up).astype(BF16)
        dg = (dh * up * sig * (1.0 + gate * (1.0 - sig))).astype(BF16)
        du = (dh * gate * sig).astype(BF16)
        d_gate[:] = dg
        d_up[:] = du
        if len(rest) > 1:
            rest[1][:, pair] = jnp.concatenate([dg, du], axis=1)

    if len(rest) > 1:
        grad, grads = rest[:2]

        @pl.when(i >= tiles)
        def _():
            wide = grad.shape[1]
            grad[:] = nn(grads[:], both[:, pl.ds(pl.multiple_of((i - tiles) * wide, wide), wide)])


def mlp_block(act, dy, wg, wu, wd, with_grad, block=256, wide=512):
    rows, dim = act.shape
    limit = wg.shape[0]
    tiles = pl.cdiv(limit, block)
    steps = tiles + with_grad * dim // wide
    cols = pl.BlockSpec((rows, block), lambda i: (0, jnp.minimum(i, tiles - 1)))
    tile = pl.BlockSpec((block, dim), lambda i: (jnp.minimum(i, tiles - 1), 0))
    full = pl.BlockSpec((rows, dim), lambda i: (0, 0), pipeline_mode=pl.Buffered(1))
    deep = 2 * block * (tiles if with_grad else 1)
    return pl.pallas_call(
        functools.partial(mlp_kernel, limit=limit, tiles=tiles),
        out_shape=[jax.ShapeDtypeStruct((rows, tiles * block), BF16)] * 3 + [jax.ShapeDtypeStruct((rows, dim), F32)] * with_grad,
        grid=(steps,),
        in_specs=[full, full, tile, tile, tile],
        out_specs=[cols] * 3 + [pl.BlockSpec((rows, wide), lambda i: (0, jnp.maximum(i - tiles, 0)))] * with_grad,
        scratch_shapes=[pltpu.VMEM((rows, deep), BF16)] * with_grad + [pltpu.VMEM((deep, dim), BF16)],
        compiler_params=pltpu.CompilerParams(vmem_limit_bytes=FULL),
        cost_estimate=cost((6 + 4 * with_grad) * rows * dim * limit),
        name="mlp_block",
    )(act, dy, wg, wu, wd)


def zero_kernel(after, *refs, begin, end):
    out, zeros, sem = refs[-3:]
    zeros[:] = jnp.zeros_like(zeros)
    step = zeros.shape[0]

    def send(i, c):
        pltpu.make_async_copy(zeros, out.at[pl.ds(pl.multiple_of(i * step, step), step), :], sem).start()
        return c

    def wait(i, c):
        pltpu.make_async_copy(zeros, out.at[pl.ds(0, step), :], sem).wait()
        return c

    lax.fori_loop(begin // step, end // step, send, 0)
    lax.fori_loop(begin // step, end // step, wait, 0)


def zero_rows(after, shape, begin, end, base=(), step=200):
    return pl.pallas_call(
        functools.partial(zero_kernel, begin=begin, end=end),
        out_shape=jax.ShapeDtypeStruct(shape, F32),
        in_specs=[pl.BlockSpec(memory_space=pltpu.SMEM)] + [pl.BlockSpec(memory_space=pl.ANY)] * len(base),
        out_specs=pl.BlockSpec(memory_space=pl.ANY),
        scratch_shapes=[pltpu.VMEM((step, shape[1]), F32), pltpu.SemaphoreType.DMA],
        input_output_aliases={1: 0} if base else {},
        compiler_params=pltpu.CompilerParams(vmem_limit_bytes=8 * MIB),
        cost_estimate=cost((end - begin) * shape[1]),
        name="zero_rows",
    )(after, *base)


def scatter_kernel(order, sid, runs, bounds, rows, base_hbm, out_hbm, sums, row_sem, sum_sem):
    lo = bounds[0]
    hi = bounds[1]

    def one(c):
        p, singles, multi = c
        n = runs[p]
        t = order[p]
        single = n == 1

        @pl.when(single)
        def _():
            pltpu.make_async_copy(rows.at[pl.ds(t, 1), :], out_hbm.at[pl.ds(sid[p], 1), :], row_sem).start()

        @pl.when(jnp.logical_not(single))
        def _():
            def add(j, acc):
                return acc + rows[pl.ds(order[p + j], 1), :]

            sums[pl.ds(multi, 1), :] = lax.fori_loop(1, n, add, rows[pl.ds(t, 1), :])

        return p + n, singles + single.astype(I32), multi + 1 - single.astype(I32)

    _, singles, multi = lax.while_loop(lambda c: c[0] < hi, one, (lo, 0, 0))

    def two(c):
        p, k = c
        n = runs[p]

        @pl.when(n > 1)
        def _():
            pltpu.make_async_copy(sums.at[pl.ds(k, 1), :], out_hbm.at[pl.ds(sid[p], 1), :], sum_sem).start()

        return p + n, k + (n > 1).astype(I32)

    lax.while_loop(lambda c: c[0] < hi, two, (lo, 0))

    def wait(sem):
        def body(i, c):
            pltpu.make_async_copy(sums.at[pl.ds(0, 1), :], out_hbm.at[pl.ds(0, 1), :], sem).wait()
            return c

        return body

    lax.fori_loop(0, singles, wait(row_sem), 0)
    lax.fori_loop(0, multi, wait(sum_sem), 0)


def scatter_rows(order, sid, runs, bounds, grads, base, tokens):
    _, dim = grads.shape
    rows = base.shape[0]
    return pl.pallas_call(
        scatter_kernel,
        out_shape=jax.ShapeDtypeStruct((rows, dim), F32),
        grid_spec=pltpu.PrefetchScalarGridSpec(
            num_scalar_prefetch=4,
            grid=(),
            in_specs=[pl.BlockSpec(memory_space=pltpu.VMEM), pl.BlockSpec(memory_space=pl.ANY)],
            out_specs=pl.BlockSpec(memory_space=pl.ANY),
            scratch_shapes=[pltpu.VMEM((tokens // 2, dim), F32), pltpu.SemaphoreType.DMA, pltpu.SemaphoreType.DMA],
        ),
        input_output_aliases={5: 0},
        compiler_params=pltpu.CompilerParams(vmem_limit_bytes=FULL),
        name="scatter_rows",
    )(order, sid, runs, bounds, grads, base)


def solution(mesh):
    cp_count = mesh.shape["cp"]
    tp_count = mesh.shape["tp"]
    both = ("cp", "tp")
    x_swap = [(i, i ^ 2) for i in range(cp_count)]
    core_swap = [(i, i ^ 1) for i in range(cp_count)]

    def compute(tokens, pos, doc_id, dy, table, w_q, w_k, w_v, w_o, w_gate, w_up, w_down, gain_one, gain_two, inv_freq):
        span = tokens.shape[0]
        total = span * cp_count
        part = span // tp_count
        rows, dim = table.shape
        head_dim = 2 * inv_freq.shape[0]
        heads = w_q.shape[1] // head_dim
        width = heads * head_dim
        tp_rank = lax.axis_index("tp")
        cp_rank = lax.axis_index("cp")
        core = cp_rank % 2
        gain_a = gain_one.astype(F32)
        gain_b = gain_two.astype(F32)

        barrier = lax.optimization_barrier
        join = lambda arr, axis: lax.all_gather(arr, axis, axis=0, tiled=True)
        add_up = lambda arr: lax.psum_scatter(arr, "tp", scatter_dimension=0, tiled=True)
        swap = lambda arr, pairs, axis="cp": lax.ppermute(arr, axis, pairs)
        local_ids = tokens - tp_rank * rows
        owned = (local_ids >= 0) & (local_ids < rows)
        safe_ids = jnp.where(owned, local_ids, jnp.arange(span) * (rows // span))
        picked = jnp.where(owned[:, None], jnp.take(table, safe_ids, axis=0), 0).astype(BF16)
        info = jnp.stack([cp_rank, core]).astype(I32)
        half = dim // 2
        angle = pos.astype(F32)[:, None] * inv_freq[None, :]
        side_f = jnp.concatenate([jnp.cos(angle), jnp.sin(angle)], axis=1)
        side_i = jnp.stack([tokens, doc_id] * 4)
        x_all, x_slice, angles, ints = embed_gather(picked.reshape(tp_count, part, dim), side_f, side_i)
        angles = angles.reshape(total, head_dim)
        tok_all = ints[:, 0, :].reshape(total)
        doc_all = ints[:, 1, :].reshape(total)
        wo_half = barrier((lax.dynamic_slice_in_dim(w_o, core * half, half, 1), x_all))[0]
        wo_half = join(wo_half, "tp")

        dy_x = swap(barrier((dy, x_all))[0], x_swap)
        act_a, query, key, value = project_qkv(x_all, gain_a[None, :], w_q, w_k, w_v, angles)

        blk = span // 2
        blocks = total // blk
        doc_col = doc_all[:, None]
        doc_row = doc_all.reshape(blocks, 1, blk)
        attended, lse = attend(info, ints, query, key, value, doc_col, doc_row, head_dim, blk)

        tok_all = barrier((tok_all, attended))[0]
        slot_ids = jnp.arange(total, dtype=I32)
        before = (tok_all[None, :] < tok_all[:, None]) | ((tok_all[None, :] == tok_all[:, None]) & (slot_ids[None, :] < slot_ids[:, None]))
        rank = jnp.sum(before.astype(I32), axis=1)
        count = jnp.sum((tok_all[None, :] == tok_all[:, None]).astype(I32), axis=1)
        at_rank = rank[None, :] == slot_ids[:, None]
        runs = jnp.sum(jnp.where(at_rank, count[None, :], 0), axis=1)
        order = jnp.sum(jnp.where(at_rank, slot_ids[None, :], 0), axis=1)
        sid = jnp.sum(jnp.where(at_rank, tok_all[None, :], 0), axis=1) - tp_rank * rows
        order = order + 8 * (order // part)
        bounds = jnp.stack([jnp.sum((tok_all < tp_rank * rows).astype(I32)), jnp.sum((tok_all < (tp_rank + 1) * rows).astype(I32))])
        wo_half, runs, order, sid, bounds = barrier((wo_half, runs, order, sid, bounds))
        heads_x = swap(attended, x_swap)
        lse_all, residual, act_b = att_project(attended, lse, x_all, wo_half, gain_b[None, :])
        lse_all = lse_all.reshape(total, 8)
        act_x = swap(act_b, x_swap)
        wg, wu = w_gate.T, w_up.T
        ffn = wg.shape[0]
        hidden, d_gate, d_up, d_act_b = mlp_block(act_b, dy, wg, wu, w_down, True)
        d_act_b = add_up(d_act_b)
        hidden_x, d_gate_x, d_up_x = mlp_block(act_x, dy_x, wg, wu, w_down, False)
        out_part = nn(hidden[:, :ffn], w_down)
        split = rows // 1000 * 600
        base = zero_rows(bounds, (rows, dim), 0, split)
        heads_x = barrier((heads_x, act_b))[0]
        head_parts = (attended, swap(attended, core_swap), heads_x, swap(heads_x, core_swap))
        att_heads = jnp.zeros((total, width), BF16)
        for k, piece in enumerate(head_parts):
            att_heads = lax.dynamic_update_slice_in_dim(att_heads, piece, (cp_rank ^ k) * span, 0)
        d_act_b, hidden_x, d_gate_x, d_up_x, out_part, base, att_heads = barrier((d_act_b, hidden_x, d_gate_x, d_up_x, out_part, base, att_heads))
        acts, dys, hiddens, d_gates, d_ups = [(a, swap(a, core_swap), b, swap(b, core_swap)) for a, b in (
            (act_b, act_x), (dy, dy_x), (hidden, hidden_x), (d_gate, d_gate_x), (d_up, d_up_x))]
        grad_down = weight_grad(info, hiddens, dys, rows=ffn)
        grad_gate = weight_grad(info, d_gates, acts, rows=ffn)
        grad_up = weight_grad(info, d_ups, acts, rows=ffn)

        def mine(arr):
            return lax.dynamic_slice_in_dim(arr, tp_rank * part, part, 0)

        res_part = mine(residual)
        d_resid_all, d_resid, d_gain_b = spread(d_act_b, res_part, mine(dy), gain_b[None])
        d_resid_all, out_part = barrier((d_resid_all, out_part))
        out_slice = add_up(out_part)
        out_slice = (res_part + out_slice).astype(BF16)

        d_att = nt(d_resid_all, w_o)
        d_att_b = d_att.astype(BF16)
        head_of = (jnp.arange(width)[None, :] // head_dim == jnp.arange(8)[:, None]).astype(F32)
        prod = att_heads.astype(F32) * d_att_b.astype(F32)
        delta = lax.dot_general(head_of, prod, (((1,), (1,)), ((), ())), precision=lax.Precision.HIGHEST, preferred_element_type=F32)

        def by_block(arr):
            return jnp.transpose(arr.reshape(8, blocks, blk), (1, 0, 2))

        dqkv = attend_back(info, ints, query, key, value, d_att_b, doc_col, doc_row, lse_all, by_block(lse_all.T), delta.T, by_block(delta), angles, blk)
        d_act_a = sum(nt(dqkv[:, i * width:(i + 1) * width], w) for i, w in enumerate((w_q, w_k, w_v)))
        d_act_a, out_slice = barrier((d_act_a, out_slice))
        d_act_a = add_up(d_act_a)
        dqkv_x = swap(dqkv, x_swap)
        dqkvs = (dqkv, swap(dqkv, core_swap), dqkv_x, swap(dqkv_x, core_swap))
        grad_out = weight_grad(info, head_parts, [d_resid_all.reshape(cp_count, span, dim)] * 4)
        base = zero_rows(bounds, (rows, dim), split, rows, (barrier((base, dqkv))[0],))
        d_act_a, dqkv_x, grad_out, grad_up, base = barrier((d_act_a, dqkv_x, grad_out, grad_up, base))
        payload = payload_rows(d_act_a, x_slice, d_resid, gain_a[None], d_gain_b)
        gathered = join(payload, both)
        grad_qkv = weight_grad(info, [act_a.reshape(cp_count, span, dim)] * 4, dqkvs, splits=3)
        gathered, grad_qkv, grad_gate, grad_down = barrier((gathered, grad_qkv, grad_gate, grad_down))
        out_slice = barrier((out_slice, grad_qkv))[0]
        layer_out = jnp.concatenate([out_slice] * tp_count)
        for k in range(1, tp_count):
            piece = swap(out_slice, [(i, i ^ k) for i in range(tp_count)], "tp")
            layer_out = lax.dynamic_update_slice_in_dim(layer_out, piece, (tp_rank ^ k) * part, 0)
        gain_grads = jnp.sum(gathered.reshape(cp_count * tp_count, part + 8, dim)[:, part:part + 2], axis=0)
        grad_table = scatter_rows(order, sid, runs, bounds, gathered, base, total)
        return (layer_out, grad_table, *grad_qkv, grad_out, grad_gate.T, grad_up.T, grad_down, gain_grads[0], gain_grads[1])

    col_spec = P(None, "tp")
    row_spec = P("tp")
    tok_spec = P("cp")
    rep_spec = P()
    in_specs = (tok_spec, tok_spec, tok_spec, P("cp"), row_spec, col_spec, col_spec, col_spec, row_spec, col_spec, col_spec, row_spec, rep_spec, rep_spec, rep_spec)
    out_specs = (P("cp"), row_spec, col_spec, col_spec, col_spec, row_spec, col_spec, col_spec, row_spec, rep_spec, rep_spec)
    return jax.shard_map(compute, mesh=mesh, in_specs=in_specs, out_specs=out_specs, check_vma=False)
```

```python
import functools
import jax
import jax.numpy as jnp
from jax import lax
from jax.experimental import pallas as pl
from jax.experimental.pallas import tpu as pltpu
from jax.sharding import PartitionSpec as P

NORM_EPS = 1e-5
NEG_BIG = -1e30
MIB = 2 ** 20
FULL = 62 * MIB
F32 = jnp.float32
BF16 = jnp.bfloat16
I32 = jnp.int32


def rms_stats(feats):
    inv_rms = lax.rsqrt(mean_row(feats * feats) + NORM_EPS)
    return feats * inv_rms, inv_rms


def rms_back(d_normed, normed, inv_rms):
    return inv_rms * (d_normed - normed * mean_row(d_normed * normed))


def to_bf16(feats):
    return feats.astype(BF16).astype(F32)


def contract(a, b, ca, cb):
    return lax.dot_general(a, b, (((ca,), (cb,)), ((), ())), preferred_element_type=F32)


def row_sum(t):
    return jnp.sum(t, 1, keepdims=True)


def mean_row(t):
    return row_sum(t) / t.shape[1]


def whole(a):
    return pl.BlockSpec(a.shape, lambda *i: (0,) * a.ndim)


def cost(flops):
    return pl.CostEstimate(flops=flops, bytes_accessed=flops // 512, transcendentals=0)


def nn(a, b):
    return contract(a, b, 1, 0)


def nt(a, b):
    return contract(a, b, 1, 1)


def tn(a, b):
    return contract(a, b, 0, 0)


DIMS = ("x", "y", "z")


class Place:
    def __init__(self):
        tp = lax.axis_index("tp")
        cp = lax.axis_index("cp")
        self.at = {"x": cp // 2, "core": cp % 2, "z": tp // 2, "y": tp % 2}

    def coord(self, dim, flip):
        return 1 - self.at[dim] if dim in flip else self.at[dim]

    def tp(self, flip=()):
        return self.coord("z", flip) * 2 + self.coord("y", flip)

    def cp(self, flip=()):
        return self.coord("x", flip) * 2 + self.coord("core", flip)

    def device(self, flip):
        return {"tp": self.tp(flip), "cp": self.cp(flip)}

    def slot(self, flip=()):
        return self.cp(flip) * 4 + self.tp(flip)

    def meet(self, dims):
        barrier = pltpu.get_barrier_semaphore()
        for d in dims:
            pl.semaphore_signal(barrier, inc=1, device_id=self.device((d,)), device_id_type=MESH)
        pl.semaphore_wait(barrier, len(dims))


MESH = pl.DeviceIdType.MESH
ORDERS = (("x", "y", "z"), ("y", "z", "x"), ("z", "x", "y"))
COUNTS = (21, 21, 24, 24, 48)
FLIPS = tuple(tuple(d for i, d in enumerate(DIMS) if n >> i & 1) for n in range(8))


def flip_code(flip):
    return sum(1 << DIMS.index(d) for d in flip)


def column_parts(width, count):
    tiles = width // 128
    sizes = [(tiles // count + (i < tiles % count)) * 128 for i in range(count)]
    return [(sum(sizes[:i]), n) for i, n in enumerate(sizes)]


class Gather:
    def __init__(self, place, buf, out, send, recv, core_send, core_recv, out_sem):
        self.place, self.buf, self.out = place, buf, out
        self.send, self.recv, self.core_send, self.core_recv, self.out_sem = send, recv, core_send, core_recv, out_sem
        self.parts = column_parts(buf.shape[2], 3)
        self.started, self.stores = [], []

    def view(self, part, flip):
        start, size = self.parts[part]
        return self.buf.at[self.place.slot(flip), :, pl.ds(start, size)]

    def hop(self, part, flip, dim):
        there = tuple(d for d in DIMS if (d in flip) != (d == dim))
        index = part * 7 + flip_code(there) - 1
        ref = self.view(part, flip)
        return pltpu.make_async_remote_copy(src_ref=ref, dst_ref=ref, send_sem=self.send.at[index], recv_sem=self.recv.at[index], device_id=self.place.device((dim,)), device_id_type=MESH)

    def core_hop(self, part, flip):
        index = part * 8 + flip_code(flip)
        ref = self.view(part, flip)
        return pltpu.make_async_remote_copy(src_ref=ref, dst_ref=ref, send_sem=self.core_send.at[index], recv_sem=self.core_recv.at[index], device_id=self.place.device(("core",)), device_id_type=MESH)

    def go(self, copy):
        copy.start()
        self.started.append(copy)

    def wait(self, part, flip):
        order = ORDERS[part]
        last = max(order.index(d) for d in flip)
        came = tuple(d for d in flip if d != order[last])
        self.hop(part, came, order[last]).wait_recv()
        for dim in order[last + 1:]:
            self.go(self.hop(part, flip, dim))
        self.go(self.core_hop(part, flip))
        self.store(part, flip)

    def take(self, part, flip):
        index = part * 8 + flip_code(flip)
        there = flip + ("core",)
        ref = self.view(part, there)
        pltpu.make_async_remote_copy(src_ref=ref, dst_ref=ref, send_sem=self.core_send.at[index], recv_sem=self.core_recv.at[index], device_id=self.place.device(("core",)), device_id_type=MESH).wait_recv()
        self.store(part, there)

    def store(self, part, flip):
        start, size = self.parts[part]
        rows = self.buf.shape[1]
        dst = self.out.at[pl.ds(self.place.slot(flip) * rows, rows), pl.ds(start, size)]
        copy = pltpu.make_async_copy(self.view(part, flip), dst, self.out_sem.at[len(self.stores)])
        copy.start()
        self.stores.append(copy)

    def run(self):
        for step in range(3):
            for part, order in enumerate(ORDERS):
                self.go(self.hop(part, (), order[step]))
        pending = [(part, ()) for part in range(3)]
        for item in pending:
            self.go(self.core_hop(*item))
            self.store(*item)
        for step in range(3):
            batch = [(part, flip) for flip in sorted(FLIPS[1:], key=len) for part, order in enumerate(ORDERS) if max(order.index(d) for d in flip) == step]
            for item in batch:
                self.wait(*item)
            for item in pending:
                self.take(*item)
            pending = batch
        for item in pending:
            self.take(*item)
        for c in self.started:
            c.wait_send()
        for c in self.stores:
            c.wait()


def embed_kernel(picked, side_f, side_i, out, slice_out, all_f, all_i, buf, r1, r2, tmp, send, recv, core_send, core_recv, out_sem, rs_send, rs_recv, side_send, side_recv, slice_sem):
    place = Place()
    place.meet(("x", "y", "z", "core"))
    half = buf.shape[2] // 2
    near = ("y", "z")

    sides = ((side_f, all_f), (side_i, all_i))
    started, keeps = [], []

    def side_hop(i, step):
        src, dst = sides[i]
        if step == 0:
            src_ref, slot, dim = src, place.cp(), "x"
        elif step == 1:
            src_ref, slot, dim = src, place.cp(), "core"
        else:
            src_ref, slot, dim = dst.at[place.cp(("x",))], place.cp(("x",)), "core"
        return pltpu.make_async_remote_copy(src_ref=src_ref, dst_ref=dst.at[slot], send_sem=side_send.at[i, step], recv_sem=side_recv.at[i, step], device_id=place.device((dim,)), device_id_type=MESH)

    def first(h, k):
        a, b = near[h], near[1 - h]
        target = place.tp((a,)) if k == 0 else place.tp((a, b))
        cols = pl.ds(h * half, half)
        return pltpu.make_async_remote_copy(src_ref=picked.at[target, :, cols], dst_ref=r1.at[h, k], send_sem=rs_send.at[h, k], recv_sem=rs_recv.at[h, k], device_id=place.device((a,)), device_id_type=MESH)

    def second(h):
        return pltpu.make_async_remote_copy(src_ref=tmp.at[h], dst_ref=r2.at[h], send_sem=rs_send.at[h, 2], recv_sem=rs_recv.at[h, 2], device_id=place.device((near[1 - h],)), device_id_type=MESH)

    def go(copy):
        copy.start()
        started.append(copy)

    for k in (1, 0):
        for h in range(2):
            go(first(h, k))
    for i in range(2):
        go(side_hop(i, 0))
        go(side_hop(i, 1))
        keeps.append(pltpu.make_async_copy(sides[i][0], sides[i][1].at[place.cp()], slice_sem.at[i]))
        keeps[i].start()
    for h in range(2):
        cols = slice(h * half, (h + 1) * half)
        first(h, 1).wait_recv()
        tmp[h] = picked[place.tp((near[1 - h],)), :, cols] + r1[h, 1]
        go(second(h))
    for i in range(2):
        side_hop(i, 0).wait_recv()
        go(side_hop(i, 2))
    mine = place.slot()
    for h in range(2):
        cols = slice(h * half, (h + 1) * half)
        first(h, 0).wait_recv()
        part = picked[place.tp(), :, cols] + r1[h, 0]
        second(h).wait_recv()
        buf[mine, :, cols] = part + r2[h]
    keeps.append(pltpu.make_async_copy(buf.at[mine], slice_out, slice_sem.at[2]))
    keeps[-1].start()
    Gather(place, buf, out, send, recv, core_send, core_recv, out_sem).run()
    for c in keeps:
        c.wait()
    for i in range(2):
        side_hop(i, 1).wait_recv()
        side_hop(i, 2).wait_recv()
    for c in started:
        c.wait_send()


def embed_gather(picked, side_f, side_i):
    _, rows, dim = picked.shape
    half = dim // 2
    dma = pltpu.SemaphoreType.DMA
    vmem = pl.BlockSpec(memory_space=pltpu.VMEM)
    hbm = pl.BlockSpec(memory_space=pl.ANY)
    return pl.pallas_call(
        embed_kernel,
        out_shape=[
            jax.ShapeDtypeStruct((16 * rows, dim), BF16),
            jax.ShapeDtypeStruct((rows, dim), BF16),
            jax.ShapeDtypeStruct((4,) + side_f.shape, F32),
            jax.ShapeDtypeStruct((4,) + side_i.shape, I32),
        ],
        in_specs=[vmem, vmem, vmem],
        out_specs=[pl.BlockSpec(memory_space=pltpu.HBM)] * 4,
        scratch_shapes=[
            pltpu.VMEM((16, rows, dim), BF16),
            pltpu.VMEM((2, 2, rows, half), BF16),
            pltpu.VMEM((2, rows, half), BF16),
            pltpu.VMEM((2, rows, half), BF16),
            *[dma((n,)) for n in COUNTS],
            *[dma((2, 3))] * 4, dma((3,)),
        ],
        compiler_params=pltpu.CompilerParams(collective_id=0, has_side_effects=True, vmem_limit_bytes=FULL),
        name="embed_gather",
    )(picked, side_f, side_i)


def spread_kernel(d_act, res, dy, gain, out, d_resid, d_gain, buf, send, recv, core_send, core_recv, out_sem):
    place = Place()
    d = to_bf16(d_act[:])
    normed, inv = rms_stats(res[:])
    t = dy[:].astype(F32) + rms_back(d * gain[:], normed, inv)
    d_resid[:] = t
    d_gain[:] = jnp.sum(d * normed, 0, keepdims=True)
    buf[place.slot()] = t.astype(BF16)
    place.meet(("x", "y", "z", "core"))
    Gather(place, buf, out, send, recv, core_send, core_recv, out_sem).run()


def spread(d_act, res, dy, gain):
    rows, dim = res.shape
    dma = pltpu.SemaphoreType.DMA
    vmem = pl.BlockSpec(memory_space=pltpu.VMEM)
    return pl.pallas_call(
        spread_kernel,
        out_shape=[jax.ShapeDtypeStruct((16 * rows, dim), BF16), jax.ShapeDtypeStruct((rows, dim), F32), jax.ShapeDtypeStruct((1, dim), F32)],
        in_specs=[vmem] * 4,
        out_specs=[pl.BlockSpec(memory_space=pltpu.HBM), vmem, vmem],
        scratch_shapes=[pltpu.VMEM((16, rows, dim), BF16), *[dma((n,)) for n in COUNTS]],
        compiler_params=pltpu.CompilerParams(collective_id=2, has_side_effects=True, vmem_limit_bytes=FULL),
        name="spread",
    )(d_act, res, dy, gain)


def payload_kernel(d_act, x, d_resid, gain, d_gain_b, out):
    rows = x.shape[0]
    d = to_bf16(d_act[:])
    normed, inv = rms_stats(x[:].astype(F32))
    out[:rows] = d_resid[:] + rms_back(d * gain[:], normed, inv)
    d_gain_a = jnp.sum(d * normed, 0, keepdims=True)
    extra = (out.shape[0] - rows, out.shape[1])
    out[rows:] = jnp.where(lax.broadcasted_iota(I32, extra, 0) == 0, d_gain_a, d_gain_b[:])


def payload_rows(d_act, x, d_resid, gain, d_gain_b):
    rows, dim = x.shape
    return pl.pallas_call(
        payload_kernel,
        out_shape=jax.ShapeDtypeStruct((rows + 8, dim), F32),
        compiler_params=pltpu.CompilerParams(vmem_limit_bytes=FULL),
        name="payload_rows",
    )(d_act, x, d_resid, gain, d_gain_b)


def slot_block(j):
    return jnp.where(j < 4, 2 * j, 15 - 2 * j)


def unpack_angles(packed):
    turned = pltpu.roll(packed, packed.shape[1] // 2, 1)
    low = lax.broadcasted_iota(I32, packed.shape, 1) < packed.shape[1] // 2
    return jnp.where(low, packed, turned), jnp.where(low, -turned, packed)


def qkv_kernel(x, gain, wq, wk, wv, angles, act, q, k, v, wide, *, head_dim):
    width = wq.shape[1]

    @pl.when(pl.program_id(0) == 0)
    def _():
        for i, w in enumerate((wq, wk, wv)):
            wide[:, i * width:(i + 1) * width] = w[:]

    feats = x[:].astype(F32)
    inv = lax.rsqrt(mean_row(feats * feats) + NORM_EPS)
    a = (feats * inv * gain[:]).astype(BF16)
    act[:] = a
    t = nn(a, wide[:])
    cos, sin = unpack_angles(angles[:])
    for i, out in enumerate((q, k, v)):
        for h in range(width // head_dim):
            th = t[:, i * width + h * head_dim:i * width + (h + 1) * head_dim]
            if i < 2:
                th = th * cos + pltpu.roll(th, head_dim // 2, 1) * sin
            out[:, h * head_dim:(h + 1) * head_dim] = th.astype(BF16)


def project_qkv(x_all, gain, wq, wk, wv, angles, block=512):
    total, dim = x_all.shape
    width = wq.shape[1]
    head_dim = angles.shape[1]
    rows = lambda n: pl.BlockSpec((block, n), lambda i: (i, 0))
    whole = lambda a: pl.BlockSpec(a.shape, lambda i: (0, 0), pipeline_mode=pl.Buffered(1))
    return pl.pallas_call(
        functools.partial(qkv_kernel, head_dim=head_dim),
        out_shape=[jax.ShapeDtypeStruct((total, n), BF16) for n in (dim, width, width, width)],
        grid=(total // block,),
        in_specs=[rows(dim), whole(gain), whole(wq), whole(wk), whole(wv), rows(head_dim)],
        out_specs=[rows(dim), rows(width), rows(width), rows(width)],
        scratch_shapes=[pltpu.VMEM((dim, 3 * width), BF16)],
        compiler_params=pltpu.CompilerParams(vmem_limit_bytes=FULL),
        cost_estimate=cost(6 * total * dim * width),
        name="project_qkv",
    )(x_all, gain, wq, wk, wv, angles)


def block_range(info, ids, i, blocks):
    r = info[0]
    blk = ids.shape[2] // 2
    b = jnp.where(i == 0, r, blocks - 1 - r)

    def docs(shard, half):
        return ids[shard, 1, half * blk], ids[shard, 1, half * blk + blk - 1]

    first, last = docs(r, i)
    jmin, imax = 0, -1
    for j in range(blocks):
        begin, end = docs(min(j, blocks - 1 - j), int(j >= blocks // 2))
        jmin = jmin + (end < first).astype(I32)
        imax = imax + (begin <= last).astype(I32)
    return b, jmin, imax


def attend_kernel(info, ids, q, k, v, doc_col, doc_row, out, lse, sc, *, heads, head_dim, scale):
    blk = q.shape[0]
    b, jmin, _ = block_range(info, ids, pl.program_id(0), doc_row.shape[0])
    row_n = lax.broadcasted_iota(I32, (blk, blk), 0) + b * blk
    col_n = lax.broadcasted_iota(I32, (blk, blk), 1)

    def score(j, peaks):
        sb = slot_block(j)
        off = pl.multiple_of(sb * blk, blk)
        allowed = (doc_col[:] == doc_row[sb]) & (col_n + j * blk <= row_n)
        new = []
        for h in range(heads):
            cols = slice(h * head_dim, (h + 1) * head_dim)
            s = nt(q[:, cols], k[pl.ds(off, blk), cols]) * scale
            s = jnp.where(allowed, s, NEG_BIG)
            sc[j, h] = s
            new.append(jnp.maximum(peaks[h], jnp.max(s, axis=1, keepdims=True)))
        return tuple(new)

    peaks = lax.fori_loop(jmin, b + 1, score, tuple(jnp.full((blk, 1), NEG_BIG, F32) for _ in range(heads)))

    def weigh(j, sums):
        new = []
        for h in range(heads):
            p = jnp.exp(sc[j, h] - peaks[h])
            sc[j, h] = p
            new.append(sums[h] + row_sum(p))
        return tuple(new)

    sums = lax.fori_loop(jmin, b + 1, weigh, tuple(jnp.zeros((blk, 1), F32) for _ in range(heads)))
    inv = tuple(1.0 / t for t in sums)
    for h in range(heads):
        lse[:, h:h + 1] = peaks[h] + jnp.log(sums[h])

    def mix(j, acc):
        off = pl.multiple_of(slot_block(j) * blk, blk)
        new = []
        for h in range(heads):
            cols = slice(h * head_dim, (h + 1) * head_dim)
            new.append(acc[h] + nn((sc[j, h] * inv[h]).astype(BF16), v[pl.ds(off, blk), cols]))
        return tuple(new)

    acc = lax.fori_loop(jmin, b + 1, mix, tuple(jnp.zeros((blk, head_dim), F32) for _ in range(heads)))
    for h in range(heads):
        out[:, h * head_dim:(h + 1) * head_dim] = acc[h].astype(BF16)


def attend(info, ids, q, k, v, doc_col, doc_row, head_dim, blk):
    total, width = k.shape
    heads = width // head_dim
    mine = lambda n: pl.BlockSpec((blk, n), lambda i, info, ids: (2 * info[0] + i, 0))
    return pl.pallas_call(
        functools.partial(attend_kernel, heads=heads, head_dim=head_dim, scale=head_dim ** -0.5),
        out_shape=[jax.ShapeDtypeStruct((2 * blk, width), BF16), jax.ShapeDtypeStruct((2 * blk, 8), F32)],
        grid_spec=pltpu.PrefetchScalarGridSpec(
            num_scalar_prefetch=2,
            grid=(2,),
            in_specs=[mine(width), whole(k), whole(v), mine(1), whole(doc_row)],
            out_specs=[pl.BlockSpec((blk, width), lambda i, info, ids: (i, 0)), pl.BlockSpec((blk, 8), lambda i, info, ids: (i, 0))],
            scratch_shapes=[pltpu.VMEM((total // blk, heads, blk, blk), F32)],
        ),
        compiler_params=pltpu.CompilerParams(vmem_limit_bytes=FULL),
        cost_estimate=cost(4 * 2 * blk * total * width),
        name="attend",
    )(info, ids, q, k, v, doc_col, doc_row)


def attend_back_kernel(info, ids, q, k, v, do, doc_col, doc_row, lse_col, lse_row, del_col, del_row, angles, out, acc, *, heads, head_dim, scale):
    blk = angles.shape[0]
    width = heads * head_dim
    i = pl.program_id(0)
    b, jmin, imax = block_range(info, ids, i, doc_row.shape[0])
    me = pl.multiple_of((2 * info[0] + i) * blk, blk)
    mine = pl.ds(me, blk)
    iota_r = lax.broadcasted_iota(I32, (blk, blk), 0)
    iota_c = lax.broadcasted_iota(I32, (blk, blk), 1)
    acc[:] = jnp.zeros_like(acc)
    spans = [slice(h * head_dim, (h + 1) * head_dim) for h in range(heads)]

    def for_query(j, c):
        sb = slot_block(j)
        there = pl.ds(pl.multiple_of(sb * blk, blk), blk)
        allowed = (doc_col[mine, :] == doc_row[sb]) & (iota_c + j * blk <= iota_r + b * blk)
        for h, cols in enumerate(spans):
            s = jnp.where(allowed, nt(q[mine, cols], k[there, cols]) * scale, NEG_BIG)
            p = jnp.exp(s - lse_col[mine, h:h + 1])
            dp = to_bf16(nt(do[mine, cols], v[there, cols]))
            ds = (p * (dp - del_col[mine, h:h + 1]) * scale).astype(BF16)
            acc[0, :, cols] += nn(ds, k[there, cols])
        return c

    lax.fori_loop(jmin, b + 1, for_query, 0)

    def for_key(j, c):
        sb = slot_block(j)
        there = pl.ds(pl.multiple_of(sb * blk, blk), blk)
        allowed = (doc_col[mine, :] == doc_row[sb]) & (iota_r + b * blk <= iota_c + j * blk)
        for h, cols in enumerate(spans):
            s = jnp.where(allowed, nt(k[mine, cols], q[there, cols]) * scale, NEG_BIG)
            p = jnp.exp(s - lse_row[sb, h:h + 1, :])
            dp = to_bf16(nt(v[mine, cols], do[there, cols]))
            ds = (p * (dp - del_row[sb, h:h + 1, :]) * scale).astype(BF16)
            acc[2, :, cols] += nn(p.astype(BF16), do[there, cols])
            acc[1, :, cols] += nn(ds, q[there, cols])
        return c

    lax.fori_loop(b, imax + 1, for_key, 0)
    cos, sin = unpack_angles(angles[:])
    for part in range(3):
        for h, cols in enumerate(spans):
            t = acc[part, :, cols]
            if part < 2:
                t = to_bf16(t)
                t = t * cos - pltpu.roll(t, head_dim // 2, 1) * sin
            out[:, part * width + h * head_dim:part * width + (h + 1) * head_dim] = t.astype(BF16)


def attend_back(info, ids, q, k, v, do, doc_col, doc_row, lse_col, lse_row, del_col, del_row, angles, blk):
    total, width = k.shape
    head_dim = angles.shape[1]
    heads = width // head_dim
    mine = lambda n: pl.BlockSpec((blk, n), lambda i, info, ids: (2 * info[0] + i, 0))
    arrays = (q, k, v, do, doc_col, doc_row, lse_col, lse_row, del_col, del_row)
    return pl.pallas_call(
        functools.partial(attend_back_kernel, heads=heads, head_dim=head_dim, scale=head_dim ** -0.5),
        out_shape=jax.ShapeDtypeStruct((2 * blk, 3 * width), BF16),
        grid_spec=pltpu.PrefetchScalarGridSpec(
            num_scalar_prefetch=2,
            grid=(2,),
            in_specs=[whole(a) for a in arrays] + [mine(head_dim)],
            out_specs=pl.BlockSpec((blk, 3 * width), lambda i, info, ids: (i, 0)),
            scratch_shapes=[pltpu.VMEM((3, blk, width), F32)],
        ),
        compiler_params=pltpu.CompilerParams(vmem_limit_bytes=FULL),
        cost_estimate=cost(14 * 2 * blk * total * width // 2),
        name="attend_back",
    )(info, ids, *arrays, angles)


def att_kernel(att, lse, x_all, w, gain, lse_out, res, act, parts, x, wide, send, recv, lse_send, lse_recv, load, swap_send, swap_recv):
    place = Place()
    rows, width = att.shape
    half = w.shape[1]
    mine = place.cp()
    loads = [pltpu.make_async_copy(src, dst, load.at[i]) for i, (src, dst) in enumerate(((x_all.at[pl.ds(mine * rows, rows), :], x), (w, wide.at[0])))]
    for c in loads:
        c.start()
    place.meet(("y", "z", "x", "core"))
    started = []
    near = ("y", "z")
    spans = column_parts(width, 2)

    def hop(p, flip, dim):
        there = tuple(d for d in near if (d in flip) != (d == dim))
        index = p * 3 + (there == ("y",)) + 2 * (there == ("z",))
        start, size = spans[p]
        cols = pl.ds(start, size)
        slot = place.tp(flip)
        src = parts.at[slot, :, cols] if flip else att.at[:, cols]
        return pltpu.make_async_remote_copy(src_ref=src, dst_ref=parts.at[slot, :, cols], send_sem=send.at[index], recv_sem=recv.at[index], device_id=place.device((dim,)), device_id_type=MESH)

    def lse_hop(step):
        src, slot, dim = ((lse, mine, "x"), (lse, mine, "core"), (lse_out.at[place.cp(("x",))], place.cp(("x",)), "core"))[step]
        return pltpu.make_async_remote_copy(src_ref=src, dst_ref=lse_out.at[slot], send_sem=lse_send.at[step], recv_sem=lse_recv.at[step], device_id=place.device((dim,)), device_id_type=MESH)

    def go(copy):
        copy.start()
        started.append(copy)

    other = pltpu.make_async_remote_copy(src_ref=w, dst_ref=wide.at[1], send_sem=swap_send, recv_sem=swap_recv, device_id=place.device(("core",)), device_id_type=MESH)
    for step in range(2):
        for p in range(2):
            go(hop(p, (), near[(p + step) % 2]))
    go(other)
    go(lse_hop(0))
    go(lse_hop(1))
    lse_out[mine] = lse[:]
    for c in loads:
        c.wait()

    def add(piece, slot, halves=(0, 1), first=False):
        for i in halves:
            cols = pl.ds(pl.multiple_of(place.coord("core", ("core",) if i else ()) * half, 128), half)
            t = nn(piece, wide[i, pl.ds(pl.multiple_of(slot * width, width), width), :])
            res[:, cols] = t + (x[:, cols].astype(F32) if first else res[:, cols])

    add(att[:], place.tp(), (0,), True)
    for p in range(2):
        hop(p, (), near[p]).wait_recv()
        go(hop(p, (near[p],), near[1 - p]))
    lse_hop(0).wait_recv()
    go(lse_hop(2))
    other.wait_recv()
    add(att[:], place.tp(), (1,), True)
    for p in (1, 0):
        hop(p, (), near[1 - p]).wait_recv()
        slot = place.tp((near[1 - p],))
        add(parts[slot], slot)
    for p in range(2):
        hop(p, (near[p],), near[1 - p]).wait_recv()
    slot = place.tp(near)
    add(parts[slot], slot)
    h = res[:]
    act[:] = (h * lax.rsqrt(mean_row(h * h) + NORM_EPS) * gain[:]).astype(BF16)
    lse_hop(1).wait_recv()
    lse_hop(2).wait_recv()
    for c in started:
        c.wait_send()


def att_project(att, lse, x_all, w, gain):
    rows, width = att.shape
    dim = x_all.shape[1]
    dma = pltpu.SemaphoreType.DMA
    vmem = pl.BlockSpec(memory_space=pltpu.VMEM)
    hbm = pl.BlockSpec(memory_space=pl.ANY)
    return pl.pallas_call(
        att_kernel,
        out_shape=[jax.ShapeDtypeStruct((4,) + lse.shape, F32), jax.ShapeDtypeStruct((rows, dim), F32), jax.ShapeDtypeStruct((rows, dim), BF16)],
        in_specs=[vmem, vmem, hbm, hbm, vmem],
        out_specs=[vmem] * 3,
        scratch_shapes=[
            pltpu.VMEM((4, rows, width), BF16), pltpu.VMEM((rows, dim), BF16), pltpu.VMEM((2,) + w.shape, BF16),
            *[dma((n,)) for n in (6, 6, 3, 3, 2)], dma, dma,
        ],
        compiler_params=pltpu.CompilerParams(collective_id=1, has_side_effects=True, vmem_limit_bytes=FULL),
        name="att_project",
    )(att, lse, x_all, w, gain)


def weight_grad_kernel(info, *refs, pieces, splits):
    lhs = refs[:pieces]
    rhs = refs[pieces:2 * pieces]
    outs = refs[2 * pieces:]
    t = tn(lhs[0][:], rhs[0][:])
    for a, b in zip(lhs[1:], rhs[1:]):
        t += tn(a[:], b[:])
    width = t.shape[1] // splits
    for i, out in enumerate(outs):
        out[:] = t[:, i * width:(i + 1) * width]


def weight_grad(info, lhs, rhs, block=256, splits=1, rows=None):
    def spec(arr, p, cols, moving):
        if arr.ndim == 3:
            return pl.BlockSpec((None, arr.shape[1], cols), lambda i, info: (info[0] ^ p, 0, i if moving else 0))
        return pl.BlockSpec((arr.shape[0], cols), lambda i, info: (0, i if moving else 0))

    tokens = lhs[0].shape[-2]
    rows, dim = rows or lhs[0].shape[-1], rhs[0].shape[-1]
    n = len(lhs)
    width = dim // splits
    outs = pl.pallas_call(
        functools.partial(weight_grad_kernel, pieces=n, splits=splits),
        out_shape=[jax.ShapeDtypeStruct((rows, width), F32)] * splits,
        grid_spec=pltpu.PrefetchScalarGridSpec(
            num_scalar_prefetch=1,
            grid=(pl.cdiv(rows, block),),
            in_specs=[spec(a, p, block, True) for p, a in enumerate(lhs)] + [spec(b, p, dim, False) for p, b in enumerate(rhs)],
            out_specs=[pl.BlockSpec((block, width), lambda i, info: (i, 0))] * splits,
        ),
        compiler_params=pltpu.CompilerParams(vmem_limit_bytes=56 * MIB),
        cost_estimate=cost(2 * n * tokens * rows * dim),
        name="weight_grad",
    )(info, *lhs, *rhs)
    return outs if splits > 1 else outs[0]


def mlp_kernel(act, dy, wg, wu, wd, hidden, d_gate, d_up, *rest, limit, tiles):
    i = pl.program_id(0)
    block = wg.shape[0]
    both = rest[-1]

    @pl.when(i < tiles)
    def _():
        left = limit - i * block
        row_ok = lax.broadcasted_iota(I32, (block, 1), 0) < left
        col_ok = lax.broadcasted_iota(I32, (1, block), 1) < left
        pair = pl.ds(pl.multiple_of(2 * i * block, block), 2 * block) if tiles < pl.num_programs(0) else slice(2 * block)
        both[pair] = jnp.concatenate([jnp.where(row_ok, w[:], 0).astype(BF16) for w in (wg, wu)])
        t = nt(act[:], both[pair])
        gate, up = t[:, :block], t[:, block:]
        dh = jnp.where(col_ok, to_bf16(nt(dy[:], wd[:])), 0)
        sig = jax.nn.sigmoid(gate)
        hidden[:] = (gate * sig * up).astype(BF16)
        dg = (dh * up * sig * (1.0 + gate * (1.0 - sig))).astype(BF16)
        du = (dh * gate * sig).astype(BF16)
        d_gate[:] = dg
        d_up[:] = du
        if len(rest) > 1:
            rest[1][:, pair] = jnp.concatenate([dg, du], axis=1)

    if len(rest) > 1:
        grad, grads = rest[:2]

        @pl.when(i >= tiles)
        def _():
            wide = grad.shape[1]
            grad[:] = nn(grads[:], both[:, pl.ds(pl.multiple_of((i - tiles) * wide, wide), wide)])


def mlp_block(act, dy, wg, wu, wd, with_grad, block=256, wide=512):
    rows, dim = act.shape
    limit = wg.shape[0]
    tiles = pl.cdiv(limit, block)
    steps = tiles + with_grad * dim // wide
    cols = pl.BlockSpec((rows, block), lambda i: (0, jnp.minimum(i, tiles - 1)))
    tile = pl.BlockSpec((block, dim), lambda i: (jnp.minimum(i, tiles - 1), 0))
    full = pl.BlockSpec((rows, dim), lambda i: (0, 0), pipeline_mode=pl.Buffered(1))
    deep = 2 * block * (tiles if with_grad else 1)
    return pl.pallas_call(
        functools.partial(mlp_kernel, limit=limit, tiles=tiles),
        out_shape=[jax.ShapeDtypeStruct((rows, tiles * block), BF16)] * 3 + [jax.ShapeDtypeStruct((rows, dim), F32)] * with_grad,
        grid=(steps,),
        in_specs=[full, full, tile, tile, tile],
        out_specs=[cols] * 3 + [pl.BlockSpec((rows, wide), lambda i: (0, jnp.maximum(i - tiles, 0)))] * with_grad,
        scratch_shapes=[pltpu.VMEM((rows, deep), BF16)] * with_grad + [pltpu.VMEM((deep, dim), BF16)],
        compiler_params=pltpu.CompilerParams(vmem_limit_bytes=FULL),
        cost_estimate=cost((6 + 4 * with_grad) * rows * dim * limit),
        name="mlp_block",
    )(act, dy, wg, wu, wd)


def zero_kernel(after, *refs, begin, end):
    out, zeros, sem = refs[-3:]
    zeros[:] = jnp.zeros_like(zeros)
    step = zeros.shape[0]

    def send(i, c):
        pltpu.make_async_copy(zeros, out.at[pl.ds(pl.multiple_of(i * step, step), step), :], sem).start()
        return c

    def wait(i, c):
        pltpu.make_async_copy(zeros, out.at[pl.ds(0, step), :], sem).wait()
        return c

    lax.fori_loop(begin // step, end // step, send, 0)
    lax.fori_loop(begin // step, end // step, wait, 0)


def zero_rows(after, shape, begin, end, base=(), step=200):
    return pl.pallas_call(
        functools.partial(zero_kernel, begin=begin, end=end),
        out_shape=jax.ShapeDtypeStruct(shape, F32),
        in_specs=[pl.BlockSpec(memory_space=pltpu.SMEM)] + [pl.BlockSpec(memory_space=pl.ANY)] * len(base),
        out_specs=pl.BlockSpec(memory_space=pl.ANY),
        scratch_shapes=[pltpu.VMEM((step, shape[1]), F32), pltpu.SemaphoreType.DMA],
        input_output_aliases={1: 0} if base else {},
        compiler_params=pltpu.CompilerParams(vmem_limit_bytes=8 * MIB),
        cost_estimate=cost((end - begin) * shape[1]),
        name="zero_rows",
    )(after, *base)


def scatter_kernel(order, sid, runs, bounds, rows, base_hbm, out_hbm, sums, row_sem, sum_sem):
    lo = bounds[0]
    hi = bounds[1]

    def one(c):
        p, singles, multi = c
        n = runs[p]
        t = order[p]
        single = n == 1

        @pl.when(single)
        def _():
            pltpu.make_async_copy(rows.at[pl.ds(t, 1), :], out_hbm.at[pl.ds(sid[p], 1), :], row_sem).start()

        @pl.when(jnp.logical_not(single))
        def _():
            def add(j, acc):
                return acc + rows[pl.ds(order[p + j], 1), :]

            sums[pl.ds(multi, 1), :] = lax.fori_loop(1, n, add, rows[pl.ds(t, 1), :])

        return p + n, singles + single.astype(I32), multi + 1 - single.astype(I32)

    _, singles, multi = lax.while_loop(lambda c: c[0] < hi, one, (lo, 0, 0))

    def two(c):
        p, k = c
        n = runs[p]

        @pl.when(n > 1)
        def _():
            pltpu.make_async_copy(sums.at[pl.ds(k, 1), :], out_hbm.at[pl.ds(sid[p], 1), :], sum_sem).start()

        return p + n, k + (n > 1).astype(I32)

    lax.while_loop(lambda c: c[0] < hi, two, (lo, 0))

    def wait(sem):
        def body(i, c):
            pltpu.make_async_copy(sums.at[pl.ds(0, 1), :], out_hbm.at[pl.ds(0, 1), :], sem).wait()
            return c

        return body

    lax.fori_loop(0, singles, wait(row_sem), 0)
    lax.fori_loop(0, multi, wait(sum_sem), 0)


def scatter_rows(order, sid, runs, bounds, grads, base, tokens):
    _, dim = grads.shape
    rows = base.shape[0]
    return pl.pallas_call(
        scatter_kernel,
        out_shape=jax.ShapeDtypeStruct((rows, dim), F32),
        grid_spec=pltpu.PrefetchScalarGridSpec(
            num_scalar_prefetch=4,
            grid=(),
            in_specs=[pl.BlockSpec(memory_space=pltpu.VMEM), pl.BlockSpec(memory_space=pl.ANY)],
            out_specs=pl.BlockSpec(memory_space=pl.ANY),
            scratch_shapes=[pltpu.VMEM((tokens // 2, dim), F32), pltpu.SemaphoreType.DMA, pltpu.SemaphoreType.DMA],
        ),
        input_output_aliases={5: 0},
        compiler_params=pltpu.CompilerParams(vmem_limit_bytes=FULL),
        name="scatter_rows",
    )(order, sid, runs, bounds, grads, base)


def solution(mesh):
    cp_count = mesh.shape["cp"]
    tp_count = mesh.shape["tp"]
    both = ("cp", "tp")
    x_swap = [(i, i ^ 2) for i in range(cp_count)]
    core_swap = [(i, i ^ 1) for i in range(cp_count)]

    def compute(tokens, pos, doc_id, dy, table, w_q, w_k, w_v, w_o, w_gate, w_up, w_down, gain_one, gain_two, inv_freq):
        span = tokens.shape[0]
        total = span * cp_count
        part = span // tp_count
        rows, dim = table.shape
        head_dim = 2 * inv_freq.shape[0]
        heads = w_q.shape[1] // head_dim
        width = heads * head_dim
        tp_rank = lax.axis_index("tp")
        cp_rank = lax.axis_index("cp")
        core = cp_rank % 2
        gain_a = gain_one.astype(F32)
        gain_b = gain_two.astype(F32)

        barrier = lax.optimization_barrier
        join = lambda arr, axis: lax.all_gather(arr, axis, axis=0, tiled=True)
        add_up = lambda arr: lax.psum_scatter(arr, "tp", scatter_dimension=0, tiled=True)
        swap = lambda arr, pairs, axis="cp": lax.ppermute(arr, axis, pairs)
        local_ids = tokens - tp_rank * rows
        owned = (local_ids >= 0) & (local_ids < rows)
        safe_ids = jnp.where(owned, local_ids, jnp.arange(span) * (rows // span))
        picked = jnp.where(owned[:, None], jnp.take(table, safe_ids, axis=0), 0).astype(BF16)
        info = jnp.stack([cp_rank, core]).astype(I32)
        half = dim // 2
        angle = pos.astype(F32)[:, None] * inv_freq[None, :]
        side_f = jnp.concatenate([jnp.cos(angle), jnp.sin(angle)], axis=1)
        side_i = jnp.stack([tokens, doc_id] * 4)
        x_all, x_slice, angles, ints = embed_gather(picked.reshape(tp_count, part, dim), side_f, side_i)
        angles = angles.reshape(total, head_dim)
        tok_all = ints[:, 0, :].reshape(total)
        doc_all = ints[:, 1, :].reshape(total)
        wo_half = barrier((lax.dynamic_slice_in_dim(w_o, core * half, half, 1), x_all))[0]
        wo_half = join(wo_half, "tp")

        dy_x = swap(barrier((dy, x_all))[0], x_swap)
        act_a, query, key, value = project_qkv(x_all, gain_a[None, :], w_q, w_k, w_v, angles)

        blk = span // 2
        blocks = total // blk
        doc_col = doc_all[:, None]
        doc_row = doc_all.reshape(blocks, 1, blk)
        attended, lse = attend(info, ints, query, key, value, doc_col, doc_row, head_dim, blk)

        tok_all = barrier((tok_all, attended))[0]
        slot_ids = jnp.arange(total, dtype=I32)
        before = (tok_all[None, :] < tok_all[:, None]) | ((tok_all[None, :] == tok_all[:, None]) & (slot_ids[None, :] < slot_ids[:, None]))
        rank = jnp.sum(before.astype(I32), axis=1)
        count = jnp.sum((tok_all[None, :] == tok_all[:, None]).astype(I32), axis=1)
        at_rank = rank[None, :] == slot_ids[:, None]
        runs = jnp.sum(jnp.where(at_rank, count[None, :], 0), axis=1)
        order = jnp.sum(jnp.where(at_rank, slot_ids[None, :], 0), axis=1)
        sid = jnp.sum(jnp.where(at_rank, tok_all[None, :], 0), axis=1) - tp_rank * rows
        order = order + 8 * (order // part)
        bounds = jnp.stack([jnp.sum((tok_all < tp_rank * rows).astype(I32)), jnp.sum((tok_all < (tp_rank + 1) * rows).astype(I32))])
        wo_half, runs, order, sid, bounds = barrier((wo_half, runs, order, sid, bounds))
        heads_x = swap(attended, x_swap)
        lse_all, residual, act_b = att_project(attended, lse, x_all, wo_half, gain_b[None, :])
        lse_all = lse_all.reshape(total, 8)
        act_x = swap(act_b, x_swap)
        wg, wu = w_gate.T, w_up.T
        ffn = wg.shape[0]
        hidden, d_gate, d_up, d_act_b = mlp_block(act_b, dy, wg, wu, w_down, True)
        d_act_b = add_up(d_act_b)
        hidden_x, d_gate_x, d_up_x = mlp_block(act_x, dy_x, wg, wu, w_down, False)
        out_part = nn(hidden[:, :ffn], w_down)
        split = rows // 1000 * 600
        base = zero_rows(bounds, (rows, dim), 0, split)
        heads_x = barrier((heads_x, act_b))[0]
        head_parts = (attended, swap(attended, core_swap), heads_x, swap(heads_x, core_swap))
        att_heads = jnp.zeros((total, width), BF16)
        for k, piece in enumerate(head_parts):
            att_heads = lax.dynamic_update_slice_in_dim(att_heads, piece, (cp_rank ^ k) * span, 0)
        d_act_b, hidden_x, d_gate_x, d_up_x, out_part, base, att_heads = barrier((d_act_b, hidden_x, d_gate_x, d_up_x, out_part, base, att_heads))
        four = lambda a, b: (a, swap(a, core_swap), b, swap(b, core_swap))
        acts, d_ups = four(act_b, act_x), four(d_up, d_up_x)
        dys, hiddens, d_gates = four(dy, dy_x), four(hidden, hidden_x), four(d_gate, d_gate_x)
        grad_down = weight_grad(info, hiddens, dys, rows=ffn)
        grad_gate = weight_grad(info, d_gates, acts, rows=ffn)
        grad_up = weight_grad(info, d_ups, acts, rows=ffn)

        def mine(arr):
            return lax.dynamic_slice_in_dim(arr, tp_rank * part, part, 0)

        res_part = mine(residual)
        d_resid_all, d_resid, d_gain_b = spread(d_act_b, res_part, mine(dy), gain_b[None])
        d_resid_all, out_part = barrier((d_resid_all, out_part))
        out_slice = add_up(out_part)
        out_slice = (res_part + out_slice).astype(BF16)

        d_att = nt(d_resid_all, w_o)
        d_att_b = d_att.astype(BF16)
        head_of = (jnp.arange(width)[None, :] // head_dim == jnp.arange(8)[:, None]).astype(F32)
        prod = att_heads.astype(F32) * d_att_b.astype(F32)
        delta = lax.dot_general(head_of, prod, (((1,), (1,)), ((), ())), precision=lax.Precision.HIGHEST, preferred_element_type=F32)

        def by_block(arr):
            return jnp.transpose(arr.reshape(8, blocks, blk), (1, 0, 2))

        dqkv = attend_back(info, ints, query, key, value, d_att_b, doc_col, doc_row, lse_all, by_block(lse_all.T), delta.T, by_block(delta), angles, blk)
        d_act_a = sum(nt(dqkv[:, i * width:(i + 1) * width], w) for i, w in enumerate((w_q, w_k, w_v)))
        d_act_a, out_slice = barrier((d_act_a, out_slice))
        d_act_a = add_up(d_act_a)
        dqkv_x = swap(dqkv, x_swap)
        dqkvs = (dqkv, swap(dqkv, core_swap), dqkv_x, swap(dqkv_x, core_swap))
        grad_out = weight_grad(info, head_parts, [d_resid_all.reshape(cp_count, span, dim)] * 4)
        base = zero_rows(bounds, (rows, dim), split, rows, (barrier((base, dqkv))[0],))
        d_act_a, dqkv_x, grad_out, grad_up, base = barrier((d_act_a, dqkv_x, grad_out, grad_up, base))
        payload = payload_rows(d_act_a, x_slice, d_resid, gain_a[None], d_gain_b)
        gathered = join(payload, both)
        grad_qkv = weight_grad(info, [act_a.reshape(cp_count, span, dim)] * 4, dqkvs, splits=3)
        gathered, grad_qkv, grad_gate, grad_down = barrier((gathered, grad_qkv, grad_gate, grad_down))
        out_slice = barrier((out_slice, grad_qkv))[0]
        layer_out = jnp.concatenate([out_slice] * tp_count)
        for k in range(1, tp_count):
            piece = swap(out_slice, [(i, i ^ k) for i in range(tp_count)], "tp")
            layer_out = lax.dynamic_update_slice_in_dim(layer_out, piece, (tp_rank ^ k) * part, 0)
        gain_grads = jnp.sum(gathered.reshape(cp_count * tp_count, part + 8, dim)[:, part:part + 2], axis=0)
        grad_table = scatter_rows(order, sid, runs, bounds, gathered, base, total)
        return (layer_out, grad_table, *grad_qkv, grad_out, grad_gate.T, grad_up.T, grad_down, gain_grads[0], gain_grads[1])

    col_spec = P(None, "tp")
    row_spec = P("tp")
    tok_spec = P("cp")
    rep_spec = P()
    in_specs = (tok_spec, tok_spec, tok_spec, P("cp"), row_spec, col_spec, col_spec, col_spec, row_spec, col_spec, col_spec, row_spec, rep_spec, rep_spec, rep_spec)
    out_specs = (P("cp"), row_spec, col_spec, col_spec, col_spec, row_spec, col_spec, col_spec, row_spec, rep_spec, rep_spec)
    return jax.shard_map(compute, mesh=mesh, in_specs=in_specs, out_specs=out_specs, check_vma=False)
```
